768 devices in a mesh: wall: 64 (over x, y, core), span: 12 (over z).
Axes of the slice: x: 4, y: 8, z: 12, core: 2. Of those that a mesh axis runs over, the one named last changes fastest.
Arguments:
- velocity_old: float32 [3, 1024, 192, 128], P(None, 'wall', 'span'), may hold values from -12 to 12, as said below
- heights: float32 [16], replicated, may hold values from 0.04 to 0.25
- owner_device: int32 [393216, 1], P(('wall', 'span')), may hold values from 0 to 63, as said below
- owner_element: int32 [393216, 1], P(('wall', 'span')), may hold values from 0 to 63, as said below
- ref_coords: float32 [3, 393216], P(None, ('wall', 'span')), may hold values from -1 to 1
- roughness: float32 [393216], P(('wall', 'span')), may hold values from 0.0001 to 0.01
Outputs:
- velocity_new: float32 [3, 1024, 192, 128], P(None, 'wall', 'span')
- neumann: float32 [2, 393216], P(None, ('wall', 'span'))
The draws below stay inside these ranges and needn't reach their ends.
Inputs may be any that keep to these rules, and one draw needn't show every extreme that they name: `velocity_old`: values at coinciding nodes of neighbouring elements are equal. `owner_device`: the owner is the streamwise index w of the point's own device, or w + 1 or w - 1 modulo 64. Among the rows of one device at most 128 name w + 1 and at most 128 name w - 1; some device has exactly 128 for w + 1 and some device exactly 128 for w - 1. `owner_element`: the element index is (ex * 2 + ez) * 16 + ey with ex = i // 8 and ez = j // 8 of the wall point; ey < 2 for points of the first wall, ey >= 14 for the second.
All inputs are finite; a program needn't handle non-finite values.
Results may differ from the reference program's by a relative error of at most 0.0003.
Values sent between devices are 32-bit elements; how exact they have to be, the bound alone decides.
A program may use at most 128 MiB of HBM per device.

```python
import math
import jax
import jax.numpy as jnp
import numpy as np
from jax import lax

ORDER = 7
QN = 8
EXD = 2
EZD = 2
EY = 16
NEAR = 2
ITERS = 3
XLOC = 16
ZLOC = 16
YNODES = 128
XNODES = 1024
ZNODES = 192
P_DEV = 512
WALLPTS = 393216
CAP = 128
N_WALL = 64
N_SPAN = 12
DEVICES = 768


def draw_velocity_old(key, part):
    unique_x = XNODES // QN * ORDER
    unique_z = ZNODES // QN * ORDER
    unique_y = EY * ORDER + 1
    index_x = (jnp.arange(XNODES) // QN * ORDER + jnp.arange(XNODES) % QN) % unique_x
    index_z = (jnp.arange(ZNODES) // QN * ORDER + jnp.arange(ZNODES) % QN) % unique_z
    index_y = jnp.arange(YNODES) // QN * ORDER + jnp.arange(YNODES) % QN
    shape_grid = (3, unique_x, unique_z, unique_y)
    values_grid = jax.random.truncated_normal(key, -4.0, 4.0, shape_grid, jnp.float32)
    rising = jnp.exp(jnp.log(3.0) * jnp.arange(unique_x, dtype=jnp.float32) / unique_x)
    values_grid = values_grid * rising[None, :, None, None]
    values_grid = jnp.take(values_grid, index_x, axis=1)
    values_grid = jnp.take(values_grid, index_z, axis=2)
    return jnp.take(values_grid, index_y, axis=3)


def draw_owner_device(key, part):
    block_keys = jax.random.split(jax.random.fold_in(key, 21), DEVICES)
    ranks = jax.vmap(lambda single: jax.random.permutation(single, P_DEV))(block_keys).astype(jnp.int32)
    blocks = jnp.arange(DEVICES, dtype=jnp.int32)
    count_next = jax.random.randint(jax.random.fold_in(key, 22), (DEVICES,), CAP // 3, CAP + 1)
    count_prev = jax.random.randint(jax.random.fold_in(key, 23), (DEVICES,), CAP // 3, CAP + 1)
    full_next = jax.random.randint(jax.random.fold_in(key, 24), (), 0, DEVICES)
    full_prev = jax.random.randint(jax.random.fold_in(key, 25), (), 0, DEVICES)
    count_next = jnp.where(blocks == full_next, CAP, count_next)
    count_prev = jnp.where(blocks == full_prev, CAP, count_prev)
    offset = jnp.where(ranks < count_next[:, None], 1, jnp.where(ranks < (count_next + count_prev)[:, None], -1, 0))
    own_wall = (blocks // N_SPAN)[:, None]
    owner = (own_wall + offset + N_WALL) % N_WALL
    return owner.astype(jnp.int32).reshape(WALLPTS, 1)


def draw_owner_element(key, part):
    position = jnp.arange(WALLPTS, dtype=jnp.int32) % P_DEV
    side_flag = position // (P_DEV // 2)
    node_i = position // ZLOC % XLOC
    node_j = position % ZLOC
    elem_x = node_i // QN
    elem_z = node_j // QN
    layer = jax.random.randint(jax.random.fold_in(key, 13), (WALLPTS,), 0, NEAR)
    elem_y = jnp.where(side_flag == 1, EY - 1 - layer, layer)
    return ((elem_x * EZD + elem_z) * EY + elem_y).astype(jnp.int32).reshape(WALLPTS, 1)


def levels(rng, shape, cuts, low, high):
    level = 1.0
    for axis_at, parts in cuts:
        steps = jax.random.uniform(jax.random.fold_in(jax.random.fold_in(rng, 6), axis_at), (parts,), jnp.float32, low / len(cuts), high / len(cuts))
        level = level * jnp.repeat(jnp.exp(steps), shape[axis_at] // parts).reshape((-1,) + (1,) * (len(shape) - 1 - axis_at))
    return level


def setup_inputs(seed: int = 0) -> dict:
    keys = jax.random.split(jax.random.key(seed), 7)
    return {
        "velocity_old": draw_velocity_old(jax.random.fold_in(keys[6], 71), 0),
        "heights": jnp.clip(jnp.exp(jax.random.uniform(keys[1], (EY,), jnp.float32, math.log(0.04), math.log(0.25))), 0.04, 0.25),
        "owner_device": draw_owner_device(jax.random.fold_in(keys[6], 71), 0),
        "owner_element": draw_owner_element(jax.random.fold_in(keys[6], 71), 0),
        "ref_coords": jnp.clip(jax.random.uniform(keys[4], (3, WALLPTS), jnp.float32, -1.0, 1.0) * levels(keys[4], (3, WALLPTS), ((1, 768),), -0.4, 0.0), -1.0, 1.0),
        "roughness": jnp.clip(jnp.exp(math.log(0.01) - 4.6051702 * jax.random.uniform(keys[5], (WALLPTS,), jnp.float32) ** levels(keys[5], (WALLPTS,), ((0, 768),), -0.2, 0.2)), 0.0001, 0.01),
    }


GLL_NODES = (-1.0, -0.8717401485096066, -0.5917001814331423, -0.2092992179024789, 0.2092992179024789, 0.5917001814331423, 0.8717401485096066, 1.0)
GLL_WEIGHTS = (0.03571428571428571, 0.2107042271435061, 0.3411226924835044, 0.4124587946587038, 0.4124587946587038, 0.3411226924835044, 0.2107042271435061, 0.03571428571428571)
viscosity = 0.02
inverse_step = 20.0
karman = 0.41
sample_height = 0.1
speed_floor = 0.01
element_dx = 0.05
element_dz = 0.13
precise = lax.Precision.HIGHEST

def stiffness_table():
    points = np.array(GLL_NODES)
    weights = np.array(GLL_WEIGHTS)
    previous = np.ones(8)
    current = points.copy()
    for degree in range(1, 7):
        previous, current = (current, ((2 * degree + 1) * points * current - degree * previous) / (degree + 1))
    derivative = np.zeros((8, 8))
    for target in range(8):
        for source in range(8):
            if target != source:
                derivative[target, source] = current[target] / current[source] / (points[target] - points[source])
    derivative[0, 0] = -14.0
    derivative[7, 7] = 14.0
    return derivative.T @ (weights[:, None] * derivative)

def lagrange(coord):
    points = np.array(GLL_NODES)
    gaps_table = points[:, None] - points[None, :] + np.eye(8)
    scale_row = jnp.asarray(1.0 / np.prod(gaps_table, axis=1), jnp.float32)
    gaps = coord[:, None] - jnp.asarray(points, jnp.float32)[None, :]
    filled = jnp.where(jnp.asarray(np.eye(8) > 0.5)[None], jnp.float32(1.0), gaps[:, None, :])
    return jnp.prod(filled, axis=2) * scale_row[None, :]

def face_weights(length, open_ends):
    values = np.ones(length)
    position = np.arange(length) % 8
    values[(position == 0) | (position == 7)] = 0.5
    if open_ends:
        values[0] = 1.0
        values[-1] = 1.0
    return values

def join_faces(core, before, after, axis):
    count = core.shape[axis] // 8
    blocks = core.reshape(core.shape[:axis] + (count, 8) + core.shape[axis + 1:])
    first = lax.slice_in_dim(blocks, 0, 1, axis=axis + 1)
    last = lax.slice_in_dim(blocks, 7, 8, axis=axis + 1)
    before_b = jnp.expand_dims(before, axis + 1)
    after_b = jnp.expand_dims(after, axis + 1)
    prev_last = jnp.concatenate([before_b, lax.slice_in_dim(last, 0, count - 1, axis=axis)], axis)
    next_first = jnp.concatenate([lax.slice_in_dim(first, 1, count, axis=axis), after_b], axis)
    middle = lax.slice_in_dim(blocks, 1, 7, axis=axis + 1)
    joined = jnp.concatenate([first + prev_last, middle, last + next_first], axis + 1)
    return joined.reshape(core.shape)

def assemble(field):
    joined_x = join_faces(field, field[:, -1:], field[:, :1], 1)
    joined_z = join_faces(joined_x, joined_x[:, :, -1:], joined_x[:, :, :1], 2)
    border = jnp.zeros(joined_z.shape[:3] + (1,), jnp.float32)
    return join_faces(joined_z, border, border, 3)

def reference(velocity_old, heights, owner_device, owner_element, ref_coords, roughness):
    weights = np.array(GLL_WEIGHTS)
    stiffness = jnp.asarray(stiffness_table(), jnp.float32)
    length_x, length_z, length_y = (velocity_old.shape[1], velocity_old.shape[2], velocity_old.shape[3])
    count_x, count_z, count_y = (length_x // 8, length_z // 8, length_y // 8)
    mass_x = jnp.asarray(np.tile(0.5 * element_dx * weights, count_x), jnp.float32)
    mass_z = jnp.asarray(np.tile(0.5 * element_dz * weights, count_z), jnp.float32)
    mass_y = (0.5 * heights[:, None] * jnp.asarray(weights, jnp.float32)[None, :]).reshape(length_y)
    mass_all = mass_x[:, None, None] * mass_z[None, :, None] * mass_y[None, None, :]
    inverse_count = jnp.asarray(face_weights(length_x, False)[:, None, None] * face_weights(length_z, False)[None, :, None] * face_weights(length_y, True)[None, None, :], jnp.float32)
    blocks = (2.0 / heights)[:, None, None] * stiffness[None]

    def operate(field):
        along_x = jnp.einsum('ab,cebzy->ceazy', stiffness * (2.0 / element_dx), field.reshape(3, count_x, 8, length_z, length_y), precision=precise).reshape(field.shape)
        along_z = jnp.einsum('ab,cxeby->cxeay', stiffness * (2.0 / element_dz), field.reshape(3, length_x, count_z, 8, length_y), precision=precise).reshape(field.shape)
        along_y = jnp.einsum('eab,cxzeb->cxzea', blocks, field.reshape(3, length_x, length_z, count_y, 8), precision=precise).reshape(field.shape)
        mass_xb = mass_x[None, :, None, None]
        mass_zb = mass_z[None, None, :, None]
        mass_yb = mass_y[None, None, None, :]
        local = viscosity * (along_x * mass_zb * mass_yb + mass_xb * along_z * mass_yb + mass_xb * mass_zb * along_y) + inverse_step * mass_all[None] * field
        return assemble(local)
    element_rows = velocity_old.reshape(3, count_x, 8, count_z, 8, count_y, 8).transpose(1, 3, 5, 0, 2, 4, 6).reshape(count_x * count_z * count_y, 3 * 512)
    points = jnp.arange(WALLPTS, dtype=jnp.int32)
    span_index = points // P_DEV % N_SPAN
    local_elem = owner_element[:, 0]
    elem_x = owner_device[:, 0] * EXD + local_elem // (EZD * EY)
    elem_z = span_index * EZD + local_elem // EY % EZD
    elem_y = local_elem % EY
    row_ids = ((elem_x * count_z + elem_z) * count_y + elem_y).astype(jnp.int32)

    def evaluate(pieces):
        rows_here, coords = pieces
        values = element_rows[rows_here].reshape(rows_here.shape[0], 3, 8, 8, 8)
        return jnp.einsum('gcabd,ga,gb,gd->gc', values, lagrange(coords[:, 0]), lagrange(coords[:, 1]), lagrange(coords[:, 2]), precision=precise)
    sampled = lax.map(evaluate, (row_ids.reshape(DEVICES, P_DEV), ref_coords.T.reshape(DEVICES, P_DEV, 3))).reshape(WALLPTS, 3)
    stream = sampled[:, 0]
    spanwise = sampled[:, 2]
    wall_speed = jnp.sqrt(stream * stream + spanwise * spanwise + speed_floor)
    drag_coeff = (karman / jnp.log(sample_height / roughness)) ** 2
    neumann = -(drag_coeff * wall_speed / viscosity)[None, :] * jnp.stack([stream, spanwise])
    traction = (viscosity * neumann).reshape(2, N_WALL, N_SPAN, 2, XLOC, ZLOC).transpose(0, 3, 1, 4, 2, 5).reshape(2, 2, length_x, length_z)
    traction = traction * (mass_x[:, None] * mass_z[None, :])[None, None]
    zero_plane = jnp.zeros((1, length_x, length_z), jnp.float32)
    bottom = jnp.concatenate([traction[0:1, 0], zero_plane, traction[1:2, 0]], axis=0)
    top_wall = jnp.concatenate([traction[0:1, 1], zero_plane, traction[1:2, 1]], axis=0)
    forcing = inverse_step * mass_all[None] * velocity_old
    forcing = forcing.at[:, :, :, 0].add(bottom).at[:, :, :, -1].add(top_wall)
    right_side = assemble(forcing)

    def weighted(first, second):
        return lax.optimization_barrier(jnp.sum(first * second * inverse_count[None], axis=(1, 2, 3)))

    def spread(values):
        return values[:, None, None, None]
    solution = jnp.zeros_like(right_side)
    residual = right_side
    direction = residual
    norm_now = weighted(residual, residual)
    for sweep in range(ITERS):
        applied = operate(direction)
        step_size = norm_now / weighted(direction, applied)
        solution = solution + spread(step_size) * direction
        residual = residual - spread(step_size) * applied
        norm_next = weighted(residual, residual)
        direction = residual + spread(norm_next / norm_now) * direction
        norm_now = norm_next
    return (solution, neumann)
```

```python
import functools

import jax
import jax.numpy as jnp
import numpy as np
from jax import lax
from jax.experimental import pallas as pl
from jax.experimental.pallas import tpu as pltpu
from jax.sharding import Mesh
from jax.sharding import PartitionSpec as P

AXES = ("wall_0", "wall_1", "wall_2", "span")
WALL_SPAN = AXES
WALL = ("wall_0", "wall_1", "wall_2")
MESH_ID = pl.DeviceIdType.MESH

GLL_NODES = (
    -1.0,
    -0.8717401485096066,
    -0.5917001814331423,
    -0.2092992179024789,
    0.2092992179024789,
    0.5917001814331423,
    0.8717401485096066,
    1.0,
)
GLL_WEIGHTS = (
    0.03571428571428571,
    0.2107042271435061,
    0.3411226924835044,
    0.4124587946587038,
    0.4124587946587038,
    0.3411226924835044,
    0.2107042271435061,
    0.03571428571428571,
)
viscosity = 0.02
inverse_step = 20.0
karman = 0.41
sample_height = 0.1
speed_floor = 0.01
element_dx = 0.05
element_dz = 0.13
precise = lax.Precision.HIGHEST

SCALE = 64.0

SHIFTS = ((1, 0), (-1, 0), (0, 1), (0, -1), (1, 1), (1, -1), (-1, 1), (-1, -1))

MZ, QMZ, COUNT, LAG, PLANE, HALFW, LAST, FIRST, KZ = range(9)


def stiffness_table():
    points = np.array(GLL_NODES)
    weights = np.array(GLL_WEIGHTS)
    previous = np.ones(8)
    current = points.copy()
    for degree in range(1, 7):
        previous, current = (
            current,
            ((2 * degree + 1) * points * current - degree * previous) / (degree + 1),
        )
    derivative = np.zeros((8, 8))
    for target in range(8):
        for source in range(8):
            if target != source:
                derivative[target, source] = (
                    current[target] / current[source] / (points[target] - points[source])
                )
    derivative[0, 0] = -14.0
    derivative[7, 7] = 14.0
    return derivative.T @ (weights[:, None] * derivative)


def tables():
    weights = np.array(GLL_WEIGHTS)
    points = np.array(GLL_NODES)
    stiffness = stiffness_table()
    ones = np.ones((8, 128))
    lane = np.arange(128)
    ends = np.array([2.0, 1, 1, 1, 1, 1, 1, 2.0])
    mass_x = 0.5 * element_dx * weights
    mass_z = 0.5 * element_dz * weights
    count_y = np.where((lane % 8 == 0) | (lane % 8 == 7), 0.5, 1.0)
    count_y[0] = count_y[127] = 1.0
    gaps = points[:, None] - points[None, :] + np.eye(8)
    kz = SCALE * (
        viscosity * (2.0 / element_dz) * stiffness + inverse_step * np.diag(mass_z)
    )
    rows = [
        mass_z[:, None] * ones,
        (mass_z * ends)[:, None] * ones,
        (1.0 / ends)[:, None] * count_y[None, :],
        (1.0 / np.prod(gaps, axis=1))[:, None] * ones,
        ones * (mass_x[lane // 16] * mass_z[lane % 8])[None, :],
        ones * (0.5 * weights[lane % 8])[None, :],
        ones * ((lane % 8 == 7) & (lane < 127))[None, :],
        ones * ((lane % 8 == 0) & (lane > 0))[None, :],
    ]
    rows += [kz[:, b][:, None] * ones for b in range(8)]
    block = np.kron(np.eye(16), SCALE * viscosity * 2.0 * stiffness)
    lift = np.zeros((8, 512))
    for comp in range(2):
        for half in range(2):
            column = (comp * 2 + half) * 128
            lift[comp * 4 + half, column] = 1.0
            lift[comp * 4 + 2 + half, column + 127] = 1.0
    as32 = lambda value: np.asarray(value, np.float32)
    return as32(np.stack(rows)), as32(block), as32(lift)


def kernel(sizes, velocity, heights, owner, element, coords, roughness, table, block, lift,
           out, neumann, res, one, two, stiff, slab, slab_in, plane, plane_in, face, face_in,
           edge, edge_in, mom, part, part_in, send, recv, slab_send, slab_recv, sum_send,
           sum_recv):
    nx, ny, nc, ns = sizes
    nw = nx * ny * nc
    wx, wy, wc, sp = (lax.axis_index(name) for name in AXES)
    wall = (wx * ny + wy) * nc + wc
    weights = np.array(GLL_WEIGHTS)
    stiffness = stiffness_table()
    mass_x = [float(v) for v in 0.5 * element_dx * weights]
    ends = [2.0, 1.0, 1.0, 1.0, 1.0, 1.0, 1.0, 2.0]

    def shifted(dw, ds):
        there = (wall + dw + nw) % nw
        return (there // (ny * nc), there // nc % ny, there % nc, (sp + ds + ns) % ns)

    neighbours = [shifted(dw, ds) for dw, ds in SHIFTS]
    pair = wx * nc + wc
    groups = [
        (nx * nc, pair, lambda q: (q // nc, wy, q % nc, sp)),
        (ny, wy, lambda q: (wx, q, wc, sp)),
        (ns, sp, lambda q: (wx, wy, wc, q)),
    ]
    peers = list(neighbours)
    for count, mine, place in groups:
        peers += [place((mine + k) % count) for k in range(1, count)]
    barrier = pltpu.get_barrier_semaphore()
    for peer in peers:
        pl.semaphore_signal(barrier, inc=1, device_id=peer, device_id_type=MESH_ID)

    lane = lax.broadcasted_iota(jnp.int32, (1, 128), 1)
    sub8 = lax.broadcasted_iota(jnp.int32, (8, 128), 0)
    lane8 = lax.broadcasted_iota(jnp.int32, (8, 128), 1)

    height = jnp.zeros((8, 128), jnp.float32)
    for layer in range(16):
        height = jnp.where(lane8 // 8 == layer, heights[layer], height)
    mass_y = height * table[HALFW]
    stiff[...] = block[...] * (1.0 / height)[:1]
    joined_y = (
        mass_y
        + table[LAST] * pltpu.roll(mass_y, 127, 1)
        + table[FIRST] * pltpu.roll(mass_y, 1, 1)
    )
    both = lambda value: jnp.concatenate([value, value], axis=0)
    mass_zy = both(table[MZ] * mass_y)
    mass_y2 = both(mass_y)
    mass_z2 = both(table[MZ])
    last2, first2 = both(table[LAST]), both(table[FIRST])
    count2 = both(table[COUNT])

    for comp in range(2):
        quarters = []
        for k in range(4):
            quarters.append(velocity[2 * comp, 4 * k : 4 * k + 4].reshape(64, 128))
        packed = jnp.zeros((64, 128), jnp.float32)
        where_to = lax.broadcasted_iota(jnp.int32, (64, 128), 1)
        for k in range(4):
            low = pltpu.roll(quarters[k], 32 * k, 1) if k else quarters[k]
            shift = (32 * k + 32) % 128
            high = pltpu.roll(quarters[k], shift, 1) if shift else quarters[k]
            packed = jnp.where(where_to // 16 == 2 * k, low, packed)
            packed = jnp.where(where_to // 16 == 2 * k + 1, high, packed)
        slab[comp] = packed.reshape(4, 16, 128)

    scale_zy = both(table[QMZ] * joined_y) * inverse_step
    for comp in range(3):
        for i in range(16):
            res[comp, 16 * i : 16 * i + 16] = velocity[comp, i] * (
                scale_zy * (mass_x[i % 8] * ends[i % 8])
            )

    def regroup(blocks):
        upper = (lane // 8) % 2 == 1
        result = []
        for ex in range(2):
            low, high = blocks[ex], blocks[2 + ex]
            result.append(jnp.where(upper, pltpu.roll(high, 8, 1), low))
            result.append(jnp.where(upper, high, pltpu.roll(low, 120, 1)))
        return result

    def ungroup(values):
        upper = (lane // 8) % 2 == 1
        low, high = [], []
        for ex in range(2):
            a, b = values[2 * ex], values[2 * ex + 1]
            low.append(jnp.where(upper, pltpu.roll(b, 8, 1), a))
            high.append(jnp.where(upper, b, pltpu.roll(a, 120, 1)))
        return low + high

    wide = lambda row: jnp.broadcast_to(row, (8, 128))
    quarter = lambda ref, row, q: ref[row : row + 1, 128 * q : 128 * q + 128]
    distance = [(quarter(owner, 0, q) - wall + nw) % nw for q in range(4)]
    to_next = regroup([wide(jnp.where(d == 1, 1.0, 0.0)) for d in distance])
    to_prev = regroup([wide(jnp.where(d == nw - 1, 1.0, 0.0)) for d in distance])
    layer = regroup([wide((quarter(element, 0, q) % 2).astype(jnp.float32)) for q in range(4)])
    axes = [regroup([wide(quarter(coords, k, q)) for q in range(4)]) for k in range(3)]

    def lagrange(coord):
        value = table[LAG]
        for b in range(8):
            value = value * jnp.where(sub8 == b, 1.0, coord - GLL_NODES[b])
        return value

    pl.semaphore_wait(barrier, len(peers))

    copies = []
    slab_copies = []
    for d in range(2):
        copy = pltpu.make_async_remote_copy(
            src_ref=slab,
            dst_ref=slab_in.at[d],
            send_sem=slab_send.at[d],
            recv_sem=slab_recv.at[d],
            device_id=neighbours[d],
            device_id_type=MESH_ID,
        )
        copy.start()
        slab_copies.append(copy)
        copies.append(copy)

    basis = [[lagrange(axes[k][g]) for k in range(3)] for g in range(4)]
    second_wall = (lane // 8) % 2 == 1
    columns = []
    for g in range(4):
        ly = basis[g][2]
        blocks = []
        for side in range(2):
            for ey in range(2):
                chosen = jnp.logical_and(
                    wide(second_wall) == (side == 1), layer[g] == float(ey)
                )
                blocks.append(jnp.where(chosen, ly, 0.0))
        columns.append(jnp.concatenate(blocks, axis=0))

    nothing = jnp.zeros((32, 128), jnp.float32)
    masks = [[1.0 - to_next[g] - to_prev[g], to_prev[g], to_next[g]] for g in range(4)]

    def sample(source, g):
        ex, ez = g // 2, g % 2
        right = [
            jnp.concatenate(
                [columns[g] if k == 2 * ex + kk else nothing for k in range(4)], axis=0
            )
            for kk in range(2)
        ]
        rows = source[:, :, 8 * ez : 8 * ez + 8, :].reshape(64, 128)
        total = [jnp.zeros((8, 128), jnp.float32) for _ in range(2)]
        for kk in range(2):
            values = jnp.dot(
                rows, right[kk], precision=precise, preferred_element_type=jnp.float32
            ).reshape(2, 4, 8, 128)
            for comp in range(2):
                for x in range(4):
                    a = 4 * kk + x
                    total[comp] = total[comp] + values[comp, x] * basis[g][0][a : a + 1]
        return total

    sums = []
    for g in range(4):
        own = sample(slab, g)
        sums.append([own[comp] * masks[g][0] for comp in range(2)])
    for d in range(2):
        slab_copies[d].wait_recv()
        for g in range(4):
            far = sample(slab_in.at[d], g)
            for comp in range(2):
                sums[g][comp] = sums[g][comp] + far[comp] * masks[g][1 + d]
    stream = ungroup(
        [wide(jnp.sum(sums[g][0] * basis[g][1], axis=0, keepdims=True)) for g in range(4)]
    )
    spanwise = ungroup(
        [wide(jnp.sum(sums[g][1] * basis[g][1], axis=0, keepdims=True)) for g in range(4)]
    )

    for q in range(4):
        u, v = stream[q], spanwise[q]
        speed = jnp.sqrt(u * u + v * v + speed_floor)
        ratio = karman / jnp.log(sample_height / wide(quarter(roughness, 0, q)))
        factor = -(ratio * ratio * speed / viscosity)
        for comp, value in enumerate((u, v)):
            slope = factor * value
            neumann[comp : comp + 1, 128 * q : 128 * q + 128] = slope[:1]
            plane[comp * 4 + q : comp * 4 + q + 1, :] = (viscosity * slope * table[PLANE])[:1]

    plane_copies = []
    for d in range(8):
        copy = pltpu.make_async_remote_copy(
            src_ref=plane,
            dst_ref=plane_in.at[d],
            send_sem=send.at[0, d],
            recv_sem=recv.at[0, d],
            device_id=neighbours[d],
            device_id_type=MESH_ID,
        )
        copy.start()
        plane_copies.append(copy)
        copies.append(copy)

    node_z = lane8 % 16
    node_x = lane8 // 16
    half = sub8 % 2

    def join_span(mine, before, after):
        return (
            mine
            + jnp.where(node_z == 7, pltpu.roll(mine, 127, 1), 0.0)
            + jnp.where(node_z == 8, pltpu.roll(mine, 1, 1), 0.0)
            + jnp.where(node_z == 0, pltpu.roll(before, 113, 1), 0.0)
            + jnp.where(node_z == 15, pltpu.roll(after, 15, 1), 0.0)
        )

    def join_wall(mine, before, after):
        later = jnp.where(half == 0, pltpu.roll(mine, 7, 0), pltpu.roll(after, 1, 0))
        earlier = jnp.where(half == 0, pltpu.roll(before, 7, 0), pltpu.roll(mine, 1, 0))
        return (
            mine
            + jnp.where(node_x == 7, pltpu.roll(later, 112, 1), 0.0)
            + jnp.where(node_x == 0, pltpu.roll(earlier, 16, 1), 0.0)
        )

    for d in range(8):
        plane_copies[d].wait_recv()
    own_line = join_span(plane[...], plane_in[2], plane_in[3])
    before_line = join_span(plane_in[0], plane_in[4], plane_in[5])
    after_line = join_span(plane_in[1], plane_in[6], plane_in[7])
    stress = join_wall(own_line, before_line, after_line)
    lifted = lax.dot_general(
        stress,
        lift[...],
        (((0,), (0,)), ((), ())),
        precision=precise,
        preferred_element_type=jnp.float32,
    )
    for comp in range(2):
        for ex in range(2):
            column = (comp * 2 + ex) * 128
            here = res[2 * comp, 128 * ex : 128 * ex + 128]
            res[2 * comp, 128 * ex : 128 * ex + 128] = here + lifted[:, column : column + 128]

    cx = SCALE * viscosity * (2.0 / element_dx) * stiffness
    even = 0.5 * (cx[:4, :4] + cx[:4, 7:3:-1])
    odd = 0.5 * (cx[:4, :4] - cx[:4, 7:3:-1])

    def fold(value):
        return value[:8] + value[8:]

    def operate(source, target, index):
        for comp in range(3):
            total = jnp.zeros((16, 128), jnp.float32)
            for ex in range(2):
                base = 128 * ex
                along_y = jnp.dot(
                    source[comp, base : base + 128],
                    stiff[...],
                    precision=precise,
                    preferred_element_type=jnp.float32,
                )
                nodes = [source[comp, base + 16 * b : base + 16 * b + 16] for b in range(8)]
                plus = [nodes[b] + nodes[7 - b] for b in range(4)]
                minus = [nodes[b] - nodes[7 - b] for b in range(4)]
                along_x = [None] * 8
                for a in range(4):
                    sum_e = plus[0] * float(even[a, 0])
                    sum_o = minus[0] * float(odd[a, 0])
                    for b in range(1, 4):
                        sum_e = sum_e + plus[b] * float(even[a, b])
                        sum_o = sum_o + minus[b] * float(odd[a, b])
                    along_x[a] = sum_e + sum_o
                    along_x[7 - a] = sum_e - sum_o
                for a in range(8):
                    start = base + 16 * a
                    halves = []
                    for h in range(2):
                        along_z = None
                        for b in range(8):
                            row = start + 8 * h + b
                            term = source[comp, row : row + 1] * table[KZ + b]
                            along_z = term if along_z is None else along_z + term
                        halves.append(along_z)
                    along_z = jnp.concatenate(halves, axis=0)
                    local = along_x[a] * mass_zy + (
                        along_z * mass_y2 + along_y[16 * a : 16 * a + 16] * mass_z2
                    ) * mass_x[a]
                    total = total + local * nodes[a]
                    if target is not None:
                        target[comp, start : start + 16] = (
                            local
                            + last2 * pltpu.roll(local, 127, 1)
                            + first2 * pltpu.roll(local, 1, 1)
                        )
            mom[3 * index + comp] = fold(total)

    def exchange(target, turn):
        for comp in range(3):
            both_x = target[comp, 112:128] + target[comp, 128:144]
            target[comp, 112:128] = both_x
            target[comp, 128:144] = both_x
            inner, outer = pl.ds(7, 16, stride=16), pl.ds(8, 16, stride=16)
            both_z = target[comp, inner, :] + target[comp, outer, :]
            target[comp, inner, :] = both_z
            target[comp, outer, :] = both_z
        started = []

        def put(d, source, into):
            copy = pltpu.make_async_remote_copy(
                src_ref=source,
                dst_ref=into,
                send_sem=send.at[turn, d],
                recv_sem=recv.at[turn, d],
                device_id=neighbours[d],
                device_id_type=MESH_ID,
            )
            copy.start()
            started.append(copy)
            copies.append(copy)

        faces = (pl.ds(240, 16), pl.ds(0, 16), pl.ds(15, 16, stride=16), pl.ds(0, 16, stride=16))
        corners = (255, 240, 15, 0)
        for d in range(4):
            for comp in range(3):
                face[turn - 1, d, comp] = target[comp, faces[d], :]
            put(d, face.at[turn - 1, d], face_in.at[turn - 1, d])
        for d in range(4):
            for comp in range(3):
                row = corners[d]
                edge[turn - 1, d, comp : comp + 1, :] = target[comp, row : row + 1, :]
            put(4 + d, edge.at[turn - 1, d], edge_in.at[turn - 1, d])
        for copy in started:
            copy.wait_recv()
        into = (faces[1], faces[0], faces[3], faces[2])
        corner_into = (0, 15, 240, 255)
        for d in range(4):
            for comp in range(3):
                target[comp, into[d], :] = target[comp, into[d], :] + face_in[turn - 1, d, comp]
        for d in range(4):
            for comp in range(3):
                row = corner_into[d]
                target[comp, row : row + 1, :] = (
                    target[comp, row : row + 1, :] + edge_in[turn - 1, d, comp : comp + 1, :]
                )

    def weighted(pairs):
        for comp in range(3):
            totals = [jnp.zeros((16, 128), jnp.float32) for _ in pairs]
            edges = [jnp.zeros((16, 128), jnp.float32) for _ in pairs]
            for i in range(16):
                for n, (first, second, _) in enumerate(pairs):
                    term = (
                        first[comp, 16 * i : 16 * i + 16] * second[comp, 16 * i : 16 * i + 16]
                    )
                    if i % 8 in (0, 7):
                        edges[n] = edges[n] + term
                    else:
                        totals[n] = totals[n] + term
            for n, (_, _, index) in enumerate(pairs):
                mom[3 * index + comp] = fold((totals[n] + 0.5 * edges[n]) * count2)

    operate(res, one, 1)
    exchange(one, 1)
    operate(one, two, 3)
    exchange(two, 2)
    weighted([(res, res, 0), (one, one, 2), (two, two, 4)])
    operate(two, None, 5)

    row = jnp.zeros((8, 128), jnp.float32)
    for k in range(18):
        value = jnp.sum(mom[k], axis=1, keepdims=True)
        row = row + jnp.where(lane8 == k, value, 0.0)
    row = jnp.sum(row, axis=0, keepdims=True)

    start = 0
    for phase, (count, mine, place) in enumerate(groups):
        part[phase] = row
        started = []
        for k in range(1, count):
            copy = pltpu.make_async_remote_copy(
                src_ref=part.at[phase],
                dst_ref=part_in.at[start + mine],
                send_sem=sum_send.at[start + k],
                recv_sem=sum_recv.at[start + k],
                device_id=place((mine + k) % count),
                device_id_type=MESH_ID,
            )
            copy.start()
            started.append(copy)
            copies.append(copy)
        part_in[start + mine] = row
        for copy in started:
            copy.wait_recv()
        row = part_in[start]
        for k in range(1, count):
            row = row + part_in[start + k]
        start += count

    row = jnp.broadcast_to(row, (8, 128))
    moments = [row if j == 0 else pltpu.roll(row, 128 - 3 * j, 1) for j in range(6)]

    def inner(first, second, raise_by):
        total = None
        for i, a in enumerate(first):
            for j, b in enumerate(second):
                term = a * b * moments[i + j + raise_by]
                total = term if total is None else total + term
        return total

    unit = jnp.ones((8, 128), jnp.float32)
    direction, residual = [unit], [unit]
    answer = [jnp.zeros((8, 128), jnp.float32)] * 3
    norm = moments[0]
    for step in range(3):
        alpha = norm / inner(direction, direction, 1)
        for i, value in enumerate(direction):
            answer[i] = answer[i] + alpha * value
        if step == 2:
            break
        lowered = [-alpha * value for value in direction]
        residual = [residual[0]] + [
            lowered[i] + residual[i + 1] if i + 1 < len(residual) else lowered[i]
            for i in range(len(lowered))
        ]
        newer = inner(residual, residual, 0)
        growth = newer / norm
        direction = [
            value + growth * direction[i] if i < len(direction) else value
            for i, value in enumerate(residual)
        ]
        norm = newer
    for comp in range(3):
        c0, c1, c2 = (
            jnp.broadcast_to(value[:1, comp : comp + 1] * SCALE, (16, 128)) for value in answer
        )
        for i in range(16):
            rows = pl.ds(16 * i, 16)
            out[comp, i] = (
                c0 * res[comp, rows, :] + c1 * one[comp, rows, :] + c2 * two[comp, rows, :]
            )
    for copy in copies:
        copy.wait_send()


def body(sizes, velocity_old, heights, owner_device, owner_element, ref_coords, roughness):
    nx, ny, nc, ns = sizes
    slots = nx * nc + ny + ns
    vmem = pl.BlockSpec(memory_space=pltpu.VMEM)
    smem = pl.BlockSpec(memory_space=pltpu.SMEM)
    f32 = jnp.float32
    constants = [jnp.asarray(value) for value in tables()]
    return pl.pallas_call(
        functools.partial(kernel, sizes),
        out_shape=(
            jax.ShapeDtypeStruct((3, 16, 16, 128), f32),
            jax.ShapeDtypeStruct((2, 512), f32),
        ),
        in_specs=[vmem, smem] + [vmem] * 7,
        out_specs=(vmem, vmem),
        scratch_shapes=[
            pltpu.VMEM((3, 256, 128), f32),
            pltpu.VMEM((3, 256, 128), f32),
            pltpu.VMEM((3, 256, 128), f32),
            pltpu.VMEM((128, 128), f32),
            pltpu.VMEM((2, 4, 16, 128), f32),
            pltpu.VMEM((2, 2, 4, 16, 128), f32),
            pltpu.VMEM((8, 128), f32),
            pltpu.VMEM((8, 8, 128), f32),
            pltpu.VMEM((2, 4, 3, 16, 128), f32),
            pltpu.VMEM((2, 4, 3, 16, 128), f32),
            pltpu.VMEM((2, 4, 3, 128), f32),
            pltpu.VMEM((2, 4, 3, 128), f32),
            pltpu.VMEM((18, 8, 128), f32),
            pltpu.VMEM((3, 1, 128), f32),
            pltpu.VMEM((slots, 1, 128), f32),
            pltpu.SemaphoreType.DMA((3, 8)),
            pltpu.SemaphoreType.DMA((3, 8)),
            pltpu.SemaphoreType.DMA((2,)),
            pltpu.SemaphoreType.DMA((2,)),
            pltpu.SemaphoreType.DMA((slots,)),
            pltpu.SemaphoreType.DMA((slots,)),
        ],
        compiler_params=pltpu.CompilerParams(collective_id=0, has_side_effects=True),
        name="channel_step",
    )(
        velocity_old,
        heights,
        owner_device.reshape(1, -1),
        owner_element.reshape(1, -1),
        ref_coords,
        roughness.reshape(1, -1),
        *constants,
    )


def torus_program(torus):
    sizes = tuple(torus.shape[name] for name in AXES)
    return jax.shard_map(
        functools.partial(body, sizes),
        mesh=torus,
        in_specs=(
            P(None, WALL, "span", None),
            P(),
            P(WALL_SPAN, None),
            P(WALL_SPAN, None),
            P(None, WALL_SPAN),
            P(WALL_SPAN),
        ),
        out_specs=(P(None, WALL, "span", None), P(None, WALL_SPAN)),
        check_vma=False,
    )


def solution(mesh):
    return torus_program(Mesh(mesh.devices.reshape(4, 8, 2, mesh.shape["span"]), AXES))
```

```python
import functools

import jax
import jax.numpy as jnp
import numpy as np
from jax import lax
from jax.experimental import pallas as pl
from jax.experimental.pallas import tpu as pltpu
from jax.sharding import Mesh
from jax.sharding import PartitionSpec as P

AXES = ("wall_0", "wall_1", "wall_2", "span")
WALL_SPAN = AXES
WALL = ("wall_0", "wall_1", "wall_2")
MESH_ID = pl.DeviceIdType.MESH

GLL_NODES = (
    -1.0,
    -0.8717401485096066,
    -0.5917001814331423,
    -0.2092992179024789,
    0.2092992179024789,
    0.5917001814331423,
    0.8717401485096066,
    1.0,
)
GLL_WEIGHTS = (
    0.03571428571428571,
    0.2107042271435061,
    0.3411226924835044,
    0.4124587946587038,
    0.4124587946587038,
    0.3411226924835044,
    0.2107042271435061,
    0.03571428571428571,
)
viscosity = 0.02
inverse_step = 20.0
karman = 0.41
sample_height = 0.1
speed_floor = 0.01
element_dx = 0.05
element_dz = 0.13
precise = lax.Precision.HIGHEST

SCALE = 64.0

SHIFTS = ((1, 0), (-1, 0), (0, 1), (0, -1), (1, 1), (1, -1), (-1, 1), (-1, -1))

MZ, QMZ, COUNT, LAG, PLANE, HALFW, LAST, FIRST, KZ = range(9)


def stiffness_table():
    points = np.array(GLL_NODES)
    weights = np.array(GLL_WEIGHTS)
    previous = np.ones(8)
    current = points.copy()
    for degree in range(1, 7):
        previous, current = (
            current,
            ((2 * degree + 1) * points * current - degree * previous) / (degree + 1),
        )
    derivative = np.zeros((8, 8))
    for target in range(8):
        for source in range(8):
            if target != source:
                derivative[target, source] = (
                    current[target] / current[source] / (points[target] - points[source])
                )
    derivative[0, 0] = -14.0
    derivative[7, 7] = 14.0
    return derivative.T @ (weights[:, None] * derivative)


def tables():
    weights = np.array(GLL_WEIGHTS)
    points = np.array(GLL_NODES)
    stiffness = stiffness_table()
    ones = np.ones((8, 128))
    lane = np.arange(128)
    ends = np.array([2.0, 1, 1, 1, 1, 1, 1, 2.0])
    mass_x = 0.5 * element_dx * weights
    mass_z = 0.5 * element_dz * weights
    count_y = np.where((lane % 8 == 0) | (lane % 8 == 7), 0.5, 1.0)
    count_y[0] = count_y[127] = 1.0
    gaps = points[:, None] - points[None, :] + np.eye(8)
    kz = SCALE * (
        viscosity * (2.0 / element_dz) * stiffness + inverse_step * np.diag(mass_z)
    )
    rows = [
        mass_z[:, None] * ones,
        (mass_z * ends)[:, None] * ones,
        (1.0 / ends)[:, None] * count_y[None, :],
        (1.0 / np.prod(gaps, axis=1))[:, None] * ones,
        ones * (mass_x[lane // 16] * mass_z[lane % 8])[None, :],
        ones * (0.5 * weights[lane % 8])[None, :],
        ones * ((lane % 8 == 7) & (lane < 127))[None, :],
        ones * ((lane % 8 == 0) & (lane > 0))[None, :],
    ]
    rows += [kz[:, b][:, None] * ones for b in range(8)]
    block = np.kron(np.eye(16), SCALE * viscosity * 2.0 * stiffness)
    lift = np.zeros((8, 512))
    for comp in range(2):
        for half in range(2):
            column = (comp * 2 + half) * 128
            lift[comp * 4 + half, column] = 1.0
            lift[comp * 4 + 2 + half, column + 127] = 1.0
    as32 = lambda value: np.asarray(value, np.float32)
    return as32(np.stack(rows)), as32(block), as32(lift)


def kernel(sizes, *refs):
    operands, refs = refs[:9], refs[9:]
    (res, one, two, scalars, neumann), refs = refs[:5], refs[5:]
    local, refs = refs[:9], refs[9:]
    velocity, heights, owner, element, coords, roughness, table, block, lift = local
    (stiff, slab, slab_in, plane, plane_in, face, face_in, edge, edge_in, mom, part, part_in,
     load, send, recv, slab_send, slab_recv, sum_send, sum_recv) = refs
    loads = [
        pltpu.make_async_copy(source, target, load.at[n])
        for n, (source, target) in enumerate(zip(operands, local))
    ]
    nx, ny, nc, ns = sizes
    nw = nx * ny * nc
    wx, wy, wc, sp = (lax.axis_index(name) for name in AXES)
    wall = (wx * ny + wy) * nc + wc
    weights = np.array(GLL_WEIGHTS)
    stiffness = stiffness_table()
    mass_x = [float(v) for v in 0.5 * element_dx * weights]
    ends = [2.0, 1.0, 1.0, 1.0, 1.0, 1.0, 1.0, 2.0]

    def shifted(dw, ds):
        there = (wall + dw + nw) % nw
        return (there // (ny * nc), there // nc % ny, there % nc, (sp + ds + ns) % ns)

    neighbours = [shifted(dw, ds) for dw, ds in SHIFTS]
    pair = wx * nc + wc
    groups = [
        (nx * nc, pair, lambda q: (q // nc, wy, q % nc, sp)),
        (ny, wy, lambda q: (wx, q, wc, sp)),
        (ns, sp, lambda q: (wx, wy, wc, q)),
    ]
    peers = list(neighbours)
    for count, mine, place in groups:
        peers += [place((mine + k) % count) for k in range(1, count)]
    for copy in loads:
        copy.start()
    barrier = pltpu.get_barrier_semaphore()
    for peer in peers:
        pl.semaphore_signal(barrier, inc=1, device_id=peer, device_id_type=MESH_ID)
    for copy in loads:
        copy.wait()

    lane = lax.broadcasted_iota(jnp.int32, (1, 128), 1)
    sub8 = lax.broadcasted_iota(jnp.int32, (8, 128), 0)
    lane8 = lax.broadcasted_iota(jnp.int32, (8, 128), 1)

    height = jnp.zeros((8, 128), jnp.float32)
    for layer in range(16):
        height = jnp.where(lane8 // 8 == layer, heights[layer], height)
    mass_y = height * table[HALFW]
    stiff[...] = block[...] * (1.0 / height)[:1]
    joined_y = (
        mass_y
        + table[LAST] * pltpu.roll(mass_y, 127, 1)
        + table[FIRST] * pltpu.roll(mass_y, 1, 1)
    )
    both = lambda value: jnp.concatenate([value, value], axis=0)
    mass_zy = both(table[MZ] * mass_y)
    mass_y2 = both(mass_y)
    mass_z2 = both(table[MZ])
    last2, first2 = both(table[LAST]), both(table[FIRST])
    count2 = both(table[COUNT])

    for comp in range(2):
        quarters = []
        for k in range(4):
            quarters.append(velocity[2 * comp, 4 * k : 4 * k + 4].reshape(64, 128))
        packed = jnp.zeros((64, 128), jnp.float32)
        where_to = lax.broadcasted_iota(jnp.int32, (64, 128), 1)
        for k in range(4):
            low = pltpu.roll(quarters[k], 32 * k, 1) if k else quarters[k]
            shift = (32 * k + 32) % 128
            high = pltpu.roll(quarters[k], shift, 1) if shift else quarters[k]
            packed = jnp.where(where_to // 16 == 2 * k, low, packed)
            packed = jnp.where(where_to // 16 == 2 * k + 1, high, packed)
        slab[comp] = packed.reshape(4, 16, 128)

    scale_zy = both(table[QMZ] * joined_y) * inverse_step
    for comp in range(3):
        for i in range(16):
            res[comp, 16 * i : 16 * i + 16] = velocity[comp, i] * (
                scale_zy * (mass_x[i % 8] * ends[i % 8])
            )

    def regroup(blocks):
        upper = (lane // 8) % 2 == 1
        result = []
        for ex in range(2):
            low, high = blocks[ex], blocks[2 + ex]
            result.append(jnp.where(upper, pltpu.roll(high, 8, 1), low))
            result.append(jnp.where(upper, high, pltpu.roll(low, 120, 1)))
        return result

    def ungroup(values):
        upper = (lane // 8) % 2 == 1
        low, high = [], []
        for ex in range(2):
            a, b = values[2 * ex], values[2 * ex + 1]
            low.append(jnp.where(upper, pltpu.roll(b, 8, 1), a))
            high.append(jnp.where(upper, b, pltpu.roll(a, 120, 1)))
        return low + high

    wide = lambda row: jnp.broadcast_to(row, (8, 128))
    quarter = lambda ref, row, q: ref[row : row + 1, 128 * q : 128 * q + 128]
    distance = [(quarter(owner, 0, q) - wall + nw) % nw for q in range(4)]
    to_next = regroup([wide(jnp.where(d == 1, 1.0, 0.0)) for d in distance])
    to_prev = regroup([wide(jnp.where(d == nw - 1, 1.0, 0.0)) for d in distance])
    layer = regroup([wide((quarter(element, 0, q) % 2).astype(jnp.float32)) for q in range(4)])
    axes = [regroup([wide(quarter(coords, k, q)) for q in range(4)]) for k in range(3)]

    def lagrange(coord):
        value = table[LAG]
        for b in range(8):
            value = value * jnp.where(sub8 == b, 1.0, coord - GLL_NODES[b])
        return value

    pl.semaphore_wait(barrier, len(peers))

    copies = []
    slab_copies = []
    for d in range(2):
        copy = pltpu.make_async_remote_copy(
            src_ref=slab,
            dst_ref=slab_in.at[d],
            send_sem=slab_send.at[d],
            recv_sem=slab_recv.at[d],
            device_id=neighbours[d],
            device_id_type=MESH_ID,
        )
        copy.start()
        slab_copies.append(copy)
        copies.append(copy)

    basis = [[lagrange(axes[k][g]) for k in range(3)] for g in range(4)]
    second_wall = (lane // 8) % 2 == 1
    columns = []
    for g in range(4):
        ly = basis[g][2]
        blocks = []
        for side in range(2):
            for ey in range(2):
                chosen = jnp.logical_and(
                    wide(second_wall) == (side == 1), layer[g] == float(ey)
                )
                blocks.append(jnp.where(chosen, ly, 0.0))
        columns.append(jnp.concatenate(blocks, axis=0))

    nothing = jnp.zeros((32, 128), jnp.float32)
    masks = [[1.0 - to_next[g] - to_prev[g], to_prev[g], to_next[g]] for g in range(4)]

    def sample(source, g):
        ex, ez = g // 2, g % 2
        right = [
            jnp.concatenate(
                [columns[g] if k == 2 * ex + kk else nothing for k in range(4)], axis=0
            )
            for kk in range(2)
        ]
        rows = source[:, :, 8 * ez : 8 * ez + 8, :].reshape(64, 128)
        total = [jnp.zeros((8, 128), jnp.float32) for _ in range(2)]
        for kk in range(2):
            values = jnp.dot(
                rows, right[kk], precision=precise, preferred_element_type=jnp.float32
            ).reshape(2, 4, 8, 128)
            for comp in range(2):
                for x in range(4):
                    a = 4 * kk + x
                    total[comp] = total[comp] + values[comp, x] * basis[g][0][a : a + 1]
        return total

    sums = []
    for g in range(4):
        own = sample(slab, g)
        sums.append([own[comp] * masks[g][0] for comp in range(2)])
    for d in range(2):
        slab_copies[d].wait_recv()
        for g in range(4):
            far = sample(slab_in.at[d], g)
            for comp in range(2):
                sums[g][comp] = sums[g][comp] + far[comp] * masks[g][1 + d]
    stream = ungroup(
        [wide(jnp.sum(sums[g][0] * basis[g][1], axis=0, keepdims=True)) for g in range(4)]
    )
    spanwise = ungroup(
        [wide(jnp.sum(sums[g][1] * basis[g][1], axis=0, keepdims=True)) for g in range(4)]
    )

    for q in range(4):
        u, v = stream[q], spanwise[q]
        speed = jnp.sqrt(u * u + v * v + speed_floor)
        ratio = karman / jnp.log(sample_height / wide(quarter(roughness, 0, q)))
        factor = -(ratio * ratio * speed / viscosity)
        for comp, value in enumerate((u, v)):
            slope = factor * value
            neumann[comp : comp + 1, 128 * q : 128 * q + 128] = slope[:1]
            plane[comp * 4 + q : comp * 4 + q + 1, :] = (viscosity * slope * table[PLANE])[:1]

    plane_copies = []
    for d in range(8):
        copy = pltpu.make_async_remote_copy(
            src_ref=plane,
            dst_ref=plane_in.at[d],
            send_sem=send.at[0, d],
            recv_sem=recv.at[0, d],
            device_id=neighbours[d],
            device_id_type=MESH_ID,
        )
        copy.start()
        plane_copies.append(copy)
        copies.append(copy)

    node_z = lane8 % 16
    node_x = lane8 // 16
    half = sub8 % 2

    def join_span(mine, before, after):
        return (
            mine
            + jnp.where(node_z == 7, pltpu.roll(mine, 127, 1), 0.0)
            + jnp.where(node_z == 8, pltpu.roll(mine, 1, 1), 0.0)
            + jnp.where(node_z == 0, pltpu.roll(before, 113, 1), 0.0)
            + jnp.where(node_z == 15, pltpu.roll(after, 15, 1), 0.0)
        )

    def join_wall(mine, before, after):
        later = jnp.where(half == 0, pltpu.roll(mine, 7, 0), pltpu.roll(after, 1, 0))
        earlier = jnp.where(half == 0, pltpu.roll(before, 7, 0), pltpu.roll(mine, 1, 0))
        return (
            mine
            + jnp.where(node_x == 7, pltpu.roll(later, 112, 1), 0.0)
            + jnp.where(node_x == 0, pltpu.roll(earlier, 16, 1), 0.0)
        )

    for d in range(8):
        plane_copies[d].wait_recv()
    own_line = join_span(plane[...], plane_in[2], plane_in[3])
    before_line = join_span(plane_in[0], plane_in[4], plane_in[5])
    after_line = join_span(plane_in[1], plane_in[6], plane_in[7])
    stress = join_wall(own_line, before_line, after_line)
    lifted = lax.dot_general(
        stress,
        lift[...],
        (((0,), (0,)), ((), ())),
        precision=precise,
        preferred_element_type=jnp.float32,
    )
    for comp in range(2):
        for ex in range(2):
            column = (comp * 2 + ex) * 128
            here = res[2 * comp, 128 * ex : 128 * ex + 128]
            res[2 * comp, 128 * ex : 128 * ex + 128] = here + lifted[:, column : column + 128]

    cx = SCALE * viscosity * (2.0 / element_dx) * stiffness
    even = 0.5 * (cx[:4, :4] + cx[:4, 7:3:-1])
    odd = 0.5 * (cx[:4, :4] - cx[:4, 7:3:-1])

    def fold(value):
        return value[:8] + value[8:]

    def operate(source, target, index):
        for comp in range(3):
            total = jnp.zeros((16, 128), jnp.float32)
            for ex in range(2):
                base = 128 * ex
                along_y = jnp.dot(
                    source[comp, base : base + 128],
                    stiff[...],
                    precision=precise,
                    preferred_element_type=jnp.float32,
                )
                nodes = [source[comp, base + 16 * b : base + 16 * b + 16] for b in range(8)]
                plus = [nodes[b] + nodes[7 - b] for b in range(4)]
                minus = [nodes[b] - nodes[7 - b] for b in range(4)]
                along_x = [None] * 8
                for a in range(4):
                    sum_e = plus[0] * float(even[a, 0])
                    sum_o = minus[0] * float(odd[a, 0])
                    for b in range(1, 4):
                        sum_e = sum_e + plus[b] * float(even[a, b])
                        sum_o = sum_o + minus[b] * float(odd[a, b])
                    along_x[a] = sum_e + sum_o
                    along_x[7 - a] = sum_e - sum_o
                for a in range(8):
                    start = base + 16 * a
                    halves = []
                    for h in range(2):
                        along_z = None
                        for b in range(8):
                            row = start + 8 * h + b
                            term = source[comp, row : row + 1] * table[KZ + b]
                            along_z = term if along_z is None else along_z + term
                        halves.append(along_z)
                    along_z = jnp.concatenate(halves, axis=0)
                    local = along_x[a] * mass_zy + (
                        along_z * mass_y2 + along_y[16 * a : 16 * a + 16] * mass_z2
                    ) * mass_x[a]
                    total = total + local * nodes[a]
                    if target is not None:
                        target[comp, start : start + 16] = (
                            local
                            + last2 * pltpu.roll(local, 127, 1)
                            + first2 * pltpu.roll(local, 1, 1)
                        )
            mom[3 * index + comp] = fold(total)

    def exchange(target, turn):
        for comp in range(3):
            both_x = target[comp, 112:128] + target[comp, 128:144]
            target[comp, 112:128] = both_x
            target[comp, 128:144] = both_x
            inner, outer = pl.ds(7, 16, stride=16), pl.ds(8, 16, stride=16)
            both_z = target[comp, inner, :] + target[comp, outer, :]
            target[comp, inner, :] = both_z
            target[comp, outer, :] = both_z
        started = []

        def put(d, source, into):
            copy = pltpu.make_async_remote_copy(
                src_ref=source,
                dst_ref=into,
                send_sem=send.at[turn, d],
                recv_sem=recv.at[turn, d],
                device_id=neighbours[d],
                device_id_type=MESH_ID,
            )
            copy.start()
            started.append(copy)
            copies.append(copy)

        faces = (pl.ds(240, 16), pl.ds(0, 16), pl.ds(15, 16, stride=16), pl.ds(0, 16, stride=16))
        corners = (255, 240, 15, 0)
        for d in range(4):
            for comp in range(3):
                face[turn - 1, d, comp] = target[comp, faces[d], :]
            put(d, face.at[turn - 1, d], face_in.at[turn - 1, d])
        for d in range(4):
            for comp in range(3):
                row = corners[d]
                edge[turn - 1, d, comp : comp + 1, :] = target[comp, row : row + 1, :]
            put(4 + d, edge.at[turn - 1, d], edge_in.at[turn - 1, d])
        for copy in started:
            copy.wait_recv()
        into = (faces[1], faces[0], faces[3], faces[2])
        corner_into = (0, 15, 240, 255)
        for d in range(4):
            for comp in range(3):
                target[comp, into[d], :] = target[comp, into[d], :] + face_in[turn - 1, d, comp]
        for d in range(4):
            for comp in range(3):
                row = corner_into[d]
                target[comp, row : row + 1, :] = (
                    target[comp, row : row + 1, :] + edge_in[turn - 1, d, comp : comp + 1, :]
                )

    def weighted(pairs):
        for comp in range(3):
            totals = [jnp.zeros((16, 128), jnp.float32) for _ in pairs]
            edges = [jnp.zeros((16, 128), jnp.float32) for _ in pairs]
            for i in range(16):
                for n, (first, second, _) in enumerate(pairs):
                    term = (
                        first[comp, 16 * i : 16 * i + 16] * second[comp, 16 * i : 16 * i + 16]
                    )
                    if i % 8 in (0, 7):
                        edges[n] = edges[n] + term
                    else:
                        totals[n] = totals[n] + term
            for n, (_, _, index) in enumerate(pairs):
                mom[3 * index + comp] = fold((totals[n] + 0.5 * edges[n]) * count2)

    operate(res, one, 1)
    exchange(one, 1)
    operate(one, two, 3)
    exchange(two, 2)
    weighted([(res, res, 0), (one, one, 2), (two, two, 4)])
    operate(two, None, 5)

    row = jnp.zeros((8, 128), jnp.float32)
    for k in range(18):
        value = jnp.sum(mom[k], axis=1, keepdims=True)
        row = row + jnp.where(lane8 == k, value, 0.0)
    row = jnp.sum(row, axis=0, keepdims=True)

    start = 0
    for phase, (count, mine, place) in enumerate(groups):
        part[phase] = row
        started = []
        for k in range(1, count):
            copy = pltpu.make_async_remote_copy(
                src_ref=part.at[phase],
                dst_ref=part_in.at[start + mine],
                send_sem=sum_send.at[start + k],
                recv_sem=sum_recv.at[start + k],
                device_id=place((mine + k) % count),
                device_id_type=MESH_ID,
            )
            copy.start()
            started.append(copy)
            copies.append(copy)
        part_in[start + mine] = row
        for copy in started:
            copy.wait_recv()
        row = part_in[start]
        for k in range(1, count):
            row = row + part_in[start + k]
        start += count

    row = jnp.broadcast_to(row, (8, 128))
    moments = [row if j == 0 else pltpu.roll(row, 128 - 3 * j, 1) for j in range(6)]

    def inner(first, second, raise_by):
        total = None
        for i, a in enumerate(first):
            for j, b in enumerate(second):
                term = a * b * moments[i + j + raise_by]
                total = term if total is None else total + term
        return total

    unit = jnp.ones((8, 128), jnp.float32)
    direction, residual = [unit], [unit]
    answer = [jnp.zeros((8, 128), jnp.float32)] * 3
    norm = moments[0]
    for step in range(3):
        alpha = norm / inner(direction, direction, 1)
        for i, value in enumerate(direction):
            answer[i] = answer[i] + alpha * value
        if step == 2:
            break
        lowered = [-alpha * value for value in direction]
        residual = [residual[0]] + [
            lowered[i] + residual[i + 1] if i + 1 < len(residual) else lowered[i]
            for i in range(len(lowered))
        ]
        newer = inner(residual, residual, 0)
        growth = newer / norm
        direction = [
            value + growth * direction[i] if i < len(direction) else value
            for i, value in enumerate(residual)
        ]
        norm = newer
    for i, value in enumerate(answer):
        scalars[i : i + 1, :] = value[:1] * SCALE
    for copy in copies:
        copy.wait_send()


def combine(res, one, two, scalars, slopes, out, neumann, sums, sent):
    copies = [pltpu.make_async_copy(slopes, neumann, sent.at[3])]
    copies[0].start()
    for comp in range(3):
        c0, c1, c2 = (
            jnp.broadcast_to(scalars[k : k + 1, comp : comp + 1], (16, 128)) for k in range(3)
        )
        for i in range(16):
            rows = pl.ds(16 * i, 16)
            sums[comp, i] = (
                c0 * res[comp, rows, :] + c1 * one[comp, rows, :] + c2 * two[comp, rows, :]
            )
        copy = pltpu.make_async_copy(sums.at[comp], out.at[comp], sent.at[comp])
        copy.start()
        copies.append(copy)
    for copy in copies:
        copy.wait()


def body(sizes, velocity_old, heights, owner_device, owner_element, ref_coords, roughness):
    nx, ny, nc, ns = sizes
    slots = nx * nc + ny + ns
    f32, i32 = jnp.float32, jnp.int32
    vmem = pl.BlockSpec(memory_space=pltpu.VMEM)
    anywhere = pl.BlockSpec(memory_space=pl.ANY)
    constants = [jnp.asarray(value) for value in tables()]
    res, one, two, scalars, slopes = pl.pallas_call(
        functools.partial(kernel, sizes),
        out_shape=(
            pltpu.VMEM((3, 256, 128), f32),
            pltpu.VMEM((3, 256, 128), f32),
            pltpu.VMEM((3, 256, 128), f32),
            pltpu.VMEM((8, 128), f32),
            pltpu.VMEM((2, 512), f32),
        ),
        in_specs=[anywhere] * 9,
        out_specs=(vmem,) * 5,
        scratch_shapes=[
            pltpu.VMEM((3, 16, 16, 128), f32),
            pltpu.SMEM((16,), f32),
            pltpu.VMEM((1, 512), i32),
            pltpu.VMEM((1, 512), i32),
            pltpu.VMEM((3, 512), f32),
            pltpu.VMEM((1, 512), f32),
            pltpu.VMEM(constants[0].shape, f32),
            pltpu.VMEM(constants[1].shape, f32),
            pltpu.VMEM(constants[2].shape, f32),
            pltpu.VMEM((128, 128), f32),
            pltpu.VMEM((2, 4, 16, 128), f32),
            pltpu.VMEM((2, 2, 4, 16, 128), f32),
            pltpu.VMEM((8, 128), f32),
            pltpu.VMEM((8, 8, 128), f32),
            pltpu.VMEM((2, 4, 3, 16, 128), f32),
            pltpu.VMEM((2, 4, 3, 16, 128), f32),
            pltpu.VMEM((2, 4, 3, 128), f32),
            pltpu.VMEM((2, 4, 3, 128), f32),
            pltpu.VMEM((18, 8, 128), f32),
            pltpu.VMEM((3, 1, 128), f32),
            pltpu.VMEM((slots, 1, 128), f32),
            pltpu.SemaphoreType.DMA((9,)),
            pltpu.SemaphoreType.DMA((3, 8)),
            pltpu.SemaphoreType.DMA((3, 8)),
            pltpu.SemaphoreType.DMA((2,)),
            pltpu.SemaphoreType.DMA((2,)),
            pltpu.SemaphoreType.DMA((slots,)),
            pltpu.SemaphoreType.DMA((slots,)),
        ],
        compiler_params=pltpu.CompilerParams(collective_id=0, has_side_effects=True),
        name="channel_step",
    )(
        velocity_old,
        heights,
        owner_device.reshape(1, -1),
        owner_element.reshape(1, -1),
        ref_coords,
        roughness.reshape(1, -1),
        *constants,
    )
    return pl.pallas_call(
        combine,
        out_shape=(
            jax.ShapeDtypeStruct((3, 16, 16, 128), f32),
            jax.ShapeDtypeStruct((2, 512), f32),
        ),
        in_specs=[vmem] * 5,
        out_specs=(anywhere, anywhere),
        scratch_shapes=[
            pltpu.VMEM((3, 16, 16, 128), f32),
            pltpu.SemaphoreType.DMA((4,)),
        ],
        name="combine",
    )(
        *(
            pltpu.with_memory_space_constraint(value, pltpu.VMEM)
            for value in (res, one, two, scalars, slopes)
        )
    )


def torus_program(torus):
    sizes = tuple(torus.shape[name] for name in AXES)
    return jax.shard_map(
        functools.partial(body, sizes),
        mesh=torus,
        in_specs=(
            P(None, WALL, "span", None),
            P(),
            P(WALL_SPAN, None),
            P(WALL_SPAN, None),
            P(None, WALL_SPAN),
            P(WALL_SPAN),
        ),
        out_specs=(P(None, WALL, "span", None), P(None, WALL_SPAN)),
        check_vma=False,
    )


def solution(mesh):
    return torus_program(Mesh(mesh.devices.reshape(4, 8, 2, mesh.shape["span"]), AXES))
```

```python
import functools

import jax
import jax.numpy as jnp
import numpy as np
from jax import lax
from jax.experimental import pallas as pl
from jax.experimental.pallas import tpu as pltpu
from jax.sharding import Mesh
from jax.sharding import PartitionSpec as P

AXES = ("wall_0", "wall_1", "wall_2", "span")
WALL_SPAN = AXES
WALL = ("wall_0", "wall_1", "wall_2")
MESH_ID = pl.DeviceIdType.MESH

GLL_NODES = (
    -1.0,
    -0.8717401485096066,
    -0.5917001814331423,
    -0.2092992179024789,
    0.2092992179024789,
    0.5917001814331423,
    0.8717401485096066,
    1.0,
)
GLL_WEIGHTS = (
    0.03571428571428571,
    0.2107042271435061,
    0.3411226924835044,
    0.4124587946587038,
    0.4124587946587038,
    0.3411226924835044,
    0.2107042271435061,
    0.03571428571428571,
)
viscosity = 0.02
inverse_step = 20.0
karman = 0.41
sample_height = 0.1
speed_floor = 0.01
element_dx = 0.05
element_dz = 0.13
precise = lax.Precision.HIGHEST

SCALE = 64.0

SHIFTS = ((1, 0), (-1, 0), (0, 1), (0, -1), (1, 1), (1, -1), (-1, 1), (-1, -1))

MZ, QMZ, COUNT, LAG, PLANE, HALFW, LAST, FIRST, KZ = range(9)
BLOCK, LIFT = 16, 32


def stiffness_table():
    points = np.array(GLL_NODES)
    weights = np.array(GLL_WEIGHTS)
    previous = np.ones(8)
    current = points.copy()
    for degree in range(1, 7):
        previous, current = (
            current,
            ((2 * degree + 1) * points * current - degree * previous) / (degree + 1),
        )
    derivative = np.zeros((8, 8))
    for target in range(8):
        for source in range(8):
            if target != source:
                derivative[target, source] = (
                    current[target] / current[source] / (points[target] - points[source])
                )
    derivative[0, 0] = -14.0
    derivative[7, 7] = 14.0
    return derivative.T @ (weights[:, None] * derivative)


def tables():
    weights = np.array(GLL_WEIGHTS)
    points = np.array(GLL_NODES)
    stiffness = stiffness_table()
    ones = np.ones((8, 128))
    lane = np.arange(128)
    ends = np.array([2.0, 1, 1, 1, 1, 1, 1, 2.0])
    mass_x = 0.5 * element_dx * weights
    mass_z = 0.5 * element_dz * weights
    count_y = np.where((lane % 8 == 0) | (lane % 8 == 7), 0.5, 1.0)
    count_y[0] = count_y[127] = 1.0
    gaps = points[:, None] - points[None, :] + np.eye(8)
    kz = SCALE * (
        viscosity * (2.0 / element_dz) * stiffness + inverse_step * np.diag(mass_z)
    )
    rows = [
        mass_z[:, None] * ones,
        (mass_z * ends)[:, None] * ones,
        (1.0 / ends)[:, None] * count_y[None, :],
        (1.0 / np.prod(gaps, axis=1))[:, None] * ones,
        ones * (mass_x[lane // 16] * mass_z[lane % 8])[None, :],
        ones * (0.5 * weights[lane % 8])[None, :],
        ones * ((lane % 8 == 7) & (lane < 127))[None, :],
        ones * ((lane % 8 == 0) & (lane > 0))[None, :],
    ]
    rows += [kz[:, b][:, None] * ones for b in range(8)]
    block = np.kron(np.eye(16), SCALE * viscosity * 2.0 * stiffness)
    lift = np.zeros((8, 512))
    for comp in range(2):
        for half in range(2):
            column = (comp * 2 + half) * 128
            lift[comp * 4 + half, column] = 1.0
            lift[comp * 4 + 2 + half, column + 127] = 1.0
    pieces = [np.stack(rows), block.reshape(16, 8, 128), lift.reshape(8, 4, 128).transpose(1, 0, 2)]
    return np.concatenate(pieces).astype(np.float32)


def kernel(sizes, *refs):
    operands, refs = refs[:7], refs[7:]
    (res, one, two, scalars, neumann), refs = refs[:5], refs[5:]
    local, refs = refs[:7], refs[7:]
    velocity, heights, owner, element, coords, roughness, table = local
    (stiff, stiff_joined, slab, slab_in, plane, plane_in, face, face_in, mom, part, part_in,
     load, send, slab_recv, recv, ready) = refs
    nx, ny, nc, ns = sizes
    nw = nx * ny * nc
    loads = [
        pltpu.make_async_copy(source, target, load.at[n])
        for n, (source, target) in enumerate(zip(operands, local))
    ]
    for copy in loads:
        copy.start()
    wx, wy, wc, sp = (lax.axis_index(name) for name in AXES)
    wall = (wx * ny + wy) * nc + wc
    weights = np.array(GLL_WEIGHTS)
    stiffness = stiffness_table()
    mass_x = [float(v) for v in 0.5 * element_dx * weights]
    ends = [2.0, 1.0, 1.0, 1.0, 1.0, 1.0, 1.0, 2.0]

    def ring(value, shift, count):
        if shift > 0:
            return jnp.where(value >= count - shift, value + shift - count, value + shift)
        return jnp.where(value < -shift, value + shift + count, value + shift)

    def beside(dw):
        if dw == 0:
            return wx, wy, wc
        turn = wc == (nc - 1 if dw > 0 else 0)
        turn_y = jnp.logical_and(turn, wy == (ny - 1 if dw > 0 else 0))
        return (
            jnp.where(turn_y, ring(wx, dw, nx), wx),
            jnp.where(turn, ring(wy, dw, ny), wy),
            ring(wc, dw, nc),
        )

    along = {dw: beside(dw) for dw in (-1, 0, 1)}
    across = {0: sp, 1: ring(sp, 1, ns), -1: ring(sp, -1, ns)}
    neighbours = [(*along[dw], across[ds]) for dw, ds in SHIFTS]
    over_x = lambda k: (ring(wx, k, nx), wy, wc, sp)
    over_y = lambda k: (wx, ring(wy, k, ny), wc, sp)
    over_z = lambda k: (wx, wy, wc, ring(sp, k, ns))
    over_pair = lambda k: (
        ring(wx, k // nc, nx) if k // nc else wx,
        wy,
        ring(wc, k % nc, nc) if k % nc else wc,
        sp,
    )
    groups = [
        (nx * nc, wx * nc + wc, over_pair),
        (ny, wy, over_y),
        (ns, sp, over_z),
    ]

    barrier = pltpu.get_barrier_semaphore()
    near = list(neighbours) + [over_pair(k) for k in range(nc)][1:]
    near += [over_pair(k * nc + c) for k in (1, nx - 1) for c in range(nc)]
    near += [over_y(1), over_y(-1)]
    for peer in near:
        pl.semaphore_signal(barrier, inc=1, device_id=peer, device_id_type=MESH_ID)
    relays = [
        [over_x(1), over_x(-1), over_y(1), over_y(-1), over_z(1), over_z(-1)],
        [over_y(2), over_y(-2), over_z(2), over_z(-2)],
        [over_z(2), over_z(-2)],
    ]

    def tell(n):
        for peer in relays[n]:
            pl.semaphore_signal(ready.at[n], inc=1, device_id=peer, device_id_type=MESH_ID)

    def hear(n):
        pl.semaphore_wait(ready.at[n], len(relays[n]))

    def push(source, target, send_sem, recv_sem, peer):
        pltpu.make_async_remote_copy(
            src_ref=source,
            dst_ref=target,
            send_sem=send_sem,
            recv_sem=recv_sem,
            device_id=peer,
            device_id_type=MESH_ID,
        ).start()

    def wait_bytes(like, sem):
        pltpu.make_async_copy(like, like, sem).wait()

    for copy in loads:
        copy.wait()

    lane = lax.broadcasted_iota(jnp.int32, (1, 128), 1)
    sub8 = lax.broadcasted_iota(jnp.int32, (8, 128), 0)
    lane8 = lax.broadcasted_iota(jnp.int32, (8, 128), 1)

    height = jnp.zeros((8, 128), jnp.float32)
    for layer in range(16):
        height = jnp.where(lane8 // 8 == layer, heights[layer], height)
    mass_y = height * table[HALFW]
    block = table[BLOCK : BLOCK + 16].reshape(128, 128) * (1.0 / height)[:1]
    stiff[...] = block
    stiff_joined[...] = (
        block
        + table[LAST][:1] * pltpu.roll(block, 127, 1)
        + table[FIRST][:1] * pltpu.roll(block, 1, 1)
    )
    joined_y = (
        mass_y
        + table[LAST] * pltpu.roll(mass_y, 127, 1)
        + table[FIRST] * pltpu.roll(mass_y, 1, 1)
    )
    both = lambda value: jnp.concatenate([value, value], axis=0)
    mass_zy = both(table[MZ] * mass_y)
    mass_y2 = both(mass_y)
    mass_z2 = both(table[MZ])
    joined_y2 = both(joined_y)
    joined_z2 = both(table[QMZ])
    joined_zy = both(table[QMZ] * joined_y)
    count2 = both(table[COUNT])

    for comp in range(2):
        quarters = []
        for k in range(4):
            quarters.append(velocity[2 * comp, 4 * k : 4 * k + 4].reshape(64, 128))
        packed = jnp.zeros((64, 128), jnp.float32)
        where_to = lax.broadcasted_iota(jnp.int32, (64, 128), 1)
        for k in range(4):
            low = pltpu.roll(quarters[k], 32 * k, 1) if k else quarters[k]
            shift = (32 * k + 32) % 128
            high = pltpu.roll(quarters[k], shift, 1) if shift else quarters[k]
            packed = jnp.where(where_to // 16 == 2 * k, low, packed)
            packed = jnp.where(where_to // 16 == 2 * k + 1, high, packed)
        slab[comp] = packed.reshape(4, 16, 128)

    scale_zy = both(table[QMZ] * joined_y) * inverse_step
    for comp in range(3):
        for i in range(16):
            res[comp, 16 * i : 16 * i + 16] = velocity[comp, i] * (
                scale_zy * (mass_x[i % 8] * ends[i % 8])
            )

    def regroup(blocks):
        upper = (lane // 8) % 2 == 1
        result = []
        for ex in range(2):
            low, high = blocks[ex], blocks[2 + ex]
            result.append(jnp.where(upper, pltpu.roll(high, 8, 1), low))
            result.append(jnp.where(upper, high, pltpu.roll(low, 120, 1)))
        return result

    def ungroup(values):
        upper = (lane // 8) % 2 == 1
        low, high = [], []
        for ex in range(2):
            a, b = values[2 * ex], values[2 * ex + 1]
            low.append(jnp.where(upper, pltpu.roll(b, 8, 1), a))
            high.append(jnp.where(upper, b, pltpu.roll(a, 120, 1)))
        return low + high

    wide = lambda row: jnp.broadcast_to(row, (8, 128))
    quarter = lambda ref, row, q: ref[row : row + 1, 128 * q : 128 * q + 128]
    distance = [(quarter(owner, 0, q) - wall + nw) % nw for q in range(4)]
    to_next = regroup([wide(jnp.where(d == 1, 1.0, 0.0)) for d in distance])
    to_prev = regroup([wide(jnp.where(d == nw - 1, 1.0, 0.0)) for d in distance])
    layer = regroup([wide((quarter(element, 0, q) % 2).astype(jnp.float32)) for q in range(4)])
    axes = [regroup([wide(quarter(coords, k, q)) for q in range(4)]) for k in range(3)]

    def lagrange(coord):
        value = table[LAG]
        for b in range(8):
            value = value * jnp.where(sub8 == b, 1.0, coord - GLL_NODES[b])
        return value

    pl.semaphore_wait(barrier, len(near))

    tell(0)
    for d in range(2):
        push(slab, slab_in.at[d], send.at[0], slab_recv.at[d], neighbours[d])

    basis = [[lagrange(axes[k][g]) for k in range(3)] for g in range(4)]
    second_wall = (lane // 8) % 2 == 1
    columns = []
    for g in range(4):
        ly = basis[g][2]
        blocks = []
        for side in range(2):
            for ey in range(2):
                chosen = jnp.logical_and(
                    wide(second_wall) == (side == 1), layer[g] == float(ey)
                )
                blocks.append(jnp.where(chosen, ly, 0.0))
        columns.append(jnp.concatenate(blocks, axis=0))

    nothing = jnp.zeros((32, 128), jnp.float32)
    masks = [[1.0 - to_next[g] - to_prev[g], to_prev[g], to_next[g]] for g in range(4)]

    def sample(source, g):
        ex, ez = g // 2, g % 2
        right = [
            jnp.concatenate(
                [columns[g] if k == 2 * ex + kk else nothing for k in range(4)], axis=0
            )
            for kk in range(2)
        ]
        rows = source[:, :, 8 * ez : 8 * ez + 8, :].reshape(64, 128)
        total = [jnp.zeros((8, 128), jnp.float32) for _ in range(2)]
        for kk in range(2):
            values = jnp.dot(
                rows, right[kk], precision=precise, preferred_element_type=jnp.float32
            ).reshape(2, 4, 8, 128)
            for comp in range(2):
                for x in range(4):
                    a = 4 * kk + x
                    total[comp] = total[comp] + values[comp, x] * basis[g][0][a : a + 1]
        return total

    sums = []
    for g in range(4):
        own = sample(slab, g)
        sums.append([own[comp] * masks[g][0] for comp in range(2)])
    for d in range(2):
        wait_bytes(slab_in.at[d], slab_recv.at[d])
        for g in range(4):
            far = sample(slab_in.at[d], g)
            for comp in range(2):
                sums[g][comp] = sums[g][comp] + far[comp] * masks[g][1 + d]
    stream = ungroup(
        [wide(jnp.sum(sums[g][0] * basis[g][1], axis=0, keepdims=True)) for g in range(4)]
    )
    spanwise = ungroup(
        [wide(jnp.sum(sums[g][1] * basis[g][1], axis=0, keepdims=True)) for g in range(4)]
    )

    for q in range(4):
        u, v = stream[q], spanwise[q]
        speed = jnp.sqrt(u * u + v * v + speed_floor)
        ratio = karman / jnp.log(sample_height / wide(quarter(roughness, 0, q)))
        factor = -(ratio * ratio * speed / viscosity)
        for comp, value in enumerate((u, v)):
            slope = factor * value
            neumann[comp : comp + 1, 128 * q : 128 * q + 128] = slope[:1]
            plane[comp * 4 + q : comp * 4 + q + 1, :] = (viscosity * slope * table[PLANE])[:1]

    for d in range(8):
        push(plane, plane_in.at[d], send.at[1], recv.at[0], neighbours[d])
    hear(0)
    tell(1)

    node_z = lane8 % 16
    node_x = lane8 // 16
    half = sub8 % 2

    def join_span(mine, before, after):
        return (
            mine
            + jnp.where(node_z == 7, pltpu.roll(mine, 127, 1), 0.0)
            + jnp.where(node_z == 8, pltpu.roll(mine, 1, 1), 0.0)
            + jnp.where(node_z == 0, pltpu.roll(before, 113, 1), 0.0)
            + jnp.where(node_z == 15, pltpu.roll(after, 15, 1), 0.0)
        )

    def join_wall(mine, before, after):
        later = jnp.where(half == 0, pltpu.roll(mine, 7, 0), pltpu.roll(after, 1, 0))
        earlier = jnp.where(half == 0, pltpu.roll(before, 7, 0), pltpu.roll(mine, 1, 0))
        return (
            mine
            + jnp.where(node_x == 7, pltpu.roll(later, 112, 1), 0.0)
            + jnp.where(node_x == 0, pltpu.roll(earlier, 16, 1), 0.0)
        )

    wait_bytes(plane_in, recv.at[0])
    own_line = join_span(plane[...], plane_in[2], plane_in[3])
    before_line = join_span(plane_in[0], plane_in[4], plane_in[5])
    after_line = join_span(plane_in[1], plane_in[6], plane_in[7])
    stress = join_wall(own_line, before_line, after_line)
    lifted = lax.dot_general(
        stress,
        jnp.concatenate([table[LIFT + k] for k in range(4)], axis=1),
        (((0,), (0,)), ((), ())),
        precision=precise,
        preferred_element_type=jnp.float32,
    )
    for comp in range(2):
        for ex in range(2):
            column = (comp * 2 + ex) * 128
            here = res[2 * comp, 128 * ex : 128 * ex + 128]
            res[2 * comp, 128 * ex : 128 * ex + 128] = here + lifted[:, column : column + 128]

    cx = SCALE * viscosity * (2.0 / element_dx) * stiffness
    even = 0.5 * (cx[:4, :4] + cx[:4, 7:3:-1])
    odd = 0.5 * (cx[:4, :4] - cx[:4, 7:3:-1])

    def fold(value):
        return value[:8] + value[8:]

    def spectral_x(nodes):
        plus = [nodes[b] + nodes[7 - b] for b in range(4)]
        minus = [nodes[b] - nodes[7 - b] for b in range(4)]
        result = [None] * 8
        for a in range(4):
            sum_e = plus[0] * float(even[a, 0])
            sum_o = minus[0] * float(odd[a, 0])
            for b in range(1, 4):
                sum_e = sum_e + plus[b] * float(even[a, b])
                sum_o = sum_o + minus[b] * float(odd[a, b])
            result[a] = sum_e + sum_o
            result[7 - a] = sum_e - sum_o
        return result

    def spectral_z(source, comp, start):
        halves = []
        for h in range(2):
            total = None
            for b in range(8):
                row = start + 8 * h + b
                term = source[comp, row : row + 1] * table[KZ + b]
                total = term if total is None else total + term
            halves.append(total)
        return halves

    def along_y(source, comp, base, matrix):
        return jnp.dot(
            source[comp, base : base + 128],
            matrix[...],
            precision=precise,
            preferred_element_type=jnp.float32,
        )

    def operate(source, target, turn):
        for comp in range(3):
            seam = None
            for ex in range(2):
                base = 128 * ex
                normal = along_y(source, comp, base, stiff_joined)
                nodes = [source[comp, base + 16 * b : base + 16 * b + 16] for b in range(8)]
                stream = [value * joined_zy for value in spectral_x(nodes)]
                if ex == 0:
                    face[turn, 1, comp] = stream[0]
                    seam = stream[7]
                else:
                    face[turn, 0, comp] = stream[7]
                    target[comp, 112:128] = target[comp, 112:128] + stream[0]
                    stream[0] = stream[0] + seam
                for a in range(8):
                    start = base + 16 * a
                    low, high = spectral_z(source, comp, start)
                    i = 8 * ex + a
                    edge = mass_x[a] * ends[a]
                    face[turn, 3, comp, i : i + 1] = (low * joined_y)[:1] * edge
                    face[turn, 2, comp, i : i + 1] = (high * joined_y)[7:] * edge
                    joined = jnp.concatenate(
                        [
                            low + jnp.where(sub8 == 7, pltpu.roll(high, 7, 0), 0.0),
                            high + jnp.where(sub8 == 0, pltpu.roll(low, 1, 0), 0.0),
                        ],
                        axis=0,
                    )
                    target[comp, start : start + 16] = stream[a] + edge * (
                        joined * joined_y2 + normal[16 * a : 16 * a + 16] * joined_z2
                    )
        for d in range(4):
            push(
                face.at[turn, d], face_in.at[turn, d], send.at[2 + turn], recv.at[1 + turn],
                neighbours[d],
            )

    def receive(target, turn):
        wait_bytes(face_in.at[turn], recv.at[1 + turn])
        into = (
            pl.ds(0, 16),
            pl.ds(240, 16),
            pl.ds(0, 16, stride=16),
            pl.ds(15, 16, stride=16),
        )
        for d in range(4):
            for comp in range(3):
                target[comp, into[d], :] = target[comp, into[d], :] + face_in[turn, d, comp]

    def energy(source, index):
        for comp in range(3):
            total = jnp.zeros((16, 128), jnp.float32)
            for ex in range(2):
                base = 128 * ex
                normal = along_y(source, comp, base, stiff)
                nodes = [source[comp, base + 16 * b : base + 16 * b + 16] for b in range(8)]
                stream = spectral_x(nodes)
                for a in range(8):
                    spanned = jnp.concatenate(spectral_z(source, comp, base + 16 * a), axis=0)
                    local = stream[a] * mass_zy + mass_x[a] * (
                        spanned * mass_y2 + normal[16 * a : 16 * a + 16] * mass_z2
                    )
                    total = total + local * nodes[a]
            mom[3 * index + comp] = fold(total)

    def weighted(pairs):
        for comp in range(3):
            totals = [jnp.zeros((16, 128), jnp.float32) for _ in pairs]
            edges = [jnp.zeros((16, 128), jnp.float32) for _ in pairs]
            for i in range(16):
                for n, (first, second, _) in enumerate(pairs):
                    term = (
                        first[comp, 16 * i : 16 * i + 16] * second[comp, 16 * i : 16 * i + 16]
                    )
                    if i % 8 in (0, 7):
                        edges[n] = edges[n] + term
                    else:
                        totals[n] = totals[n] + term
            for n, (_, _, index) in enumerate(pairs):
                mom[3 * index + comp] = fold((totals[n] + 0.5 * edges[n]) * count2)

    operate(res, one, 0)
    hear(1)
    tell(2)
    receive(one, 0)
    operate(one, two, 1)
    weighted([(res, res, 0), (res, one, 1), (one, one, 2)])
    hear(2)
    receive(two, 1)
    weighted([(one, two, 3), (two, two, 4)])
    energy(two, 5)

    row = jnp.zeros((8, 128), jnp.float32)
    for k in range(18):
        value = jnp.sum(mom[k], axis=1, keepdims=True)
        row = row + jnp.where(lane8 == k, value, 0.0)
    row = jnp.sum(row, axis=0, keepdims=True)

    start = 0
    for phase, (count, mine, place) in enumerate(groups):
        part[phase] = row
        for k in range(1, count):
            push(
                part.at[phase], part_in.at[start + mine], send.at[4 + phase], recv.at[3 + phase],
                place(k),
            )
        part_in[start + mine] = row
        wait_bytes(part_in.at[pl.ds(start, count - 1)], recv.at[3 + phase])
        row = part_in[start]
        for k in range(1, count):
            row = row + part_in[start + k]
        start += count

    row = jnp.broadcast_to(row, (8, 128))
    moments = [row if j == 0 else pltpu.roll(row, 128 - 3 * j, 1) for j in range(6)]

    def inner(first, second, raise_by):
        total = None
        for i, a in enumerate(first):
            for j, b in enumerate(second):
                term = a * b * moments[i + j + raise_by]
                total = term if total is None else total + term
        return total

    unit = jnp.ones((8, 128), jnp.float32)
    direction, residual = [unit], [unit]
    answer = [jnp.zeros((8, 128), jnp.float32)] * 3
    norm = moments[0]
    for step in range(3):
        alpha = norm / inner(direction, direction, 1)
        for i, value in enumerate(direction):
            answer[i] = answer[i] + alpha * value
        if step == 2:
            break
        lowered = [-alpha * value for value in direction]
        residual = [residual[0]] + [
            lowered[i] + residual[i + 1] if i + 1 < len(residual) else lowered[i]
            for i in range(len(lowered))
        ]
        newer = inner(residual, residual, 0)
        growth = newer / norm
        direction = [
            value + growth * direction[i] if i < len(direction) else value
            for i, value in enumerate(residual)
        ]
        norm = newer
    for i, value in enumerate(answer):
        scalars[i : i + 1, :] = value[:1] * SCALE
    wait_bytes(slab_in, send.at[0])
    wait_bytes(plane_in, send.at[1])
    for turn in range(2):
        wait_bytes(face_in.at[turn], send.at[2 + turn])
    start = 0
    for phase, (count, _, _) in enumerate(groups):
        wait_bytes(part_in.at[pl.ds(start, count - 1)], send.at[4 + phase])
        start += count


def combine(res, one, two, scalars, slopes, out, neumann, sums, sent):
    copies = [pltpu.make_async_copy(slopes, neumann, sent.at[3])]
    copies[0].start()
    for comp in range(3):
        c0, c1, c2 = (
            jnp.broadcast_to(scalars[k : k + 1, comp : comp + 1], (16, 128)) for k in range(3)
        )
        for i in range(16):
            rows = pl.ds(16 * i, 16)
            sums[comp, i] = (
                c0 * res[comp, rows, :] + c1 * one[comp, rows, :] + c2 * two[comp, rows, :]
            )
        copy = pltpu.make_async_copy(sums.at[comp], out.at[comp], sent.at[comp])
        copy.start()
        copies.append(copy)
    for copy in copies:
        copy.wait()


def body(sizes, velocity_old, heights, owner_device, owner_element, ref_coords, roughness):
    nx, ny, nc, ns = sizes
    slots = nx * nc + ny + ns
    f32, i32 = jnp.float32, jnp.int32
    vmem = pl.BlockSpec(memory_space=pltpu.VMEM)
    anywhere = pl.BlockSpec(memory_space=pl.ANY)
    constants = jnp.asarray(tables())
    res, one, two, scalars, slopes = pl.pallas_call(
        functools.partial(kernel, sizes),
        out_shape=(
            pltpu.VMEM((3, 256, 128), f32),
            pltpu.VMEM((3, 256, 128), f32),
            pltpu.VMEM((3, 256, 128), f32),
            pltpu.VMEM((8, 128), f32),
            pltpu.VMEM((2, 512), f32),
        ),
        in_specs=[anywhere] * 7,
        out_specs=(vmem,) * 5,
        scratch_shapes=[
            pltpu.VMEM((3, 16, 16, 128), f32),
            pltpu.SMEM((16,), f32),
            pltpu.VMEM((1, 512), i32),
            pltpu.VMEM((1, 512), i32),
            pltpu.VMEM((3, 512), f32),
            pltpu.VMEM((1, 512), f32),
            pltpu.VMEM(constants.shape, f32),
            pltpu.VMEM((128, 128), f32),
            pltpu.VMEM((128, 128), f32),
            pltpu.VMEM((2, 4, 16, 128), f32),
            pltpu.VMEM((2, 2, 4, 16, 128), f32),
            pltpu.VMEM((8, 128), f32),
            pltpu.VMEM((8, 8, 128), f32),
            pltpu.VMEM((2, 4, 3, 16, 128), f32),
            pltpu.VMEM((2, 4, 3, 16, 128), f32),
            pltpu.VMEM((18, 8, 128), f32),
            pltpu.VMEM((3, 1, 128), f32),
            pltpu.VMEM((slots, 1, 128), f32),
            pltpu.SemaphoreType.DMA((7,)),
            pltpu.SemaphoreType.DMA((7,)),
            pltpu.SemaphoreType.DMA((2,)),
            pltpu.SemaphoreType.DMA((6,)),
            pltpu.SemaphoreType.REGULAR((3,)),
        ],
        compiler_params=pltpu.CompilerParams(collective_id=0, has_side_effects=True),
        name="channel_step",
    )(
        velocity_old,
        heights,
        owner_device.reshape(1, -1),
        owner_element.reshape(1, -1),
        ref_coords,
        roughness.reshape(1, -1),
        constants,
    )
    return pl.pallas_call(
        combine,
        out_shape=(
            jax.ShapeDtypeStruct((3, 16, 16, 128), f32),
            jax.ShapeDtypeStruct((2, 512), f32),
        ),
        in_specs=[vmem] * 5,
        out_specs=(anywhere, anywhere),
        scratch_shapes=[
            pltpu.VMEM((3, 16, 16, 128), f32),
            pltpu.SemaphoreType.DMA((4,)),
        ],
        name="combine",
    )(
        *(
            pltpu.with_memory_space_constraint(value, pltpu.VMEM)
            for value in (res, one, two, scalars, slopes)
        )
    )


def torus_program(torus):
    sizes = tuple(torus.shape[name] for name in AXES)
    return jax.shard_map(
        functools.partial(body, sizes),
        mesh=torus,
        in_specs=(
            P(None, WALL, "span", None),
            P(),
            P(WALL_SPAN, None),
            P(WALL_SPAN, None),
            P(None, WALL_SPAN),
            P(WALL_SPAN),
        ),
        out_specs=(P(None, WALL, "span", None), P(None, WALL_SPAN)),
        check_vma=False,
    )


def solution(mesh):
    return torus_program(Mesh(mesh.devices.reshape(4, 8, 2, mesh.shape["span"]), AXES))
```

```python
import functools

import jax
import jax.numpy as jnp
import numpy as np
from jax import lax
from jax.experimental import pallas as pl
from jax.experimental.pallas import tpu as pltpu
from jax.sharding import Mesh
from jax.sharding import PartitionSpec as P

AXES = ("wall_0", "wall_1", "wall_2", "span")
WALL_SPAN = AXES
WALL = ("wall_0", "wall_1", "wall_2")
MESH_ID = pl.DeviceIdType.MESH

GLL_NODES = (
    -1.0,
    -0.8717401485096066,
    -0.5917001814331423,
    -0.2092992179024789,
    0.2092992179024789,
    0.5917001814331423,
    0.8717401485096066,
    1.0,
)
GLL_WEIGHTS = (
    0.03571428571428571,
    0.2107042271435061,
    0.3411226924835044,
    0.4124587946587038,
    0.4124587946587038,
    0.3411226924835044,
    0.2107042271435061,
    0.03571428571428571,
)
viscosity = 0.02
inverse_step = 20.0
karman = 0.41
sample_height = 0.1
speed_floor = 0.01
element_dx = 0.05
element_dz = 0.13
precise = lax.Precision.HIGHEST

SCALE = 64.0

SHIFTS = ((1, 0), (-1, 0), (0, 1), (0, -1), (1, 1), (1, -1), (-1, 1), (-1, -1))

MZ, QMZ, COUNT, LAG, PLANE, HALFW, LAST, FIRST = range(8)
BLOCK, LIFT, FLAT = 8, 24, 28


def stiffness_table():
    points = np.array(GLL_NODES)
    weights = np.array(GLL_WEIGHTS)
    previous = np.ones(8)
    current = points.copy()
    for degree in range(1, 7):
        previous, current = (
            current,
            ((2 * degree + 1) * points * current - degree * previous) / (degree + 1),
        )
    derivative = np.zeros((8, 8))
    for target in range(8):
        for source in range(8):
            if target != source:
                derivative[target, source] = (
                    current[target] / current[source] / (points[target] - points[source])
                )
    derivative[0, 0] = -14.0
    derivative[7, 7] = 14.0
    return derivative.T @ (weights[:, None] * derivative)


def tables():
    weights = np.array(GLL_WEIGHTS)
    points = np.array(GLL_NODES)
    stiffness = stiffness_table()
    ones = np.ones((8, 128))
    lane = np.arange(128)
    ends = np.array([2.0, 1, 1, 1, 1, 1, 1, 2.0])
    mass_x = 0.5 * element_dx * weights
    mass_z = 0.5 * element_dz * weights
    count_y = np.where((lane % 8 == 0) | (lane % 8 == 7), 0.5, 1.0)
    count_y[0] = count_y[127] = 1.0
    gaps = points[:, None] - points[None, :] + np.eye(8)
    rows = [
        mass_z[:, None] * ones,
        (mass_z * ends)[:, None] * ones,
        (1.0 / ends)[:, None] * count_y[None, :],
        (1.0 / np.prod(gaps, axis=1))[:, None] * ones,
        ones * (mass_x[lane // 16] * mass_z[lane % 8])[None, :],
        ones * (0.5 * weights[lane % 8])[None, :],
        ones * ((lane % 8 == 7) & (lane < 127))[None, :],
        ones * ((lane % 8 == 0) & (lane > 0))[None, :],
    ]
    block = np.kron(np.eye(16), SCALE * viscosity * 2.0 * stiffness)
    lift = np.zeros((8, 512))
    for comp in range(2):
        for half in range(2):
            column = (comp * 2 + half) * 128
            lift[comp * 4 + half, column] = 1.0
            lift[comp * 4 + 2 + half, column + 127] = 1.0
    joined_x = np.tile(mass_x * ends, 2)
    joined_z = np.tile(mass_z * ends, 2)

    def chain(length):
        scaled = SCALE * viscosity * (2.0 / length) * stiffness
        full = np.kron(np.eye(2), scaled)
        ends_only = full[[15, 0]]
        full[7] = full[8] = full[7] + full[8]
        return full, ends_only

    chain_x, ends_x = chain(element_dx)
    chain_z, ends_z = chain(element_dz)
    flat = np.kron(chain_x, np.diag(joined_z)) + np.kron(np.diag(joined_x), chain_z)
    flat += SCALE * inverse_step * np.diag(np.kron(joined_x, joined_z))
    faces = [np.kron(ends_x[d : d + 1], np.diag(joined_z)) for d in range(2)]
    faces += [np.kron(np.diag(joined_x), ends_z[d : d + 1]) for d in range(2)]
    flat = np.concatenate([flat] + faces).astype(np.float32)
    flat_high = flat.astype(jnp.bfloat16)
    flat_low = (flat - flat_high.astype(np.float32)).astype(jnp.bfloat16)
    pieces = [np.stack(rows), block.reshape(16, 8, 128), lift.reshape(8, 4, 128).transpose(1, 0, 2)]
    pieces += [joined_x[:, None, None] * (mass_z * ends)[None, :, None] * np.ones((16, 8, 128))]
    return np.concatenate(pieces).astype(np.float32), np.stack([flat_high, flat_low])


def kernel(sizes, *refs):
    operands, refs = refs[:8], refs[8:]
    (res, one, two, scalars, neumann), refs = refs[:5], refs[5:]
    local, refs = refs[:8], refs[8:]
    velocity, heights, owner, element, coords, roughness, table, flat = local
    (normal, right_high, right_low, slab, slab_in, plane, plane_in, face, face_in, mom, part, part_in,
     load, send, slab_recv, recv, ready) = refs
    nx, ny, nc, ns = sizes
    nw = nx * ny * nc
    loads = [
        pltpu.make_async_copy(source, target, load.at[n])
        for n, (source, target) in enumerate(zip(operands, local))
    ]
    for copy in loads:
        copy.start()
    wx, wy, wc, sp = (lax.axis_index(name) for name in AXES)
    wall = (wx * ny + wy) * nc + wc
    weights = np.array(GLL_WEIGHTS)
    stiffness = stiffness_table()
    mass_x = [float(v) for v in 0.5 * element_dx * weights]
    ends = [2.0, 1.0, 1.0, 1.0, 1.0, 1.0, 1.0, 2.0]

    def ring(value, shift, count):
        if shift > 0:
            return jnp.where(value >= count - shift, value + shift - count, value + shift)
        return jnp.where(value < -shift, value + shift + count, value + shift)

    def beside(dw):
        if dw == 0:
            return wx, wy, wc
        turn = wc == (nc - 1 if dw > 0 else 0)
        turn_y = jnp.logical_and(turn, wy == (ny - 1 if dw > 0 else 0))
        return (
            jnp.where(turn_y, ring(wx, dw, nx), wx),
            jnp.where(turn, ring(wy, dw, ny), wy),
            ring(wc, dw, nc),
        )

    along = {dw: beside(dw) for dw in (-1, 0, 1)}
    across = {0: sp, 1: ring(sp, 1, ns), -1: ring(sp, -1, ns)}
    neighbours = [(*along[dw], across[ds]) for dw, ds in SHIFTS]
    place_x = {0: wx, 1: ring(wx, 1, nx), -1: ring(wx, -1, nx), 2: ring(wx, 2, nx)}
    place_y = {k: ring(wy, k, ny) if k else wy for k in range(-(ny // 2) + 1, ny // 2 + 1)}
    place_y[-2] = ring(wy, -2, ny)
    place_z = {k: ring(sp, k, ns) if k else sp for k in range(-(ns // 2) + 1, ns // 2 + 1)}
    place_z[-2] = ring(sp, -2, ns)
    other = ring(wc, 1, nc)
    flat_peer = lambda dx, dy: (place_x[dx], place_y[dy], wc, sp)
    deep_peer = lambda c, ds: (wx, wy, c, place_z[ds])

    def far_first(keys):
        return sorted(keys, key=lambda key: -abs(key[0]) - abs(key[1]))

    deep = far_first([(c, k) for c in (0, 1) for k in range(-(ns // 2) + 1, ns // 2 + 1)])
    deep = [key for key in deep if key != (0, 0)]
    wide_x = [k for k in (-1, 0, 1, 2) if -(nx // 2) < k <= nx // 2]
    plain = far_first([(a, b) for a in wide_x for b in range(-(ny // 2) + 1, ny // 2 + 1)])
    plain = [key for key in plain if key != (0, 0)]
    groups = [
        (nc * ns, wc * ns + sp, [deep_peer((wc, other)[c], k) for c, k in deep]),
        (nx * ny, wx * ny + wy, [flat_peer(a, b) for a, b in plain]),
    ]

    barrier = pltpu.get_barrier_semaphore()
    near = neighbours[:4] + [deep_peer(other, 0)]
    near += [flat_peer(1, 0), flat_peer(-1, 0), flat_peer(0, 1), flat_peer(0, -1)]
    for peer in near:
        pl.semaphore_signal(barrier, inc=1, device_id=peer, device_id_type=MESH_ID)
    relays = [
        near,
        [flat_peer(1, 0), flat_peer(-1, 0), flat_peer(0, 2), flat_peer(0, -2)]
        + [deep_peer(wc, 2), deep_peer(wc, -2)],
        [flat_peer(1, 0), flat_peer(-1, 0), flat_peer(0, 2), flat_peer(0, -2)]
        + [flat_peer(2, 2), flat_peer(2, -2), deep_peer(wc, 4), deep_peer(wc, -4)],
    ]

    def tell(n):
        for peer in relays[n]:
            pl.semaphore_signal(ready.at[n], inc=1, device_id=peer, device_id_type=MESH_ID)

    def hear(n):
        pl.semaphore_wait(ready.at[n], len(relays[n]))

    def push(source, target, send_sem, recv_sem, peer):
        pltpu.make_async_remote_copy(
            src_ref=source,
            dst_ref=target,
            send_sem=send_sem,
            recv_sem=recv_sem,
            device_id=peer,
            device_id_type=MESH_ID,
        ).start()

    def wait_bytes(like, sem):
        pltpu.make_async_copy(like, like, sem).wait()

    for copy in loads:
        copy.wait()

    lane = lax.broadcasted_iota(jnp.int32, (1, 128), 1)
    sub8 = lax.broadcasted_iota(jnp.int32, (8, 128), 0)
    lane8 = lax.broadcasted_iota(jnp.int32, (8, 128), 1)

    height = jnp.zeros((8, 128), jnp.float32)
    for layer in range(16):
        height = jnp.where(lane8 // 8 == layer, heights[layer], height)
    mass_y = height * table[HALFW]
    block = table[BLOCK : BLOCK + 16].reshape(128, 128) * (1.0 / height)[:1]
    block = (
        block
        + table[LAST][:1] * pltpu.roll(block, 127, 1)
        + table[FIRST][:1] * pltpu.roll(block, 1, 1)
    )

    def split(value):
        high = value.astype(jnp.bfloat16)
        return high, (value - high.astype(jnp.float32)).astype(jnp.bfloat16)

    block_high, block_low = split(block)
    normal[:128, :128] = block_high
    normal[128:, :128] = block_high
    normal[:128, 128:] = block_low
    normal[128:, 128:] = jnp.zeros((128, 128), jnp.bfloat16)
    right_high[...] = jnp.zeros(right_high.shape, jnp.bfloat16)
    right_low[...] = jnp.zeros(right_low.shape, jnp.bfloat16)
    joined_y = (
        mass_y
        + table[LAST] * pltpu.roll(mass_y, 127, 1)
        + table[FIRST] * pltpu.roll(mass_y, 1, 1)
    )
    both = lambda value: jnp.concatenate([value, value], axis=0)
    joined_y2 = both(joined_y)
    count2 = both(table[COUNT])

    for comp in range(2):
        quarters = []
        for k in range(4):
            quarters.append(velocity[2 * comp, 4 * k : 4 * k + 4].reshape(64, 128))
        packed = jnp.zeros((64, 128), jnp.float32)
        where_to = lax.broadcasted_iota(jnp.int32, (64, 128), 1)
        for k in range(4):
            low = pltpu.roll(quarters[k], 32 * k, 1) if k else quarters[k]
            shift = (32 * k + 32) % 128
            high = pltpu.roll(quarters[k], shift, 1) if shift else quarters[k]
            packed = jnp.where(where_to // 16 == 2 * k, low, packed)
            packed = jnp.where(where_to // 16 == 2 * k + 1, high, packed)
        slab[comp] = packed.reshape(4, 16, 128)

    scale_zy = both(table[QMZ] * joined_y) * inverse_step
    for comp in range(3):
        for i in range(16):
            res[comp, 16 * i : 16 * i + 16] = velocity[comp, i] * (
                scale_zy * (mass_x[i % 8] * ends[i % 8])
            )

    def regroup(blocks):
        upper = (lane // 8) % 2 == 1
        result = []
        for ex in range(2):
            low, high = blocks[ex], blocks[2 + ex]
            result.append(jnp.where(upper, pltpu.roll(high, 8, 1), low))
            result.append(jnp.where(upper, high, pltpu.roll(low, 120, 1)))
        return result

    def ungroup(values):
        upper = (lane // 8) % 2 == 1
        low, high = [], []
        for ex in range(2):
            a, b = values[2 * ex], values[2 * ex + 1]
            low.append(jnp.where(upper, pltpu.roll(b, 8, 1), a))
            high.append(jnp.where(upper, b, pltpu.roll(a, 120, 1)))
        return low + high

    wide = lambda row: jnp.broadcast_to(row, (8, 128))
    quarter = lambda ref, row, q: ref[row : row + 1, 128 * q : 128 * q + 128]
    distance = [(quarter(owner, 0, q) - wall + nw) % nw for q in range(4)]
    to_next = regroup([wide(jnp.where(d == 1, 1.0, 0.0)) for d in distance])
    to_prev = regroup([wide(jnp.where(d == nw - 1, 1.0, 0.0)) for d in distance])
    layer = regroup([wide((quarter(element, 0, q) % 2).astype(jnp.float32)) for q in range(4)])
    axes = [regroup([wide(quarter(coords, k, q)) for q in range(4)]) for k in range(3)]

    def lagrange(coord):
        value = table[LAG]
        for b in range(8):
            value = value * jnp.where(sub8 == b, 1.0, coord - GLL_NODES[b])
        return value

    pl.semaphore_wait(barrier, len(near))

    tell(0)
    for d in range(2):
        push(slab, slab_in.at[d], send.at[0], slab_recv.at[d], neighbours[d])

    basis = [[lagrange(axes[k][g]) for k in range(3)] for g in range(4)]
    second_wall = (lane // 8) % 2 == 1
    for g in range(4):
        ly = basis[g][2]
        blocks = []
        for side in range(2):
            for ey in range(2):
                chosen = jnp.logical_and(
                    wide(second_wall) == (side == 1), layer[g] == float(ey)
                )
                blocks.append(jnp.where(chosen, ly, 0.0))
        high, low = split(jnp.concatenate(blocks, axis=0))
        for kk in range(2):
            k = 2 * (g // 2) + kk
            column = slice(128 * kk, 128 * kk + 128)
            right_high[g, 32 * k : 32 * k + 32, column] = high
            right_high[g, 128 + 32 * k : 160 + 32 * k, column] = high
            right_low[g, 32 * k : 32 * k + 32, column] = low

    masks = [[1.0 - to_next[g] - to_prev[g], to_prev[g], to_next[g]] for g in range(4)]

    def sample(source, g):
        ez = g % 2
        high, low = split(source[:, :, 8 * ez : 8 * ez + 8, :].reshape(64, 128))
        product = jnp.dot(
            jnp.concatenate([high, low], axis=1), right_high[g],
            preferred_element_type=jnp.float32,
        ) + jnp.dot(high, right_low[g], preferred_element_type=jnp.float32)
        total = [jnp.zeros((8, 128), jnp.float32) for _ in range(2)]
        for kk in range(2):
            values = product[:, 128 * kk : 128 * kk + 128].reshape(2, 4, 8, 128)
            for comp in range(2):
                for x in range(4):
                    a = 4 * kk + x
                    total[comp] = total[comp] + values[comp, x] * basis[g][0][a : a + 1]
        return total

    sums = []
    for g in range(4):
        own = sample(slab, g)
        sums.append([own[comp] * masks[g][0] for comp in range(2)])
    for d in range(2):
        wait_bytes(slab_in.at[d], slab_recv.at[d])
        for g in range(4):
            far = sample(slab_in.at[d], g)
            for comp in range(2):
                sums[g][comp] = sums[g][comp] + far[comp] * masks[g][1 + d]
    stream = ungroup(
        [wide(jnp.sum(sums[g][0] * basis[g][1], axis=0, keepdims=True)) for g in range(4)]
    )
    spanwise = ungroup(
        [wide(jnp.sum(sums[g][1] * basis[g][1], axis=0, keepdims=True)) for g in range(4)]
    )

    for q in range(4):
        u, v = stream[q], spanwise[q]
        speed = jnp.sqrt(u * u + v * v + speed_floor)
        ratio = karman / jnp.log(sample_height / wide(quarter(roughness, 0, q)))
        factor = -(ratio * ratio * speed / viscosity)
        for comp, value in enumerate((u, v)):
            slope = factor * value
            neumann[comp : comp + 1, 128 * q : 128 * q + 128] = slope[:1]
            plane[comp * 4 + q : comp * 4 + q + 1, :] = (viscosity * slope * table[PLANE])[:1]

    hear(0)
    for d in range(8):
        push(plane, plane_in.at[d], send.at[1], recv.at[0], neighbours[d])
    tell(1)

    node_z = lane8 % 16
    node_x = lane8 // 16
    half = sub8 % 2

    def join_span(mine, before, after):
        return (
            mine
            + jnp.where(node_z == 7, pltpu.roll(mine, 127, 1), 0.0)
            + jnp.where(node_z == 8, pltpu.roll(mine, 1, 1), 0.0)
            + jnp.where(node_z == 0, pltpu.roll(before, 113, 1), 0.0)
            + jnp.where(node_z == 15, pltpu.roll(after, 15, 1), 0.0)
        )

    def join_wall(mine, before, after):
        later = jnp.where(half == 0, pltpu.roll(mine, 7, 0), pltpu.roll(after, 1, 0))
        earlier = jnp.where(half == 0, pltpu.roll(before, 7, 0), pltpu.roll(mine, 1, 0))
        return (
            mine
            + jnp.where(node_x == 7, pltpu.roll(later, 112, 1), 0.0)
            + jnp.where(node_x == 0, pltpu.roll(earlier, 16, 1), 0.0)
        )

    wait_bytes(plane_in, recv.at[0])
    own_line = join_span(plane[...], plane_in[2], plane_in[3])
    before_line = join_span(plane_in[0], plane_in[4], plane_in[5])
    after_line = join_span(plane_in[1], plane_in[6], plane_in[7])
    stress = join_wall(own_line, before_line, after_line)
    lift = jnp.concatenate([table[LIFT + k] for k in range(4)], axis=1)
    stress_high = stress.astype(jnp.bfloat16).astype(jnp.float32)
    lifted = lax.dot_general(
        jnp.concatenate([stress_high, stress - stress_high], axis=0),
        jnp.concatenate([lift, lift], axis=0),
        (((0,), (0,)), ((), ())),
        preferred_element_type=jnp.float32,
    )
    for comp in range(2):
        for ex in range(2):
            column = (comp * 2 + ex) * 128
            here = res[2 * comp, 128 * ex : 128 * ex + 128]
            res[2 * comp, 128 * ex : 128 * ex + 128] = here + lifted[:, column : column + 128]

    row16 = lax.broadcasted_iota(jnp.int32, (16, 128), 0) % 8
    share_x = jnp.where(jnp.logical_or(row16 == 0, row16 == 7), 0.5, 1.0)
    half_y = wide(table[COUNT][:1])

    def fold(value):
        return value[:8] + value[8:]

    def apply(source, comp):
        high, low = split(source[comp])
        parts = jnp.concatenate([high, low], axis=1)
        along = jnp.dot(flat[0], parts, preferred_element_type=jnp.float32)
        along = along[:, :128] + along[:, 128:]
        along = along + jnp.dot(flat[1], high, preferred_element_type=jnp.float32)
        across_y = jnp.dot(parts, normal[...], preferred_element_type=jnp.float32)
        return along, across_y[:, :128] + across_y[:, 128:]

    def operate(source, target, turn):
        for comp in range(3):
            along, across_y = apply(source, comp)
            for d in range(4):
                rows = slice(256 + 16 * d, 272 + 16 * d)
                face[turn, d, comp] = along[rows] * joined_y2
                push(
                    face.at[turn, d, comp], face_in.at[turn, d, comp], send.at[2 + turn],
                    recv.at[1 + turn], neighbours[d],
                )
            for i in range(16):
                rows = slice(16 * i, 16 * i + 16)
                target[comp, rows] = along[rows] * joined_y2 + across_y[rows] * both(
                    table[FLAT + i]
                )

    def receive(target, turn):
        wait_bytes(face_in.at[turn], recv.at[1 + turn])
        into = (
            pl.ds(0, 16),
            pl.ds(240, 16),
            pl.ds(0, 16, stride=16),
            pl.ds(15, 16, stride=16),
        )
        for d in range(4):
            for comp in range(3):
                target[comp, into[d], :] = target[comp, into[d], :] + face_in[turn, d, comp]

    def energy(source, index):
        for comp in range(3):
            along, across_y = apply(source, comp)
            inside = jnp.zeros((16, 128), jnp.float32)
            edges = jnp.zeros((16, 128), jnp.float32)
            for i in range(16):
                rows = slice(16 * i, 16 * i + 16)
                term = source[comp, rows] * (
                    along[rows] * joined_y2 + across_y[rows] * both(table[FLAT + i])
                )
                if i % 8 in (0, 7):
                    edges = edges + term
                else:
                    inside = inside + term
            for d, i in ((0, 15), (1, 0)):
                sent = along[256 + 16 * d : 272 + 16 * d] * joined_y2
                edges = edges + sent * source[comp, 16 * i : 16 * i + 16]
            total = fold((inside + 0.5 * edges) * count2)
            for d, first in ((2, 15), (3, 0)):
                sent = along[256 + 16 * d : 272 + 16 * d] * joined_y2
                term = sent * source[comp, pl.ds(first, 16, stride=16), :]
                total = total + fold(term * share_x) * half_y
            mom[3 * index + comp] = total

    def weighted(pairs):
        for comp in range(3):
            totals = [jnp.zeros((16, 128), jnp.float32) for _ in pairs]
            edges = [jnp.zeros((16, 128), jnp.float32) for _ in pairs]
            for i in range(16):
                for n, (first, second, _) in enumerate(pairs):
                    term = (
                        first[comp, 16 * i : 16 * i + 16] * second[comp, 16 * i : 16 * i + 16]
                    )
                    if i % 8 in (0, 7):
                        edges[n] = edges[n] + term
                    else:
                        totals[n] = totals[n] + term
            for n, (_, _, index) in enumerate(pairs):
                mom[3 * index + comp] = fold((totals[n] + 0.5 * edges[n]) * count2)

    operate(res, one, 0)
    hear(1)
    tell(2)
    receive(one, 0)
    operate(one, two, 1)
    weighted([(res, res, 0), (res, one, 1), (one, one, 2)])
    hear(2)
    receive(two, 1)
    weighted([(one, two, 3), (two, two, 4)])
    energy(two, 5)

    row = jnp.zeros((8, 128), jnp.float32)
    for k in range(18):
        value = jnp.sum(mom[k], axis=1, keepdims=True)
        row = row + jnp.where(lane8 == k, value, 0.0)
    row = jnp.sum(row, axis=0, keepdims=True)

    start = 0
    for phase, (count, mine, peers) in enumerate(groups):
        part[phase] = row
        for peer in peers:
            push(
                part.at[phase], part_in.at[start + mine], send.at[4 + phase], recv.at[3 + phase],
                peer,
            )
        part_in[start + mine] = row
        wait_bytes(part_in.at[pl.ds(start, count - 1)], recv.at[3 + phase])
        row = part_in[start]
        for k in range(1, count):
            row = row + part_in[start + k]
        start += count

    row = jnp.broadcast_to(row, (8, 128))
    moments = [row if j == 0 else pltpu.roll(row, 128 - 3 * j, 1) for j in range(6)]

    def inner(first, second, raise_by):
        total = None
        for i, a in enumerate(first):
            for j, b in enumerate(second):
                term = a * b * moments[i + j + raise_by]
                total = term if total is None else total + term
        return total

    unit = jnp.ones((8, 128), jnp.float32)
    direction, residual = [unit], [unit]
    answer = [jnp.zeros((8, 128), jnp.float32)] * 3
    norm = moments[0]
    for step in range(3):
        alpha = norm / inner(direction, direction, 1)
        for i, value in enumerate(direction):
            answer[i] = answer[i] + alpha * value
        if step == 2:
            break
        lowered = [-alpha * value for value in direction]
        residual = [residual[0]] + [
            lowered[i] + residual[i + 1] if i + 1 < len(residual) else lowered[i]
            for i in range(len(lowered))
        ]
        newer = inner(residual, residual, 0)
        growth = newer / norm
        direction = [
            value + growth * direction[i] if i < len(direction) else value
            for i, value in enumerate(residual)
        ]
        norm = newer
    for i, value in enumerate(answer):
        scalars[i : i + 1, :] = value[:1] * SCALE
    wait_bytes(slab_in, send.at[0])
    wait_bytes(plane_in, send.at[1])
    for turn in range(2):
        wait_bytes(face_in.at[turn], send.at[2 + turn])
    start = 0
    for phase, (count, _, _) in enumerate(groups):
        wait_bytes(part_in.at[pl.ds(start, count - 1)], send.at[4 + phase])
        start += count


def combine(res, one, two, scalars, slopes, out, neumann, sums, sent):
    copies = [pltpu.make_async_copy(slopes, neumann, sent.at[3])]
    copies[0].start()
    for comp in range(3):
        c0, c1, c2 = (
            jnp.broadcast_to(scalars[k : k + 1, comp : comp + 1], (16, 128)) for k in range(3)
        )
        for i in range(16):
            rows = pl.ds(16 * i, 16)
            sums[comp, i] = (
                c0 * res[comp, rows, :] + c1 * one[comp, rows, :] + c2 * two[comp, rows, :]
            )
        copy = pltpu.make_async_copy(sums.at[comp], out.at[comp], sent.at[comp])
        copy.start()
        copies.append(copy)
    for copy in copies:
        copy.wait()


def body(sizes, velocity_old, heights, owner_device, owner_element, ref_coords, roughness):
    nx, ny, nc, ns = sizes
    slots = nc * ns + nx * ny
    f32, i32 = jnp.float32, jnp.int32
    vmem = pl.BlockSpec(memory_space=pltpu.VMEM)
    anywhere = pl.BlockSpec(memory_space=pl.ANY)
    constants, flat = (jnp.asarray(value) for value in tables())
    res, one, two, scalars, slopes = pl.pallas_call(
        functools.partial(kernel, sizes),
        out_shape=(
            pltpu.VMEM((3, 256, 128), f32),
            pltpu.VMEM((3, 256, 128), f32),
            pltpu.VMEM((3, 256, 128), f32),
            pltpu.VMEM((8, 128), f32),
            pltpu.VMEM((2, 512), f32),
        ),
        in_specs=[anywhere] * 8,
        out_specs=(vmem,) * 5,
        scratch_shapes=[
            pltpu.VMEM((3, 16, 16, 128), f32),
            pltpu.SMEM((16,), f32),
            pltpu.VMEM((1, 512), i32),
            pltpu.VMEM((1, 512), i32),
            pltpu.VMEM((3, 512), f32),
            pltpu.VMEM((1, 512), f32),
            pltpu.VMEM(constants.shape, f32),
            pltpu.VMEM(flat.shape, jnp.bfloat16),
            pltpu.VMEM((256, 256), jnp.bfloat16),
            pltpu.VMEM((4, 256, 256), jnp.bfloat16),
            pltpu.VMEM((4, 128, 256), jnp.bfloat16),
            pltpu.VMEM((2, 4, 16, 128), f32),
            pltpu.VMEM((2, 2, 4, 16, 128), f32),
            pltpu.VMEM((8, 128), f32),
            pltpu.VMEM((8, 8, 128), f32),
            pltpu.VMEM((2, 4, 3, 16, 128), f32),
            pltpu.VMEM((2, 4, 3, 16, 128), f32),
            pltpu.VMEM((18, 8, 128), f32),
            pltpu.VMEM((2, 1, 128), f32),
            pltpu.VMEM((slots, 1, 128), f32),
            pltpu.SemaphoreType.DMA((8,)),
            pltpu.SemaphoreType.DMA((6,)),
            pltpu.SemaphoreType.DMA((2,)),
            pltpu.SemaphoreType.DMA((5,)),
            pltpu.SemaphoreType.REGULAR((3,)),
        ],
        compiler_params=pltpu.CompilerParams(collective_id=0, has_side_effects=True),
        name="channel_step",
    )(
        velocity_old,
        heights,
        owner_device.reshape(1, -1),
        owner_element.reshape(1, -1),
        ref_coords,
        roughness.reshape(1, -1),
        constants,
        flat,
    )
    return pl.pallas_call(
        combine,
        out_shape=(
            jax.ShapeDtypeStruct((3, 16, 16, 128), f32),
            jax.ShapeDtypeStruct((2, 512), f32),
        ),
        in_specs=[vmem] * 5,
        out_specs=(anywhere, anywhere),
        scratch_shapes=[
            pltpu.VMEM((3, 16, 16, 128), f32),
            pltpu.SemaphoreType.DMA((4,)),
        ],
        name="combine",
    )(
        *(
            pltpu.with_memory_space_constraint(value, pltpu.VMEM)
            for value in (res, one, two, scalars, slopes)
        )
    )


def torus_program(torus):
    sizes = tuple(torus.shape[name] for name in AXES)
    return jax.shard_map(
        functools.partial(body, sizes),
        mesh=torus,
        in_specs=(
            P(None, WALL, "span", None),
            P(),
            P(WALL_SPAN, None),
            P(WALL_SPAN, None),
            P(None, WALL_SPAN),
            P(WALL_SPAN),
        ),
        out_specs=(P(None, WALL, "span", None), P(None, WALL_SPAN)),
        check_vma=False,
    )


def solution(mesh):
    return torus_program(Mesh(mesh.devices.reshape(4, 8, 2, mesh.shape["span"]), AXES))
```

```python
import functools

import jax
import jax.numpy as jnp
import numpy as np
from jax import lax
from jax.experimental import pallas as pl
from jax.experimental.pallas import tpu as pltpu
from jax.sharding import Mesh
from jax.sharding import PartitionSpec as P

AXES = ("wall_0", "wall_1", "wall_2", "span")
WALL_SPAN = AXES
WALL = ("wall_0", "wall_1", "wall_2")
MESH_ID = pl.DeviceIdType.MESH

GLL_NODES = (
    -1.0,
    -0.8717401485096066,
    -0.5917001814331423,
    -0.2092992179024789,
    0.2092992179024789,
    0.5917001814331423,
    0.8717401485096066,
    1.0,
)
GLL_WEIGHTS = (
    0.03571428571428571,
    0.2107042271435061,
    0.3411226924835044,
    0.4124587946587038,
    0.4124587946587038,
    0.3411226924835044,
    0.2107042271435061,
    0.03571428571428571,
)
viscosity = 0.02
inverse_step = 20.0
karman = 0.41
sample_height = 0.1
speed_floor = 0.01
element_dx = 0.05
element_dz = 0.13
precise = lax.Precision.HIGHEST

SCALE = 64.0

SHIFTS = ((1, 0), (-1, 0), (0, 1), (0, -1), (1, 1), (1, -1), (-1, 1), (-1, -1))

MZ, QMZ, COUNT, LAG, PLANE, HALFW, LAST, FIRST, LANEX, LANEZ = range(10)
BLOCK, LIFT, FLAT = 10, 26, 30


def stiffness_table():
    points = np.array(GLL_NODES)
    weights = np.array(GLL_WEIGHTS)
    previous = np.ones(8)
    current = points.copy()
    for degree in range(1, 7):
        previous, current = (
            current,
            ((2 * degree + 1) * points * current - degree * previous) / (degree + 1),
        )
    derivative = np.zeros((8, 8))
    for target in range(8):
        for source in range(8):
            if target != source:
                derivative[target, source] = (
                    current[target] / current[source] / (points[target] - points[source])
                )
    derivative[0, 0] = -14.0
    derivative[7, 7] = 14.0
    return derivative.T @ (weights[:, None] * derivative)


def tables():
    weights = np.array(GLL_WEIGHTS)
    points = np.array(GLL_NODES)
    stiffness = stiffness_table()
    ones = np.ones((8, 128))
    lane = np.arange(128)
    ends = np.array([2.0, 1, 1, 1, 1, 1, 1, 2.0])
    mass_x = 0.5 * element_dx * weights
    mass_z = 0.5 * element_dz * weights
    count_y = np.where((lane % 8 == 0) | (lane % 8 == 7), 0.5, 1.0)
    count_y[0] = count_y[127] = 1.0
    gaps = points[:, None] - points[None, :] + np.eye(8)
    rows = [
        mass_z[:, None] * ones,
        (mass_z * ends)[:, None] * ones,
        (1.0 / ends)[:, None] * count_y[None, :],
        (1.0 / np.prod(gaps, axis=1))[:, None] * ones,
        ones * (mass_x[lane // 16] * mass_z[lane % 8])[None, :],
        ones * (0.5 * weights[lane % 8])[None, :],
        ones * ((lane % 8 == 7) & (lane < 127))[None, :],
        ones * ((lane % 8 == 0) & (lane > 0))[None, :],
    ]
    block = np.kron(np.eye(16), SCALE * viscosity * 2.0 * stiffness)
    lift = np.zeros((8, 512))
    for comp in range(2):
        for half in range(2):
            column = (comp * 2 + half) * 128
            lift[comp * 4 + half, column] = 1.0
            lift[comp * 4 + 2 + half, column + 127] = 1.0
    joined_x = np.tile(mass_x * ends, 2)
    joined_z = np.tile(mass_z * ends, 2)

    def chain(length):
        scaled = SCALE * viscosity * (2.0 / length) * stiffness
        full = np.kron(np.eye(2), scaled)
        ends_only = full[[15, 0]]
        full[7] = full[8] = full[7] + full[8]
        return full, ends_only

    chain_x, ends_x = chain(element_dx)
    chain_z, ends_z = chain(element_dz)
    flat = np.kron(chain_x, np.diag(joined_z)) + np.kron(np.diag(joined_x), chain_z)
    flat += SCALE * inverse_step * np.diag(np.kron(joined_x, joined_z))
    faces = [np.kron(ends_x[d : d + 1], np.diag(joined_z)) for d in range(2)]
    faces += [np.kron(np.diag(joined_x), ends_z[d : d + 1]) for d in range(2)]
    flat = np.concatenate([flat] + faces).astype(np.float32)
    flat_high = flat.astype(jnp.bfloat16)
    flat_low = (flat - flat_high.astype(np.float32)).astype(jnp.bfloat16)
    line_x = SCALE * viscosity * (2.0 / element_dx) * stiffness
    line_z = SCALE * viscosity * (2.0 / element_dz) * stiffness
    line = np.concatenate([np.kron(line_x.T, np.eye(16)), np.kron(np.eye(16), line_z.T)], axis=1)
    line_high = line.astype(np.float32).astype(jnp.bfloat16)
    line_low = (line.astype(np.float32) - line_high.astype(np.float32)).astype(jnp.bfloat16)
    lines = np.concatenate([line_high, line_high, line_low])
    rows += [
        ones * (mass_x * ends)[lane // 16][None, :],
        ones * (mass_z * ends)[lane % 8][None, :],
    ]
    pieces = [np.stack(rows), block.reshape(16, 8, 128), lift.reshape(8, 4, 128).transpose(1, 0, 2)]
    pieces += [joined_x[:, None, None] * (mass_z * ends)[None, :, None] * np.ones((16, 8, 128))]
    return np.concatenate(pieces).astype(np.float32), np.stack([flat_high, flat_low]), lines


def kernel(sizes, *refs):
    operands, refs = refs[:9], refs[9:]
    (res, one, two, scalars, neumann), refs = refs[:5], refs[5:]
    local, refs = refs[:9], refs[9:]
    velocity, heights, owner, element, coords, roughness, table, flat, lines = local
    (normal, lifting, right_high, right_low, slab, slab_in, plane, plane_in, face, face_in, mom, part, part_in,
     load, send, slab_recv, recv, ready) = refs
    nx, ny, nc, ns = sizes
    nw = nx * ny * nc
    loads = [
        pltpu.make_async_copy(source, target, load.at[n])
        for n, (source, target) in enumerate(zip(operands, local))
    ]
    for copy in loads:
        copy.start()
    wx, wy, wc, sp = (lax.axis_index(name) for name in AXES)
    wall = (wx * ny + wy) * nc + wc
    weights = np.array(GLL_WEIGHTS)
    stiffness = stiffness_table()
    mass_x = [float(v) for v in 0.5 * element_dx * weights]
    ends = [2.0, 1.0, 1.0, 1.0, 1.0, 1.0, 1.0, 2.0]

    def ring(value, shift, count):
        if shift > 0:
            return jnp.where(value >= count - shift, value + shift - count, value + shift)
        return jnp.where(value < -shift, value + shift + count, value + shift)

    def beside(dw):
        if dw == 0:
            return wx, wy, wc
        turn = wc == (nc - 1 if dw > 0 else 0)
        turn_y = jnp.logical_and(turn, wy == (ny - 1 if dw > 0 else 0))
        return (
            jnp.where(turn_y, ring(wx, dw, nx), wx),
            jnp.where(turn, ring(wy, dw, ny), wy),
            ring(wc, dw, nc),
        )

    along = {dw: beside(dw) for dw in (-1, 0, 1)}
    across = {0: sp, 1: ring(sp, 1, ns), -1: ring(sp, -1, ns)}
    neighbours = [(*along[dw], across[ds]) for dw, ds in SHIFTS]
    place_x = {0: wx, 1: ring(wx, 1, nx), -1: ring(wx, -1, nx), 2: ring(wx, 2, nx)}
    place_y = {k: ring(wy, k, ny) if k else wy for k in range(-(ny // 2) + 1, ny // 2 + 1)}
    place_y[-2] = ring(wy, -2, ny)
    place_z = {k: ring(sp, k, ns) if k else sp for k in range(-(ns // 2) + 1, ns // 2 + 1)}
    place_z[-2] = ring(sp, -2, ns)
    other = ring(wc, 1, nc)
    flat_peer = lambda dx, dy: (place_x[dx], place_y[dy], wc, sp)
    deep_peer = lambda c, ds: (wx, wy, c, place_z[ds])

    def far_first(keys):
        return sorted(keys, key=lambda key: -abs(key[0]) - abs(key[1]))

    deep = far_first([(c, k) for c in (0, 1) for k in range(-(ns // 2) + 1, ns // 2 + 1)])
    deep = [key for key in deep if key != (0, 0)]
    wide_x = [k for k in (-1, 0, 1, 2) if -(nx // 2) < k <= nx // 2]
    plain = far_first([(a, b) for a in wide_x for b in range(-(ny // 2) + 1, ny // 2 + 1)])
    plain = [key for key in plain if key != (0, 0)]
    groups = [
        (nc * ns, wc * ns + sp, [deep_peer((wc, other)[c], k) for c, k in deep]),
        (nx * ny, wx * ny + wy, [flat_peer(a, b) for a, b in plain]),
    ]

    barrier = pltpu.get_barrier_semaphore()
    near = neighbours[:4] + [deep_peer(other, 0)]
    near += [flat_peer(1, 0), flat_peer(-1, 0), flat_peer(0, 1), flat_peer(0, -1)]
    for peer in near:
        pl.semaphore_signal(barrier, inc=1, device_id=peer, device_id_type=MESH_ID)
    relays = [
        near,
        [flat_peer(1, 0), flat_peer(-1, 0), flat_peer(0, 2), flat_peer(0, -2)]
        + [deep_peer(wc, 2), deep_peer(wc, -2)],
        [flat_peer(1, 0), flat_peer(-1, 0), flat_peer(0, 2), flat_peer(0, -2)]
        + [flat_peer(2, 2), flat_peer(2, -2), deep_peer(wc, 4), deep_peer(wc, -4)],
    ]

    def tell(n):
        for peer in relays[n]:
            pl.semaphore_signal(ready.at[n], inc=1, device_id=peer, device_id_type=MESH_ID)

    def hear(n):
        pl.semaphore_wait(ready.at[n], len(relays[n]))

    def push(source, target, send_sem, recv_sem, peer):
        pltpu.make_async_remote_copy(
            src_ref=source,
            dst_ref=target,
            send_sem=send_sem,
            recv_sem=recv_sem,
            device_id=peer,
            device_id_type=MESH_ID,
        ).start()

    def wait_bytes(like, sem):
        pltpu.make_async_copy(like, like, sem).wait()

    loads[0].wait()

    lane = lax.broadcasted_iota(jnp.int32, (1, 128), 1)
    sub8 = lax.broadcasted_iota(jnp.int32, (8, 128), 0)
    lane8 = lax.broadcasted_iota(jnp.int32, (8, 128), 1)

    for comp in range(2):
        quarters = []
        for k in range(4):
            quarters.append(velocity[2 * comp, 4 * k : 4 * k + 4].reshape(64, 128))
        packed = jnp.zeros((64, 128), jnp.float32)
        where_to = lax.broadcasted_iota(jnp.int32, (64, 128), 1)
        for k in range(4):
            low = pltpu.roll(quarters[k], 32 * k, 1) if k else quarters[k]
            shift = (32 * k + 32) % 128
            high = pltpu.roll(quarters[k], shift, 1) if shift else quarters[k]
            packed = jnp.where(where_to // 16 == 2 * k, low, packed)
            packed = jnp.where(where_to // 16 == 2 * k + 1, high, packed)
        slab[comp] = packed.reshape(4, 16, 128)

    pl.semaphore_wait(barrier, len(near))

    tell(0)
    for d in range(2):
        push(slab, slab_in.at[d], send.at[0], slab_recv.at[d], neighbours[d])

    for copy in loads[1:]:
        copy.wait()
    height = jnp.zeros((8, 128), jnp.float32)
    for layer in range(16):
        height = jnp.where(lane8 // 8 == layer, heights[layer], height)
    mass_y = height * table[HALFW]
    block = table[BLOCK : BLOCK + 16].reshape(128, 128) * (1.0 / height)[:1]
    block = (
        block
        + table[LAST][:1] * pltpu.roll(block, 127, 1)
        + table[FIRST][:1] * pltpu.roll(block, 1, 1)
    )

    def split(value):
        high = value.astype(jnp.bfloat16)
        return high, (value - high.astype(jnp.float32)).astype(jnp.bfloat16)

    block_high, block_low = split(block)
    normal[:128, :128] = block_high
    normal[128:, :128] = block_high
    normal[:128, 128:] = block_low
    normal[128:, 128:] = jnp.zeros((128, 128), jnp.bfloat16)
    right_high[...] = jnp.zeros(right_high.shape, jnp.bfloat16)
    right_low[...] = jnp.zeros(right_low.shape, jnp.bfloat16)
    side = sub8 // 2 % 2
    wall_row = jnp.where(side == 0, block[:1], block[127:])
    lift = jnp.concatenate([table[LIFT + k] for k in range(4)], axis=1)
    home = (sub8 // 4 * 2 + sub8 % 2)[:, :1]
    rises = jnp.concatenate([jnp.where(home == k, wall_row, 0.0) for k in range(4)], axis=1)
    rises_high = rises.astype(jnp.bfloat16).astype(jnp.float32)
    for n, part_of in enumerate((lift, lift, rises_high, rises_high, rises - rises_high)):
        lifting[8 * n : 8 * n + 8] = part_of
    lifting[40:] = jnp.zeros((8, 512), jnp.float32)
    joined_y = (
        mass_y
        + table[LAST] * pltpu.roll(mass_y, 127, 1)
        + table[FIRST] * pltpu.roll(mass_y, 1, 1)
    )
    both = lambda value: jnp.concatenate([value, value], axis=0)
    joined_y2 = both(joined_y)
    count2 = both(table[COUNT])

    wall_mass = jnp.where(side == 0, joined_y[:, :1], joined_y[:, 127:])
    scale_zy = both(table[QMZ] * joined_y) * inverse_step
    for comp in range(3):
        for i in range(16):
            res[comp, 16 * i : 16 * i + 16] = velocity[comp, i] * (
                scale_zy * (mass_x[i % 8] * ends[i % 8])
            )

    row16 = lax.broadcasted_iota(jnp.int32, (16, 128), 0) % 8
    share_x = jnp.where(jnp.logical_or(row16 == 0, row16 == 7), 0.5, 1.0)
    half_y = jnp.broadcast_to(table[COUNT][:1], (8, 128))

    def fold(value):
        return value[:8] + value[8:]

    def apply(source, comp):
        high, low = split(source[comp])
        parts = jnp.concatenate([high, low], axis=1)
        along = jnp.dot(flat[0], parts, preferred_element_type=jnp.float32)
        along = along[:, :128] + along[:, 128:]
        along = along + jnp.dot(flat[1], high, preferred_element_type=jnp.float32)
        across_y = jnp.dot(parts, normal[...], preferred_element_type=jnp.float32)
        return along, across_y[:, :128] + across_y[:, 128:]

    def operate(source, target, turn):
        for comp in range(3):
            along, across_y = apply(source, comp)
            for d in range(4):
                rows = slice(256 + 16 * d, 272 + 16 * d)
                face[turn, d, comp] = along[rows] * joined_y2
                push(
                    face.at[turn, d, comp], face_in.at[turn, d, comp], send.at[2 + turn],
                    recv.at[1 + turn], neighbours[d],
                )
            for i in range(16):
                rows = slice(16 * i, 16 * i + 16)
                target[comp, rows] = along[rows] * joined_y2 + across_y[rows] * both(
                    table[FLAT + i]
                )

    operate(res, one, 0)
    def regroup(blocks):
        upper = (lane // 8) % 2 == 1
        result = []
        for ex in range(2):
            low, high = blocks[ex], blocks[2 + ex]
            result.append(jnp.where(upper, pltpu.roll(high, 8, 1), low))
            result.append(jnp.where(upper, high, pltpu.roll(low, 120, 1)))
        return result

    def ungroup(values):
        upper = (lane // 8) % 2 == 1
        low, high = [], []
        for ex in range(2):
            a, b = values[2 * ex], values[2 * ex + 1]
            low.append(jnp.where(upper, pltpu.roll(b, 8, 1), a))
            high.append(jnp.where(upper, b, pltpu.roll(a, 120, 1)))
        return low + high

    wide = lambda row: jnp.broadcast_to(row, (8, 128))
    quarter = lambda ref, row, q: ref[row : row + 1, 128 * q : 128 * q + 128]
    distance = [(quarter(owner, 0, q) - wall + nw) % nw for q in range(4)]
    to_next = regroup([wide(jnp.where(d == 1, 1.0, 0.0)) for d in distance])
    to_prev = regroup([wide(jnp.where(d == nw - 1, 1.0, 0.0)) for d in distance])
    layer = regroup([wide((quarter(element, 0, q) % 2).astype(jnp.float32)) for q in range(4)])
    axes = [regroup([wide(quarter(coords, k, q)) for q in range(4)]) for k in range(3)]

    def lagrange(coord):
        value = table[LAG]
        for b in range(8):
            value = value * jnp.where(sub8 == b, 1.0, coord - GLL_NODES[b])
        return value

    basis = [[lagrange(axes[k][g]) for k in range(3)] for g in range(4)]
    second_wall = (lane // 8) % 2 == 1
    for g in range(4):
        ly = basis[g][2]
        blocks = []
        for side in range(2):
            for ey in range(2):
                chosen = jnp.logical_and(
                    wide(second_wall) == (side == 1), layer[g] == float(ey)
                )
                blocks.append(jnp.where(chosen, ly, 0.0))
        high, low = split(jnp.concatenate(blocks, axis=0))
        for kk in range(2):
            k = 2 * (g // 2) + kk
            column = slice(128 * kk, 128 * kk + 128)
            right_high[g, 32 * k : 32 * k + 32, column] = high
            right_high[g, 128 + 32 * k : 160 + 32 * k, column] = high
            right_low[g, 32 * k : 32 * k + 32, column] = low

    masks = [[1.0 - to_next[g] - to_prev[g], to_prev[g], to_next[g]] for g in range(4)]

    def sample(source, g):
        ez = g % 2
        high, low = split(source[:, :, 8 * ez : 8 * ez + 8, :].reshape(64, 128))
        product = jnp.dot(
            jnp.concatenate([high, low], axis=1), right_high[g],
            preferred_element_type=jnp.float32,
        ) + jnp.dot(high, right_low[g], preferred_element_type=jnp.float32)
        total = [jnp.zeros((8, 128), jnp.float32) for _ in range(2)]
        for kk in range(2):
            values = product[:, 128 * kk : 128 * kk + 128].reshape(2, 4, 8, 128)
            for comp in range(2):
                for x in range(4):
                    a = 4 * kk + x
                    total[comp] = total[comp] + values[comp, x] * basis[g][0][a : a + 1]
        return total

    sums = []
    for g in range(4):
        own = sample(slab, g)
        sums.append([own[comp] * masks[g][0] for comp in range(2)])
    for d in range(2):
        wait_bytes(slab_in.at[d], slab_recv.at[d])
        for g in range(4):
            far = sample(slab_in.at[d], g)
            for comp in range(2):
                sums[g][comp] = sums[g][comp] + far[comp] * masks[g][1 + d]
    stream = ungroup(
        [wide(jnp.sum(sums[g][0] * basis[g][1], axis=0, keepdims=True)) for g in range(4)]
    )
    spanwise = ungroup(
        [wide(jnp.sum(sums[g][1] * basis[g][1], axis=0, keepdims=True)) for g in range(4)]
    )

    for q in range(4):
        u, v = stream[q], spanwise[q]
        speed = jnp.sqrt(u * u + v * v + speed_floor)
        ratio = karman / jnp.log(sample_height / wide(quarter(roughness, 0, q)))
        factor = -(ratio * ratio * speed / viscosity)
        for comp, value in enumerate((u, v)):
            slope = factor * value
            neumann[comp : comp + 1, 128 * q : 128 * q + 128] = slope[:1]
            plane[comp * 4 + q : comp * 4 + q + 1, :] = (viscosity * slope * table[PLANE])[:1]

    hear(0)
    for d in range(8):
        push(plane, plane_in.at[d], send.at[1], recv.at[0], neighbours[d])
    tell(1)

    node_z = lane8 % 16
    node_x = lane8 // 16
    half = sub8 % 2

    def join_span(mine, before, after):
        return (
            mine
            + jnp.where(node_z == 7, pltpu.roll(mine, 127, 1), 0.0)
            + jnp.where(node_z == 8, pltpu.roll(mine, 1, 1), 0.0)
            + jnp.where(node_z == 0, pltpu.roll(before, 113, 1), 0.0)
            + jnp.where(node_z == 15, pltpu.roll(after, 15, 1), 0.0)
        )

    def join_wall(mine, before, after):
        later = jnp.where(half == 0, pltpu.roll(mine, 7, 0), pltpu.roll(after, 1, 0))
        earlier = jnp.where(half == 0, pltpu.roll(before, 7, 0), pltpu.roll(mine, 1, 0))
        return (
            mine
            + jnp.where(node_x == 7, pltpu.roll(later, 112, 1), 0.0)
            + jnp.where(node_x == 0, pltpu.roll(earlier, 16, 1), 0.0)
        )

    def receive(target, turn):
        wait_bytes(face_in.at[turn], recv.at[1 + turn])
        into = (
            pl.ds(0, 16),
            pl.ds(240, 16),
            pl.ds(0, 16, stride=16),
            pl.ds(15, 16, stride=16),
        )
        for d in range(4):
            for comp in range(3):
                target[comp, into[d], :] = target[comp, into[d], :] + face_in[turn, d, comp]

    receive(one, 0)
    wait_bytes(plane_in, recv.at[0])
    raw = {(-dw, -ds): plane_in[d] for d, (dw, ds) in enumerate(SHIFTS)}
    raw[0, 0] = plane[...]
    none = jnp.zeros((8, 128), jnp.float32)
    line_of = {
        (dw, ds): join_span(raw[dw, ds], raw.get((dw, ds - 1), none), raw.get((dw, ds + 1), none))
        for dw in (-1, 0, 1)
        for ds in (-1, 0, 1)
    }
    cross = ((0, 0), (-1, 0), (1, 0), (0, -1), (0, 1))
    sums_of = [
        join_wall(
            line_of[dw, ds], line_of.get((dw - 1, ds), none), line_of.get((dw + 1, ds), none)
        )
        for dw, ds in cross
    ]
    stress = sums_of[0]
    high, low = split(jnp.concatenate(sums_of + [none], axis=0))
    pulls = jnp.dot(
        jnp.concatenate([high, low, high], axis=1), lines[...], preferred_element_type=jnp.float32
    )
    in_x = [pulls[8 * n : 8 * n + 8, :128] for n in range(5)]
    in_z = [pulls[8 * n : 8 * n + 8, 128:] for n in range(5)]
    plane_mass = table[LANEX] * table[LANEZ] * stress
    plane_pull = (
        table[LANEZ] * join_wall(in_x[0], in_x[1], in_x[2])
        + table[LANEX] * join_span(in_z[0], in_z[3], in_z[4])
        + SCALE * inverse_step * plane_mass
    ) * wall_mass
    def coarse(value):
        return value.astype(jnp.bfloat16).astype(jnp.float32)

    def raised(parts, rows):
        return lax.dot_general(
            jnp.concatenate(parts, axis=0),
            lifting[:rows],
            (((0,), (0,)), ((), ())),
            preferred_element_type=jnp.float32,
        )

    stress_high, pull_high, mass_high = coarse(stress), coarse(plane_pull), coarse(plane_mass)
    lifted = raised([stress_high, stress - stress_high], 16)
    lifted_one = raised(
        [pull_high, plane_pull - pull_high, mass_high, plane_mass - mass_high, mass_high, none], 48
    )
    for comp in range(2):
        for ex in range(2):
            column = (comp * 2 + ex) * 128
            here = res[2 * comp, 128 * ex : 128 * ex + 128]
            res[2 * comp, 128 * ex : 128 * ex + 128] = here + lifted[:, column : column + 128]
            here = one[2 * comp, 128 * ex : 128 * ex + 128]
            one[2 * comp, 128 * ex : 128 * ex + 128] = here + lifted_one[:, column : column + 128]

    def energy(source, index):
        for comp in range(3):
            along, across_y = apply(source, comp)
            inside = jnp.zeros((16, 128), jnp.float32)
            edges = jnp.zeros((16, 128), jnp.float32)
            for i in range(16):
                rows = slice(16 * i, 16 * i + 16)
                term = source[comp, rows] * (
                    along[rows] * joined_y2 + across_y[rows] * both(table[FLAT + i])
                )
                if i % 8 in (0, 7):
                    edges = edges + term
                else:
                    inside = inside + term
            for d, i in ((0, 15), (1, 0)):
                sent = along[256 + 16 * d : 272 + 16 * d] * joined_y2
                edges = edges + sent * source[comp, 16 * i : 16 * i + 16]
            total = fold((inside + 0.5 * edges) * count2)
            for d, first in ((2, 15), (3, 0)):
                sent = along[256 + 16 * d : 272 + 16 * d] * joined_y2
                term = sent * source[comp, pl.ds(first, 16, stride=16), :]
                total = total + fold(term * share_x) * half_y
            mom[3 * index + comp] = total

    def weighted(pairs):
        for comp in range(3):
            totals = [jnp.zeros((16, 128), jnp.float32) for _ in pairs]
            edges = [jnp.zeros((16, 128), jnp.float32) for _ in pairs]
            for i in range(16):
                for n, (first, second, _) in enumerate(pairs):
                    term = (
                        first[comp, 16 * i : 16 * i + 16] * second[comp, 16 * i : 16 * i + 16]
                    )
                    if i % 8 in (0, 7):
                        edges[n] = edges[n] + term
                    else:
                        totals[n] = totals[n] + term
            for n, (_, _, index) in enumerate(pairs):
                mom[3 * index + comp] = fold((totals[n] + 0.5 * edges[n]) * count2)

    hear(1)
    tell(2)
    operate(one, two, 1)
    weighted([(res, res, 0), (res, one, 1), (one, one, 2)])
    receive(two, 1)
    hear(2)
    weighted([(one, two, 3), (two, two, 4)])
    energy(two, 5)

    row = jnp.zeros((8, 128), jnp.float32)
    for k in range(18):
        value = jnp.sum(mom[k], axis=1, keepdims=True)
        row = row + jnp.where(lane8 == k, value, 0.0)
    row = jnp.sum(row, axis=0, keepdims=True)

    start = 0
    for phase, (count, mine, peers) in enumerate(groups):
        part[phase] = row
        for peer in peers:
            push(
                part.at[phase], part_in.at[start + mine], send.at[4 + phase], recv.at[3 + phase],
                peer,
            )
        part_in[start + mine] = row
        wait_bytes(part_in.at[pl.ds(start, count - 1)], recv.at[3 + phase])
        row = part_in[start]
        for k in range(1, count):
            row = row + part_in[start + k]
        start += count

    row = jnp.broadcast_to(row, (8, 128))
    moments = [row if j == 0 else pltpu.roll(row, 128 - 3 * j, 1) for j in range(6)]

    def inner(first, second, raise_by):
        total = None
        for i, a in enumerate(first):
            for j, b in enumerate(second):
                term = a * b * moments[i + j + raise_by]
                total = term if total is None else total + term
        return total

    unit = jnp.ones((8, 128), jnp.float32)
    direction, residual = [unit], [unit]
    answer = [jnp.zeros((8, 128), jnp.float32)] * 3
    norm = moments[0]
    for step in range(3):
        alpha = norm / inner(direction, direction, 1)
        for i, value in enumerate(direction):
            answer[i] = answer[i] + alpha * value
        if step == 2:
            break
        lowered = [-alpha * value for value in direction]
        residual = [residual[0]] + [
            lowered[i] + residual[i + 1] if i + 1 < len(residual) else lowered[i]
            for i in range(len(lowered))
        ]
        newer = inner(residual, residual, 0)
        growth = newer / norm
        direction = [
            value + growth * direction[i] if i < len(direction) else value
            for i, value in enumerate(residual)
        ]
        norm = newer
    for i, value in enumerate(answer):
        scalars[i : i + 1, :] = value[:1] * SCALE
    wait_bytes(slab_in, send.at[0])
    wait_bytes(plane_in, send.at[1])
    for turn in range(2):
        wait_bytes(face_in.at[turn], send.at[2 + turn])
    start = 0
    for phase, (count, _, _) in enumerate(groups):
        wait_bytes(part_in.at[pl.ds(start, count - 1)], send.at[4 + phase])
        start += count


def combine(res, one, two, scalars, slopes, out, neumann, sums, sent):
    copies = [pltpu.make_async_copy(slopes, neumann, sent.at[3])]
    copies[0].start()
    for comp in range(3):
        c0, c1, c2 = (
            jnp.broadcast_to(scalars[k : k + 1, comp : comp + 1], (16, 128)) for k in range(3)
        )
        for i in range(16):
            rows = pl.ds(16 * i, 16)
            sums[comp, i] = (
                c0 * res[comp, rows, :] + c1 * one[comp, rows, :] + c2 * two[comp, rows, :]
            )
        copy = pltpu.make_async_copy(sums.at[comp], out.at[comp], sent.at[comp])
        copy.start()
        copies.append(copy)
    for copy in copies:
        copy.wait()


def body(sizes, velocity_old, heights, owner_device, owner_element, ref_coords, roughness):
    nx, ny, nc, ns = sizes
    slots = nc * ns + nx * ny
    f32, i32 = jnp.float32, jnp.int32
    vmem = pl.BlockSpec(memory_space=pltpu.VMEM)
    anywhere = pl.BlockSpec(memory_space=pl.ANY)
    constants, flat, lines = (jnp.asarray(value) for value in tables())
    res, one, two, scalars, slopes = pl.pallas_call(
        functools.partial(kernel, sizes),
        out_shape=(
            pltpu.VMEM((3, 256, 128), f32),
            pltpu.VMEM((3, 256, 128), f32),
            pltpu.VMEM((3, 256, 128), f32),
            pltpu.VMEM((8, 128), f32),
            pltpu.VMEM((2, 512), f32),
        ),
        in_specs=[anywhere] * 9,
        out_specs=(vmem,) * 5,
        scratch_shapes=[
            pltpu.VMEM((3, 16, 16, 128), f32),
            pltpu.SMEM((16,), f32),
            pltpu.VMEM((1, 512), i32),
            pltpu.VMEM((1, 512), i32),
            pltpu.VMEM((3, 512), f32),
            pltpu.VMEM((1, 512), f32),
            pltpu.VMEM(constants.shape, f32),
            pltpu.VMEM(flat.shape, jnp.bfloat16),
            pltpu.VMEM(lines.shape, jnp.bfloat16),
            pltpu.VMEM((256, 256), jnp.bfloat16),
            pltpu.VMEM((48, 512), f32),
            pltpu.VMEM((4, 256, 256), jnp.bfloat16),
            pltpu.VMEM((4, 128, 256), jnp.bfloat16),
            pltpu.VMEM((2, 4, 16, 128), f32),
            pltpu.VMEM((2, 2, 4, 16, 128), f32),
            pltpu.VMEM((8, 128), f32),
            pltpu.VMEM((8, 8, 128), f32),
            pltpu.VMEM((2, 4, 3, 16, 128), f32),
            pltpu.VMEM((2, 4, 3, 16, 128), f32),
            pltpu.VMEM((18, 8, 128), f32),
            pltpu.VMEM((2, 1, 128), f32),
            pltpu.VMEM((slots, 1, 128), f32),
            pltpu.SemaphoreType.DMA((9,)),
            pltpu.SemaphoreType.DMA((6,)),
            pltpu.SemaphoreType.DMA((2,)),
            pltpu.SemaphoreType.DMA((5,)),
            pltpu.SemaphoreType.REGULAR((3,)),
        ],
        compiler_params=pltpu.CompilerParams(collective_id=0, has_side_effects=True),
        name="channel_step",
    )(
        velocity_old,
        heights,
        owner_device.reshape(1, -1),
        owner_element.reshape(1, -1),
        ref_coords,
        roughness.reshape(1, -1),
        constants,
        flat,
        lines,
    )
    return pl.pallas_call(
        combine,
        out_shape=(
            jax.ShapeDtypeStruct((3, 16, 16, 128), f32),
            jax.ShapeDtypeStruct((2, 512), f32),
        ),
        in_specs=[vmem] * 5,
        out_specs=(anywhere, anywhere),
        scratch_shapes=[
            pltpu.VMEM((3, 16, 16, 128), f32),
            pltpu.SemaphoreType.DMA((4,)),
        ],
        name="combine",
    )(
        *(
            pltpu.with_memory_space_constraint(value, pltpu.VMEM)
            for value in (res, one, two, scalars, slopes)
        )
    )


def torus_program(torus):
    sizes = tuple(torus.shape[name] for name in AXES)
    return jax.shard_map(
        functools.partial(body, sizes),
        mesh=torus,
        in_specs=(
            P(None, WALL, "span", None),
            P(),
            P(WALL_SPAN, None),
            P(WALL_SPAN, None),
            P(None, WALL_SPAN),
            P(WALL_SPAN),
        ),
        out_specs=(P(None, WALL, "span", None), P(None, WALL_SPAN)),
        check_vma=False,
    )


def solution(mesh):
    return torus_program(Mesh(mesh.devices.reshape(4, 8, 2, mesh.shape["span"]), AXES))
```

```python
import functools

import jax
import jax.numpy as jnp
import numpy as np
from jax import lax
from jax.experimental import pallas as pl
from jax.experimental.pallas import tpu as pltpu
from jax.sharding import Mesh
from jax.sharding import PartitionSpec as P

AXES = ("wall_0", "wall_1", "wall_2", "span")
WALL_SPAN = AXES
WALL = ("wall_0", "wall_1", "wall_2")
MESH_ID = pl.DeviceIdType.MESH

GLL_NODES = (
    -1.0,
    -0.8717401485096066,
    -0.5917001814331423,
    -0.2092992179024789,
    0.2092992179024789,
    0.5917001814331423,
    0.8717401485096066,
    1.0,
)
GLL_WEIGHTS = (
    0.03571428571428571,
    0.2107042271435061,
    0.3411226924835044,
    0.4124587946587038,
    0.4124587946587038,
    0.3411226924835044,
    0.2107042271435061,
    0.03571428571428571,
)
viscosity = 0.02
inverse_step = 20.0
karman = 0.41
sample_height = 0.1
speed_floor = 0.01
element_dx = 0.05
element_dz = 0.13
precise = lax.Precision.HIGHEST

SCALE = 64.0

SHIFTS = ((1, 0), (-1, 0), (0, 1), (0, -1), (1, 1), (1, -1), (-1, 1), (-1, -1))

FAR_SHIFTS = (
    (2, 0), (2, 1), (2, -1), (-2, 0), (-2, 1), (-2, -1),
    (0, 2), (1, 2), (-1, 2), (0, -2), (1, -2), (-1, -2),
)

MZ, QMZ, COUNT, LAG, PLANE, HALFW, LAST, FIRST, LANEX, LANEZ = range(10)
BLOCK, LIFT, FLAT = 10, 26, 30


def stiffness_table():
    points = np.array(GLL_NODES)
    weights = np.array(GLL_WEIGHTS)
    previous = np.ones(8)
    current = points.copy()
    for degree in range(1, 7):
        previous, current = (
            current,
            ((2 * degree + 1) * points * current - degree * previous) / (degree + 1),
        )
    derivative = np.zeros((8, 8))
    for target in range(8):
        for source in range(8):
            if target != source:
                derivative[target, source] = (
                    current[target] / current[source] / (points[target] - points[source])
                )
    derivative[0, 0] = -14.0
    derivative[7, 7] = 14.0
    return derivative.T @ (weights[:, None] * derivative)


def tables():
    weights = np.array(GLL_WEIGHTS)
    points = np.array(GLL_NODES)
    stiffness = stiffness_table()
    ones = np.ones((8, 128))
    lane = np.arange(128)
    ends = np.array([2.0, 1, 1, 1, 1, 1, 1, 2.0])
    mass_x = 0.5 * element_dx * weights
    mass_z = 0.5 * element_dz * weights
    count_y = np.where((lane % 8 == 0) | (lane % 8 == 7), 0.5, 1.0)
    count_y[0] = count_y[127] = 1.0
    gaps = points[:, None] - points[None, :] + np.eye(8)
    rows = [
        mass_z[:, None] * ones,
        (mass_z * ends)[:, None] * ones,
        (1.0 / ends)[:, None] * count_y[None, :],
        (1.0 / np.prod(gaps, axis=1))[:, None] * ones,
        ones * (mass_x[lane // 16] * mass_z[lane % 8])[None, :],
        ones * (0.5 * weights[lane % 8])[None, :],
        ones * ((lane % 8 == 7) & (lane < 127))[None, :],
        ones * ((lane % 8 == 0) & (lane > 0))[None, :],
    ]
    block = np.kron(np.eye(16), SCALE * viscosity * 2.0 * stiffness)
    lift = np.zeros((8, 512))
    for comp in range(2):
        for half in range(2):
            column = (comp * 2 + half) * 128
            lift[comp * 4 + half, column] = 1.0
            lift[comp * 4 + 2 + half, column + 127] = 1.0
    joined_x = np.tile(mass_x * ends, 2)
    joined_z = np.tile(mass_z * ends, 2)

    def chain(length):
        scaled = SCALE * viscosity * (2.0 / length) * stiffness
        full = np.kron(np.eye(2), scaled)
        ends_only = full[[15, 0]]
        full[7] = full[8] = full[7] + full[8]
        return full, ends_only

    chain_x, ends_x = chain(element_dx)
    chain_z, ends_z = chain(element_dz)
    flat = np.kron(chain_x, np.diag(joined_z)) + np.kron(np.diag(joined_x), chain_z)
    flat += SCALE * inverse_step * np.diag(np.kron(joined_x, joined_z))
    faces = [np.kron(ends_x[d : d + 1], np.diag(joined_z)) for d in range(2)]
    faces += [np.kron(np.diag(joined_x), ends_z[d : d + 1]) for d in range(2)]
    flat = np.concatenate([flat] + faces).astype(np.float32)
    flat_high = flat.astype(jnp.bfloat16)
    flat_low = (flat - flat_high.astype(np.float32)).astype(jnp.bfloat16)
    line_x = SCALE * viscosity * (2.0 / element_dx) * stiffness
    line_z = SCALE * viscosity * (2.0 / element_dz) * stiffness
    line = np.concatenate([np.kron(line_x.T, np.eye(16)), np.kron(np.eye(16), line_z.T)], axis=1)
    line_high = line.astype(np.float32).astype(jnp.bfloat16)
    line_low = (line.astype(np.float32) - line_high.astype(np.float32)).astype(jnp.bfloat16)
    lines = np.concatenate([line_high, line_high, line_low])
    rows += [
        ones * (mass_x * ends)[lane // 16][None, :],
        ones * (mass_z * ends)[lane % 8][None, :],
    ]
    pieces = [np.stack(rows), block.reshape(16, 8, 128), lift.reshape(8, 4, 128).transpose(1, 0, 2)]
    pieces += [joined_x[:, None, None] * (mass_z * ends)[None, :, None] * np.ones((16, 8, 128))]
    return np.concatenate(pieces).astype(np.float32), np.stack([flat_high, flat_low]), lines


def kernel(sizes, *refs):
    operands, refs = refs[:9], refs[9:]
    (res, one, two, scalars, neumann), refs = refs[:5], refs[5:]
    local, refs = refs[:9], refs[9:]
    velocity, heights, owner, element, coords, roughness, table, flat, lines = local
    (normal, lifting, lifting_two, right_high, right_low, slab, slab_in, plane, plane_in,
     verge, verge_in, face, face_in, mom, part, part_in,
     load, send, slab_recv, recv, ready) = refs
    nx, ny, nc, ns = sizes
    nw = nx * ny * nc
    loads = [
        pltpu.make_async_copy(source, target, load.at[n])
        for n, (source, target) in enumerate(zip(operands, local))
    ]
    for copy in loads:
        copy.start()
    wx, wy, wc, sp = (lax.axis_index(name) for name in AXES)
    wall = (wx * ny + wy) * nc + wc
    weights = np.array(GLL_WEIGHTS)
    stiffness = stiffness_table()
    mass_x = [float(v) for v in 0.5 * element_dx * weights]
    ends = [2.0, 1.0, 1.0, 1.0, 1.0, 1.0, 1.0, 2.0]

    def ring(value, shift, count):
        if shift > 0:
            return jnp.where(value >= count - shift, value + shift - count, value + shift)
        return jnp.where(value < -shift, value + shift + count, value + shift)

    def beside(dw):
        if dw == 0:
            return wx, wy, wc
        sign = 1 if dw > 0 else -1
        if abs(dw) == 2:
            turn_y = wy == (ny - 1 if dw > 0 else 0)
            return jnp.where(turn_y, ring(wx, sign, nx), wx), ring(wy, sign, ny), wc
        turn = wc == (nc - 1 if dw > 0 else 0)
        turn_y = jnp.logical_and(turn, wy == (ny - 1 if dw > 0 else 0))
        return (
            jnp.where(turn_y, ring(wx, dw, nx), wx),
            jnp.where(turn, ring(wy, dw, ny), wy),
            ring(wc, dw, nc),
        )

    along = {dw: beside(dw) for dw in (-2, -1, 0, 1, 2)}
    across = {k: ring(sp, k, ns) if k else sp for k in (-2, -1, 0, 1, 2)}
    neighbours = [(*along[dw], across[ds]) for dw, ds in SHIFTS]
    distant = [(*along[dw], across[ds]) for dw, ds in FAR_SHIFTS]
    place_x = {0: wx, 1: ring(wx, 1, nx), -1: ring(wx, -1, nx), 2: ring(wx, 2, nx)}
    place_y = {k: ring(wy, k, ny) if k else wy for k in range(-(ny // 2) + 1, ny // 2 + 1)}
    place_y[-2] = ring(wy, -2, ny)
    place_z = {k: ring(sp, k, ns) if k else sp for k in range(-(ns // 2) + 1, ns // 2 + 1)}
    place_z[-2] = ring(sp, -2, ns)
    other = ring(wc, 1, nc)
    flat_peer = lambda dx, dy: (place_x[dx], place_y[dy], wc, sp)
    deep_peer = lambda c, ds: (wx, wy, c, place_z[ds])

    def far_first(keys):
        return sorted(keys, key=lambda key: -abs(key[0]) - abs(key[1]))

    deep = far_first([(c, k) for c in (0, 1) for k in range(-(ns // 2) + 1, ns // 2 + 1)])
    deep = [key for key in deep if key != (0, 0)]
    wide_x = [k for k in (-1, 0, 1, 2) if -(nx // 2) < k <= nx // 2]
    plain = far_first([(a, b) for a in wide_x for b in range(-(ny // 2) + 1, ny // 2 + 1)])
    plain = [key for key in plain if key != (0, 0)]
    groups = [
        (nc * ns, wc * ns + sp, [deep_peer((wc, other)[c], k) for c, k in deep]),
        (nx * ny, wx * ny + wy, [flat_peer(a, b) for a, b in plain]),
    ]

    barrier = pltpu.get_barrier_semaphore()
    near = neighbours[:4] + [deep_peer(other, 0)]
    near += [(*along[2], sp), (*along[-2], sp), (*along[0], across[2]), (*along[0], across[-2])]
    near += [flat_peer(1, 0), flat_peer(-1, 0), flat_peer(0, 1), flat_peer(0, -1)]
    for peer in near:
        pl.semaphore_signal(barrier, inc=1, device_id=peer, device_id_type=MESH_ID)
    relays = [
        near,
        [flat_peer(1, 0), flat_peer(-1, 0), flat_peer(0, 2), flat_peer(0, -2)]
        + [deep_peer(wc, 2), deep_peer(wc, -2)],
        [flat_peer(1, 0), flat_peer(-1, 0), flat_peer(0, 2), flat_peer(0, -2)]
        + [flat_peer(2, 2), flat_peer(2, -2), deep_peer(wc, 4), deep_peer(wc, -4)],
    ]

    def tell(n):
        for peer in relays[n]:
            pl.semaphore_signal(ready.at[n], inc=1, device_id=peer, device_id_type=MESH_ID)

    def hear(n):
        pl.semaphore_wait(ready.at[n], len(relays[n]))

    def push(source, target, send_sem, recv_sem, peer):
        pltpu.make_async_remote_copy(
            src_ref=source,
            dst_ref=target,
            send_sem=send_sem,
            recv_sem=recv_sem,
            device_id=peer,
            device_id_type=MESH_ID,
        ).start()

    def wait_bytes(like, sem):
        pltpu.make_async_copy(like, like, sem).wait()

    loads[0].wait()

    lane = lax.broadcasted_iota(jnp.int32, (1, 128), 1)
    sub8 = lax.broadcasted_iota(jnp.int32, (8, 128), 0)
    lane8 = lax.broadcasted_iota(jnp.int32, (8, 128), 1)

    for comp in range(2):
        quarters = []
        for k in range(4):
            quarters.append(velocity[2 * comp, 4 * k : 4 * k + 4].reshape(64, 128))
        packed = jnp.zeros((64, 128), jnp.float32)
        where_to = lax.broadcasted_iota(jnp.int32, (64, 128), 1)
        for k in range(4):
            low = pltpu.roll(quarters[k], 32 * k, 1) if k else quarters[k]
            shift = (32 * k + 32) % 128
            high = pltpu.roll(quarters[k], shift, 1) if shift else quarters[k]
            packed = jnp.where(where_to // 16 == 2 * k, low, packed)
            packed = jnp.where(where_to // 16 == 2 * k + 1, high, packed)
        slab[comp] = packed.reshape(4, 16, 128)

    pl.semaphore_wait(barrier, len(near))

    tell(0)
    for d in range(2):
        push(slab, slab_in.at[d], send.at[0], slab_recv.at[d], neighbours[d])

    for copy in loads[1:]:
        copy.wait()
    height = jnp.zeros((8, 128), jnp.float32)
    for layer in range(16):
        height = jnp.where(lane8 // 8 == layer, heights[layer], height)
    mass_y = height * table[HALFW]
    block = table[BLOCK : BLOCK + 16].reshape(128, 128) * (1.0 / height)[:1]
    block = (
        block
        + table[LAST][:1] * pltpu.roll(block, 127, 1)
        + table[FIRST][:1] * pltpu.roll(block, 1, 1)
    )

    def split(value):
        high = value.astype(jnp.bfloat16)
        return high, (value - high.astype(jnp.float32)).astype(jnp.bfloat16)

    block_high, block_low = split(block)
    normal[:128, :128] = block_high
    normal[128:, :128] = block_high
    normal[:128, 128:] = block_low
    normal[128:, 128:] = jnp.zeros((128, 128), jnp.bfloat16)
    right_high[...] = jnp.zeros(right_high.shape, jnp.bfloat16)
    right_low[...] = jnp.zeros(right_low.shape, jnp.bfloat16)
    side = sub8 // 2 % 2
    wall_row = jnp.where(side == 0, block[:1], block[127:])
    lift = jnp.concatenate([table[LIFT + k] for k in range(4)], axis=1)
    home = (sub8 // 4 * 2 + sub8 % 2)[:, :1]
    joined_y = (
        mass_y
        + table[LAST] * pltpu.roll(mass_y, 127, 1)
        + table[FIRST] * pltpu.roll(mass_y, 1, 1)
    )
    both = lambda value: jnp.concatenate([value, value], axis=0)
    joined_y2 = both(joined_y)
    count2 = both(table[COUNT])

    def at_home(value):
        return jnp.concatenate([jnp.where(home == k, value, 0.0) for k in range(4)], axis=1)

    def coarse(value):
        return value.astype(jnp.bfloat16).astype(jnp.float32)

    twice = jnp.dot(wall_row, block, precision=precise, preferred_element_type=jnp.float32)
    pieces, pieces_two = [lift, lift], [lift, lift]
    for n, value in enumerate((wall_row, joined_y * wall_row, wall_row, twice)):
        rises = at_home(value)
        high = coarse(rises)
        triple = [high, high, rises - high]
        if n == 0:
            pieces += triple
        else:
            pieces_two += triple
    for n, value in enumerate(pieces):
        lifting[8 * n : 8 * n + 8] = value
    lifting[40:] = jnp.zeros((8, 512), jnp.float32)
    for n, value in enumerate(pieces_two):
        lifting_two[8 * n : 8 * n + 8] = value
    lifting_two[88:] = jnp.zeros((8, 512), jnp.float32)
    wall_mass = jnp.where(side == 0, joined_y[:, :1], joined_y[:, 127:])
    scale_zy = both(table[QMZ] * joined_y) * inverse_step
    for comp in range(3):
        for i in range(16):
            res[comp, 16 * i : 16 * i + 16] = velocity[comp, i] * (
                scale_zy * (mass_x[i % 8] * ends[i % 8])
            )

    row16 = lax.broadcasted_iota(jnp.int32, (16, 128), 0) % 8
    share_x = jnp.where(jnp.logical_or(row16 == 0, row16 == 7), 0.5, 1.0)
    half_y = jnp.broadcast_to(table[COUNT][:1], (8, 128))

    def fold(value):
        return value[:8] + value[8:]

    def apply(source, comp):
        high, low = split(source[comp])
        parts = jnp.concatenate([high, low], axis=1)
        along = jnp.dot(flat[0], parts, preferred_element_type=jnp.float32)
        along = along[:, :128] + along[:, 128:]
        along = along + jnp.dot(flat[1], high, preferred_element_type=jnp.float32)
        across_y = jnp.dot(parts, normal[...], preferred_element_type=jnp.float32)
        return along, across_y[:, :128] + across_y[:, 128:]

    def operate(source, target, turn):
        for comp in range(3):
            along, across_y = apply(source, comp)
            for d in range(4):
                rows = slice(256 + 16 * d, 272 + 16 * d)
                face[turn, d, comp] = along[rows] * joined_y2
                push(
                    face.at[turn, d, comp], face_in.at[turn, d, comp], send.at[2 + turn],
                    recv.at[1 + turn], neighbours[d],
                )
            for i in range(16):
                rows = slice(16 * i, 16 * i + 16)
                target[comp, rows] = along[rows] * joined_y2 + across_y[rows] * both(
                    table[FLAT + i]
                )

    operate(res, one, 0)
    def regroup(blocks):
        upper = (lane // 8) % 2 == 1
        result = []
        for ex in range(2):
            low, high = blocks[ex], blocks[2 + ex]
            result.append(jnp.where(upper, pltpu.roll(high, 8, 1), low))
            result.append(jnp.where(upper, high, pltpu.roll(low, 120, 1)))
        return result

    def ungroup(values):
        upper = (lane // 8) % 2 == 1
        low, high = [], []
        for ex in range(2):
            a, b = values[2 * ex], values[2 * ex + 1]
            low.append(jnp.where(upper, pltpu.roll(b, 8, 1), a))
            high.append(jnp.where(upper, b, pltpu.roll(a, 120, 1)))
        return low + high

    wide = lambda row: jnp.broadcast_to(row, (8, 128))
    quarter = lambda ref, row, q: ref[row : row + 1, 128 * q : 128 * q + 128]
    distance = [(quarter(owner, 0, q) - wall + nw) % nw for q in range(4)]
    to_next = regroup([wide(jnp.where(d == 1, 1.0, 0.0)) for d in distance])
    to_prev = regroup([wide(jnp.where(d == nw - 1, 1.0, 0.0)) for d in distance])
    layer = regroup([wide((quarter(element, 0, q) % 2).astype(jnp.float32)) for q in range(4)])
    axes = [regroup([wide(quarter(coords, k, q)) for q in range(4)]) for k in range(3)]

    def lagrange(coord):
        value = table[LAG]
        for b in range(8):
            value = value * jnp.where(sub8 == b, 1.0, coord - GLL_NODES[b])
        return value

    basis = [[lagrange(axes[k][g]) for k in range(3)] for g in range(4)]
    second_wall = (lane // 8) % 2 == 1
    for g in range(4):
        ly = basis[g][2]
        blocks = []
        for side in range(2):
            for ey in range(2):
                chosen = jnp.logical_and(
                    wide(second_wall) == (side == 1), layer[g] == float(ey)
                )
                blocks.append(jnp.where(chosen, ly, 0.0))
        high, low = split(jnp.concatenate(blocks, axis=0))
        for kk in range(2):
            k = 2 * (g // 2) + kk
            column = slice(128 * kk, 128 * kk + 128)
            right_high[g, 32 * k : 32 * k + 32, column] = high
            right_high[g, 128 + 32 * k : 160 + 32 * k, column] = high
            right_low[g, 32 * k : 32 * k + 32, column] = low

    masks = [[1.0 - to_next[g] - to_prev[g], to_prev[g], to_next[g]] for g in range(4)]

    def sample(source, g):
        ez = g % 2
        high, low = split(source[:, :, 8 * ez : 8 * ez + 8, :].reshape(64, 128))
        product = jnp.dot(
            jnp.concatenate([high, low], axis=1), right_high[g],
            preferred_element_type=jnp.float32,
        ) + jnp.dot(high, right_low[g], preferred_element_type=jnp.float32)
        total = [jnp.zeros((8, 128), jnp.float32) for _ in range(2)]
        for kk in range(2):
            values = product[:, 128 * kk : 128 * kk + 128].reshape(2, 4, 8, 128)
            for comp in range(2):
                for x in range(4):
                    a = 4 * kk + x
                    total[comp] = total[comp] + values[comp, x] * basis[g][0][a : a + 1]
        return total

    sums = []
    for g in range(4):
        own = sample(slab, g)
        sums.append([own[comp] * masks[g][0] for comp in range(2)])
    for d in range(2):
        wait_bytes(slab_in.at[d], slab_recv.at[d])
        for g in range(4):
            far = sample(slab_in.at[d], g)
            for comp in range(2):
                sums[g][comp] = sums[g][comp] + far[comp] * masks[g][1 + d]
    stream = ungroup(
        [wide(jnp.sum(sums[g][0] * basis[g][1], axis=0, keepdims=True)) for g in range(4)]
    )
    spanwise = ungroup(
        [wide(jnp.sum(sums[g][1] * basis[g][1], axis=0, keepdims=True)) for g in range(4)]
    )

    for q in range(4):
        u, v = stream[q], spanwise[q]
        speed = jnp.sqrt(u * u + v * v + speed_floor)
        ratio = karman / jnp.log(sample_height / wide(quarter(roughness, 0, q)))
        factor = -(ratio * ratio * speed / viscosity)
        for comp, value in enumerate((u, v)):
            slope = factor * value
            neumann[comp : comp + 1, 128 * q : 128 * q + 128] = slope[:1]
            plane[comp * 4 + q : comp * 4 + q + 1, :] = (viscosity * slope * table[PLANE])[:1]

    mine = plane[...]
    lines_x = jnp.zeros((8, 128), jnp.float32)
    for q in range(4):
        here = jnp.logical_and(sub8 == 2 * q + 1, lane8 // 16 == 3 - q)
        lines_x = jnp.where(here, pltpu.roll(mine, (16 * (3 - q) - 112) % 128, 1), lines_x)
        here = jnp.logical_and(sub8 == 2 * q, lane8 // 16 == 7 - q)
        lines_x = jnp.where(here, pltpu.roll(mine, (64 + 16 * (3 - q)) % 128, 1), lines_x)
    lines_z = jnp.zeros((8, 128), jnp.float32)
    for r in range(8):
        here = jnp.logical_and(sub8 == r, lane8 % 16 == 7 - r)
        lines_z = jnp.where(here, pltpu.roll(mine, (7 - r - 15) % 128, 1), lines_z)
        here = jnp.logical_and(sub8 == r, lane8 % 16 == 15 - r)
        lines_z = jnp.where(here, pltpu.roll(mine, (15 - r) % 128, 1), lines_z)
    verge[0] = jnp.sum(lines_x, axis=0, keepdims=True)
    verge[1] = jnp.sum(lines_z, axis=0, keepdims=True)
    hear(0)
    for d, (dw, ds) in enumerate(FAR_SHIFTS):
        push(
            verge.at[0 if abs(dw) == 2 else 1], verge_in.at[d], send.at[6], recv.at[5], distant[d]
        )
    for d in range(8):
        push(plane, plane_in.at[d], send.at[1], recv.at[0], neighbours[d])
    tell(1)

    node_z = lane8 % 16
    node_x = lane8 // 16
    half = sub8 % 2

    def join_span(mine, before, after):
        return (
            mine
            + jnp.where(node_z == 7, pltpu.roll(mine, 127, 1), 0.0)
            + jnp.where(node_z == 8, pltpu.roll(mine, 1, 1), 0.0)
            + jnp.where(node_z == 0, pltpu.roll(before, 113, 1), 0.0)
            + jnp.where(node_z == 15, pltpu.roll(after, 15, 1), 0.0)
        )

    def join_wall(mine, before, after):
        later = jnp.where(half == 0, pltpu.roll(mine, 7, 0), pltpu.roll(after, 1, 0))
        earlier = jnp.where(half == 0, pltpu.roll(before, 7, 0), pltpu.roll(mine, 1, 0))
        return (
            mine
            + jnp.where(node_x == 7, pltpu.roll(later, 112, 1), 0.0)
            + jnp.where(node_x == 0, pltpu.roll(earlier, 16, 1), 0.0)
        )

    def receive(target, turn):
        wait_bytes(face_in.at[turn], recv.at[1 + turn])
        into = (
            pl.ds(0, 16),
            pl.ds(240, 16),
            pl.ds(0, 16, stride=16),
            pl.ds(15, 16, stride=16),
        )
        for d in range(4):
            for comp in range(3):
                target[comp, into[d], :] = target[comp, into[d], :] + face_in[turn, d, comp]

    receive(one, 0)
    operate(one, two, 1)
    hear(1)
    tell(2)
    wait_bytes(plane_in, recv.at[0])
    wait_bytes(verge_in, recv.at[5])
    raw = {(-dw, -ds): plane_in[d] for d, (dw, ds) in enumerate(SHIFTS)}
    raw[0, 0] = plane[...]
    for d, (dw, ds) in enumerate(FAR_SHIFTS):
        row = wide(verge_in[d])
        if abs(dw) == 2:
            value = pltpu.roll(row, 56 if dw > 0 else 16, 1, stride=8, stride_axis=0)
        else:
            value = pltpu.roll(row, 8 if ds > 0 else 113, 1, stride=1, stride_axis=0)
        raw[-dw, -ds] = value
    none = jnp.zeros((8, 128), jnp.float32)
    square = [(dw, ds) for dw in (-1, 0, 1) for ds in (-1, 0, 1)]
    cross = [(0, 0), (-1, 0), (1, 0), (0, -1), (0, 1)]

    def spans(values, at):
        dw, ds = at
        return join_span(
            values[at], values.get((dw, ds - 1), none), values.get((dw, ds + 1), none)
        )

    def walls(values, at):
        dw, ds = at
        return join_wall(
            values[at], values.get((dw - 1, ds), none), values.get((dw + 1, ds), none)
        )

    def pulled(values):
        fill = [none] * (len(values) % 2)
        high, low = split(jnp.concatenate(list(values) + fill, axis=0))
        product = jnp.dot(
            jnp.concatenate([high, low, high], axis=1),
            lines[...],
            preferred_element_type=jnp.float32,
        )
        return [
            (product[8 * n : 8 * n + 8, :128], product[8 * n : 8 * n + 8, 128:])
            for n in range(len(values))
        ]

    mass_flat = table[LANEX] * table[LANEZ]

    def plane_operator(in_x, in_z, value, at):
        return (
            table[LANEZ] * walls(in_x, at)
            + table[LANEX] * spans(in_z, at)
            + (SCALE * inverse_step) * mass_flat * value
        )

    line_of = {at: spans(raw, at) for at in square + [(-2, 0), (2, 0)]}
    stress = {at: walls(line_of, at) for at in square}
    pulls = pulled([stress[at] for at in square])
    in_x = {at: pulls[n][0] for n, at in enumerate(square)}
    in_z = {at: pulls[n][1] for n, at in enumerate(square)}
    first = {at: plane_operator(in_x, in_z, stress[at], at) for at in cross}
    mass_of = {at: mass_flat * stress[at] for at in cross}
    pulls = pulled([first[at] for at in cross] + [mass_of[at] for at in cross])
    seconds = []
    for offset, values in ((0, first), (5, mass_of)):
        in_x = {at: pulls[offset + n][0] for n, at in enumerate(cross)}
        in_z = {at: pulls[offset + n][1] for n, at in enumerate(cross)}
        seconds.append(plane_operator(in_x, in_z, values[0, 0], (0, 0)))

    def raised(doubles, triples, rights, rows):
        parts = []
        for value in doubles:
            parts += [coarse(value), value - coarse(value)]
        for value in triples:
            parts += [coarse(value), value - coarse(value), coarse(value)]
        parts += [none] * (rows // 8 - len(parts))
        return lax.dot_general(
            jnp.concatenate(parts, axis=0),
            rights[:rows],
            (((0,), (0,)), ((), ())),
            preferred_element_type=jnp.float32,
        )

    here, pull, mass_here = stress[0, 0], first[0, 0] * wall_mass, mass_of[0, 0]
    lifted = raised([here], [], lifting, 16)
    lifted_one = raised([pull], [mass_here], lifting, 48)
    lifted_two = raised(
        [seconds[0] * wall_mass * wall_mass],
        [seconds[1], mass_flat * pull, mass_flat * mass_here],
        lifting_two,
        96,
    )
    receive(two, 1)
    hear(2)
    for comp in range(2):
        for ex in range(2):
            column = (comp * 2 + ex) * 128
            rows = slice(128 * ex, 128 * ex + 128)
            for target, value in ((res, lifted), (one, lifted_one), (two, lifted_two)):
                target[2 * comp, rows] = target[2 * comp, rows] + value[:, column : column + 128]

    def energy(source, index):
        for comp in range(3):
            along, across_y = apply(source, comp)
            inside = jnp.zeros((16, 128), jnp.float32)
            edges = jnp.zeros((16, 128), jnp.float32)
            for i in range(16):
                rows = slice(16 * i, 16 * i + 16)
                term = source[comp, rows] * (
                    along[rows] * joined_y2 + across_y[rows] * both(table[FLAT + i])
                )
                if i % 8 in (0, 7):
                    edges = edges + term
                else:
                    inside = inside + term
            for d, i in ((0, 15), (1, 0)):
                sent = along[256 + 16 * d : 272 + 16 * d] * joined_y2
                edges = edges + sent * source[comp, 16 * i : 16 * i + 16]
            total = fold((inside + 0.5 * edges) * count2)
            for d, first in ((2, 15), (3, 0)):
                sent = along[256 + 16 * d : 272 + 16 * d] * joined_y2
                term = sent * source[comp, pl.ds(first, 16, stride=16), :]
                total = total + fold(term * share_x) * half_y
            mom[3 * index + comp] = total

    def weighted(pairs):
        for comp in range(3):
            totals = [jnp.zeros((16, 128), jnp.float32) for _ in pairs]
            edges = [jnp.zeros((16, 128), jnp.float32) for _ in pairs]
            for i in range(16):
                for n, (first, second, _) in enumerate(pairs):
                    term = (
                        first[comp, 16 * i : 16 * i + 16] * second[comp, 16 * i : 16 * i + 16]
                    )
                    if i % 8 in (0, 7):
                        edges[n] = edges[n] + term
                    else:
                        totals[n] = totals[n] + term
            for n, (_, _, index) in enumerate(pairs):
                mom[3 * index + comp] = fold((totals[n] + 0.5 * edges[n]) * count2)

    weighted([(res, res, 0), (res, one, 1), (one, one, 2), (one, two, 3), (two, two, 4)])
    energy(two, 5)

    row = jnp.zeros((8, 128), jnp.float32)
    for k in range(18):
        value = jnp.sum(mom[k], axis=1, keepdims=True)
        row = row + jnp.where(lane8 == k, value, 0.0)
    row = jnp.sum(row, axis=0, keepdims=True)

    start = 0
    for phase, (count, mine, peers) in enumerate(groups):
        part[phase] = row
        for peer in peers:
            push(
                part.at[phase], part_in.at[start + mine], send.at[4 + phase], recv.at[3 + phase],
                peer,
            )
        part_in[start + mine] = row
        wait_bytes(part_in.at[pl.ds(start, count - 1)], recv.at[3 + phase])
        row = part_in[start]
        for k in range(1, count):
            row = row + part_in[start + k]
        start += count

    row = jnp.broadcast_to(row, (8, 128))
    moments = [row if j == 0 else pltpu.roll(row, 128 - 3 * j, 1) for j in range(6)]

    def inner(first, second, raise_by):
        total = None
        for i, a in enumerate(first):
            for j, b in enumerate(second):
                term = a * b * moments[i + j + raise_by]
                total = term if total is None else total + term
        return total

    unit = jnp.ones((8, 128), jnp.float32)
    direction, residual = [unit], [unit]
    answer = [jnp.zeros((8, 128), jnp.float32)] * 3
    norm = moments[0]
    for step in range(3):
        alpha = norm / inner(direction, direction, 1)
        for i, value in enumerate(direction):
            answer[i] = answer[i] + alpha * value
        if step == 2:
            break
        lowered = [-alpha * value for value in direction]
        residual = [residual[0]] + [
            lowered[i] + residual[i + 1] if i + 1 < len(residual) else lowered[i]
            for i in range(len(lowered))
        ]
        newer = inner(residual, residual, 0)
        growth = newer / norm
        direction = [
            value + growth * direction[i] if i < len(direction) else value
            for i, value in enumerate(residual)
        ]
        norm = newer
    for i, value in enumerate(answer):
        scalars[i : i + 1, :] = value[:1] * SCALE
    wait_bytes(slab_in, send.at[0])
    wait_bytes(plane_in, send.at[1])
    wait_bytes(verge_in, send.at[6])
    for turn in range(2):
        wait_bytes(face_in.at[turn], send.at[2 + turn])
    start = 0
    for phase, (count, _, _) in enumerate(groups):
        wait_bytes(part_in.at[pl.ds(start, count - 1)], send.at[4 + phase])
        start += count


def combine(res, one, two, scalars, slopes, out, neumann, sums, sent):
    copies = [pltpu.make_async_copy(slopes, neumann, sent.at[3])]
    copies[0].start()
    for comp in range(3):
        c0, c1, c2 = (
            jnp.broadcast_to(scalars[k : k + 1, comp : comp + 1], (16, 128)) for k in range(3)
        )
        for i in range(16):
            rows = pl.ds(16 * i, 16)
            sums[comp, i] = (
                c0 * res[comp, rows, :] + c1 * one[comp, rows, :] + c2 * two[comp, rows, :]
            )
        copy = pltpu.make_async_copy(sums.at[comp], out.at[comp], sent.at[comp])
        copy.start()
        copies.append(copy)
    for copy in copies:
        copy.wait()


def body(sizes, velocity_old, heights, owner_device, owner_element, ref_coords, roughness):
    nx, ny, nc, ns = sizes
    slots = nc * ns + nx * ny
    f32, i32 = jnp.float32, jnp.int32
    vmem = pl.BlockSpec(memory_space=pltpu.VMEM)
    anywhere = pl.BlockSpec(memory_space=pl.ANY)
    constants, flat, lines = (jnp.asarray(value) for value in tables())
    res, one, two, scalars, slopes = pl.pallas_call(
        functools.partial(kernel, sizes),
        out_shape=(
            pltpu.VMEM((3, 256, 128), f32),
            pltpu.VMEM((3, 256, 128), f32),
            pltpu.VMEM((3, 256, 128), f32),
            pltpu.VMEM((8, 128), f32),
            pltpu.VMEM((2, 512), f32),
        ),
        in_specs=[anywhere] * 9,
        out_specs=(vmem,) * 5,
        scratch_shapes=[
            pltpu.VMEM((3, 16, 16, 128), f32),
            pltpu.SMEM((16,), f32),
            pltpu.VMEM((1, 512), i32),
            pltpu.VMEM((1, 512), i32),
            pltpu.VMEM((3, 512), f32),
            pltpu.VMEM((1, 512), f32),
            pltpu.VMEM(constants.shape, f32),
            pltpu.VMEM(flat.shape, jnp.bfloat16),
            pltpu.VMEM(lines.shape, jnp.bfloat16),
            pltpu.VMEM((256, 256), jnp.bfloat16),
            pltpu.VMEM((48, 512), f32),
            pltpu.VMEM((96, 512), f32),
            pltpu.VMEM((4, 256, 256), jnp.bfloat16),
            pltpu.VMEM((4, 128, 256), jnp.bfloat16),
            pltpu.VMEM((2, 4, 16, 128), f32),
            pltpu.VMEM((2, 2, 4, 16, 128), f32),
            pltpu.VMEM((8, 128), f32),
            pltpu.VMEM((8, 8, 128), f32),
            pltpu.VMEM((2, 1, 128), f32),
            pltpu.VMEM((12, 1, 128), f32),
            pltpu.VMEM((2, 4, 3, 16, 128), f32),
            pltpu.VMEM((2, 4, 3, 16, 128), f32),
            pltpu.VMEM((18, 8, 128), f32),
            pltpu.VMEM((2, 1, 128), f32),
            pltpu.VMEM((slots, 1, 128), f32),
            pltpu.SemaphoreType.DMA((9,)),
            pltpu.SemaphoreType.DMA((7,)),
            pltpu.SemaphoreType.DMA((2,)),
            pltpu.SemaphoreType.DMA((6,)),
            pltpu.SemaphoreType.REGULAR((3,)),
        ],
        compiler_params=pltpu.CompilerParams(collective_id=0, has_side_effects=True),
        name="channel_step",
    )(
        velocity_old,
        heights,
        owner_device.reshape(1, -1),
        owner_element.reshape(1, -1),
        ref_coords,
        roughness.reshape(1, -1),
        constants,
        flat,
        lines,
    )
    return pl.pallas_call(
        combine,
        out_shape=(
            jax.ShapeDtypeStruct((3, 16, 16, 128), f32),
            jax.ShapeDtypeStruct((2, 512), f32),
        ),
        in_specs=[vmem] * 5,
        out_specs=(anywhere, anywhere),
        scratch_shapes=[
            pltpu.VMEM((3, 16, 16, 128), f32),
            pltpu.SemaphoreType.DMA((4,)),
        ],
        name="combine",
    )(
        *(
            pltpu.with_memory_space_constraint(value, pltpu.VMEM)
            for value in (res, one, two, scalars, slopes)
        )
    )


def torus_program(torus):
    sizes = tuple(torus.shape[name] for name in AXES)
    return jax.shard_map(
        functools.partial(body, sizes),
        mesh=torus,
        in_specs=(
            P(None, WALL, "span", None),
            P(),
            P(WALL_SPAN, None),
            P(WALL_SPAN, None),
            P(None, WALL_SPAN),
            P(WALL_SPAN),
        ),
        out_specs=(P(None, WALL, "span", None), P(None, WALL_SPAN)),
        check_vma=False,
    )


def solution(mesh):
    return torus_program(Mesh(mesh.devices.reshape(4, 8, 2, mesh.shape["span"]), AXES))
```

```python
import functools

import jax
import jax.numpy as jnp
import numpy as np
from jax import lax
from jax.experimental import pallas as pl
from jax.experimental.pallas import tpu as pltpu
from jax.sharding import Mesh
from jax.sharding import PartitionSpec as P

AXES = ("wall_0", "wall_1", "wall_2", "span")
WALL_SPAN = AXES
WALL = ("wall_0", "wall_1", "wall_2")
MESH_ID = pl.DeviceIdType.MESH

GLL_NODES = (
    -1.0,
    -0.8717401485096066,
    -0.5917001814331423,
    -0.2092992179024789,
    0.2092992179024789,
    0.5917001814331423,
    0.8717401485096066,
    1.0,
)
GLL_WEIGHTS = (
    0.03571428571428571,
    0.2107042271435061,
    0.3411226924835044,
    0.4124587946587038,
    0.4124587946587038,
    0.3411226924835044,
    0.2107042271435061,
    0.03571428571428571,
)
viscosity = 0.02
inverse_step = 20.0
karman = 0.41
sample_height = 0.1
speed_floor = 0.01
element_dx = 0.05
element_dz = 0.13
precise = lax.Precision.HIGHEST

SCALE = 64.0

SHIFTS = ((1, 0), (-1, 0), (0, 1), (0, -1), (1, 1), (1, -1), (-1, 1), (-1, -1))

FAR_SHIFTS = (
    (2, 0), (2, 1), (2, -1), (-2, 0), (-2, 1), (-2, -1),
    (0, 2), (1, 2), (-1, 2), (0, -2), (1, -2), (-1, -2),
)

MZ, QMZ, COUNT, LAG, PLANE, HALFW, LAST, FIRST, LANEX, LANEZ = range(10)
BLOCK, LIFT, FLAT = 10, 26, 30


def stiffness_table():
    points = np.array(GLL_NODES)
    weights = np.array(GLL_WEIGHTS)
    previous = np.ones(8)
    current = points.copy()
    for degree in range(1, 7):
        previous, current = (
            current,
            ((2 * degree + 1) * points * current - degree * previous) / (degree + 1),
        )
    derivative = np.zeros((8, 8))
    for target in range(8):
        for source in range(8):
            if target != source:
                derivative[target, source] = (
                    current[target] / current[source] / (points[target] - points[source])
                )
    derivative[0, 0] = -14.0
    derivative[7, 7] = 14.0
    return derivative.T @ (weights[:, None] * derivative)


def tables():
    weights = np.array(GLL_WEIGHTS)
    points = np.array(GLL_NODES)
    stiffness = stiffness_table()
    ones = np.ones((8, 128))
    lane = np.arange(128)
    ends = np.array([2.0, 1, 1, 1, 1, 1, 1, 2.0])
    mass_x = 0.5 * element_dx * weights
    mass_z = 0.5 * element_dz * weights
    count_y = np.where((lane % 8 == 0) | (lane % 8 == 7), 0.5, 1.0)
    count_y[0] = count_y[127] = 1.0
    gaps = points[:, None] - points[None, :] + np.eye(8)
    rows = [
        mass_z[:, None] * ones,
        (mass_z * ends)[:, None] * ones,
        (1.0 / ends)[:, None] * count_y[None, :],
        (1.0 / np.prod(gaps, axis=1))[:, None] * ones,
        ones * (mass_x[lane // 16] * mass_z[lane % 8])[None, :],
        ones * (0.5 * weights[lane % 8])[None, :],
        ones * ((lane % 8 == 7) & (lane < 127))[None, :],
        ones * ((lane % 8 == 0) & (lane > 0))[None, :],
    ]
    block = np.kron(np.eye(16), SCALE * viscosity * 2.0 * stiffness)
    lift = np.zeros((8, 512))
    for comp in range(2):
        for half in range(2):
            column = (comp * 2 + half) * 128
            lift[comp * 4 + half, column] = 1.0
            lift[comp * 4 + 2 + half, column + 127] = 1.0
    joined_x = np.tile(mass_x * ends, 2)
    joined_z = np.tile(mass_z * ends, 2)

    def chain(length):
        scaled = SCALE * viscosity * (2.0 / length) * stiffness
        full = np.kron(np.eye(2), scaled)
        ends_only = full[[15, 0]]
        full[7] = full[8] = full[7] + full[8]
        return full, ends_only

    chain_x, ends_x = chain(element_dx)
    chain_z, ends_z = chain(element_dz)
    flat = np.kron(chain_x, np.diag(joined_z)) + np.kron(np.diag(joined_x), chain_z)
    flat += SCALE * inverse_step * np.diag(np.kron(joined_x, joined_z))
    faces = [np.kron(ends_x[d : d + 1], np.diag(joined_z)) for d in range(2)]
    faces += [np.kron(np.diag(joined_x), ends_z[d : d + 1]) for d in range(2)]
    flat = np.concatenate([flat] + faces).astype(np.float32)
    flat_high = flat.astype(jnp.bfloat16)
    flat_low = (flat - flat_high.astype(np.float32)).astype(jnp.bfloat16)
    line_x = SCALE * viscosity * (2.0 / element_dx) * stiffness
    line_z = SCALE * viscosity * (2.0 / element_dz) * stiffness
    line = np.concatenate([np.kron(line_x.T, np.eye(16)), np.kron(np.eye(16), line_z.T)], axis=1)
    line_high = line.astype(np.float32).astype(jnp.bfloat16)
    line_low = (line.astype(np.float32) - line_high.astype(np.float32)).astype(jnp.bfloat16)
    lines = np.concatenate([line_high, line_high, line_low])
    rows += [
        ones * (mass_x * ends)[lane // 16][None, :],
        ones * (mass_z * ends)[lane % 8][None, :],
    ]
    pieces = [np.stack(rows), block.reshape(16, 8, 128), lift.reshape(8, 4, 128).transpose(1, 0, 2)]
    pieces += [joined_x[:, None, None] * (mass_z * ends)[None, :, None] * np.ones((16, 8, 128))]
    return np.concatenate(pieces).astype(np.float32), np.stack([flat_high, flat_low]), lines


def kernel(sizes, *refs):
    operands, refs = refs[:9], refs[9:]
    (res, one, two, scalars, neumann), refs = refs[:5], refs[5:]
    local, refs = refs[:9], refs[9:]
    velocity, heights, owner, element, coords, roughness, table, flat, lines = local
    (normal, lifting, lifting_two, right_high, right_low, slab, slab_in, plane, plane_in,
     verge, verge_in, face, face_in, mom, part, part_in,
     load, send, slab_recv, recv, ready) = refs
    nx, ny, nc, ns = sizes
    nw = nx * ny * nc
    loads = [
        pltpu.make_async_copy(source, target, load.at[n])
        for n, (source, target) in enumerate(zip(operands, local))
    ]
    for copy in loads:
        copy.start()
    wx, wy, wc, sp = (lax.axis_index(name) for name in AXES)
    wall = (wx * ny + wy) * nc + wc
    weights = np.array(GLL_WEIGHTS)
    stiffness = stiffness_table()
    mass_x = [float(v) for v in 0.5 * element_dx * weights]
    ends = [2.0, 1.0, 1.0, 1.0, 1.0, 1.0, 1.0, 2.0]

    def ring(value, shift, count):
        if shift > 0:
            return jnp.where(value >= count - shift, value + shift - count, value + shift)
        return jnp.where(value < -shift, value + shift + count, value + shift)

    def beside(dw):
        if dw == 0:
            return wx, wy, wc
        sign = 1 if dw > 0 else -1
        if abs(dw) == 2:
            turn_y = wy == (ny - 1 if dw > 0 else 0)
            return jnp.where(turn_y, ring(wx, sign, nx), wx), ring(wy, sign, ny), wc
        turn = wc == (nc - 1 if dw > 0 else 0)
        turn_y = jnp.logical_and(turn, wy == (ny - 1 if dw > 0 else 0))
        return (
            jnp.where(turn_y, ring(wx, dw, nx), wx),
            jnp.where(turn, ring(wy, dw, ny), wy),
            ring(wc, dw, nc),
        )

    along = {dw: beside(dw) for dw in (-2, -1, 0, 1, 2)}
    across = {k: ring(sp, k, ns) if k else sp for k in (-2, -1, 0, 1, 2)}
    neighbours = [(*along[dw], across[ds]) for dw, ds in SHIFTS]
    distant = [(*along[dw], across[ds]) for dw, ds in FAR_SHIFTS]
    place_x = {0: wx, 1: ring(wx, 1, nx), -1: ring(wx, -1, nx), 2: ring(wx, 2, nx)}
    place_y = {k: ring(wy, k, ny) if k else wy for k in range(-(ny // 2) + 1, ny // 2 + 1)}
    place_y[-2] = ring(wy, -2, ny)
    place_z = {k: ring(sp, k, ns) if k else sp for k in range(-(ns // 2) + 1, ns // 2 + 1)}
    place_z[-2] = ring(sp, -2, ns)
    other = ring(wc, 1, nc)
    flat_peer = lambda dx, dy: (place_x[dx], place_y[dy], wc, sp)
    deep_peer = lambda c, ds: (wx, wy, c, place_z[ds])

    def far_first(keys):
        return sorted(keys, key=lambda key: -abs(key[0]) - abs(key[1]))

    deep_shifts = range(-(ns // 2) + 1, ns // 2 + 1)
    wide_x = [k for k in (-1, 0, 1, 2) if -(nx // 2) < k <= nx // 2]
    plain = far_first([(a, b) for a in wide_x for b in range(-(ny // 2) + 1, ny // 2 + 1)])
    plain = [key for key in plain if key != (0, 0)]

    barrier = pltpu.get_barrier_semaphore()
    near = neighbours[:4] + [deep_peer(other, 0)]
    near += [(*along[2], sp), (*along[-2], sp), (*along[0], across[2]), (*along[0], across[-2])]
    near += [flat_peer(1, 0), flat_peer(-1, 0), flat_peer(0, 1), flat_peer(0, -1)]
    for peer in near:
        pl.semaphore_signal(barrier, inc=1, device_id=peer, device_id_type=MESH_ID)
    relays = [
        near,
        [flat_peer(1, 0), flat_peer(-1, 0), flat_peer(0, 2), flat_peer(0, -2)]
        + [deep_peer(wc, 2), deep_peer(wc, -2)],
        [flat_peer(1, 0), flat_peer(-1, 0), flat_peer(0, 2), flat_peer(0, -2)]
        + [flat_peer(2, 2), flat_peer(2, -2), deep_peer(wc, 4), deep_peer(wc, -4)],
    ]

    def tell(n):
        for peer in relays[n]:
            pl.semaphore_signal(ready.at[n], inc=1, device_id=peer, device_id_type=MESH_ID)

    def hear(n):
        pl.semaphore_wait(ready.at[n], len(relays[n]))

    def push(source, target, send_sem, recv_sem, peer):
        pltpu.make_async_remote_copy(
            src_ref=source,
            dst_ref=target,
            send_sem=send_sem,
            recv_sem=recv_sem,
            device_id=peer,
            device_id_type=MESH_ID,
        ).start()

    def wait_bytes(like, sem):
        pltpu.make_async_copy(like, like, sem).wait()

    loads[0].wait()

    lane = lax.broadcasted_iota(jnp.int32, (1, 128), 1)
    sub8 = lax.broadcasted_iota(jnp.int32, (8, 128), 0)
    lane8 = lax.broadcasted_iota(jnp.int32, (8, 128), 1)

    for comp in range(2):
        quarters = []
        for k in range(4):
            quarters.append(velocity[2 * comp, 4 * k : 4 * k + 4].reshape(64, 128))
        packed = jnp.zeros((64, 128), jnp.float32)
        where_to = lax.broadcasted_iota(jnp.int32, (64, 128), 1)
        for k in range(4):
            low = pltpu.roll(quarters[k], 32 * k, 1) if k else quarters[k]
            shift = (32 * k + 32) % 128
            high = pltpu.roll(quarters[k], shift, 1) if shift else quarters[k]
            packed = jnp.where(where_to // 16 == 2 * k, low, packed)
            packed = jnp.where(where_to // 16 == 2 * k + 1, high, packed)
        slab[comp] = packed.reshape(4, 16, 128)

    pl.semaphore_wait(barrier, len(near))

    tell(0)
    for d in range(2):
        push(slab, slab_in.at[d], send.at[0], slab_recv.at[d], neighbours[d])

    for copy in loads[1:]:
        copy.wait()
    height = jnp.zeros((8, 128), jnp.float32)
    for layer in range(16):
        height = jnp.where(lane8 // 8 == layer, heights[layer], height)
    mass_y = height * table[HALFW]
    block = table[BLOCK : BLOCK + 16].reshape(128, 128) * (1.0 / height)[:1]
    block = (
        block
        + table[LAST][:1] * pltpu.roll(block, 127, 1)
        + table[FIRST][:1] * pltpu.roll(block, 1, 1)
    )

    def split(value):
        high = value.astype(jnp.bfloat16)
        return high, (value - high.astype(jnp.float32)).astype(jnp.bfloat16)

    block_high, block_low = split(block)
    normal[:128, :128] = block_high
    normal[128:, :128] = block_high
    normal[:128, 128:] = block_low
    normal[128:, 128:] = jnp.zeros((128, 128), jnp.bfloat16)
    right_high[...] = jnp.zeros(right_high.shape, jnp.bfloat16)
    right_low[...] = jnp.zeros(right_low.shape, jnp.bfloat16)
    side = sub8 // 2 % 2
    wall_row = jnp.where(side == 0, block[:1], block[127:])
    lift = jnp.concatenate([table[LIFT + k] for k in range(4)], axis=1)
    home = (sub8 // 4 * 2 + sub8 % 2)[:, :1]
    joined_y = (
        mass_y
        + table[LAST] * pltpu.roll(mass_y, 127, 1)
        + table[FIRST] * pltpu.roll(mass_y, 1, 1)
    )
    both = lambda value: jnp.concatenate([value, value], axis=0)
    joined_y2 = both(joined_y)
    count2 = both(table[COUNT])

    def at_home(value):
        return jnp.concatenate([jnp.where(home == k, value, 0.0) for k in range(4)], axis=1)

    def coarse(value):
        return value.astype(jnp.bfloat16).astype(jnp.float32)

    twice = jnp.dot(wall_row, block, precision=precise, preferred_element_type=jnp.float32)
    pieces, pieces_two = [lift, lift], [lift, lift]
    for n, value in enumerate((wall_row, joined_y * wall_row, wall_row, twice)):
        rises = at_home(value)
        high = coarse(rises)
        triple = [high, high, rises - high]
        if n == 0:
            pieces += triple
        else:
            pieces_two += triple
    for n, value in enumerate(pieces):
        lifting[8 * n : 8 * n + 8] = value
    lifting[40:] = jnp.zeros((8, 512), jnp.float32)
    for n, value in enumerate(pieces_two):
        lifting_two[8 * n : 8 * n + 8] = value
    lifting_two[88:] = jnp.zeros((8, 512), jnp.float32)
    wall_mass = jnp.where(side == 0, joined_y[:, :1], joined_y[:, 127:])
    scale_zy = both(table[QMZ] * joined_y) * inverse_step
    for comp in range(3):
        for i in range(16):
            res[comp, 16 * i : 16 * i + 16] = velocity[comp, i] * (
                scale_zy * (mass_x[i % 8] * ends[i % 8])
            )

    row16 = lax.broadcasted_iota(jnp.int32, (16, 128), 0) % 8
    share_x = jnp.where(jnp.logical_or(row16 == 0, row16 == 7), 0.5, 1.0)
    half_y = jnp.broadcast_to(table[COUNT][:1], (8, 128))

    def fold(value):
        return value[:8] + value[8:]

    def apply(source, comp):
        high, low = split(source[comp])
        parts = jnp.concatenate([high, low], axis=1)
        along = jnp.dot(flat[0], parts, preferred_element_type=jnp.float32)
        along = along[:, :128] + along[:, 128:]
        along = along + jnp.dot(flat[1], high, preferred_element_type=jnp.float32)
        across_y = jnp.dot(parts, normal[...], preferred_element_type=jnp.float32)
        return along, across_y[:, :128] + across_y[:, 128:]

    def operate(source, target, turn):
        for comp in range(3):
            along, across_y = apply(source, comp)
            for d in range(4):
                rows = slice(256 + 16 * d, 272 + 16 * d)
                face[turn, d, comp] = along[rows] * joined_y2
                push(
                    face.at[turn, d, comp], face_in.at[turn, d, comp], send.at[2 + turn],
                    recv.at[1 + turn], neighbours[d],
                )
            for i in range(16):
                rows = slice(16 * i, 16 * i + 16)
                target[comp, rows] = along[rows] * joined_y2 + across_y[rows] * both(
                    table[FLAT + i]
                )

    operate(res, one, 0)
    def regroup(blocks):
        upper = (lane // 8) % 2 == 1
        result = []
        for ex in range(2):
            low, high = blocks[ex], blocks[2 + ex]
            result.append(jnp.where(upper, pltpu.roll(high, 8, 1), low))
            result.append(jnp.where(upper, high, pltpu.roll(low, 120, 1)))
        return result

    def ungroup(values):
        upper = (lane // 8) % 2 == 1
        low, high = [], []
        for ex in range(2):
            a, b = values[2 * ex], values[2 * ex + 1]
            low.append(jnp.where(upper, pltpu.roll(b, 8, 1), a))
            high.append(jnp.where(upper, b, pltpu.roll(a, 120, 1)))
        return low + high

    wide = lambda row: jnp.broadcast_to(row, (8, 128))
    quarter = lambda ref, row, q: ref[row : row + 1, 128 * q : 128 * q + 128]
    distance = [(quarter(owner, 0, q) - wall + nw) % nw for q in range(4)]
    to_next = regroup([wide(jnp.where(d == 1, 1.0, 0.0)) for d in distance])
    to_prev = regroup([wide(jnp.where(d == nw - 1, 1.0, 0.0)) for d in distance])
    layer = regroup([wide((quarter(element, 0, q) % 2).astype(jnp.float32)) for q in range(4)])
    axes = [regroup([wide(quarter(coords, k, q)) for q in range(4)]) for k in range(3)]

    def lagrange(coord):
        value = table[LAG]
        for b in range(8):
            value = value * jnp.where(sub8 == b, 1.0, coord - GLL_NODES[b])
        return value

    basis = [[lagrange(axes[k][g]) for k in range(3)] for g in range(4)]
    second_wall = (lane // 8) % 2 == 1
    for g in range(4):
        ly = basis[g][2]
        blocks = []
        for side in range(2):
            for ey in range(2):
                chosen = jnp.logical_and(
                    wide(second_wall) == (side == 1), layer[g] == float(ey)
                )
                blocks.append(jnp.where(chosen, ly, 0.0))
        high, low = split(jnp.concatenate(blocks, axis=0))
        for kk in range(2):
            k = 2 * (g // 2) + kk
            column = slice(128 * kk, 128 * kk + 128)
            right_high[g, 32 * k : 32 * k + 32, column] = high
            right_high[g, 128 + 32 * k : 160 + 32 * k, column] = high
            right_low[g, 32 * k : 32 * k + 32, column] = low

    masks = [[1.0 - to_next[g] - to_prev[g], to_prev[g], to_next[g]] for g in range(4)]

    def sample(source, g):
        ez = g % 2
        high, low = split(source[:, :, 8 * ez : 8 * ez + 8, :].reshape(64, 128))
        product = jnp.dot(
            jnp.concatenate([high, low], axis=1), right_high[g],
            preferred_element_type=jnp.float32,
        ) + jnp.dot(high, right_low[g], preferred_element_type=jnp.float32)
        total = [jnp.zeros((8, 128), jnp.float32) for _ in range(2)]
        for kk in range(2):
            values = product[:, 128 * kk : 128 * kk + 128].reshape(2, 4, 8, 128)
            for comp in range(2):
                for x in range(4):
                    a = 4 * kk + x
                    total[comp] = total[comp] + values[comp, x] * basis[g][0][a : a + 1]
        return total

    sums = []
    for g in range(4):
        own = sample(slab, g)
        sums.append([own[comp] * masks[g][0] for comp in range(2)])
    hear(0)
    tell(1)
    for d in range(2):
        wait_bytes(slab_in.at[d], slab_recv.at[d])
        for g in range(4):
            far = sample(slab_in.at[d], g)
            for comp in range(2):
                sums[g][comp] = sums[g][comp] + far[comp] * masks[g][1 + d]
    stream = ungroup(
        [wide(jnp.sum(sums[g][0] * basis[g][1], axis=0, keepdims=True)) for g in range(4)]
    )
    spanwise = ungroup(
        [wide(jnp.sum(sums[g][1] * basis[g][1], axis=0, keepdims=True)) for g in range(4)]
    )

    for q in range(4):
        u, v = stream[q], spanwise[q]
        speed = jnp.sqrt(u * u + v * v + speed_floor)
        ratio = karman / jnp.log(sample_height / wide(quarter(roughness, 0, q)))
        factor = -(ratio * ratio * speed / viscosity)
        for comp, value in enumerate((u, v)):
            slope = factor * value
            neumann[comp : comp + 1, 128 * q : 128 * q + 128] = slope[:1]
            plane[comp * 4 + q : comp * 4 + q + 1, :] = (viscosity * slope * table[PLANE])[:1]

    mine = plane[...]
    lines_x = jnp.zeros((8, 128), jnp.float32)
    for q in range(4):
        here = jnp.logical_and(sub8 == 2 * q + 1, lane8 // 16 == 3 - q)
        lines_x = jnp.where(here, pltpu.roll(mine, (16 * (3 - q) - 112) % 128, 1), lines_x)
        here = jnp.logical_and(sub8 == 2 * q, lane8 // 16 == 7 - q)
        lines_x = jnp.where(here, pltpu.roll(mine, (64 + 16 * (3 - q)) % 128, 1), lines_x)
    lines_z = jnp.zeros((8, 128), jnp.float32)
    for r in range(8):
        here = jnp.logical_and(sub8 == r, lane8 % 16 == 7 - r)
        lines_z = jnp.where(here, pltpu.roll(mine, (7 - r - 15) % 128, 1), lines_z)
        here = jnp.logical_and(sub8 == r, lane8 % 16 == 15 - r)
        lines_z = jnp.where(here, pltpu.roll(mine, (15 - r) % 128, 1), lines_z)
    verge[0] = jnp.sum(lines_x, axis=0, keepdims=True)
    verge[1] = jnp.sum(lines_z, axis=0, keepdims=True)
    for d, (dw, ds) in enumerate(FAR_SHIFTS):
        push(
            verge.at[0 if abs(dw) == 2 else 1], verge_in.at[d], send.at[6], recv.at[5], distant[d]
        )
    for d in range(8):
        push(plane, plane_in.at[d], send.at[1], recv.at[0], neighbours[d])

    node_z = lane8 % 16
    node_x = lane8 // 16
    half = sub8 % 2

    def join_span(mine, before, after):
        return (
            mine
            + jnp.where(node_z == 7, pltpu.roll(mine, 127, 1), 0.0)
            + jnp.where(node_z == 8, pltpu.roll(mine, 1, 1), 0.0)
            + jnp.where(node_z == 0, pltpu.roll(before, 113, 1), 0.0)
            + jnp.where(node_z == 15, pltpu.roll(after, 15, 1), 0.0)
        )

    def join_wall(mine, before, after):
        later = jnp.where(half == 0, pltpu.roll(mine, 7, 0), pltpu.roll(after, 1, 0))
        earlier = jnp.where(half == 0, pltpu.roll(before, 7, 0), pltpu.roll(mine, 1, 0))
        return (
            mine
            + jnp.where(node_x == 7, pltpu.roll(later, 112, 1), 0.0)
            + jnp.where(node_x == 0, pltpu.roll(earlier, 16, 1), 0.0)
        )

    def receive(target, turn):
        wait_bytes(face_in.at[turn], recv.at[1 + turn])
        into = (
            pl.ds(0, 16),
            pl.ds(240, 16),
            pl.ds(0, 16, stride=16),
            pl.ds(15, 16, stride=16),
        )
        for d in range(4):
            for comp in range(3):
                target[comp, into[d], :] = target[comp, into[d], :] + face_in[turn, d, comp]

    hear(1)
    tell(2)
    receive(one, 0)
    operate(one, two, 1)
    wait_bytes(plane_in, recv.at[0])
    wait_bytes(verge_in, recv.at[5])
    raw = {(-dw, -ds): plane_in[d] for d, (dw, ds) in enumerate(SHIFTS)}
    raw[0, 0] = plane[...]
    for d, (dw, ds) in enumerate(FAR_SHIFTS):
        row = wide(verge_in[d])
        if abs(dw) == 2:
            value = pltpu.roll(row, 56 if dw > 0 else 16, 1, stride=8, stride_axis=0)
        else:
            value = pltpu.roll(row, 8 if ds > 0 else 113, 1, stride=1, stride_axis=0)
        raw[-dw, -ds] = value
    none = jnp.zeros((8, 128), jnp.float32)
    square = [(dw, ds) for dw in (-1, 0, 1) for ds in (-1, 0, 1)]
    cross = [(0, 0), (-1, 0), (1, 0), (0, -1), (0, 1)]

    def spans(values, at):
        dw, ds = at
        return join_span(
            values[at], values.get((dw, ds - 1), none), values.get((dw, ds + 1), none)
        )

    def walls(values, at):
        dw, ds = at
        return join_wall(
            values[at], values.get((dw - 1, ds), none), values.get((dw + 1, ds), none)
        )

    def pulled(values):
        fill = [none] * (len(values) % 2)
        high, low = split(jnp.concatenate(list(values) + fill, axis=0))
        product = jnp.dot(
            jnp.concatenate([high, low, high], axis=1),
            lines[...],
            preferred_element_type=jnp.float32,
        )
        return [
            (product[8 * n : 8 * n + 8, :128], product[8 * n : 8 * n + 8, 128:])
            for n in range(len(values))
        ]

    mass_flat = table[LANEX] * table[LANEZ]

    def plane_operator(in_x, in_z, value, at):
        return (
            table[LANEZ] * walls(in_x, at)
            + table[LANEX] * spans(in_z, at)
            + (SCALE * inverse_step) * mass_flat * value
        )

    line_of = {at: spans(raw, at) for at in square + [(-2, 0), (2, 0)]}
    stress = {at: walls(line_of, at) for at in square}
    pulls = pulled([stress[at] for at in square])
    in_x = {at: pulls[n][0] for n, at in enumerate(square)}
    in_z = {at: pulls[n][1] for n, at in enumerate(square)}
    first = {at: plane_operator(in_x, in_z, stress[at], at) for at in cross}
    mass_of = {at: mass_flat * stress[at] for at in cross}
    pulls = pulled([first[at] for at in cross] + [mass_of[at] for at in cross])
    seconds = []
    for offset, values in ((0, first), (5, mass_of)):
        in_x = {at: pulls[offset + n][0] for n, at in enumerate(cross)}
        in_z = {at: pulls[offset + n][1] for n, at in enumerate(cross)}
        seconds.append(plane_operator(in_x, in_z, values[0, 0], (0, 0)))

    def raised(doubles, triples, rights, rows):
        parts = []
        for value in doubles:
            parts += [coarse(value), value - coarse(value)]
        for value in triples:
            parts += [coarse(value), value - coarse(value), coarse(value)]
        parts += [none] * (rows // 8 - len(parts))
        return lax.dot_general(
            jnp.concatenate(parts, axis=0),
            rights[:rows],
            (((0,), (0,)), ((), ())),
            preferred_element_type=jnp.float32,
        )

    here, pull, mass_here = stress[0, 0], first[0, 0] * wall_mass, mass_of[0, 0]
    lifted = raised([here], [], lifting, 16)
    lifted_one = raised([pull], [mass_here], lifting, 48)
    lifted_two = raised(
        [seconds[0] * wall_mass * wall_mass],
        [seconds[1], mass_flat * pull, mass_flat * mass_here],
        lifting_two,
        96,
    )
    receive(two, 1)
    for comp in range(2):
        for ex in range(2):
            column = (comp * 2 + ex) * 128
            rows = slice(128 * ex, 128 * ex + 128)
            for target, value in ((res, lifted), (one, lifted_one), (two, lifted_two)):
                target[2 * comp, rows] = target[2 * comp, rows] + value[:, column : column + 128]

    def note(k, value):
        mom[k : k + 1, :] = jnp.sum(value, axis=0, keepdims=True)

    def energy(source, index):
        for comp in range(3):
            along, across_y = apply(source, comp)
            inside = jnp.zeros((16, 128), jnp.float32)
            edges = jnp.zeros((16, 128), jnp.float32)
            for i in range(16):
                rows = slice(16 * i, 16 * i + 16)
                term = source[comp, rows] * (
                    along[rows] * joined_y2 + across_y[rows] * both(table[FLAT + i])
                )
                if i % 8 in (0, 7):
                    edges = edges + term
                else:
                    inside = inside + term
            for d, i in ((0, 15), (1, 0)):
                sent = along[256 + 16 * d : 272 + 16 * d] * joined_y2
                edges = edges + sent * source[comp, 16 * i : 16 * i + 16]
            total = fold((inside + 0.5 * edges) * count2)
            for d, first in ((2, 15), (3, 0)):
                sent = along[256 + 16 * d : 272 + 16 * d] * joined_y2
                term = sent * source[comp, pl.ds(first, 16, stride=16), :]
                total = total + fold(term * share_x) * half_y
            note(3 * index + comp, total)

    def weighted(pairs):
        for comp in range(3):
            totals = [jnp.zeros((16, 128), jnp.float32) for _ in pairs]
            edges = [jnp.zeros((16, 128), jnp.float32) for _ in pairs]
            for i in range(16):
                for n, (first, second, _) in enumerate(pairs):
                    term = (
                        first[comp, 16 * i : 16 * i + 16] * second[comp, 16 * i : 16 * i + 16]
                    )
                    if i % 8 in (0, 7):
                        edges[n] = edges[n] + term
                    else:
                        totals[n] = totals[n] + term
            for n, (_, _, index) in enumerate(pairs):
                note(3 * index + comp, fold((totals[n] + 0.5 * edges[n]) * count2))

    weighted([(res, res, 0), (res, one, 1), (one, one, 2), (one, two, 3), (two, two, 4)])
    energy(two, 5)

    mom[18:24, :] = jnp.zeros((6, 128), jnp.float32)
    total = jnp.sum(mom[...], axis=1, keepdims=True)
    row = jnp.zeros((8, 128), jnp.float32)
    for k in range(3):
        row = row + jnp.where(lane8 == 8 * k + sub8, total[8 * k : 8 * k + 8], 0.0)
    part[0] = jnp.sum(row, axis=0, keepdims=True)
    hear(2)
    line_slots, plane_slots = nc * ns, nx * ny
    for ds in sorted(deep_shifts, key=lambda k: -abs(k)):
        if ds:
            push(
                part.at[0], part_in.at[wc * ns + sp], send.at[4], recv.at[3], deep_peer(1, ds)
            )
    relays_sums = wc == 1

    @pl.when(jnp.logical_not(relays_sums))
    def _():
        push(part.at[0], part_in.at[wc * ns + sp], send.at[4], recv.at[3], deep_peer(1, 0))
        wait_bytes(part_in.at[pl.ds(line_slots, plane_slots)], recv.at[4])
        wait_bytes(part_in.at[pl.ds(0, ns)], send.at[4])

    @pl.when(relays_sums)
    def _():
        part_in[wc * ns + sp] = part[0]
        wait_bytes(part_in.at[pl.ds(0, line_slots - 1)], recv.at[3])
        row = part_in[0]
        for k in range(1, line_slots):
            row = row + part_in[k]
        part[1] = row
        slot = line_slots + wx * ny + wy
        for a, b in plain:
            for c in (0, 1):
                push(
                    part.at[1], part_in.at[slot], send.at[5 if c else 7], recv.at[4],
                    (place_x[a], place_y[b], c, sp),
                )
        push(part.at[1], part_in.at[slot], send.at[7], recv.at[4], (wx, wy, 0, sp))
        part_in[slot] = row
        wait_bytes(part_in.at[pl.ds(line_slots, plane_slots - 1)], recv.at[4])
        wait_bytes(part_in.at[pl.ds(0, ns - 1)], send.at[4])
        wait_bytes(part_in.at[pl.ds(line_slots, plane_slots - 1)], send.at[5])
        wait_bytes(part_in.at[pl.ds(line_slots, plane_slots)], send.at[7])

    row = part_in[line_slots]
    for k in range(1, plane_slots):
        row = row + part_in[line_slots + k]

    row = jnp.broadcast_to(row, (8, 128))
    moments = [row if j == 0 else pltpu.roll(row, 128 - 3 * j, 1) for j in range(6)]

    def inner(first, second, raise_by):
        total = None
        for i, a in enumerate(first):
            for j, b in enumerate(second):
                term = a * b * moments[i + j + raise_by]
                total = term if total is None else total + term
        return total

    unit = jnp.ones((8, 128), jnp.float32)
    direction, residual = [unit], [unit]
    answer = [jnp.zeros((8, 128), jnp.float32)] * 3
    norm = moments[0]
    for step in range(3):
        alpha = norm / inner(direction, direction, 1)
        for i, value in enumerate(direction):
            answer[i] = answer[i] + alpha * value
        if step == 2:
            break
        lowered = [-alpha * value for value in direction]
        residual = [residual[0]] + [
            lowered[i] + residual[i + 1] if i + 1 < len(residual) else lowered[i]
            for i in range(len(lowered))
        ]
        newer = inner(residual, residual, 0)
        growth = newer / norm
        direction = [
            value + growth * direction[i] if i < len(direction) else value
            for i, value in enumerate(residual)
        ]
        norm = newer
    for i, value in enumerate(answer):
        scalars[i : i + 1, :] = value[:1] * SCALE
    wait_bytes(slab_in, send.at[0])
    wait_bytes(plane_in, send.at[1])
    wait_bytes(verge_in, send.at[6])
    for turn in range(2):
        wait_bytes(face_in.at[turn], send.at[2 + turn])


def combine(res, one, two, scalars, slopes, out, neumann, sums, sent):
    copies = [pltpu.make_async_copy(slopes, neumann, sent.at[3])]
    copies[0].start()
    for comp in range(3):
        c0, c1, c2 = (
            jnp.broadcast_to(scalars[k : k + 1, comp : comp + 1], (16, 128)) for k in range(3)
        )
        for i in range(16):
            rows = pl.ds(16 * i, 16)
            sums[comp, i] = (
                c0 * res[comp, rows, :] + c1 * one[comp, rows, :] + c2 * two[comp, rows, :]
            )
        copy = pltpu.make_async_copy(sums.at[comp], out.at[comp], sent.at[comp])
        copy.start()
        copies.append(copy)
    for copy in copies:
        copy.wait()


def body(sizes, velocity_old, heights, owner_device, owner_element, ref_coords, roughness):
    nx, ny, nc, ns = sizes
    slots = nc * ns + nx * ny
    f32, i32 = jnp.float32, jnp.int32
    vmem = pl.BlockSpec(memory_space=pltpu.VMEM)
    anywhere = pl.BlockSpec(memory_space=pl.ANY)
    constants, flat, lines = (jnp.asarray(value) for value in tables())
    res, one, two, scalars, slopes = pl.pallas_call(
        functools.partial(kernel, sizes),
        out_shape=(
            pltpu.VMEM((3, 256, 128), f32),
            pltpu.VMEM((3, 256, 128), f32),
            pltpu.VMEM((3, 256, 128), f32),
            pltpu.VMEM((8, 128), f32),
            pltpu.VMEM((2, 512), f32),
        ),
        in_specs=[anywhere] * 9,
        out_specs=(vmem,) * 5,
        scratch_shapes=[
            pltpu.VMEM((3, 16, 16, 128), f32),
            pltpu.SMEM((16,), f32),
            pltpu.VMEM((1, 512), i32),
            pltpu.VMEM((1, 512), i32),
            pltpu.VMEM((3, 512), f32),
            pltpu.VMEM((1, 512), f32),
            pltpu.VMEM(constants.shape, f32),
            pltpu.VMEM(flat.shape, jnp.bfloat16),
            pltpu.VMEM(lines.shape, jnp.bfloat16),
            pltpu.VMEM((256, 256), jnp.bfloat16),
            pltpu.VMEM((48, 512), f32),
            pltpu.VMEM((96, 512), f32),
            pltpu.VMEM((4, 256, 256), jnp.bfloat16),
            pltpu.VMEM((4, 128, 256), jnp.bfloat16),
            pltpu.VMEM((2, 4, 16, 128), f32),
            pltpu.VMEM((2, 2, 4, 16, 128), f32),
            pltpu.VMEM((8, 128), f32),
            pltpu.VMEM((8, 8, 128), f32),
            pltpu.VMEM((2, 1, 128), f32),
            pltpu.VMEM((12, 1, 128), f32),
            pltpu.VMEM((2, 4, 3, 16, 128), f32),
            pltpu.VMEM((2, 4, 3, 16, 128), f32),
            pltpu.VMEM((24, 128), f32),
            pltpu.VMEM((2, 1, 128), f32),
            pltpu.VMEM((slots, 1, 128), f32),
            pltpu.SemaphoreType.DMA((9,)),
            pltpu.SemaphoreType.DMA((8,)),
            pltpu.SemaphoreType.DMA((2,)),
            pltpu.SemaphoreType.DMA((6,)),
            pltpu.SemaphoreType.REGULAR((3,)),
        ],
        compiler_params=pltpu.CompilerParams(collective_id=0, has_side_effects=True),
        name="channel_step",
    )(
        velocity_old,
        heights,
        owner_device.reshape(1, -1),
        owner_element.reshape(1, -1),
        ref_coords,
        roughness.reshape(1, -1),
        constants,
        flat,
        lines,
    )
    return pl.pallas_call(
        combine,
        out_shape=(
            jax.ShapeDtypeStruct((3, 16, 16, 128), f32),
            jax.ShapeDtypeStruct((2, 512), f32),
        ),
        in_specs=[vmem] * 5,
        out_specs=(anywhere, anywhere),
        scratch_shapes=[
            pltpu.VMEM((3, 16, 16, 128), f32),
            pltpu.SemaphoreType.DMA((4,)),
        ],
        name="combine",
    )(
        *(
            pltpu.with_memory_space_constraint(value, pltpu.VMEM)
            for value in (res, one, two, scalars, slopes)
        )
    )


def torus_program(torus):
    sizes = tuple(torus.shape[name] for name in AXES)
    return jax.shard_map(
        functools.partial(body, sizes),
        mesh=torus,
        in_specs=(
            P(None, WALL, "span", None),
            P(),
            P(WALL_SPAN, None),
            P(WALL_SPAN, None),
            P(None, WALL_SPAN),
            P(WALL_SPAN),
        ),
        out_specs=(P(None, WALL, "span", None), P(None, WALL_SPAN)),
        check_vma=False,
    )


def solution(mesh):
    return torus_program(Mesh(mesh.devices.reshape(4, 8, 2, mesh.shape["span"]), AXES))
```

```python
import functools

import jax
import jax.numpy as jnp
import numpy as np
from jax import lax
from jax.experimental import pallas as pl
from jax.experimental.pallas import tpu as pltpu
from jax.sharding import Mesh
from jax.sharding import PartitionSpec as P

AXES = ("wall_0", "wall_1", "wall_2", "span")
WALL_SPAN = AXES
WALL = ("wall_0", "wall_1", "wall_2")
MESH_ID = pl.DeviceIdType.MESH

GLL_NODES = (
    -1.0,
    -0.8717401485096066,
    -0.5917001814331423,
    -0.2092992179024789,
    0.2092992179024789,
    0.5917001814331423,
    0.8717401485096066,
    1.0,
)
GLL_WEIGHTS = (
    0.03571428571428571,
    0.2107042271435061,
    0.3411226924835044,
    0.4124587946587038,
    0.4124587946587038,
    0.3411226924835044,
    0.2107042271435061,
    0.03571428571428571,
)
viscosity = 0.02
inverse_step = 20.0
karman = 0.41
sample_height = 0.1
speed_floor = 0.01
element_dx = 0.05
element_dz = 0.13
precise = lax.Precision.HIGHEST

SCALE = 64.0

SHIFTS = ((1, 0), (-1, 0), (0, 1), (0, -1), (1, 1), (1, -1), (-1, 1), (-1, -1))

FAR_SHIFTS = (
    (2, 0), (2, 1), (2, -1), (-2, 0), (-2, 1), (-2, -1),
    (0, 2), (1, 2), (-1, 2), (0, -2), (1, -2), (-1, -2),
)

MZ, QMZ, COUNT, LAG, PLANE, HALFW, LAST, FIRST, LANEX, LANEZ = range(10)
BLOCK, LIFT, FLAT = 10, 26, 30


def stiffness_table():
    points = np.array(GLL_NODES)
    weights = np.array(GLL_WEIGHTS)
    previous = np.ones(8)
    current = points.copy()
    for degree in range(1, 7):
        previous, current = (
            current,
            ((2 * degree + 1) * points * current - degree * previous) / (degree + 1),
        )
    derivative = np.zeros((8, 8))
    for target in range(8):
        for source in range(8):
            if target != source:
                derivative[target, source] = (
                    current[target] / current[source] / (points[target] - points[source])
                )
    derivative[0, 0] = -14.0
    derivative[7, 7] = 14.0
    return derivative.T @ (weights[:, None] * derivative)


def tables():
    weights = np.array(GLL_WEIGHTS)
    points = np.array(GLL_NODES)
    stiffness = stiffness_table()
    ones = np.ones((8, 128))
    lane = np.arange(128)
    ends = np.array([2.0, 1, 1, 1, 1, 1, 1, 2.0])
    mass_x = 0.5 * element_dx * weights
    mass_z = 0.5 * element_dz * weights
    count_y = np.where((lane % 8 == 0) | (lane % 8 == 7), 0.5, 1.0)
    count_y[0] = count_y[127] = 1.0
    gaps = points[:, None] - points[None, :] + np.eye(8)
    rows = [
        mass_z[:, None] * ones,
        (mass_z * ends)[:, None] * ones,
        (1.0 / ends)[:, None] * count_y[None, :],
        (1.0 / np.prod(gaps, axis=1))[:, None] * ones,
        ones * (mass_x[lane // 16] * mass_z[lane % 8])[None, :],
        ones * (0.5 * weights[lane % 8])[None, :],
        ones * ((lane % 8 == 7) & (lane < 127))[None, :],
        ones * ((lane % 8 == 0) & (lane > 0))[None, :],
    ]
    block = np.kron(np.eye(16), SCALE * viscosity * 2.0 * stiffness)
    lift = np.zeros((8, 512))
    for comp in range(2):
        for half in range(2):
            column = (comp * 2 + half) * 128
            lift[comp * 4 + half, column] = 1.0
            lift[comp * 4 + 2 + half, column + 127] = 1.0
    joined_x = np.tile(mass_x * ends, 2)
    joined_z = np.tile(mass_z * ends, 2)

    def chain(length):
        scaled = SCALE * viscosity * (2.0 / length) * stiffness
        full = np.kron(np.eye(2), scaled)
        ends_only = full[[15, 0]]
        full[7] = full[8] = full[7] + full[8]
        return full, ends_only

    chain_x, ends_x = chain(element_dx)
    chain_z, ends_z = chain(element_dz)
    flat = np.kron(chain_x, np.diag(joined_z)) + np.kron(np.diag(joined_x), chain_z)
    flat += SCALE * inverse_step * np.diag(np.kron(joined_x, joined_z))
    faces = [np.kron(ends_x[d : d + 1], np.diag(joined_z)) for d in range(2)]
    faces += [np.kron(np.diag(joined_x), ends_z[d : d + 1]) for d in range(2)]
    flat = np.concatenate([flat] + faces).astype(np.float32)
    flat_high = flat.astype(jnp.bfloat16)
    flat_low = (flat - flat_high.astype(np.float32)).astype(jnp.bfloat16)
    line_x = SCALE * viscosity * (2.0 / element_dx) * stiffness
    line_z = SCALE * viscosity * (2.0 / element_dz) * stiffness
    line = np.concatenate([np.kron(line_x.T, np.eye(16)), np.kron(np.eye(16), line_z.T)], axis=1)
    line_high = line.astype(np.float32).astype(jnp.bfloat16)
    line_low = (line.astype(np.float32) - line_high.astype(np.float32)).astype(jnp.bfloat16)
    lines = np.concatenate([line_high, line_high, line_low])
    rows += [
        ones * (mass_x * ends)[lane // 16][None, :],
        ones * (mass_z * ends)[lane % 8][None, :],
    ]
    pieces = [np.stack(rows), block.reshape(16, 8, 128), lift.reshape(8, 4, 128).transpose(1, 0, 2)]
    pieces += [joined_x[:, None, None] * (mass_z * ends)[None, :, None] * np.ones((16, 8, 128))]
    return np.concatenate(pieces).astype(np.float32), np.stack([flat_high, flat_low]), lines


def kernel(sizes, *refs):
    operands, refs = refs[:9], refs[9:]
    (res, one, two, scalars, neumann), refs = refs[:5], refs[5:]
    local, refs = refs[:9], refs[9:]
    velocity, heights, owner, element, coords, roughness, table, flat, lines = local
    (normal, lifting, lifting_two, right_high, right_low, slab, slab_in, plane, plane_in,
     verge, verge_in, face, face_in, mom, part, part_in,
     load, send, slab_recv, recv, ready) = refs
    nx, ny, nc, ns = sizes
    nw = nx * ny * nc
    loads = [
        pltpu.make_async_copy(source, target, load.at[n])
        for n, (source, target) in enumerate(zip(operands, local))
    ]
    for copy in loads:
        copy.start()
    wx, wy, wc, sp = (lax.axis_index(name) for name in AXES)
    wall = (wx * ny + wy) * nc + wc
    weights = np.array(GLL_WEIGHTS)
    stiffness = stiffness_table()
    mass_x = [float(v) for v in 0.5 * element_dx * weights]
    ends = [2.0, 1.0, 1.0, 1.0, 1.0, 1.0, 1.0, 2.0]

    def ring(value, shift, count):
        if shift > 0:
            return jnp.where(value >= count - shift, value + shift - count, value + shift)
        return jnp.where(value < -shift, value + shift + count, value + shift)

    def beside(dw):
        if dw == 0:
            return wx, wy, wc
        sign = 1 if dw > 0 else -1
        if abs(dw) == 2:
            turn_y = wy == (ny - 1 if dw > 0 else 0)
            return jnp.where(turn_y, ring(wx, sign, nx), wx), ring(wy, sign, ny), wc
        turn = wc == (nc - 1 if dw > 0 else 0)
        turn_y = jnp.logical_and(turn, wy == (ny - 1 if dw > 0 else 0))
        return (
            jnp.where(turn_y, ring(wx, dw, nx), wx),
            jnp.where(turn, ring(wy, dw, ny), wy),
            ring(wc, dw, nc),
        )

    along = {dw: beside(dw) for dw in (-2, -1, 0, 1, 2)}
    across = {k: ring(sp, k, ns) if k else sp for k in (-2, -1, 0, 1, 2)}
    neighbours = [(*along[dw], across[ds]) for dw, ds in SHIFTS]
    distant = [(*along[dw], across[ds]) for dw, ds in FAR_SHIFTS]
    place_x = {0: wx, 1: ring(wx, 1, nx), -1: ring(wx, -1, nx), 2: ring(wx, 2, nx)}
    place_y = {k: ring(wy, k, ny) if k else wy for k in range(-(ny // 2) + 1, ny // 2 + 1)}
    place_y[-2] = ring(wy, -2, ny)
    place_z = {k: ring(sp, k, ns) if k else sp for k in range(-(ns // 2) + 1, ns // 2 + 1)}
    place_z[-2] = ring(sp, -2, ns)
    other = ring(wc, 1, nc)
    flat_peer = lambda dx, dy: (place_x[dx], place_y[dy], wc, sp)
    deep_peer = lambda c, ds: (wx, wy, c, place_z[ds])

    def far_first(keys):
        return sorted(keys, key=lambda key: -abs(key[0]) - abs(key[1]))

    deep_shifts = range(-(ns // 2) + 1, ns // 2 + 1)
    wide_x = [k for k in (-1, 0, 1, 2) if -(nx // 2) < k <= nx // 2]
    plain = far_first([(a, b) for a in wide_x for b in range(-(ny // 2) + 1, ny // 2 + 1)])
    plain = [key for key in plain if key != (0, 0)]

    barrier = pltpu.get_barrier_semaphore()
    near = neighbours[:4] + [deep_peer(other, 0)]
    near += [(*along[2], sp), (*along[-2], sp), (*along[0], across[2]), (*along[0], across[-2])]
    near += [flat_peer(1, 0), flat_peer(-1, 0), flat_peer(0, 1), flat_peer(0, -1)]
    for peer in near:
        pl.semaphore_signal(barrier, inc=1, device_id=peer, device_id_type=MESH_ID)
    relays = [
        near,
        [flat_peer(1, 0), flat_peer(-1, 0), flat_peer(0, 2), flat_peer(0, -2)]
        + [deep_peer(wc, 2), deep_peer(wc, -2)],
        [flat_peer(1, 0), flat_peer(-1, 0), flat_peer(0, 2), flat_peer(0, -2)]
        + [flat_peer(2, 2), flat_peer(2, -2), deep_peer(wc, 4), deep_peer(wc, -4)],
    ]

    def tell(n):
        for peer in relays[n]:
            pl.semaphore_signal(ready.at[n], inc=1, device_id=peer, device_id_type=MESH_ID)

    def hear(n):
        pl.semaphore_wait(ready.at[n], len(relays[n]))

    def push(source, target, send_sem, recv_sem, peer):
        pltpu.make_async_remote_copy(
            src_ref=source,
            dst_ref=target,
            send_sem=send_sem,
            recv_sem=recv_sem,
            device_id=peer,
            device_id_type=MESH_ID,
        ).start()

    def wait_bytes(like, sem):
        pltpu.make_async_copy(like, like, sem).wait()

    loads[0].wait()

    lane = lax.broadcasted_iota(jnp.int32, (1, 128), 1)
    sub8 = lax.broadcasted_iota(jnp.int32, (8, 128), 0)
    lane8 = lax.broadcasted_iota(jnp.int32, (8, 128), 1)

    for comp in range(2):
        quarters = []
        for k in range(4):
            quarters.append(velocity[2 * comp, 4 * k : 4 * k + 4].reshape(64, 128))
        packed = jnp.zeros((64, 128), jnp.float32)
        where_to = lax.broadcasted_iota(jnp.int32, (64, 128), 1)
        for k in range(4):
            low = pltpu.roll(quarters[k], 32 * k, 1) if k else quarters[k]
            shift = (32 * k + 32) % 128
            high = pltpu.roll(quarters[k], shift, 1) if shift else quarters[k]
            packed = jnp.where(where_to // 16 == 2 * k, low, packed)
            packed = jnp.where(where_to // 16 == 2 * k + 1, high, packed)
        slab[comp] = packed.reshape(4, 16, 128)

    pl.semaphore_wait(barrier, len(near))

    tell(0)
    for d in range(2):
        push(slab, slab_in.at[d], send.at[0], slab_recv.at[d], neighbours[d])

    for copy in loads[1:]:
        copy.wait()
    height = jnp.zeros((8, 128), jnp.float32)
    for layer in range(16):
        height = jnp.where(lane8 // 8 == layer, heights[layer], height)
    mass_y = height * table[HALFW]
    block = table[BLOCK : BLOCK + 16].reshape(128, 128) * (1.0 / height)[:1]
    block = (
        block
        + table[LAST][:1] * pltpu.roll(block, 127, 1)
        + table[FIRST][:1] * pltpu.roll(block, 1, 1)
    )

    def split(value):
        high = value.astype(jnp.bfloat16)
        return high, (value - high.astype(jnp.float32)).astype(jnp.bfloat16)

    block_high, block_low = split(block)
    normal[:128, :128] = block_high
    normal[128:, :128] = block_high
    normal[:128, 128:] = block_low
    normal[128:, 128:] = jnp.zeros((128, 128), jnp.bfloat16)
    right_high[...] = jnp.zeros(right_high.shape, jnp.bfloat16)
    right_low[...] = jnp.zeros(right_low.shape, jnp.bfloat16)
    side = sub8 // 2 % 2
    wall_row = jnp.where(side == 0, block[:1], block[127:])
    lift = jnp.concatenate([table[LIFT + k] for k in range(4)], axis=1)
    home = (sub8 // 4 * 2 + sub8 % 2)[:, :1]
    joined_y = (
        mass_y
        + table[LAST] * pltpu.roll(mass_y, 127, 1)
        + table[FIRST] * pltpu.roll(mass_y, 1, 1)
    )
    both = lambda value: jnp.concatenate([value, value], axis=0)
    joined_y2 = both(joined_y)
    count2 = both(table[COUNT])

    def at_home(value):
        return jnp.concatenate([jnp.where(home == k, value, 0.0) for k in range(4)], axis=1)

    def coarse(value):
        return value.astype(jnp.bfloat16).astype(jnp.float32)

    twice = jnp.dot(wall_row, block, precision=precise, preferred_element_type=jnp.float32)
    pieces, pieces_two = [lift, lift], [lift, lift]
    for n, value in enumerate((wall_row, joined_y * wall_row, wall_row, twice)):
        rises = at_home(value)
        high = coarse(rises)
        triple = [high, high, rises - high]
        if n == 0:
            pieces += triple
        else:
            pieces_two += triple
    for n, value in enumerate(pieces):
        lifting[8 * n : 8 * n + 8] = value
    lifting[40:] = jnp.zeros((8, 512), jnp.float32)
    for n, value in enumerate(pieces_two):
        lifting_two[8 * n : 8 * n + 8] = value
    lifting_two[88:] = jnp.zeros((8, 512), jnp.float32)
    wall_mass = jnp.where(side == 0, joined_y[:, :1], joined_y[:, 127:])
    scale_zy = both(table[QMZ] * joined_y) * inverse_step
    for comp in range(3):
        for i in range(16):
            res[comp, 16 * i : 16 * i + 16] = velocity[comp, i] * (
                scale_zy * (mass_x[i % 8] * ends[i % 8])
            )

    row16 = lax.broadcasted_iota(jnp.int32, (16, 128), 0) % 8
    share_x = jnp.where(jnp.logical_or(row16 == 0, row16 == 7), 0.5, 1.0)
    half_y = jnp.broadcast_to(table[COUNT][:1], (8, 128))

    def fold(value):
        return value[:8] + value[8:]

    def apply(source, comp):
        high, low = split(source[comp])
        parts = jnp.concatenate([high, low], axis=1)
        along = jnp.dot(flat[0], parts, preferred_element_type=jnp.float32)
        along = along[:, :128] + along[:, 128:]
        along = along + jnp.dot(flat[1], high, preferred_element_type=jnp.float32)
        across_y = jnp.dot(parts, normal[...], preferred_element_type=jnp.float32)
        return along, across_y[:, :128] + across_y[:, 128:]

    def operate(source, target, turn):
        for comp in range(3):
            along, across_y = apply(source, comp)
            for d in range(4):
                rows = slice(256 + 16 * d, 272 + 16 * d)
                face[turn, d, comp] = along[rows] * joined_y2
                push(
                    face.at[turn, d, comp], face_in.at[turn, d, comp], send.at[2 + turn],
                    recv.at[1 + turn], neighbours[d],
                )
            for i in range(16):
                rows = slice(16 * i, 16 * i + 16)
                target[comp, rows] = along[rows] * joined_y2 + across_y[rows] * both(
                    table[FLAT + i]
                )

    operate(res, one, 0)
    def regroup(blocks):
        upper = (lane // 8) % 2 == 1
        result = []
        for ex in range(2):
            low, high = blocks[ex], blocks[2 + ex]
            result.append(jnp.where(upper, pltpu.roll(high, 8, 1), low))
            result.append(jnp.where(upper, high, pltpu.roll(low, 120, 1)))
        return result

    def ungroup(values):
        upper = (lane // 8) % 2 == 1
        low, high = [], []
        for ex in range(2):
            a, b = values[2 * ex], values[2 * ex + 1]
            low.append(jnp.where(upper, pltpu.roll(b, 8, 1), a))
            high.append(jnp.where(upper, b, pltpu.roll(a, 120, 1)))
        return low + high

    wide = lambda row: jnp.broadcast_to(row, (8, 128))
    quarter = lambda ref, row, q: ref[row : row + 1, 128 * q : 128 * q + 128]
    distance = [(quarter(owner, 0, q) - wall + nw) % nw for q in range(4)]
    to_next = regroup([wide(jnp.where(d == 1, 1.0, 0.0)) for d in distance])
    to_prev = regroup([wide(jnp.where(d == nw - 1, 1.0, 0.0)) for d in distance])
    layer = regroup([wide((quarter(element, 0, q) % 2).astype(jnp.float32)) for q in range(4)])
    axes = [regroup([wide(quarter(coords, k, q)) for q in range(4)]) for k in range(3)]

    def lagrange(coord):
        value = table[LAG]
        for b in range(8):
            value = value * jnp.where(sub8 == b, 1.0, coord - GLL_NODES[b])
        return value

    basis = [[lagrange(axes[k][g]) for k in range(3)] for g in range(4)]
    second_wall = (lane // 8) % 2 == 1
    for g in range(4):
        ly = basis[g][2]
        blocks = []
        for side in range(2):
            for ey in range(2):
                chosen = jnp.logical_and(
                    wide(second_wall) == (side == 1), layer[g] == float(ey)
                )
                blocks.append(jnp.where(chosen, ly, 0.0))
        high, low = split(jnp.concatenate(blocks, axis=0))
        for kk in range(2):
            k = 2 * (g // 2) + kk
            column = slice(128 * kk, 128 * kk + 128)
            right_high[g, 32 * k : 32 * k + 32, column] = high
            right_high[g, 128 + 32 * k : 160 + 32 * k, column] = high
            right_low[g, 32 * k : 32 * k + 32, column] = low

    masks = [[1.0 - to_next[g] - to_prev[g], to_prev[g], to_next[g]] for g in range(4)]

    def sample(source, g):
        ez = g % 2
        high, low = split(source[:, :, 8 * ez : 8 * ez + 8, :].reshape(64, 128))
        product = jnp.dot(
            jnp.concatenate([high, low], axis=1), right_high[g],
            preferred_element_type=jnp.float32,
        ) + jnp.dot(high, right_low[g], preferred_element_type=jnp.float32)
        total = [jnp.zeros((8, 128), jnp.float32) for _ in range(2)]
        for kk in range(2):
            values = product[:, 128 * kk : 128 * kk + 128].reshape(2, 4, 8, 128)
            for comp in range(2):
                for x in range(4):
                    a = 4 * kk + x
                    total[comp] = total[comp] + values[comp, x] * basis[g][0][a : a + 1]
        return total

    sums = []
    for g in range(4):
        own = sample(slab, g)
        sums.append([own[comp] * masks[g][0] for comp in range(2)])
    for d in range(2):
        wait_bytes(slab_in.at[d], slab_recv.at[d])
        for g in range(4):
            far = sample(slab_in.at[d], g)
            for comp in range(2):
                sums[g][comp] = sums[g][comp] + far[comp] * masks[g][1 + d]
    stream = ungroup(
        [wide(jnp.sum(sums[g][0] * basis[g][1], axis=0, keepdims=True)) for g in range(4)]
    )
    spanwise = ungroup(
        [wide(jnp.sum(sums[g][1] * basis[g][1], axis=0, keepdims=True)) for g in range(4)]
    )

    for q in range(4):
        u, v = stream[q], spanwise[q]
        speed = jnp.sqrt(u * u + v * v + speed_floor)
        ratio = karman / jnp.log(sample_height / wide(quarter(roughness, 0, q)))
        factor = -(ratio * ratio * speed / viscosity)
        for comp, value in enumerate((u, v)):
            slope = factor * value
            neumann[comp : comp + 1, 128 * q : 128 * q + 128] = slope[:1]
            plane[comp * 4 + q : comp * 4 + q + 1, :] = (viscosity * slope * table[PLANE])[:1]

    mine = plane[...]
    lines_x = jnp.zeros((8, 128), jnp.float32)
    for q in range(4):
        here = jnp.logical_and(sub8 == 2 * q + 1, lane8 // 16 == 3 - q)
        lines_x = jnp.where(here, pltpu.roll(mine, (16 * (3 - q) - 112) % 128, 1), lines_x)
        here = jnp.logical_and(sub8 == 2 * q, lane8 // 16 == 7 - q)
        lines_x = jnp.where(here, pltpu.roll(mine, (64 + 16 * (3 - q)) % 128, 1), lines_x)
    lines_z = jnp.zeros((8, 128), jnp.float32)
    for r in range(8):
        here = jnp.logical_and(sub8 == r, lane8 % 16 == 7 - r)
        lines_z = jnp.where(here, pltpu.roll(mine, (7 - r - 15) % 128, 1), lines_z)
        here = jnp.logical_and(sub8 == r, lane8 % 16 == 15 - r)
        lines_z = jnp.where(here, pltpu.roll(mine, (15 - r) % 128, 1), lines_z)
    verge[0] = jnp.sum(lines_x, axis=0, keepdims=True)
    verge[1] = jnp.sum(lines_z, axis=0, keepdims=True)
    hear(0)
    for d, (dw, ds) in enumerate(FAR_SHIFTS):
        push(
            verge.at[0 if abs(dw) == 2 else 1], verge_in.at[d], send.at[6], recv.at[5], distant[d]
        )
    for d in range(8):
        push(plane, plane_in.at[d], send.at[1], recv.at[0], neighbours[d])
    tell(1)

    node_z = lane8 % 16
    node_x = lane8 // 16
    half = sub8 % 2

    def join_span(mine, before, after):
        return (
            mine
            + jnp.where(node_z == 7, pltpu.roll(mine, 127, 1), 0.0)
            + jnp.where(node_z == 8, pltpu.roll(mine, 1, 1), 0.0)
            + jnp.where(node_z == 0, pltpu.roll(before, 113, 1), 0.0)
            + jnp.where(node_z == 15, pltpu.roll(after, 15, 1), 0.0)
        )

    def join_wall(mine, before, after):
        later = jnp.where(half == 0, pltpu.roll(mine, 7, 0), pltpu.roll(after, 1, 0))
        earlier = jnp.where(half == 0, pltpu.roll(before, 7, 0), pltpu.roll(mine, 1, 0))
        return (
            mine
            + jnp.where(node_x == 7, pltpu.roll(later, 112, 1), 0.0)
            + jnp.where(node_x == 0, pltpu.roll(earlier, 16, 1), 0.0)
        )

    def receive(target, turn):
        wait_bytes(face_in.at[turn], recv.at[1 + turn])
        into = (
            pl.ds(0, 16),
            pl.ds(240, 16),
            pl.ds(0, 16, stride=16),
            pl.ds(15, 16, stride=16),
        )
        for d in range(4):
            for comp in range(3):
                target[comp, into[d], :] = target[comp, into[d], :] + face_in[turn, d, comp]

    def note(k, value):
        mom[k : k + 1, :] = jnp.sum(value, axis=0, keepdims=True)

    def energy(source, index, comps):
        for comp in comps:
            along, across_y = apply(source, comp)
            inside = jnp.zeros((16, 128), jnp.float32)
            edges = jnp.zeros((16, 128), jnp.float32)
            for i in range(16):
                rows = slice(16 * i, 16 * i + 16)
                term = source[comp, rows] * (
                    along[rows] * joined_y2 + across_y[rows] * both(table[FLAT + i])
                )
                if i % 8 in (0, 7):
                    edges = edges + term
                else:
                    inside = inside + term
            for d, i in ((0, 15), (1, 0)):
                sent = along[256 + 16 * d : 272 + 16 * d] * joined_y2
                edges = edges + sent * source[comp, 16 * i : 16 * i + 16]
            total = fold((inside + 0.5 * edges) * count2)
            for d, first in ((2, 15), (3, 0)):
                sent = along[256 + 16 * d : 272 + 16 * d] * joined_y2
                term = sent * source[comp, pl.ds(first, 16, stride=16), :]
                total = total + fold(term * share_x) * half_y
            note(3 * index + comp, total)

    def weighted(pairs, comps):
        for comp in comps:
            totals = [jnp.zeros((16, 128), jnp.float32) for _ in pairs]
            edges = [jnp.zeros((16, 128), jnp.float32) for _ in pairs]
            for i in range(16):
                for n, (first, second, _) in enumerate(pairs):
                    term = (
                        first[comp, 16 * i : 16 * i + 16] * second[comp, 16 * i : 16 * i + 16]
                    )
                    if i % 8 in (0, 7):
                        edges[n] = edges[n] + term
                    else:
                        totals[n] = totals[n] + term
            for n, (_, _, index) in enumerate(pairs):
                note(3 * index + comp, fold((totals[n] + 0.5 * edges[n]) * count2))

    receive(one, 0)
    operate(one, two, 1)
    hear(1)
    tell(2)
    receive(two, 1)
    products = [(res, res, 0), (res, one, 1), (one, one, 2), (one, two, 3), (two, two, 4)]
    weighted(products, (1,))
    energy(two, 5, (1,))
    wait_bytes(plane_in, recv.at[0])
    wait_bytes(verge_in, recv.at[5])
    raw = {(-dw, -ds): plane_in[d] for d, (dw, ds) in enumerate(SHIFTS)}
    raw[0, 0] = plane[...]
    for d, (dw, ds) in enumerate(FAR_SHIFTS):
        row = wide(verge_in[d])
        if abs(dw) == 2:
            value = pltpu.roll(row, 56 if dw > 0 else 16, 1, stride=8, stride_axis=0)
        else:
            value = pltpu.roll(row, 8 if ds > 0 else 113, 1, stride=1, stride_axis=0)
        raw[-dw, -ds] = value
    none = jnp.zeros((8, 128), jnp.float32)
    square = [(dw, ds) for dw in (-1, 0, 1) for ds in (-1, 0, 1)]
    cross = [(0, 0), (-1, 0), (1, 0), (0, -1), (0, 1)]

    def spans(values, at):
        dw, ds = at
        return join_span(
            values[at], values.get((dw, ds - 1), none), values.get((dw, ds + 1), none)
        )

    def walls(values, at):
        dw, ds = at
        return join_wall(
            values[at], values.get((dw - 1, ds), none), values.get((dw + 1, ds), none)
        )

    def pulled(values):
        fill = [none] * (len(values) % 2)
        high, low = split(jnp.concatenate(list(values) + fill, axis=0))
        product = jnp.dot(
            jnp.concatenate([high, low, high], axis=1),
            lines[...],
            preferred_element_type=jnp.float32,
        )
        return [
            (product[8 * n : 8 * n + 8, :128], product[8 * n : 8 * n + 8, 128:])
            for n in range(len(values))
        ]

    mass_flat = table[LANEX] * table[LANEZ]

    def plane_operator(in_x, in_z, value, at):
        return (
            table[LANEZ] * walls(in_x, at)
            + table[LANEX] * spans(in_z, at)
            + (SCALE * inverse_step) * mass_flat * value
        )

    line_of = {at: spans(raw, at) for at in square + [(-2, 0), (2, 0)]}
    stress = {at: walls(line_of, at) for at in square}
    pulls = pulled([stress[at] for at in square])
    in_x = {at: pulls[n][0] for n, at in enumerate(square)}
    in_z = {at: pulls[n][1] for n, at in enumerate(square)}
    first = {at: plane_operator(in_x, in_z, stress[at], at) for at in cross}
    mass_of = {at: mass_flat * stress[at] for at in cross}
    pulls = pulled([first[at] for at in cross] + [mass_of[at] for at in cross])
    seconds = []
    for offset, values in ((0, first), (5, mass_of)):
        in_x = {at: pulls[offset + n][0] for n, at in enumerate(cross)}
        in_z = {at: pulls[offset + n][1] for n, at in enumerate(cross)}
        seconds.append(plane_operator(in_x, in_z, values[0, 0], (0, 0)))

    def raised(doubles, triples, rights, rows):
        parts = []
        for value in doubles:
            parts += [coarse(value), value - coarse(value)]
        for value in triples:
            parts += [coarse(value), value - coarse(value), coarse(value)]
        parts += [none] * (rows // 8 - len(parts))
        return lax.dot_general(
            jnp.concatenate(parts, axis=0),
            rights[:rows],
            (((0,), (0,)), ((), ())),
            preferred_element_type=jnp.float32,
        )

    here, pull, mass_here = stress[0, 0], first[0, 0] * wall_mass, mass_of[0, 0]
    lifted = raised([here], [], lifting, 16)
    lifted_one = raised([pull], [mass_here], lifting, 48)
    lifted_two = raised(
        [seconds[0] * wall_mass * wall_mass],
        [seconds[1], mass_flat * pull, mass_flat * mass_here],
        lifting_two,
        96,
    )
    for comp in range(2):
        for ex in range(2):
            column = (comp * 2 + ex) * 128
            rows = slice(128 * ex, 128 * ex + 128)
            for target, value in ((res, lifted), (one, lifted_one), (two, lifted_two)):
                target[2 * comp, rows] = target[2 * comp, rows] + value[:, column : column + 128]

    weighted(products, (0, 2))
    energy(two, 5, (0, 2))

    mom[18:24, :] = jnp.zeros((6, 128), jnp.float32)
    total = jnp.sum(mom[...], axis=1, keepdims=True)
    row = jnp.zeros((8, 128), jnp.float32)
    for k in range(3):
        row = row + jnp.where(lane8 == 8 * k + sub8, total[8 * k : 8 * k + 8], 0.0)
    part[0] = jnp.sum(row, axis=0, keepdims=True)
    hear(2)
    line_slots, plane_slots = nc * ns, nx * ny
    for ds in sorted(deep_shifts, key=lambda k: -abs(k)):
        if ds:
            push(
                part.at[0], part_in.at[wc * ns + sp], send.at[4], recv.at[3], deep_peer(1, ds)
            )
    relays_sums = wc == 1

    @pl.when(jnp.logical_not(relays_sums))
    def _():
        push(part.at[0], part_in.at[wc * ns + sp], send.at[4], recv.at[3], deep_peer(1, 0))
        wait_bytes(part_in.at[pl.ds(line_slots, plane_slots)], recv.at[4])
        wait_bytes(part_in.at[pl.ds(0, ns)], send.at[4])

    @pl.when(relays_sums)
    def _():
        part_in[wc * ns + sp] = part[0]
        wait_bytes(part_in.at[pl.ds(0, line_slots - 1)], recv.at[3])
        row = part_in[0]
        for k in range(1, line_slots):
            row = row + part_in[k]
        part[1] = row
        slot = line_slots + wx * ny + wy
        for a, b in plain:
            for c in (0, 1):
                push(
                    part.at[1], part_in.at[slot], send.at[5 if c else 7], recv.at[4],
                    (place_x[a], place_y[b], c, sp),
                )
        push(part.at[1], part_in.at[slot], send.at[7], recv.at[4], (wx, wy, 0, sp))
        part_in[slot] = row
        wait_bytes(part_in.at[pl.ds(line_slots, plane_slots - 1)], recv.at[4])
        wait_bytes(part_in.at[pl.ds(0, ns - 1)], send.at[4])
        wait_bytes(part_in.at[pl.ds(line_slots, plane_slots - 1)], send.at[5])
        wait_bytes(part_in.at[pl.ds(line_slots, plane_slots)], send.at[7])

    row = part_in[line_slots]
    for k in range(1, plane_slots):
        row = row + part_in[line_slots + k]

    row = jnp.broadcast_to(row, (8, 128))
    moments = [row if j == 0 else pltpu.roll(row, 128 - 3 * j, 1) for j in range(6)]

    def inner(first, second, raise_by):
        total = None
        for i, a in enumerate(first):
            for j, b in enumerate(second):
                term = a * b * moments[i + j + raise_by]
                total = term if total is None else total + term
        return total

    unit = jnp.ones((8, 128), jnp.float32)
    direction, residual = [unit], [unit]
    answer = [jnp.zeros((8, 128), jnp.float32)] * 3
    norm = moments[0]
    for step in range(3):
        alpha = norm / inner(direction, direction, 1)
        for i, value in enumerate(direction):
            answer[i] = answer[i] + alpha * value
        if step == 2:
            break
        lowered = [-alpha * value for value in direction]
        residual = [residual[0]] + [
            lowered[i] + residual[i + 1] if i + 1 < len(residual) else lowered[i]
            for i in range(len(lowered))
        ]
        newer = inner(residual, residual, 0)
        growth = newer / norm
        direction = [
            value + growth * direction[i] if i < len(direction) else value
            for i, value in enumerate(residual)
        ]
        norm = newer
    for i, value in enumerate(answer):
        scalars[i : i + 1, :] = value[:1] * SCALE
    wait_bytes(slab_in, send.at[0])
    wait_bytes(plane_in, send.at[1])
    wait_bytes(verge_in, send.at[6])
    for turn in range(2):
        wait_bytes(face_in.at[turn], send.at[2 + turn])


def combine(res, one, two, scalars, slopes, out, neumann, sums, sent):
    copies = [pltpu.make_async_copy(slopes, neumann, sent.at[3])]
    copies[0].start()
    for comp in range(3):
        c0, c1, c2 = (
            jnp.broadcast_to(scalars[k : k + 1, comp : comp + 1], (16, 128)) for k in range(3)
        )
        for i in range(16):
            rows = pl.ds(16 * i, 16)
            sums[comp, i] = (
                c0 * res[comp, rows, :] + c1 * one[comp, rows, :] + c2 * two[comp, rows, :]
            )
        copy = pltpu.make_async_copy(sums.at[comp], out.at[comp], sent.at[comp])
        copy.start()
        copies.append(copy)
    for copy in copies:
        copy.wait()


def body(sizes, velocity_old, heights, owner_device, owner_element, ref_coords, roughness):
    nx, ny, nc, ns = sizes
    slots = nc * ns + nx * ny
    f32, i32 = jnp.float32, jnp.int32
    vmem = pl.BlockSpec(memory_space=pltpu.VMEM)
    anywhere = pl.BlockSpec(memory_space=pl.ANY)
    constants, flat, lines = (jnp.asarray(value) for value in tables())
    res, one, two, scalars, slopes = pl.pallas_call(
        functools.partial(kernel, sizes),
        out_shape=(
            pltpu.VMEM((3, 256, 128), f32),
            pltpu.VMEM((3, 256, 128), f32),
            pltpu.VMEM((3, 256, 128), f32),
            pltpu.VMEM((8, 128), f32),
            pltpu.VMEM((2, 512), f32),
        ),
        in_specs=[anywhere] * 9,
        out_specs=(vmem,) * 5,
        scratch_shapes=[
            pltpu.VMEM((3, 16, 16, 128), f32),
            pltpu.SMEM((16,), f32),
            pltpu.VMEM((1, 512), i32),
            pltpu.VMEM((1, 512), i32),
            pltpu.VMEM((3, 512), f32),
            pltpu.VMEM((1, 512), f32),
            pltpu.VMEM(constants.shape, f32),
            pltpu.VMEM(flat.shape, jnp.bfloat16),
            pltpu.VMEM(lines.shape, jnp.bfloat16),
            pltpu.VMEM((256, 256), jnp.bfloat16),
            pltpu.VMEM((48, 512), f32),
            pltpu.VMEM((96, 512), f32),
            pltpu.VMEM((4, 256, 256), jnp.bfloat16),
            pltpu.VMEM((4, 128, 256), jnp.bfloat16),
            pltpu.VMEM((2, 4, 16, 128), f32),
            pltpu.VMEM((2, 2, 4, 16, 128), f32),
            pltpu.VMEM((8, 128), f32),
            pltpu.VMEM((8, 8, 128), f32),
            pltpu.VMEM((2, 1, 128), f32),
            pltpu.VMEM((12, 1, 128), f32),
            pltpu.VMEM((2, 4, 3, 16, 128), f32),
            pltpu.VMEM((2, 4, 3, 16, 128), f32),
            pltpu.VMEM((24, 128), f32),
            pltpu.VMEM((2, 1, 128), f32),
            pltpu.VMEM((slots, 1, 128), f32),
            pltpu.SemaphoreType.DMA((9,)),
            pltpu.SemaphoreType.DMA((8,)),
            pltpu.SemaphoreType.DMA((2,)),
            pltpu.SemaphoreType.DMA((6,)),
            pltpu.SemaphoreType.REGULAR((3,)),
        ],
        compiler_params=pltpu.CompilerParams(collective_id=0, has_side_effects=True),
        name="channel_step",
    )(
        velocity_old,
        heights,
        owner_device.reshape(1, -1),
        owner_element.reshape(1, -1),
        ref_coords,
        roughness.reshape(1, -1),
        constants,
        flat,
        lines,
    )
    return pl.pallas_call(
        combine,
        out_shape=(
            jax.ShapeDtypeStruct((3, 16, 16, 128), f32),
            jax.ShapeDtypeStruct((2, 512), f32),
        ),
        in_specs=[vmem] * 5,
        out_specs=(anywhere, anywhere),
        scratch_shapes=[
            pltpu.VMEM((3, 16, 16, 128), f32),
            pltpu.SemaphoreType.DMA((4,)),
        ],
        name="combine",
    )(
        *(
            pltpu.with_memory_space_constraint(value, pltpu.VMEM)
            for value in (res, one, two, scalars, slopes)
        )
    )


def torus_program(torus):
    sizes = tuple(torus.shape[name] for name in AXES)
    return jax.shard_map(
        functools.partial(body, sizes),
        mesh=torus,
        in_specs=(
            P(None, WALL, "span", None),
            P(),
            P(WALL_SPAN, None),
            P(WALL_SPAN, None),
            P(None, WALL_SPAN),
            P(WALL_SPAN),
        ),
        out_specs=(P(None, WALL, "span", None), P(None, WALL_SPAN)),
        check_vma=False,
    )


def solution(mesh):
    return torus_program(Mesh(mesh.devices.reshape(4, 8, 2, mesh.shape["span"]), AXES))
```

```python
import functools

import jax
import jax.numpy as jnp
import numpy as np
from jax import lax
from jax.experimental import pallas as pl
from jax.experimental.pallas import tpu as pltpu
from jax.sharding import Mesh
from jax.sharding import PartitionSpec as P

AXES = ("wall_0", "wall_1", "wall_2", "span")
WALL_SPAN = AXES
WALL = ("wall_0", "wall_1", "wall_2")
MESH_ID = pl.DeviceIdType.MESH

GLL_NODES = (
    -1.0,
    -0.8717401485096066,
    -0.5917001814331423,
    -0.2092992179024789,
    0.2092992179024789,
    0.5917001814331423,
    0.8717401485096066,
    1.0,
)
GLL_WEIGHTS = (
    0.03571428571428571,
    0.2107042271435061,
    0.3411226924835044,
    0.4124587946587038,
    0.4124587946587038,
    0.3411226924835044,
    0.2107042271435061,
    0.03571428571428571,
)
viscosity = 0.02
inverse_step = 20.0
karman = 0.41
sample_height = 0.1
speed_floor = 0.01
element_dx = 0.05
element_dz = 0.13
precise = lax.Precision.HIGHEST

SCALE = 64.0

SHIFTS = ((1, 0), (-1, 0), (0, 1), (0, -1), (1, 1), (1, -1), (-1, 1), (-1, -1))

FAR_SHIFTS = (
    (2, 0), (2, 1), (2, -1), (-2, 0), (-2, 1), (-2, -1),
    (0, 2), (1, 2), (-1, 2), (0, -2), (1, -2), (-1, -2),
)

MZ, QMZ, COUNT, LAG, PLANE, HALFW, LAST, FIRST, LANEX, LANEZ = range(10)
BLOCK, LIFT, FLAT = 10, 26, 30


def stiffness_table():
    points = np.array(GLL_NODES)
    weights = np.array(GLL_WEIGHTS)
    previous = np.ones(8)
    current = points.copy()
    for degree in range(1, 7):
        previous, current = (
            current,
            ((2 * degree + 1) * points * current - degree * previous) / (degree + 1),
        )
    derivative = np.zeros((8, 8))
    for target in range(8):
        for source in range(8):
            if target != source:
                derivative[target, source] = (
                    current[target] / current[source] / (points[target] - points[source])
                )
    derivative[0, 0] = -14.0
    derivative[7, 7] = 14.0
    return derivative.T @ (weights[:, None] * derivative)


def tables():
    weights = np.array(GLL_WEIGHTS)
    points = np.array(GLL_NODES)
    stiffness = stiffness_table()
    ones = np.ones((8, 128))
    lane = np.arange(128)
    ends = np.array([2.0, 1, 1, 1, 1, 1, 1, 2.0])
    mass_x = 0.5 * element_dx * weights
    mass_z = 0.5 * element_dz * weights
    count_y = np.where((lane % 8 == 0) | (lane % 8 == 7), 0.5, 1.0)
    count_y[0] = count_y[127] = 1.0
    gaps = points[:, None] - points[None, :] + np.eye(8)
    rows = [
        mass_z[:, None] * ones,
        (mass_z * ends)[:, None] * ones,
        (1.0 / ends)[:, None] * count_y[None, :],
        (1.0 / np.prod(gaps, axis=1))[:, None] * ones,
        ones * (mass_x[lane // 16] * mass_z[lane % 8])[None, :],
        ones * (0.5 * weights[lane % 8])[None, :],
        ones * ((lane % 8 == 7) & (lane < 127))[None, :],
        ones * ((lane % 8 == 0) & (lane > 0))[None, :],
    ]
    block = np.kron(np.eye(16), SCALE * viscosity * 2.0 * stiffness)
    lift = np.zeros((8, 512))
    for comp in range(2):
        for half in range(2):
            column = (comp * 2 + half) * 128
            lift[comp * 4 + half, column] = 1.0
            lift[comp * 4 + 2 + half, column + 127] = 1.0
    joined_x = np.tile(mass_x * ends, 2)
    joined_z = np.tile(mass_z * ends, 2)

    def chain(length):
        scaled = SCALE * viscosity * (2.0 / length) * stiffness
        full = np.kron(np.eye(2), scaled)
        ends_only = full[[15, 0]]
        full[7] = full[8] = full[7] + full[8]
        return full, ends_only

    chain_x, ends_x = chain(element_dx)
    chain_z, ends_z = chain(element_dz)
    flat = np.kron(chain_x, np.diag(joined_z)) + np.kron(np.diag(joined_x), chain_z)
    flat += SCALE * inverse_step * np.diag(np.kron(joined_x, joined_z))
    faces = [np.kron(ends_x[d : d + 1], np.diag(joined_z)) for d in range(2)]
    faces += [np.kron(np.diag(joined_x), ends_z[d : d + 1]) for d in range(2)]
    flat = np.concatenate([flat] + faces).astype(np.float32)
    flat_high = flat.astype(jnp.bfloat16)
    flat_low = (flat - flat_high.astype(np.float32)).astype(jnp.bfloat16)
    line_x = SCALE * viscosity * (2.0 / element_dx) * stiffness
    line_z = SCALE * viscosity * (2.0 / element_dz) * stiffness
    line = np.concatenate([np.kron(line_x.T, np.eye(16)), np.kron(np.eye(16), line_z.T)], axis=1)
    line_high = line.astype(np.float32).astype(jnp.bfloat16)
    line_low = (line.astype(np.float32) - line_high.astype(np.float32)).astype(jnp.bfloat16)
    lines = np.concatenate([line_high, line_low])
    rows += [
        ones * (mass_x * ends)[lane // 16][None, :],
        ones * (mass_z * ends)[lane % 8][None, :],
    ]
    pieces = [np.stack(rows), block.reshape(16, 8, 128), lift.reshape(8, 4, 128).transpose(1, 0, 2)]
    pieces += [joined_x[:, None, None] * (mass_z * ends)[None, :, None] * np.ones((16, 8, 128))]
    return np.concatenate(pieces).astype(np.float32), np.concatenate([flat_high, flat_low]), lines


def kernel(sizes, *refs):
    operands, refs = refs[:9], refs[9:]
    (res, one, two, scalars, neumann), refs = refs[:5], refs[5:]
    local, refs = refs[:9], refs[9:]
    velocity, heights, owner, element, coords, roughness, table, flat, lines = local
    (normal, lifting, lifting_two, right, slab, slab_in, plane, plane_in,
     verge, verge_in, face, face_in, mom, part, part_in,
     load, send, slab_recv, recv, ready) = refs
    nx, ny, nc, ns = sizes
    nw = nx * ny * nc
    loads = [
        pltpu.make_async_copy(source, target, load.at[n])
        for n, (source, target) in enumerate(zip(operands, local))
    ]
    for copy in loads:
        copy.start()
    wx, wy, wc, sp = (lax.axis_index(name) for name in AXES)
    wall = (wx * ny + wy) * nc + wc
    weights = np.array(GLL_WEIGHTS)
    stiffness = stiffness_table()
    mass_x = [float(v) for v in 0.5 * element_dx * weights]
    ends = [2.0, 1.0, 1.0, 1.0, 1.0, 1.0, 1.0, 2.0]

    def ring(value, shift, count):
        if shift > 0:
            return jnp.where(value >= count - shift, value + shift - count, value + shift)
        return jnp.where(value < -shift, value + shift + count, value + shift)

    def beside(dw):
        if dw == 0:
            return wx, wy, wc
        sign = 1 if dw > 0 else -1
        if abs(dw) == 2:
            turn_y = wy == (ny - 1 if dw > 0 else 0)
            return jnp.where(turn_y, ring(wx, sign, nx), wx), ring(wy, sign, ny), wc
        turn = wc == (nc - 1 if dw > 0 else 0)
        turn_y = jnp.logical_and(turn, wy == (ny - 1 if dw > 0 else 0))
        return (
            jnp.where(turn_y, ring(wx, dw, nx), wx),
            jnp.where(turn, ring(wy, dw, ny), wy),
            ring(wc, dw, nc),
        )

    along = {dw: beside(dw) for dw in (-2, -1, 0, 1, 2)}
    across = {k: ring(sp, k, ns) if k else sp for k in (-2, -1, 0, 1, 2)}
    neighbours = [(*along[dw], across[ds]) for dw, ds in SHIFTS]
    distant = [(*along[dw], across[ds]) for dw, ds in FAR_SHIFTS]
    place_x = {0: wx, 1: ring(wx, 1, nx), -1: ring(wx, -1, nx), 2: ring(wx, 2, nx)}
    place_y = {k: ring(wy, k, ny) if k else wy for k in range(-(ny // 2) + 1, ny // 2 + 1)}
    place_y[-2] = ring(wy, -2, ny)
    place_z = {k: ring(sp, k, ns) if k else sp for k in range(-(ns // 2) + 1, ns // 2 + 1)}
    place_z[-2] = ring(sp, -2, ns)
    other = ring(wc, 1, nc)
    flat_peer = lambda dx, dy: (place_x[dx], place_y[dy], wc, sp)
    deep_peer = lambda c, ds: (wx, wy, c, place_z[ds])

    def far_first(keys):
        return sorted(keys, key=lambda key: -abs(key[0]) - abs(key[1]))

    deep_shifts = range(-(ns // 2) + 1, ns // 2 + 1)
    wide_x = [k for k in (-1, 0, 1, 2) if -(nx // 2) < k <= nx // 2]
    plain = far_first([(a, b) for a in wide_x for b in range(-(ny // 2) + 1, ny // 2 + 1)])
    plain = [key for key in plain if key != (0, 0)]

    barrier = pltpu.get_barrier_semaphore()
    near = neighbours[:4] + [deep_peer(other, 0)]
    near += [(*along[2], sp), (*along[-2], sp), (*along[0], across[2]), (*along[0], across[-2])]
    near += [flat_peer(1, 0), flat_peer(-1, 0), flat_peer(0, 1), flat_peer(0, -1)]
    for peer in near:
        pl.semaphore_signal(barrier, inc=1, device_id=peer, device_id_type=MESH_ID)
    relays = [
        near,
        [flat_peer(1, 0), flat_peer(-1, 0), flat_peer(0, 2), flat_peer(0, -2)]
        + [deep_peer(wc, 2), deep_peer(wc, -2)],
        [flat_peer(1, 0), flat_peer(-1, 0), flat_peer(0, 2), flat_peer(0, -2)]
        + [flat_peer(2, 2), flat_peer(2, -2), deep_peer(wc, 4), deep_peer(wc, -4)],
    ]

    def tell(n):
        for peer in relays[n]:
            pl.semaphore_signal(ready.at[n], inc=1, device_id=peer, device_id_type=MESH_ID)

    def hear(n):
        pl.semaphore_wait(ready.at[n], len(relays[n]))

    def push(source, target, send_sem, recv_sem, peer):
        pltpu.make_async_remote_copy(
            src_ref=source,
            dst_ref=target,
            send_sem=send_sem,
            recv_sem=recv_sem,
            device_id=peer,
            device_id_type=MESH_ID,
        ).start()

    def wait_bytes(like, sem):
        pltpu.make_async_copy(like, like, sem).wait()

    loads[0].wait()

    lane = lax.broadcasted_iota(jnp.int32, (1, 128), 1)
    sub8 = lax.broadcasted_iota(jnp.int32, (8, 128), 0)
    lane8 = lax.broadcasted_iota(jnp.int32, (8, 128), 1)

    for comp in range(2):
        quarters = []
        for k in range(4):
            quarters.append(velocity[2 * comp, 4 * k : 4 * k + 4].reshape(64, 128))
        packed = jnp.zeros((64, 128), jnp.float32)
        where_to = lax.broadcasted_iota(jnp.int32, (64, 128), 1)
        for k in range(4):
            low = pltpu.roll(quarters[k], 32 * k, 1) if k else quarters[k]
            shift = (32 * k + 32) % 128
            high = pltpu.roll(quarters[k], shift, 1) if shift else quarters[k]
            packed = jnp.where(where_to // 16 == 2 * k, low, packed)
            packed = jnp.where(where_to // 16 == 2 * k + 1, high, packed)
        slab[comp] = packed.reshape(4, 16, 128)

    pl.semaphore_wait(barrier, len(near))

    tell(0)
    for d in range(2):
        push(slab, slab_in.at[d], send.at[0], slab_recv.at[d], neighbours[d])

    for copy in loads[1:]:
        copy.wait()
    height = jnp.zeros((8, 128), jnp.float32)
    for layer in range(16):
        height = jnp.where(lane8 // 8 == layer, heights[layer], height)
    mass_y = height * table[HALFW]
    block = table[BLOCK : BLOCK + 16].reshape(128, 128) * (1.0 / height)[:1]
    block = (
        block
        + table[LAST][:1] * pltpu.roll(block, 127, 1)
        + table[FIRST][:1] * pltpu.roll(block, 1, 1)
    )

    def split(value):
        high = value.astype(jnp.bfloat16)
        return high, (value - high.astype(jnp.float32)).astype(jnp.bfloat16)

    def split_product(left, right):
        rows = left.shape[0]
        high, low = split(left)
        product = jnp.dot(
            jnp.concatenate(
                [
                    jnp.concatenate([high, high], axis=1),
                    jnp.concatenate([low, jnp.zeros_like(low)], axis=1),
                ],
                axis=0,
            ),
            right,
            preferred_element_type=jnp.float32,
        )
        return product[:rows] + product[rows:]

    block_high, block_low = split(block)
    normal[:128, :128] = block_high
    normal[128:, :128] = block_high
    normal[:128, 128:] = block_low
    normal[128:, 128:] = jnp.zeros((128, 128), jnp.bfloat16)
    right[...] = jnp.zeros(right.shape, jnp.bfloat16)
    side = sub8 // 2 % 2
    wall_row = jnp.where(side == 0, block[:1], block[127:])
    lift = jnp.concatenate([table[LIFT + k] for k in range(4)], axis=1)
    home = (sub8 // 4 * 2 + sub8 % 2)[:, :1]
    joined_y = (
        mass_y
        + table[LAST] * pltpu.roll(mass_y, 127, 1)
        + table[FIRST] * pltpu.roll(mass_y, 1, 1)
    )
    both = lambda value: jnp.concatenate([value, value], axis=0)
    joined_y2 = both(joined_y)
    count2 = both(table[COUNT])

    def at_home(value):
        return jnp.concatenate([jnp.where(home == k, value, 0.0) for k in range(4)], axis=1)

    def coarse(value):
        return value.astype(jnp.bfloat16).astype(jnp.float32)

    twice = jnp.dot(wall_row, block, precision=precise, preferred_element_type=jnp.float32)
    pieces, pieces_two = [lift, lift], [lift, lift]
    for n, value in enumerate((wall_row, joined_y * wall_row, wall_row, twice)):
        rises = at_home(value)
        high = coarse(rises)
        triple = [high, high, rises - high]
        if n == 0:
            pieces += triple
        else:
            pieces_two += triple
    for n, value in enumerate(pieces):
        lifting[8 * n : 8 * n + 8] = value
    lifting[40:] = jnp.zeros((8, 512), jnp.float32)
    for n, value in enumerate(pieces_two):
        lifting_two[8 * n : 8 * n + 8] = value
    lifting_two[88:] = jnp.zeros((8, 512), jnp.float32)
    wall_mass = jnp.where(side == 0, joined_y[:, :1], joined_y[:, 127:])
    scale_zy = both(table[QMZ] * joined_y) * inverse_step
    for comp in range(3):
        for i in range(16):
            res[comp, 16 * i : 16 * i + 16] = velocity[comp, i] * (
                scale_zy * (mass_x[i % 8] * ends[i % 8])
            )

    row16 = lax.broadcasted_iota(jnp.int32, (16, 128), 0) % 8
    share_x = jnp.where(jnp.logical_or(row16 == 0, row16 == 7), 0.5, 1.0)
    half_y = jnp.broadcast_to(table[COUNT][:1], (8, 128))

    def fold(value):
        return value[:8] + value[8:]

    def apply(source, comp):
        high, low = split(source[comp])
        parts = jnp.concatenate([high, low], axis=1)
        product = jnp.dot(flat[...], parts, preferred_element_type=jnp.float32)
        along = product[:320, :128] + product[:320, 128:] + product[320:, :128]
        across_y = jnp.dot(parts, normal[...], preferred_element_type=jnp.float32)
        return along, across_y[:, :128] + across_y[:, 128:]

    def operate(source, target, turn):
        for comp in range(3):
            along, across_y = apply(source, comp)
            for d in range(4):
                rows = slice(256 + 16 * d, 272 + 16 * d)
                face[turn, d, comp] = along[rows] * joined_y2
                push(
                    face.at[turn, d, comp], face_in.at[turn, d, comp], send.at[2 + turn],
                    recv.at[1 + turn], neighbours[d],
                )
            for i in range(16):
                rows = slice(16 * i, 16 * i + 16)
                target[comp, rows] = along[rows] * joined_y2 + across_y[rows] * both(
                    table[FLAT + i]
                )

    operate(res, one, 0)
    def regroup(blocks):
        upper = (lane // 8) % 2 == 1
        result = []
        for ex in range(2):
            low, high = blocks[ex], blocks[2 + ex]
            result.append(jnp.where(upper, pltpu.roll(high, 8, 1), low))
            result.append(jnp.where(upper, high, pltpu.roll(low, 120, 1)))
        return result

    def ungroup(values):
        upper = (lane // 8) % 2 == 1
        low, high = [], []
        for ex in range(2):
            a, b = values[2 * ex], values[2 * ex + 1]
            low.append(jnp.where(upper, pltpu.roll(b, 8, 1), a))
            high.append(jnp.where(upper, b, pltpu.roll(a, 120, 1)))
        return low + high

    wide = lambda row: jnp.broadcast_to(row, (8, 128))
    quarter = lambda ref, row, q: ref[row : row + 1, 128 * q : 128 * q + 128]
    distance = [(quarter(owner, 0, q) - wall + nw) % nw for q in range(4)]
    to_next = regroup([wide(jnp.where(d == 1, 1.0, 0.0)) for d in distance])
    to_prev = regroup([wide(jnp.where(d == nw - 1, 1.0, 0.0)) for d in distance])
    layer = regroup([wide((quarter(element, 0, q) % 2).astype(jnp.float32)) for q in range(4)])
    axes = [regroup([wide(quarter(coords, k, q)) for q in range(4)]) for k in range(3)]

    def lagrange(coord):
        value = table[LAG]
        for b in range(8):
            value = value * jnp.where(sub8 == b, 1.0, coord - GLL_NODES[b])
        return value

    basis = [[lagrange(axes[k][g]) for k in range(3)] for g in range(4)]
    second_wall = (lane // 8) % 2 == 1
    for g in range(4):
        ly = basis[g][2]
        blocks = []
        for side in range(2):
            for ey in range(2):
                chosen = jnp.logical_and(
                    wide(second_wall) == (side == 1), layer[g] == float(ey)
                )
                blocks.append(jnp.where(chosen, ly, 0.0))
        high, low = split(jnp.concatenate(blocks, axis=0))
        for kk in range(2):
            k = 2 * (g // 2) + kk
            column = slice(128 * kk, 128 * kk + 128)
            right[g, 32 * k : 32 * k + 32, column] = high
            right[g, 128 + 32 * k : 160 + 32 * k, column] = low

    masks = [[1.0 - to_next[g] - to_prev[g], to_prev[g], to_next[g]] for g in range(4)]

    def sample(source, g):
        ez = g % 2
        product = split_product(
            source[:, :, 8 * ez : 8 * ez + 8, :].reshape(64, 128), right[g]
        )
        total = [jnp.zeros((8, 128), jnp.float32) for _ in range(2)]
        for kk in range(2):
            values = product[:, 128 * kk : 128 * kk + 128].reshape(2, 4, 8, 128)
            for comp in range(2):
                for x in range(4):
                    a = 4 * kk + x
                    total[comp] = total[comp] + values[comp, x] * basis[g][0][a : a + 1]
        return total

    sums = []
    for g in range(4):
        own = sample(slab, g)
        sums.append([own[comp] * masks[g][0] for comp in range(2)])
    for d in range(2):
        wait_bytes(slab_in.at[d], slab_recv.at[d])
        for g in range(4):
            far = sample(slab_in.at[d], g)
            for comp in range(2):
                sums[g][comp] = sums[g][comp] + far[comp] * masks[g][1 + d]
    stream = ungroup(
        [wide(jnp.sum(sums[g][0] * basis[g][1], axis=0, keepdims=True)) for g in range(4)]
    )
    spanwise = ungroup(
        [wide(jnp.sum(sums[g][1] * basis[g][1], axis=0, keepdims=True)) for g in range(4)]
    )

    for q in range(4):
        u, v = stream[q], spanwise[q]
        speed = jnp.sqrt(u * u + v * v + speed_floor)
        ratio = karman / jnp.log(sample_height / wide(quarter(roughness, 0, q)))
        factor = -(ratio * ratio * speed / viscosity)
        for comp, value in enumerate((u, v)):
            slope = factor * value
            neumann[comp : comp + 1, 128 * q : 128 * q + 128] = slope[:1]
            plane[comp * 4 + q : comp * 4 + q + 1, :] = (viscosity * slope * table[PLANE])[:1]

    mine = plane[...]
    lines_x = jnp.zeros((8, 128), jnp.float32)
    for q in range(4):
        here = jnp.logical_and(sub8 == 2 * q + 1, lane8 // 16 == 3 - q)
        lines_x = jnp.where(here, pltpu.roll(mine, (16 * (3 - q) - 112) % 128, 1), lines_x)
        here = jnp.logical_and(sub8 == 2 * q, lane8 // 16 == 7 - q)
        lines_x = jnp.where(here, pltpu.roll(mine, (64 + 16 * (3 - q)) % 128, 1), lines_x)
    lines_z = jnp.zeros((8, 128), jnp.float32)
    for r in range(8):
        here = jnp.logical_and(sub8 == r, lane8 % 16 == 7 - r)
        lines_z = jnp.where(here, pltpu.roll(mine, (7 - r - 15) % 128, 1), lines_z)
        here = jnp.logical_and(sub8 == r, lane8 % 16 == 15 - r)
        lines_z = jnp.where(here, pltpu.roll(mine, (15 - r) % 128, 1), lines_z)
    verge[0] = jnp.sum(lines_x, axis=0, keepdims=True)
    verge[1] = jnp.sum(lines_z, axis=0, keepdims=True)
    hear(0)
    for d, (dw, ds) in enumerate(FAR_SHIFTS):
        push(
            verge.at[0 if abs(dw) == 2 else 1], verge_in.at[d], send.at[6], recv.at[5], distant[d]
        )
    for d in range(8):
        push(plane, plane_in.at[d], send.at[1], recv.at[0], neighbours[d])
    tell(1)

    node_z = lane8 % 16
    node_x = lane8 // 16
    half = sub8 % 2

    def join_span(mine, before, after):
        return (
            mine
            + jnp.where(node_z == 7, pltpu.roll(mine, 127, 1), 0.0)
            + jnp.where(node_z == 8, pltpu.roll(mine, 1, 1), 0.0)
            + jnp.where(node_z == 0, pltpu.roll(before, 113, 1), 0.0)
            + jnp.where(node_z == 15, pltpu.roll(after, 15, 1), 0.0)
        )

    def join_wall(mine, before, after):
        later = jnp.where(half == 0, pltpu.roll(mine, 7, 0), pltpu.roll(after, 1, 0))
        earlier = jnp.where(half == 0, pltpu.roll(before, 7, 0), pltpu.roll(mine, 1, 0))
        return (
            mine
            + jnp.where(node_x == 7, pltpu.roll(later, 112, 1), 0.0)
            + jnp.where(node_x == 0, pltpu.roll(earlier, 16, 1), 0.0)
        )

    def receive(target, turn):
        wait_bytes(face_in.at[turn], recv.at[1 + turn])
        into = (
            pl.ds(0, 16),
            pl.ds(240, 16),
            pl.ds(0, 16, stride=16),
            pl.ds(15, 16, stride=16),
        )
        for d in range(4):
            for comp in range(3):
                target[comp, into[d], :] = target[comp, into[d], :] + face_in[turn, d, comp]

    def note(k, value):
        mom[k : k + 1, :] = jnp.sum(value, axis=0, keepdims=True)

    def energy(source, index, comps):
        for comp in comps:
            along, across_y = apply(source, comp)
            inside = jnp.zeros((16, 128), jnp.float32)
            edges = jnp.zeros((16, 128), jnp.float32)
            for i in range(16):
                rows = slice(16 * i, 16 * i + 16)
                term = source[comp, rows] * (
                    along[rows] * joined_y2 + across_y[rows] * both(table[FLAT + i])
                )
                if i % 8 in (0, 7):
                    edges = edges + term
                else:
                    inside = inside + term
            for d, i in ((0, 15), (1, 0)):
                sent = along[256 + 16 * d : 272 + 16 * d] * joined_y2
                edges = edges + sent * source[comp, 16 * i : 16 * i + 16]
            total = fold((inside + 0.5 * edges) * count2)
            for d, first in ((2, 15), (3, 0)):
                sent = along[256 + 16 * d : 272 + 16 * d] * joined_y2
                term = sent * source[comp, pl.ds(first, 16, stride=16), :]
                total = total + fold(term * share_x) * half_y
            note(3 * index + comp, total)

    def weighted(pairs, comps):
        for comp in comps:
            totals = [jnp.zeros((16, 128), jnp.float32) for _ in pairs]
            edges = [jnp.zeros((16, 128), jnp.float32) for _ in pairs]
            for i in range(16):
                for n, (first, second, _) in enumerate(pairs):
                    term = (
                        first[comp, 16 * i : 16 * i + 16] * second[comp, 16 * i : 16 * i + 16]
                    )
                    if i % 8 in (0, 7):
                        edges[n] = edges[n] + term
                    else:
                        totals[n] = totals[n] + term
            for n, (_, _, index) in enumerate(pairs):
                note(3 * index + comp, fold((totals[n] + 0.5 * edges[n]) * count2))

    receive(one, 0)
    operate(one, two, 1)
    hear(1)
    tell(2)
    receive(two, 1)
    products = [(res, res, 0), (res, one, 1), (one, one, 2), (one, two, 3), (two, two, 4)]
    weighted(products, (1,))
    energy(two, 5, (1,))
    wait_bytes(plane_in, recv.at[0])
    wait_bytes(verge_in, recv.at[5])
    raw = {(-dw, -ds): plane_in[d] for d, (dw, ds) in enumerate(SHIFTS)}
    raw[0, 0] = plane[...]
    for d, (dw, ds) in enumerate(FAR_SHIFTS):
        row = wide(verge_in[d])
        if abs(dw) == 2:
            value = pltpu.roll(row, 56 if dw > 0 else 16, 1, stride=8, stride_axis=0)
        else:
            value = pltpu.roll(row, 8 if ds > 0 else 113, 1, stride=1, stride_axis=0)
        raw[-dw, -ds] = value
    none = jnp.zeros((8, 128), jnp.float32)
    square = [(dw, ds) for dw in (-1, 0, 1) for ds in (-1, 0, 1)]
    cross = [(0, 0), (-1, 0), (1, 0), (0, -1), (0, 1)]

    def spans(values, at):
        dw, ds = at
        return join_span(
            values[at], values.get((dw, ds - 1), none), values.get((dw, ds + 1), none)
        )

    def walls(values, at):
        dw, ds = at
        return join_wall(
            values[at], values.get((dw - 1, ds), none), values.get((dw + 1, ds), none)
        )

    def pulled(values):
        fill = [none] * (len(values) % 2)
        product = split_product(jnp.concatenate(list(values) + fill, axis=0), lines[...])
        return [
            (product[8 * n : 8 * n + 8, :128], product[8 * n : 8 * n + 8, 128:])
            for n in range(len(values))
        ]

    mass_flat = table[LANEX] * table[LANEZ]

    def plane_operator(in_x, in_z, value, at):
        return (
            table[LANEZ] * walls(in_x, at)
            + table[LANEX] * spans(in_z, at)
            + (SCALE * inverse_step) * mass_flat * value
        )

    line_of = {at: spans(raw, at) for at in square + [(-2, 0), (2, 0)]}
    stress = {at: walls(line_of, at) for at in square}
    pulls = pulled([stress[at] for at in square])
    in_x = {at: pulls[n][0] for n, at in enumerate(square)}
    in_z = {at: pulls[n][1] for n, at in enumerate(square)}
    first = {at: plane_operator(in_x, in_z, stress[at], at) for at in cross}
    mass_of = {at: mass_flat * stress[at] for at in cross}
    pulls = pulled([first[at] for at in cross] + [mass_of[at] for at in cross])
    seconds = []
    for offset, values in ((0, first), (5, mass_of)):
        in_x = {at: pulls[offset + n][0] for n, at in enumerate(cross)}
        in_z = {at: pulls[offset + n][1] for n, at in enumerate(cross)}
        seconds.append(plane_operator(in_x, in_z, values[0, 0], (0, 0)))

    def raised(doubles, triples, rights, rows):
        parts = []
        for value in doubles:
            parts += [coarse(value), value - coarse(value)]
        for value in triples:
            parts += [coarse(value), value - coarse(value), coarse(value)]
        parts += [none] * (rows // 8 - len(parts))
        return lax.dot_general(
            jnp.concatenate(parts, axis=0),
            rights[:rows],
            (((0,), (0,)), ((), ())),
            preferred_element_type=jnp.float32,
        )

    here, pull, mass_here = stress[0, 0], first[0, 0] * wall_mass, mass_of[0, 0]
    lifted = raised([here], [], lifting, 16)
    lifted_one = raised([pull], [mass_here], lifting, 48)
    lifted_two = raised(
        [seconds[0] * wall_mass * wall_mass],
        [seconds[1], mass_flat * pull, mass_flat * mass_here],
        lifting_two,
        96,
    )
    for comp in range(2):
        for ex in range(2):
            column = (comp * 2 + ex) * 128
            rows = slice(128 * ex, 128 * ex + 128)
            for target, value in ((res, lifted), (one, lifted_one), (two, lifted_two)):
                target[2 * comp, rows] = target[2 * comp, rows] + value[:, column : column + 128]

    weighted(products, (0, 2))
    energy(two, 5, (0, 2))

    mom[18:24, :] = jnp.zeros((6, 128), jnp.float32)
    total = jnp.sum(mom[...], axis=1, keepdims=True)
    row = jnp.zeros((8, 128), jnp.float32)
    for k in range(3):
        row = row + jnp.where(lane8 == 8 * k + sub8, total[8 * k : 8 * k + 8], 0.0)
    part[0] = jnp.sum(row, axis=0, keepdims=True)
    hear(2)
    line_slots, plane_slots = nc * ns, nx * ny
    for ds in sorted(deep_shifts, key=lambda k: -abs(k)):
        if ds:
            push(
                part.at[0], part_in.at[wc * ns + sp], send.at[4], recv.at[3], deep_peer(1, ds)
            )
    relays_sums = wc == 1

    @pl.when(jnp.logical_not(relays_sums))
    def _():
        push(part.at[0], part_in.at[wc * ns + sp], send.at[4], recv.at[3], deep_peer(1, 0))
        wait_bytes(part_in.at[pl.ds(line_slots, plane_slots)], recv.at[4])
        wait_bytes(part_in.at[pl.ds(0, ns)], send.at[4])

    @pl.when(relays_sums)
    def _():
        part_in[wc * ns + sp] = part[0]
        wait_bytes(part_in.at[pl.ds(0, line_slots - 1)], recv.at[3])
        row = part_in[0]
        for k in range(1, line_slots):
            row = row + part_in[k]
        part[1] = row
        slot = line_slots + wx * ny + wy
        for a, b in plain:
            for c in (0, 1):
                push(
                    part.at[1], part_in.at[slot], send.at[5 if c else 7], recv.at[4],
                    (place_x[a], place_y[b], c, sp),
                )
        push(part.at[1], part_in.at[slot], send.at[7], recv.at[4], (wx, wy, 0, sp))
        part_in[slot] = row
        wait_bytes(part_in.at[pl.ds(line_slots, plane_slots - 1)], recv.at[4])
        wait_bytes(part_in.at[pl.ds(0, ns - 1)], send.at[4])
        wait_bytes(part_in.at[pl.ds(line_slots, plane_slots - 1)], send.at[5])
        wait_bytes(part_in.at[pl.ds(line_slots, plane_slots)], send.at[7])

    row = part_in[line_slots]
    for k in range(1, plane_slots):
        row = row + part_in[line_slots + k]

    row = jnp.broadcast_to(row, (8, 128))
    moments = [row if j == 0 else pltpu.roll(row, 128 - 3 * j, 1) for j in range(6)]

    def inner(first, second, raise_by):
        total = None
        for i, a in enumerate(first):
            for j, b in enumerate(second):
                term = a * b * moments[i + j + raise_by]
                total = term if total is None else total + term
        return total

    unit = jnp.ones((8, 128), jnp.float32)
    direction, residual = [unit], [unit]
    answer = [jnp.zeros((8, 128), jnp.float32)] * 3
    norm = moments[0]
    for step in range(3):
        alpha = norm / inner(direction, direction, 1)
        for i, value in enumerate(direction):
            answer[i] = answer[i] + alpha * value
        if step == 2:
            break
        lowered = [-alpha * value for value in direction]
        residual = [residual[0]] + [
            lowered[i] + residual[i + 1] if i + 1 < len(residual) else lowered[i]
            for i in range(len(lowered))
        ]
        newer = inner(residual, residual, 0)
        growth = newer / norm
        direction = [
            value + growth * direction[i] if i < len(direction) else value
            for i, value in enumerate(residual)
        ]
        norm = newer
    for i, value in enumerate(answer):
        scalars[i : i + 1, :] = value[:1] * SCALE
    wait_bytes(slab_in, send.at[0])
    wait_bytes(plane_in, send.at[1])
    wait_bytes(verge_in, send.at[6])
    for turn in range(2):
        wait_bytes(face_in.at[turn], send.at[2 + turn])


def combine(res, one, two, scalars, slopes, out, neumann, sums, sent):
    copies = [pltpu.make_async_copy(slopes, neumann, sent.at[3])]
    copies[0].start()
    for comp in range(3):
        c0, c1, c2 = (
            jnp.broadcast_to(scalars[k : k + 1, comp : comp + 1], (16, 128)) for k in range(3)
        )
        for i in range(16):
            rows = pl.ds(16 * i, 16)
            sums[comp, i] = (
                c0 * res[comp, rows, :] + c1 * one[comp, rows, :] + c2 * two[comp, rows, :]
            )
        copy = pltpu.make_async_copy(sums.at[comp], out.at[comp], sent.at[comp])
        copy.start()
        copies.append(copy)
    for copy in copies:
        copy.wait()


def body(sizes, velocity_old, heights, owner_device, owner_element, ref_coords, roughness):
    nx, ny, nc, ns = sizes
    slots = nc * ns + nx * ny
    f32, i32 = jnp.float32, jnp.int32
    vmem = pl.BlockSpec(memory_space=pltpu.VMEM)
    anywhere = pl.BlockSpec(memory_space=pl.ANY)
    constants, flat, lines = (jnp.asarray(value) for value in tables())
    res, one, two, scalars, slopes = pl.pallas_call(
        functools.partial(kernel, sizes),
        out_shape=(
            pltpu.VMEM((3, 256, 128), f32),
            pltpu.VMEM((3, 256, 128), f32),
            pltpu.VMEM((3, 256, 128), f32),
            pltpu.VMEM((8, 128), f32),
            pltpu.VMEM((2, 512), f32),
        ),
        in_specs=[anywhere] * 9,
        out_specs=(vmem,) * 5,
        scratch_shapes=[
            pltpu.VMEM((3, 16, 16, 128), f32),
            pltpu.SMEM((16,), f32),
            pltpu.VMEM((1, 512), i32),
            pltpu.VMEM((1, 512), i32),
            pltpu.VMEM((3, 512), f32),
            pltpu.VMEM((1, 512), f32),
            pltpu.VMEM(constants.shape, f32),
            pltpu.VMEM(flat.shape, jnp.bfloat16),
            pltpu.VMEM(lines.shape, jnp.bfloat16),
            pltpu.VMEM((256, 256), jnp.bfloat16),
            pltpu.VMEM((48, 512), f32),
            pltpu.VMEM((96, 512), f32),
            pltpu.VMEM((4, 256, 256), jnp.bfloat16),
            pltpu.VMEM((2, 4, 16, 128), f32),
            pltpu.VMEM((2, 2, 4, 16, 128), f32),
            pltpu.VMEM((8, 128), f32),
            pltpu.VMEM((8, 8, 128), f32),
            pltpu.VMEM((2, 1, 128), f32),
            pltpu.VMEM((12, 1, 128), f32),
            pltpu.VMEM((2, 4, 3, 16, 128), f32),
            pltpu.VMEM((2, 4, 3, 16, 128), f32),
            pltpu.VMEM((24, 128), f32),
            pltpu.VMEM((2, 1, 128), f32),
            pltpu.VMEM((slots, 1, 128), f32),
            pltpu.SemaphoreType.DMA((9,)),
            pltpu.SemaphoreType.DMA((8,)),
            pltpu.SemaphoreType.DMA((2,)),
            pltpu.SemaphoreType.DMA((6,)),
            pltpu.SemaphoreType.REGULAR((3,)),
        ],
        compiler_params=pltpu.CompilerParams(collective_id=0, has_side_effects=True),
        name="channel_step",
    )(
        velocity_old,
        heights,
        owner_device.reshape(1, -1),
        owner_element.reshape(1, -1),
        ref_coords,
        roughness.reshape(1, -1),
        constants,
        flat,
        lines,
    )
    return pl.pallas_call(
        combine,
        out_shape=(
            jax.ShapeDtypeStruct((3, 16, 16, 128), f32),
            jax.ShapeDtypeStruct((2, 512), f32),
        ),
        in_specs=[vmem] * 5,
        out_specs=(anywhere, anywhere),
        scratch_shapes=[
            pltpu.VMEM((3, 16, 16, 128), f32),
            pltpu.SemaphoreType.DMA((4,)),
        ],
        name="combine",
    )(
        *(
            pltpu.with_memory_space_constraint(value, pltpu.VMEM)
            for value in (res, one, two, scalars, slopes)
        )
    )


def torus_program(torus):
    sizes = tuple(torus.shape[name] for name in AXES)
    return jax.shard_map(
        functools.partial(body, sizes),
        mesh=torus,
        in_specs=(
            P(None, WALL, "span", None),
            P(),
            P(WALL_SPAN, None),
            P(WALL_SPAN, None),
            P(None, WALL_SPAN),
            P(WALL_SPAN),
        ),
        out_specs=(P(None, WALL, "span", None), P(None, WALL_SPAN)),
        check_vma=False,
    )


def solution(mesh):
    return torus_program(Mesh(mesh.devices.reshape(4, 8, 2, mesh.shape["span"]), AXES))
```

```python
import functools

import jax
import jax.numpy as jnp
import numpy as np
from jax import lax
from jax.experimental import pallas as pl
from jax.experimental.pallas import tpu as pltpu
from jax.sharding import Mesh
from jax.sharding import PartitionSpec as P

AXES = ("wall_0", "wall_1", "wall_2", "span")
WALL_SPAN = AXES
WALL = ("wall_0", "wall_1", "wall_2")
MESH_ID = pl.DeviceIdType.MESH

GLL_NODES = (
    -1.0,
    -0.8717401485096066,
    -0.5917001814331423,
    -0.2092992179024789,
    0.2092992179024789,
    0.5917001814331423,
    0.8717401485096066,
    1.0,
)
GLL_WEIGHTS = (
    0.03571428571428571,
    0.2107042271435061,
    0.3411226924835044,
    0.4124587946587038,
    0.4124587946587038,
    0.3411226924835044,
    0.2107042271435061,
    0.03571428571428571,
)
viscosity = 0.02
inverse_step = 20.0
karman = 0.41
sample_height = 0.1
speed_floor = 0.01
element_dx = 0.05
element_dz = 0.13
precise = lax.Precision.HIGHEST

SCALE = 64.0

SHIFTS = ((1, 0), (-1, 0), (0, 1), (0, -1), (1, 1), (1, -1), (-1, 1), (-1, -1))

FAR_SHIFTS = (
    (2, 0), (2, 1), (2, -1), (-2, 0), (-2, 1), (-2, -1),
    (0, 2), (1, 2), (-1, 2), (0, -2), (1, -2), (-1, -2),
)

MZ, QMZ, COUNT, LAG, PLANE, HALFW, LAST, FIRST, LANEX, LANEZ = range(10)
BLOCK, LIFT, FLAT = 10, 26, 30


def stiffness_table():
    points = np.array(GLL_NODES)
    weights = np.array(GLL_WEIGHTS)
    previous = np.ones(8)
    current = points.copy()
    for degree in range(1, 7):
        previous, current = (
            current,
            ((2 * degree + 1) * points * current - degree * previous) / (degree + 1),
        )
    derivative = np.zeros((8, 8))
    for target in range(8):
        for source in range(8):
            if target != source:
                derivative[target, source] = (
                    current[target] / current[source] / (points[target] - points[source])
                )
    derivative[0, 0] = -14.0
    derivative[7, 7] = 14.0
    return derivative.T @ (weights[:, None] * derivative)


def tables():
    weights = np.array(GLL_WEIGHTS)
    points = np.array(GLL_NODES)
    stiffness = stiffness_table()
    ones = np.ones((8, 128))
    lane = np.arange(128)
    ends = np.array([2.0, 1, 1, 1, 1, 1, 1, 2.0])
    mass_x = 0.5 * element_dx * weights
    mass_z = 0.5 * element_dz * weights
    count_y = np.where((lane % 8 == 0) | (lane % 8 == 7), 0.5, 1.0)
    count_y[0] = count_y[127] = 1.0
    gaps = points[:, None] - points[None, :] + np.eye(8)
    rows = [
        mass_z[:, None] * ones,
        (mass_z * ends)[:, None] * ones,
        (1.0 / ends)[:, None] * count_y[None, :],
        (1.0 / np.prod(gaps, axis=1))[:, None] * ones,
        ones * (mass_x[lane // 16] * mass_z[lane % 8])[None, :],
        ones * (0.5 * weights[lane % 8])[None, :],
        ones * ((lane % 8 == 7) & (lane < 127))[None, :],
        ones * ((lane % 8 == 0) & (lane > 0))[None, :],
    ]
    block = np.kron(np.eye(16), SCALE * viscosity * 2.0 * stiffness)
    lift = np.zeros((8, 512))
    for comp in range(2):
        for half in range(2):
            column = (comp * 2 + half) * 128
            lift[comp * 4 + half, column] = 1.0
            lift[comp * 4 + 2 + half, column + 127] = 1.0
    joined_x = np.tile(mass_x * ends, 2)
    joined_z = np.tile(mass_z * ends, 2)

    def chain(length):
        scaled = SCALE * viscosity * (2.0 / length) * stiffness
        full = np.kron(np.eye(2), scaled)
        ends_only = full[[15, 0]]
        full[7] = full[8] = full[7] + full[8]
        return full, ends_only

    chain_x, ends_x = chain(element_dx)
    chain_z, ends_z = chain(element_dz)
    flat = np.kron(chain_x, np.diag(joined_z)) + np.kron(np.diag(joined_x), chain_z)
    flat += SCALE * inverse_step * np.diag(np.kron(joined_x, joined_z))
    faces = [np.kron(ends_x[d : d + 1], np.diag(joined_z)) for d in range(2)]
    faces += [np.kron(np.diag(joined_x), ends_z[d : d + 1]) for d in range(2)]
    flat = np.concatenate([flat] + faces).astype(np.float32)
    flat_high = flat.astype(jnp.bfloat16)
    flat_low = (flat - flat_high.astype(np.float32)).astype(jnp.bfloat16)
    line_x = SCALE * viscosity * (2.0 / element_dx) * stiffness
    line_z = SCALE * viscosity * (2.0 / element_dz) * stiffness
    line = np.concatenate([np.kron(line_x.T, np.eye(16)), np.kron(np.eye(16), line_z.T)], axis=1)
    line_high = line.astype(np.float32).astype(jnp.bfloat16)
    line_low = (line.astype(np.float32) - line_high.astype(np.float32)).astype(jnp.bfloat16)
    lines = np.concatenate([line_high, line_low])
    rows += [
        ones * (mass_x * ends)[lane // 16][None, :],
        ones * (mass_z * ends)[lane % 8][None, :],
    ]
    pieces = [np.stack(rows), block.reshape(16, 8, 128), lift.reshape(8, 4, 128).transpose(1, 0, 2)]
    pieces += [joined_x[:, None, None] * (mass_z * ends)[None, :, None] * np.ones((16, 8, 128))]
    return np.concatenate(pieces).astype(np.float32), np.stack([flat_high, flat_low]), lines


def kernel(sizes, *refs):
    operands, refs = refs[:9], refs[9:]
    (res, one, two, scalars, neumann), refs = refs[:5], refs[5:]
    local, refs = refs[:9], refs[9:]
    velocity, heights, owner, element, coords, roughness, table, flat, lines = local
    (normal, lifting, lifting_two, right, slab, slab_in, plane, plane_in,
     verge, verge_in, face, face_in, mom, part, part_in,
     load, send, slab_recv, recv, ready) = refs
    nx, ny, nc, ns = sizes
    nw = nx * ny * nc
    loads = [
        pltpu.make_async_copy(source, target, load.at[n])
        for n, (source, target) in enumerate(zip(operands, local))
    ]
    for copy in loads:
        copy.start()
    wx, wy, wc, sp = (lax.axis_index(name) for name in AXES)
    wall = (wx * ny + wy) * nc + wc
    weights = np.array(GLL_WEIGHTS)
    stiffness = stiffness_table()
    mass_x = [float(v) for v in 0.5 * element_dx * weights]
    ends = [2.0, 1.0, 1.0, 1.0, 1.0, 1.0, 1.0, 2.0]

    def ring(value, shift, count):
        if shift > 0:
            return jnp.where(value >= count - shift, value + shift - count, value + shift)
        return jnp.where(value < -shift, value + shift + count, value + shift)

    def beside(dw):
        if dw == 0:
            return wx, wy, wc
        sign = 1 if dw > 0 else -1
        if abs(dw) == 2:
            turn_y = wy == (ny - 1 if dw > 0 else 0)
            return jnp.where(turn_y, ring(wx, sign, nx), wx), ring(wy, sign, ny), wc
        turn = wc == (nc - 1 if dw > 0 else 0)
        turn_y = jnp.logical_and(turn, wy == (ny - 1 if dw > 0 else 0))
        return (
            jnp.where(turn_y, ring(wx, dw, nx), wx),
            jnp.where(turn, ring(wy, dw, ny), wy),
            ring(wc, dw, nc),
        )

    along = {dw: beside(dw) for dw in (-2, -1, 0, 1, 2)}
    across = {k: ring(sp, k, ns) if k else sp for k in (-2, -1, 0, 1, 2)}
    neighbours = [(*along[dw], across[ds]) for dw, ds in SHIFTS]
    distant = [(*along[dw], across[ds]) for dw, ds in FAR_SHIFTS]
    place_x = {0: wx, 1: ring(wx, 1, nx), -1: ring(wx, -1, nx), 2: ring(wx, 2, nx)}
    place_y = {k: ring(wy, k, ny) if k else wy for k in range(-(ny // 2) + 1, ny // 2 + 1)}
    place_y[-2] = ring(wy, -2, ny)
    place_z = {k: ring(sp, k, ns) if k else sp for k in range(-(ns // 2) + 1, ns // 2 + 1)}
    place_z[-2] = ring(sp, -2, ns)
    other = ring(wc, 1, nc)
    flat_peer = lambda dx, dy: (place_x[dx], place_y[dy], wc, sp)
    deep_peer = lambda c, ds: (wx, wy, c, place_z[ds])

    def far_first(keys):
        return sorted(keys, key=lambda key: -abs(key[0]) - abs(key[1]))

    deep_shifts = range(-(ns // 2) + 1, ns // 2 + 1)
    wide_x = [k for k in (-1, 0, 1, 2) if -(nx // 2) < k <= nx // 2]
    plain = far_first([(a, b) for a in wide_x for b in range(-(ny // 2) + 1, ny // 2 + 1)])
    plain = [key for key in plain if key != (0, 0)]

    barrier = pltpu.get_barrier_semaphore()
    near = neighbours[:4] + [deep_peer(other, 0)]
    near += [(*along[2], sp), (*along[-2], sp), (*along[0], across[2]), (*along[0], across[-2])]
    near += [flat_peer(1, 0), flat_peer(-1, 0), flat_peer(0, 1), flat_peer(0, -1)]
    for peer in near:
        pl.semaphore_signal(barrier, inc=1, device_id=peer, device_id_type=MESH_ID)
    relays = [
        near,
        [flat_peer(1, 0), flat_peer(-1, 0), flat_peer(0, 2), flat_peer(0, -2)]
        + [deep_peer(wc, 2), deep_peer(wc, -2)],
        [flat_peer(1, 0), flat_peer(-1, 0), flat_peer(0, 2), flat_peer(0, -2)]
        + [flat_peer(2, 2), flat_peer(2, -2), deep_peer(wc, 4), deep_peer(wc, -4)],
    ]

    def tell(n):
        for peer in relays[n]:
            pl.semaphore_signal(ready.at[n], inc=1, device_id=peer, device_id_type=MESH_ID)

    def hear(n):
        pl.semaphore_wait(ready.at[n], len(relays[n]))

    def push(source, target, send_sem, recv_sem, peer):
        pltpu.make_async_remote_copy(
            src_ref=source,
            dst_ref=target,
            send_sem=send_sem,
            recv_sem=recv_sem,
            device_id=peer,
            device_id_type=MESH_ID,
        ).start()

    def wait_bytes(like, sem):
        pltpu.make_async_copy(like, like, sem).wait()

    loads[0].wait()

    lane = lax.broadcasted_iota(jnp.int32, (1, 128), 1)
    sub8 = lax.broadcasted_iota(jnp.int32, (8, 128), 0)
    lane8 = lax.broadcasted_iota(jnp.int32, (8, 128), 1)

    for comp in range(2):
        quarters = []
        for k in range(4):
            quarters.append(velocity[2 * comp, 4 * k : 4 * k + 4].reshape(64, 128))
        packed = jnp.zeros((64, 128), jnp.float32)
        where_to = lax.broadcasted_iota(jnp.int32, (64, 128), 1)
        for k in range(4):
            low = pltpu.roll(quarters[k], 32 * k, 1) if k else quarters[k]
            shift = (32 * k + 32) % 128
            high = pltpu.roll(quarters[k], shift, 1) if shift else quarters[k]
            packed = jnp.where(where_to // 16 == 2 * k, low, packed)
            packed = jnp.where(where_to // 16 == 2 * k + 1, high, packed)
        slab[comp] = packed.reshape(4, 16, 128)

    for copy in loads[1:]:
        copy.wait()
    height = jnp.zeros((8, 128), jnp.float32)
    for layer in range(16):
        height = jnp.where(lane8 // 8 == layer, heights[layer], height)
    mass_y = height * table[HALFW]
    block = table[BLOCK : BLOCK + 16].reshape(128, 128) * (1.0 / height)[:1]
    block = (
        block
        + table[LAST][:1] * pltpu.roll(block, 127, 1)
        + table[FIRST][:1] * pltpu.roll(block, 1, 1)
    )

    def split(value):
        high = value.astype(jnp.bfloat16)
        return high, (value - high.astype(jnp.float32)).astype(jnp.bfloat16)

    def split_product(left, right):
        rows = left.shape[0]
        high, low = split(left)
        product = jnp.dot(
            jnp.concatenate(
                [
                    jnp.concatenate([high, high], axis=1),
                    jnp.concatenate([low, jnp.zeros_like(low)], axis=1),
                ],
                axis=0,
            ),
            right,
            preferred_element_type=jnp.float32,
        )
        return product[:rows] + product[rows:]

    block_high, block_low = split(block)
    normal[:128, :128] = block_high
    normal[128:, :128] = block_high
    normal[:128, 128:] = block_low
    normal[128:, 128:] = jnp.zeros((128, 128), jnp.bfloat16)
    right[...] = jnp.zeros(right.shape, jnp.bfloat16)
    side = sub8 // 2 % 2
    wall_row = jnp.where(side == 0, block[:1], block[127:])
    lift = jnp.concatenate([table[LIFT + k] for k in range(4)], axis=1)
    home = (sub8 // 4 * 2 + sub8 % 2)[:, :1]
    joined_y = (
        mass_y
        + table[LAST] * pltpu.roll(mass_y, 127, 1)
        + table[FIRST] * pltpu.roll(mass_y, 1, 1)
    )
    both = lambda value: jnp.concatenate([value, value], axis=0)
    joined_y2 = both(joined_y)
    count2 = both(table[COUNT])

    def at_home(value):
        return jnp.concatenate([jnp.where(home == k, value, 0.0) for k in range(4)], axis=1)

    def coarse(value):
        return value.astype(jnp.bfloat16).astype(jnp.float32)

    twice = jnp.dot(wall_row, block, precision=precise, preferred_element_type=jnp.float32)
    pieces, pieces_two = [lift, lift], [lift, lift]
    for n, value in enumerate((wall_row, joined_y * wall_row, wall_row, twice)):
        rises = at_home(value)
        high = coarse(rises)
        triple = [high, high, rises - high]
        if n == 0:
            pieces += triple
        else:
            pieces_two += triple
    for n, value in enumerate(pieces):
        lifting[8 * n : 8 * n + 8] = value
    lifting[40:] = jnp.zeros((8, 512), jnp.float32)
    for n, value in enumerate(pieces_two):
        lifting_two[8 * n : 8 * n + 8] = value
    lifting_two[88:] = jnp.zeros((8, 512), jnp.float32)
    wall_mass = jnp.where(side == 0, joined_y[:, :1], joined_y[:, 127:])
    scale_zy = both(table[QMZ] * joined_y) * inverse_step
    for comp in range(3):
        for i in range(16):
            res[comp, 16 * i : 16 * i + 16] = velocity[comp, i] * (
                scale_zy * (mass_x[i % 8] * ends[i % 8])
            )

    row16 = lax.broadcasted_iota(jnp.int32, (16, 128), 0) % 8
    share_x = jnp.where(jnp.logical_or(row16 == 0, row16 == 7), 0.5, 1.0)
    half_y = jnp.broadcast_to(table[COUNT][:1], (8, 128))

    def fold(value):
        return value[:8] + value[8:]

    def apply(source, comp):
        high, low = split(source[comp])
        parts = jnp.concatenate([high, low], axis=1)
        along = jnp.dot(flat[0], parts, preferred_element_type=jnp.float32)
        along = along[:, :128] + along[:, 128:]
        along = along + jnp.dot(flat[1], high, preferred_element_type=jnp.float32)
        across_y = jnp.dot(parts, normal[...], preferred_element_type=jnp.float32)
        return along, across_y[:, :128] + across_y[:, 128:]

    def send_face(turn, d, comp):
        push(
            face.at[turn, d, comp], face_in.at[turn, d, comp], send.at[2 + turn],
            recv.at[1 + turn], neighbours[d],
        )

    def operate(source, target, turn):
        for comp in range(3):
            along, across_y = apply(source, comp)
            for d in range(4):
                rows = slice(256 + 16 * d, 272 + 16 * d)
                face[turn, d, comp] = along[rows] * joined_y2
                if turn:
                    send_face(turn, d, comp)
            for i in range(16):
                rows = slice(16 * i, 16 * i + 16)
                target[comp, rows] = along[rows] * joined_y2 + across_y[rows] * both(
                    table[FLAT + i]
                )

    operate(res, one, 0)
    pl.semaphore_wait(barrier, len(near))

    tell(0)
    for d in range(2):
        push(slab, slab_in.at[d], send.at[0], slab_recv.at[d], neighbours[d])
    for comp in range(3):
        for d in range(4):
            send_face(0, d, comp)

    def regroup(blocks):
        upper = (lane // 8) % 2 == 1
        result = []
        for ex in range(2):
            low, high = blocks[ex], blocks[2 + ex]
            result.append(jnp.where(upper, pltpu.roll(high, 8, 1), low))
            result.append(jnp.where(upper, high, pltpu.roll(low, 120, 1)))
        return result

    def ungroup(values):
        upper = (lane // 8) % 2 == 1
        low, high = [], []
        for ex in range(2):
            a, b = values[2 * ex], values[2 * ex + 1]
            low.append(jnp.where(upper, pltpu.roll(b, 8, 1), a))
            high.append(jnp.where(upper, b, pltpu.roll(a, 120, 1)))
        return low + high

    wide = lambda row: jnp.broadcast_to(row, (8, 128))
    quarter = lambda ref, row, q: ref[row : row + 1, 128 * q : 128 * q + 128]
    distance = [(quarter(owner, 0, q) - wall + nw) % nw for q in range(4)]
    to_next = regroup([wide(jnp.where(d == 1, 1.0, 0.0)) for d in distance])
    to_prev = regroup([wide(jnp.where(d == nw - 1, 1.0, 0.0)) for d in distance])
    layer = regroup([wide((quarter(element, 0, q) % 2).astype(jnp.float32)) for q in range(4)])
    axes = [regroup([wide(quarter(coords, k, q)) for q in range(4)]) for k in range(3)]

    def lagrange(coord):
        value = table[LAG]
        for b in range(8):
            value = value * jnp.where(sub8 == b, 1.0, coord - GLL_NODES[b])
        return value

    basis = [[lagrange(axes[k][g]) for k in range(3)] for g in range(4)]
    second_wall = (lane // 8) % 2 == 1
    for g in range(4):
        ly = basis[g][2]
        blocks = []
        for side in range(2):
            for ey in range(2):
                chosen = jnp.logical_and(
                    wide(second_wall) == (side == 1), layer[g] == float(ey)
                )
                blocks.append(jnp.where(chosen, ly, 0.0))
        high, low = split(jnp.concatenate(blocks, axis=0))
        for kk in range(2):
            k = 2 * (g // 2) + kk
            column = slice(128 * kk, 128 * kk + 128)
            right[g, 32 * k : 32 * k + 32, column] = high
            right[g, 128 + 32 * k : 160 + 32 * k, column] = low

    masks = [[1.0 - to_next[g] - to_prev[g], to_prev[g], to_next[g]] for g in range(4)]

    def sample(source, g):
        ez = g % 2
        product = split_product(
            source[:, :, 8 * ez : 8 * ez + 8, :].reshape(64, 128), right[g]
        )
        total = [jnp.zeros((8, 128), jnp.float32) for _ in range(2)]
        for kk in range(2):
            values = product[:, 128 * kk : 128 * kk + 128].reshape(2, 4, 8, 128)
            for comp in range(2):
                for x in range(4):
                    a = 4 * kk + x
                    total[comp] = total[comp] + values[comp, x] * basis[g][0][a : a + 1]
        return total

    sums = []
    for g in range(4):
        own = sample(slab, g)
        sums.append([own[comp] * masks[g][0] for comp in range(2)])
    for d in range(2):
        wait_bytes(slab_in.at[d], slab_recv.at[d])
        for g in range(4):
            far = sample(slab_in.at[d], g)
            for comp in range(2):
                sums[g][comp] = sums[g][comp] + far[comp] * masks[g][1 + d]
    stream = ungroup(
        [wide(jnp.sum(sums[g][0] * basis[g][1], axis=0, keepdims=True)) for g in range(4)]
    )
    spanwise = ungroup(
        [wide(jnp.sum(sums[g][1] * basis[g][1], axis=0, keepdims=True)) for g in range(4)]
    )

    for q in range(4):
        u, v = stream[q], spanwise[q]
        speed = jnp.sqrt(u * u + v * v + speed_floor)
        ratio = karman / jnp.log(sample_height / wide(quarter(roughness, 0, q)))
        factor = -(ratio * ratio * speed / viscosity)
        for comp, value in enumerate((u, v)):
            slope = factor * value
            neumann[comp : comp + 1, 128 * q : 128 * q + 128] = slope[:1]
            plane[comp * 4 + q : comp * 4 + q + 1, :] = (viscosity * slope * table[PLANE])[:1]

    mine = plane[...]
    lines_x = jnp.zeros((8, 128), jnp.float32)
    for q in range(4):
        here = jnp.logical_and(sub8 == 2 * q + 1, lane8 // 16 == 3 - q)
        lines_x = jnp.where(here, pltpu.roll(mine, (16 * (3 - q) - 112) % 128, 1), lines_x)
        here = jnp.logical_and(sub8 == 2 * q, lane8 // 16 == 7 - q)
        lines_x = jnp.where(here, pltpu.roll(mine, (64 + 16 * (3 - q)) % 128, 1), lines_x)
    lines_z = jnp.zeros((8, 128), jnp.float32)
    for r in range(8):
        here = jnp.logical_and(sub8 == r, lane8 % 16 == 7 - r)
        lines_z = jnp.where(here, pltpu.roll(mine, (7 - r - 15) % 128, 1), lines_z)
        here = jnp.logical_and(sub8 == r, lane8 % 16 == 15 - r)
        lines_z = jnp.where(here, pltpu.roll(mine, (15 - r) % 128, 1), lines_z)
    verge[0] = jnp.sum(lines_x, axis=0, keepdims=True)
    verge[1] = jnp.sum(lines_z, axis=0, keepdims=True)
    hear(0)
    for d, (dw, ds) in enumerate(FAR_SHIFTS):
        push(
            verge.at[0 if abs(dw) == 2 else 1], verge_in.at[d], send.at[6], recv.at[5], distant[d]
        )
    for d in range(8):
        push(plane, plane_in.at[d], send.at[1], recv.at[0], neighbours[d])
    tell(1)

    node_z = lane8 % 16
    node_x = lane8 // 16
    half = sub8 % 2

    def join_span(mine, before, after):
        return (
            mine
            + jnp.where(node_z == 7, pltpu.roll(mine, 127, 1), 0.0)
            + jnp.where(node_z == 8, pltpu.roll(mine, 1, 1), 0.0)
            + jnp.where(node_z == 0, pltpu.roll(before, 113, 1), 0.0)
            + jnp.where(node_z == 15, pltpu.roll(after, 15, 1), 0.0)
        )

    def join_wall(mine, before, after):
        later = jnp.where(half == 0, pltpu.roll(mine, 7, 0), pltpu.roll(after, 1, 0))
        earlier = jnp.where(half == 0, pltpu.roll(before, 7, 0), pltpu.roll(mine, 1, 0))
        return (
            mine
            + jnp.where(node_x == 7, pltpu.roll(later, 112, 1), 0.0)
            + jnp.where(node_x == 0, pltpu.roll(earlier, 16, 1), 0.0)
        )

    def receive(target, turn):
        wait_bytes(face_in.at[turn], recv.at[1 + turn])
        into = (
            pl.ds(0, 16),
            pl.ds(240, 16),
            pl.ds(0, 16, stride=16),
            pl.ds(15, 16, stride=16),
        )
        for d in range(4):
            for comp in range(3):
                target[comp, into[d], :] = target[comp, into[d], :] + face_in[turn, d, comp]

    def note(k, value):
        mom[k : k + 1, :] = jnp.sum(value, axis=0, keepdims=True)

    def energy(source, index, comps):
        for comp in comps:
            along, across_y = apply(source, comp)
            inside = jnp.zeros((16, 128), jnp.float32)
            edges = jnp.zeros((16, 128), jnp.float32)
            for i in range(16):
                rows = slice(16 * i, 16 * i + 16)
                term = source[comp, rows] * (
                    along[rows] * joined_y2 + across_y[rows] * both(table[FLAT + i])
                )
                if i % 8 in (0, 7):
                    edges = edges + term
                else:
                    inside = inside + term
            for d, i in ((0, 15), (1, 0)):
                sent = along[256 + 16 * d : 272 + 16 * d] * joined_y2
                edges = edges + sent * source[comp, 16 * i : 16 * i + 16]
            total = fold((inside + 0.5 * edges) * count2)
            for d, first in ((2, 15), (3, 0)):
                sent = along[256 + 16 * d : 272 + 16 * d] * joined_y2
                term = sent * source[comp, pl.ds(first, 16, stride=16), :]
                total = total + fold(term * share_x) * half_y
            note(3 * index + comp, total)

    def weighted(pairs, comps):
        for comp in comps:
            totals = [jnp.zeros((16, 128), jnp.float32) for _ in pairs]
            edges = [jnp.zeros((16, 128), jnp.float32) for _ in pairs]
            for i in range(16):
                for n, (first, second, _) in enumerate(pairs):
                    term = (
                        first[comp, 16 * i : 16 * i + 16] * second[comp, 16 * i : 16 * i + 16]
                    )
                    if i % 8 in (0, 7):
                        edges[n] = edges[n] + term
                    else:
                        totals[n] = totals[n] + term
            for n, (_, _, index) in enumerate(pairs):
                note(3 * index + comp, fold((totals[n] + 0.5 * edges[n]) * count2))

    receive(one, 0)
    operate(one, two, 1)
    hear(1)
    tell(2)
    receive(two, 1)
    products = [(res, res, 0), (res, one, 1), (one, one, 2), (one, two, 3), (two, two, 4)]
    weighted(products, (1,))
    energy(two, 5, (1,))
    wait_bytes(plane_in, recv.at[0])
    wait_bytes(verge_in, recv.at[5])
    raw = {(-dw, -ds): plane_in[d] for d, (dw, ds) in enumerate(SHIFTS)}
    raw[0, 0] = plane[...]
    for d, (dw, ds) in enumerate(FAR_SHIFTS):
        row = wide(verge_in[d])
        if abs(dw) == 2:
            value = pltpu.roll(row, 56 if dw > 0 else 16, 1, stride=8, stride_axis=0)
        else:
            value = pltpu.roll(row, 8 if ds > 0 else 113, 1, stride=1, stride_axis=0)
        raw[-dw, -ds] = value
    none = jnp.zeros((8, 128), jnp.float32)
    square = [(dw, ds) for dw in (-1, 0, 1) for ds in (-1, 0, 1)]
    cross = [(0, 0), (-1, 0), (1, 0), (0, -1), (0, 1)]

    def spans(values, at):
        dw, ds = at
        return join_span(
            values[at], values.get((dw, ds - 1), none), values.get((dw, ds + 1), none)
        )

    def walls(values, at):
        dw, ds = at
        return join_wall(
            values[at], values.get((dw - 1, ds), none), values.get((dw + 1, ds), none)
        )

    def pulled(values):
        fill = [none] * (len(values) % 2)
        product = split_product(jnp.concatenate(list(values) + fill, axis=0), lines[...])
        return [
            (product[8 * n : 8 * n + 8, :128], product[8 * n : 8 * n + 8, 128:])
            for n in range(len(values))
        ]

    mass_flat = table[LANEX] * table[LANEZ]

    def plane_operator(in_x, in_z, value, at):
        return (
            table[LANEZ] * walls(in_x, at)
            + table[LANEX] * spans(in_z, at)
            + (SCALE * inverse_step) * mass_flat * value
        )

    line_of = {at: spans(raw, at) for at in square + [(-2, 0), (2, 0)]}
    stress = {at: walls(line_of, at) for at in square}
    pulls = pulled([stress[at] for at in square])
    in_x = {at: pulls[n][0] for n, at in enumerate(square)}
    in_z = {at: pulls[n][1] for n, at in enumerate(square)}
    first = {at: plane_operator(in_x, in_z, stress[at], at) for at in cross}
    mass_of = {at: mass_flat * stress[at] for at in cross}
    pulls = pulled([first[at] for at in cross] + [mass_of[at] for at in cross])
    seconds = []
    for offset, values in ((0, first), (5, mass_of)):
        in_x = {at: pulls[offset + n][0] for n, at in enumerate(cross)}
        in_z = {at: pulls[offset + n][1] for n, at in enumerate(cross)}
        seconds.append(plane_operator(in_x, in_z, values[0, 0], (0, 0)))

    def raised(doubles, triples, rights, rows):
        parts = []
        for value in doubles:
            parts += [coarse(value), value - coarse(value)]
        for value in triples:
            parts += [coarse(value), value - coarse(value), coarse(value)]
        parts += [none] * (rows // 8 - len(parts))
        return lax.dot_general(
            jnp.concatenate(parts, axis=0),
            rights[:rows],
            (((0,), (0,)), ((), ())),
            preferred_element_type=jnp.float32,
        )

    here, pull, mass_here = stress[0, 0], first[0, 0] * wall_mass, mass_of[0, 0]
    lifted = raised([here], [], lifting, 16)
    lifted_one = raised([pull], [mass_here], lifting, 48)
    lifted_two = raised(
        [seconds[0] * wall_mass * wall_mass],
        [seconds[1], mass_flat * pull, mass_flat * mass_here],
        lifting_two,
        96,
    )
    for comp in range(2):
        for ex in range(2):
            column = (comp * 2 + ex) * 128
            rows = slice(128 * ex, 128 * ex + 128)
            for target, value in ((res, lifted), (one, lifted_one), (two, lifted_two)):
                target[2 * comp, rows] = target[2 * comp, rows] + value[:, column : column + 128]

    weighted(products, (0, 2))
    energy(two, 5, (0, 2))

    mom[18:24, :] = jnp.zeros((6, 128), jnp.float32)
    total = jnp.sum(mom[...], axis=1, keepdims=True)
    row = jnp.zeros((8, 128), jnp.float32)
    for k in range(3):
        row = row + jnp.where(lane8 == 8 * k + sub8, total[8 * k : 8 * k + 8], 0.0)
    part[0] = jnp.sum(row, axis=0, keepdims=True)
    hear(2)
    line_slots, plane_slots = nc * ns, nx * ny
    for ds in sorted(deep_shifts, key=lambda k: -abs(k)):
        if ds:
            push(
                part.at[0], part_in.at[wc * ns + sp], send.at[4], recv.at[3], deep_peer(1, ds)
            )
    relays_sums = wc == 1

    @pl.when(jnp.logical_not(relays_sums))
    def _():
        push(part.at[0], part_in.at[wc * ns + sp], send.at[4], recv.at[3], deep_peer(1, 0))
        wait_bytes(part_in.at[pl.ds(line_slots, plane_slots)], recv.at[4])
        wait_bytes(part_in.at[pl.ds(0, ns)], send.at[4])

    @pl.when(relays_sums)
    def _():
        part_in[wc * ns + sp] = part[0]
        wait_bytes(part_in.at[pl.ds(0, line_slots - 1)], recv.at[3])
        row = part_in[0]
        for k in range(1, line_slots):
            row = row + part_in[k]
        part[1] = row
        slot = line_slots + wx * ny + wy
        for a, b in plain:
            for c in (0, 1):
                push(
                    part.at[1], part_in.at[slot], send.at[5 if c else 7], recv.at[4],
                    (place_x[a], place_y[b], c, sp),
                )
        push(part.at[1], part_in.at[slot], send.at[7], recv.at[4], (wx, wy, 0, sp))
        part_in[slot] = row
        wait_bytes(part_in.at[pl.ds(line_slots, plane_slots - 1)], recv.at[4])
        wait_bytes(part_in.at[pl.ds(0, ns - 1)], send.at[4])
        wait_bytes(part_in.at[pl.ds(line_slots, plane_slots - 1)], send.at[5])
        wait_bytes(part_in.at[pl.ds(line_slots, plane_slots)], send.at[7])

    row = part_in[line_slots]
    for k in range(1, plane_slots):
        row = row + part_in[line_slots + k]

    row = jnp.broadcast_to(row, (8, 128))
    moments = [row if j == 0 else pltpu.roll(row, 128 - 3 * j, 1) for j in range(6)]

    def inner(first, second, raise_by):
        total = None
        for i, a in enumerate(first):
            for j, b in enumerate(second):
                term = a * b * moments[i + j + raise_by]
                total = term if total is None else total + term
        return total

    unit = jnp.ones((8, 128), jnp.float32)
    direction, residual = [unit], [unit]
    answer = [jnp.zeros((8, 128), jnp.float32)] * 3
    norm = moments[0]
    for step in range(3):
        alpha = norm / inner(direction, direction, 1)
        for i, value in enumerate(direction):
            answer[i] = answer[i] + alpha * value
        if step == 2:
            break
        lowered = [-alpha * value for value in direction]
        residual = [residual[0]] + [
            lowered[i] + residual[i + 1] if i + 1 < len(residual) else lowered[i]
            for i in range(len(lowered))
        ]
        newer = inner(residual, residual, 0)
        growth = newer / norm
        direction = [
            value + growth * direction[i] if i < len(direction) else value
            for i, value in enumerate(residual)
        ]
        norm = newer
    for i, value in enumerate(answer):
        scalars[i : i + 1, :] = value[:1] * SCALE
    wait_bytes(slab_in, send.at[0])
    wait_bytes(plane_in, send.at[1])
    wait_bytes(verge_in, send.at[6])
    for turn in range(2):
        wait_bytes(face_in.at[turn], send.at[2 + turn])


def combine(res, one, two, scalars, slopes, out, neumann, sums, sent):
    copies = [pltpu.make_async_copy(slopes, neumann, sent.at[3])]
    copies[0].start()
    for comp in range(3):
        c0, c1, c2 = (
            jnp.broadcast_to(scalars[k : k + 1, comp : comp + 1], (16, 128)) for k in range(3)
        )
        for i in range(16):
            rows = pl.ds(16 * i, 16)
            sums[comp, i] = (
                c0 * res[comp, rows, :] + c1 * one[comp, rows, :] + c2 * two[comp, rows, :]
            )
        copy = pltpu.make_async_copy(sums.at[comp], out.at[comp], sent.at[comp])
        copy.start()
        copies.append(copy)
    for copy in copies:
        copy.wait()


def body(sizes, velocity_old, heights, owner_device, owner_element, ref_coords, roughness):
    nx, ny, nc, ns = sizes
    slots = nc * ns + nx * ny
    f32, i32 = jnp.float32, jnp.int32
    vmem = pl.BlockSpec(memory_space=pltpu.VMEM)
    anywhere = pl.BlockSpec(memory_space=pl.ANY)
    constants, flat, lines = (jnp.asarray(value) for value in tables())
    res, one, two, scalars, slopes = pl.pallas_call(
        functools.partial(kernel, sizes),
        out_shape=(
            pltpu.VMEM((3, 256, 128), f32),
            pltpu.VMEM((3, 256, 128), f32),
            pltpu.VMEM((3, 256, 128), f32),
            pltpu.VMEM((8, 128), f32),
            pltpu.VMEM((2, 512), f32),
        ),
        in_specs=[anywhere] * 9,
        out_specs=(vmem,) * 5,
        scratch_shapes=[
            pltpu.VMEM((3, 16, 16, 128), f32),
            pltpu.SMEM((16,), f32),
            pltpu.VMEM((1, 512), i32),
            pltpu.VMEM((1, 512), i32),
            pltpu.VMEM((3, 512), f32),
            pltpu.VMEM((1, 512), f32),
            pltpu.VMEM(constants.shape, f32),
            pltpu.VMEM(flat.shape, jnp.bfloat16),
            pltpu.VMEM(lines.shape, jnp.bfloat16),
            pltpu.VMEM((256, 256), jnp.bfloat16),
            pltpu.VMEM((48, 512), f32),
            pltpu.VMEM((96, 512), f32),
            pltpu.VMEM((4, 256, 256), jnp.bfloat16),
            pltpu.VMEM((2, 4, 16, 128), f32),
            pltpu.VMEM((2, 2, 4, 16, 128), f32),
            pltpu.VMEM((8, 128), f32),
            pltpu.VMEM((8, 8, 128), f32),
            pltpu.VMEM((2, 1, 128), f32),
            pltpu.VMEM((12, 1, 128), f32),
            pltpu.VMEM((2, 4, 3, 16, 128), f32),
            pltpu.VMEM((2, 4, 3, 16, 128), f32),
            pltpu.VMEM((24, 128), f32),
            pltpu.VMEM((2, 1, 128), f32),
            pltpu.VMEM((slots, 1, 128), f32),
            pltpu.SemaphoreType.DMA((9,)),
            pltpu.SemaphoreType.DMA((8,)),
            pltpu.SemaphoreType.DMA((2,)),
            pltpu.SemaphoreType.DMA((6,)),
            pltpu.SemaphoreType.REGULAR((3,)),
        ],
        compiler_params=pltpu.CompilerParams(collective_id=0, has_side_effects=True),
        name="channel_step",
    )(
        velocity_old,
        heights,
        owner_device.reshape(1, -1),
        owner_element.reshape(1, -1),
        ref_coords,
        roughness.reshape(1, -1),
        constants,
        flat,
        lines,
    )
    return pl.pallas_call(
        combine,
        out_shape=(
            jax.ShapeDtypeStruct((3, 16, 16, 128), f32),
            jax.ShapeDtypeStruct((2, 512), f32),
        ),
        in_specs=[vmem] * 5,
        out_specs=(anywhere, anywhere),
        scratch_shapes=[
            pltpu.VMEM((3, 16, 16, 128), f32),
            pltpu.SemaphoreType.DMA((4,)),
        ],
        name="combine",
    )(
        *(
            pltpu.with_memory_space_constraint(value, pltpu.VMEM)
            for value in (res, one, two, scalars, slopes)
        )
    )


def torus_program(torus):
    sizes = tuple(torus.shape[name] for name in AXES)
    return jax.shard_map(
        functools.partial(body, sizes),
        mesh=torus,
        in_specs=(
            P(None, WALL, "span", None),
            P(),
            P(WALL_SPAN, None),
            P(WALL_SPAN, None),
            P(None, WALL_SPAN),
            P(WALL_SPAN),
        ),
        out_specs=(P(None, WALL, "span", None), P(None, WALL_SPAN)),
        check_vma=False,
    )


def solution(mesh):
    return torus_program(Mesh(mesh.devices.reshape(4, 8, 2, mesh.shape["span"]), AXES))
```

```python
import functools

import jax
import jax.numpy as jnp
import numpy as np
from jax import lax
from jax.experimental import pallas as pl
from jax.experimental.pallas import tpu as pltpu
from jax.sharding import Mesh
from jax.sharding import PartitionSpec as P

AXES = ("wall_0", "wall_1", "wall_2", "span")
WALL_SPAN = AXES
WALL = ("wall_0", "wall_1", "wall_2")
MESH_ID = pl.DeviceIdType.MESH

GLL_NODES = (
    -1.0,
    -0.8717401485096066,
    -0.5917001814331423,
    -0.2092992179024789,
    0.2092992179024789,
    0.5917001814331423,
    0.8717401485096066,
    1.0,
)
GLL_WEIGHTS = (
    0.03571428571428571,
    0.2107042271435061,
    0.3411226924835044,
    0.4124587946587038,
    0.4124587946587038,
    0.3411226924835044,
    0.2107042271435061,
    0.03571428571428571,
)
viscosity = 0.02
inverse_step = 20.0
karman = 0.41
sample_height = 0.1
speed_floor = 0.01
element_dx = 0.05
element_dz = 0.13
precise = lax.Precision.HIGHEST

SCALE = 64.0

SHIFTS = ((1, 0), (-1, 0), (0, 1), (0, -1), (1, 1), (1, -1), (-1, 1), (-1, -1))

FAR_SHIFTS = (
    (2, 0), (2, 1), (2, -1), (-2, 0), (-2, 1), (-2, -1),
    (0, 2), (1, 2), (-1, 2), (0, -2), (1, -2), (-1, -2),
)

MZ, QMZ, COUNT, LAG, PLANE, HALFW, LAST, FIRST, LANEX, LANEZ = range(10)
BLOCK, LIFT, FLAT = 10, 26, 30


def stiffness_table():
    points = np.array(GLL_NODES)
    weights = np.array(GLL_WEIGHTS)
    previous = np.ones(8)
    current = points.copy()
    for degree in range(1, 7):
        previous, current = (
            current,
            ((2 * degree + 1) * points * current - degree * previous) / (degree + 1),
        )
    derivative = np.zeros((8, 8))
    for target in range(8):
        for source in range(8):
            if target != source:
                derivative[target, source] = (
                    current[target] / current[source] / (points[target] - points[source])
                )
    derivative[0, 0] = -14.0
    derivative[7, 7] = 14.0
    return derivative.T @ (weights[:, None] * derivative)


def tables():
    weights = np.array(GLL_WEIGHTS)
    points = np.array(GLL_NODES)
    stiffness = stiffness_table()
    ones = np.ones((8, 128))
    lane = np.arange(128)
    ends = np.array([2.0, 1, 1, 1, 1, 1, 1, 2.0])
    mass_x = 0.5 * element_dx * weights
    mass_z = 0.5 * element_dz * weights
    count_y = np.where((lane % 8 == 0) | (lane % 8 == 7), 0.5, 1.0)
    count_y[0] = count_y[127] = 1.0
    gaps = points[:, None] - points[None, :] + np.eye(8)
    rows = [
        mass_z[:, None] * ones,
        (mass_z * ends)[:, None] * ones,
        (1.0 / ends)[:, None] * count_y[None, :],
        (1.0 / np.prod(gaps, axis=1))[:, None] * ones,
        ones * (mass_x[lane // 16] * mass_z[lane % 8])[None, :],
        ones * (0.5 * weights[lane % 8])[None, :],
        ones * ((lane % 8 == 7) & (lane < 127))[None, :],
        ones * ((lane % 8 == 0) & (lane > 0))[None, :],
    ]
    block = np.kron(np.eye(16), SCALE * viscosity * 2.0 * stiffness)
    lift = np.zeros((8, 512))
    for comp in range(2):
        for half in range(2):
            column = (comp * 2 + half) * 128
            lift[comp * 4 + half, column] = 1.0
            lift[comp * 4 + 2 + half, column + 127] = 1.0
    joined_x = np.tile(mass_x * ends, 2)
    joined_z = np.tile(mass_z * ends, 2)

    def chain(length):
        scaled = SCALE * viscosity * (2.0 / length) * stiffness
        full = np.kron(np.eye(2), scaled)
        ends_only = full[[15, 0]]
        full[7] = full[8] = full[7] + full[8]
        return full, ends_only

    chain_x, ends_x = chain(element_dx)
    chain_z, ends_z = chain(element_dz)
    flat = np.kron(chain_x, np.diag(joined_z)) + np.kron(np.diag(joined_x), chain_z)
    flat += SCALE * inverse_step * np.diag(np.kron(joined_x, joined_z))
    faces = [np.kron(ends_x[d : d + 1], np.diag(joined_z)) for d in range(2)]
    faces += [np.kron(np.diag(joined_x), ends_z[d : d + 1]) for d in range(2)]
    flat = np.concatenate([flat] + faces).astype(np.float32)
    flat_high = flat.astype(jnp.bfloat16)
    flat_low = (flat - flat_high.astype(np.float32)).astype(jnp.bfloat16)
    line_x = SCALE * viscosity * (2.0 / element_dx) * stiffness
    line_z = SCALE * viscosity * (2.0 / element_dz) * stiffness
    line = np.concatenate([np.kron(line_x.T, np.eye(16)), np.kron(np.eye(16), line_z.T)], axis=1)
    line_high = line.astype(np.float32).astype(jnp.bfloat16)
    line_low = (line.astype(np.float32) - line_high.astype(np.float32)).astype(jnp.bfloat16)
    lines = np.concatenate([line_high, line_low])
    rows += [
        ones * (mass_x * ends)[lane // 16][None, :],
        ones * (mass_z * ends)[lane % 8][None, :],
    ]
    pieces = [np.stack(rows), block.reshape(16, 8, 128), lift.reshape(8, 4, 128).transpose(1, 0, 2)]
    pieces += [joined_x[:, None, None] * (mass_z * ends)[None, :, None] * np.ones((16, 8, 128))]
    return np.concatenate(pieces).astype(np.float32), np.stack([flat_high, flat_low]), lines


def kernel(sizes, *refs):
    operands, refs = refs[:9], refs[9:]
    (res, one, two, scalars, neumann), refs = refs[:5], refs[5:]
    local, refs = refs[:9], refs[9:]
    velocity, heights, owner, element, coords, roughness, table, flat, lines = local
    (normal, lifting, lifting_two, right, slab, slab_in, plane, plane_in,
     verge, verge_in, face, face_in, mom, part, part_in,
     load, send, slab_recv, recv, ready) = refs
    nx, ny, nc, ns = sizes
    nw = nx * ny * nc
    loads = [
        pltpu.make_async_copy(source, target, load.at[n])
        for n, (source, target) in enumerate(zip(operands, local))
    ]
    for copy in loads:
        copy.start()
    wx, wy, wc, sp = (lax.axis_index(name) for name in AXES)
    wall = (wx * ny + wy) * nc + wc
    weights = np.array(GLL_WEIGHTS)
    stiffness = stiffness_table()
    mass_x = [float(v) for v in 0.5 * element_dx * weights]
    ends = [2.0, 1.0, 1.0, 1.0, 1.0, 1.0, 1.0, 2.0]

    def ring(value, shift, count):
        if shift > 0:
            return jnp.where(value >= count - shift, value + shift - count, value + shift)
        return jnp.where(value < -shift, value + shift + count, value + shift)

    def beside(dw):
        if dw == 0:
            return wx, wy, wc
        sign = 1 if dw > 0 else -1
        if abs(dw) == 2:
            turn_y = wy == (ny - 1 if dw > 0 else 0)
            return jnp.where(turn_y, ring(wx, sign, nx), wx), ring(wy, sign, ny), wc
        turn = wc == (nc - 1 if dw > 0 else 0)
        turn_y = jnp.logical_and(turn, wy == (ny - 1 if dw > 0 else 0))
        return (
            jnp.where(turn_y, ring(wx, dw, nx), wx),
            jnp.where(turn, ring(wy, dw, ny), wy),
            ring(wc, dw, nc),
        )

    along = {dw: beside(dw) for dw in (-2, -1, 0, 1, 2)}
    across = {k: ring(sp, k, ns) if k else sp for k in (-2, -1, 0, 1, 2)}
    neighbours = [(*along[dw], across[ds]) for dw, ds in SHIFTS]
    distant = [(*along[dw], across[ds]) for dw, ds in FAR_SHIFTS]
    place_x = {0: wx, 1: ring(wx, 1, nx), -1: ring(wx, -1, nx), 2: ring(wx, 2, nx)}
    place_y = {k: ring(wy, k, ny) if k else wy for k in range(-(ny // 2) + 1, ny // 2 + 1)}
    place_y[-2] = ring(wy, -2, ny)
    place_z = {k: ring(sp, k, ns) if k else sp for k in range(-(ns // 2) + 1, ns // 2 + 1)}
    place_z[-2] = ring(sp, -2, ns)
    other = ring(wc, 1, nc)
    flat_peer = lambda dx, dy: (place_x[dx], place_y[dy], wc, sp)
    deep_peer = lambda c, ds: (wx, wy, c, place_z[ds])

    def far_first(keys):
        return sorted(keys, key=lambda key: -abs(key[0]) - abs(key[1]))

    deep_shifts = range(-(ns // 2) + 1, ns // 2 + 1)
    wide_x = [k for k in (-1, 0, 1, 2) if -(nx // 2) < k <= nx // 2]
    plain = far_first([(a, b) for a in wide_x for b in range(-(ny // 2) + 1, ny // 2 + 1)])
    plain = [key for key in plain if key != (0, 0)]

    barrier = pltpu.get_barrier_semaphore()
    near = neighbours[:4] + [deep_peer(other, 0)]
    near += [(*along[2], sp), (*along[-2], sp), (*along[0], across[2]), (*along[0], across[-2])]
    near += [flat_peer(1, 0), flat_peer(-1, 0), flat_peer(0, 1), flat_peer(0, -1)]
    for peer in near:
        pl.semaphore_signal(barrier, inc=1, device_id=peer, device_id_type=MESH_ID)
    relays = [
        near,
        [flat_peer(1, 0), flat_peer(-1, 0), flat_peer(0, 2), flat_peer(0, -2)]
        + [deep_peer(wc, 2), deep_peer(wc, -2)],
        [flat_peer(1, 0), flat_peer(-1, 0), flat_peer(0, 2), flat_peer(0, -2)]
        + [flat_peer(2, 2), flat_peer(2, -2), deep_peer(wc, 4), deep_peer(wc, -4)],
    ]

    def tell(n):
        for peer in relays[n]:
            pl.semaphore_signal(ready.at[n], inc=1, device_id=peer, device_id_type=MESH_ID)

    def hear(n):
        pl.semaphore_wait(ready.at[n], len(relays[n]))

    def push(source, target, send_sem, recv_sem, peer):
        pltpu.make_async_remote_copy(
            src_ref=source,
            dst_ref=target,
            send_sem=send_sem,
            recv_sem=recv_sem,
            device_id=peer,
            device_id_type=MESH_ID,
        ).start()

    def wait_bytes(like, sem):
        pltpu.make_async_copy(like, like, sem).wait()

    loads[0].wait()

    lane = lax.broadcasted_iota(jnp.int32, (1, 128), 1)
    sub8 = lax.broadcasted_iota(jnp.int32, (8, 128), 0)
    lane8 = lax.broadcasted_iota(jnp.int32, (8, 128), 1)

    for comp in range(2):
        quarters = []
        for k in range(4):
            quarters.append(velocity[2 * comp, 4 * k : 4 * k + 4].reshape(64, 128))
        packed = jnp.zeros((64, 128), jnp.float32)
        where_to = lax.broadcasted_iota(jnp.int32, (64, 128), 1)
        for k in range(4):
            low = pltpu.roll(quarters[k], 32 * k, 1) if k else quarters[k]
            shift = (32 * k + 32) % 128
            high = pltpu.roll(quarters[k], shift, 1) if shift else quarters[k]
            packed = jnp.where(where_to // 16 == 2 * k, low, packed)
            packed = jnp.where(where_to // 16 == 2 * k + 1, high, packed)
        slab[comp] = packed.reshape(4, 16, 128)

    for copy in loads[1:]:
        copy.wait()
    height = jnp.zeros((8, 128), jnp.float32)
    for layer in range(16):
        height = jnp.where(lane8 // 8 == layer, heights[layer], height)
    mass_y = height * table[HALFW]
    block = table[BLOCK : BLOCK + 16].reshape(128, 128) * (1.0 / height)[:1]
    block = (
        block
        + table[LAST][:1] * pltpu.roll(block, 127, 1)
        + table[FIRST][:1] * pltpu.roll(block, 1, 1)
    )

    def split(value):
        high = value.astype(jnp.bfloat16)
        return high, (value - high.astype(jnp.float32)).astype(jnp.bfloat16)

    def split_product(left, right):
        rows = left.shape[0]
        high, low = split(left)
        product = jnp.dot(
            jnp.concatenate(
                [
                    jnp.concatenate([high, high], axis=1),
                    jnp.concatenate([low, jnp.zeros_like(low)], axis=1),
                ],
                axis=0,
            ),
            right,
            preferred_element_type=jnp.float32,
        )
        return product[:rows] + product[rows:]

    block_high, block_low = split(block)
    normal[:128, :128] = block_high
    normal[128:, :128] = block_high
    normal[:128, 128:] = block_low
    normal[128:, 128:] = jnp.zeros((128, 128), jnp.bfloat16)
    right[...] = jnp.zeros(right.shape, jnp.bfloat16)
    side = sub8 // 2 % 2
    wall_row = jnp.where(side == 0, block[:1], block[127:])
    lift = jnp.concatenate([table[LIFT + k] for k in range(4)], axis=1)
    home = (sub8 // 4 * 2 + sub8 % 2)[:, :1]
    joined_y = (
        mass_y
        + table[LAST] * pltpu.roll(mass_y, 127, 1)
        + table[FIRST] * pltpu.roll(mass_y, 1, 1)
    )
    both = lambda value: jnp.concatenate([value, value], axis=0)
    joined_y2 = both(joined_y)
    count2 = both(table[COUNT])

    def at_home(value):
        return jnp.concatenate([jnp.where(home == k, value, 0.0) for k in range(4)], axis=1)

    def coarse(value):
        return value.astype(jnp.bfloat16).astype(jnp.float32)

    twice = jnp.dot(wall_row, block, precision=precise, preferred_element_type=jnp.float32)
    pieces, pieces_two = [lift, lift], [lift, lift]
    for n, value in enumerate((wall_row, joined_y * wall_row, wall_row, twice)):
        rises = at_home(value)
        high = coarse(rises)
        triple = [high, high, rises - high]
        if n == 0:
            pieces += triple
        else:
            pieces_two += triple
    for n, value in enumerate(pieces):
        lifting[8 * n : 8 * n + 8] = value
    lifting[40:] = jnp.zeros((8, 512), jnp.float32)
    for n, value in enumerate(pieces_two):
        lifting_two[8 * n : 8 * n + 8] = value
    lifting_two[88:] = jnp.zeros((8, 512), jnp.float32)
    wall_mass = jnp.where(side == 0, joined_y[:, :1], joined_y[:, 127:])
    scale_zy = both(table[QMZ] * joined_y) * inverse_step
    for comp in range(3):
        for i in range(16):
            res[comp, 16 * i : 16 * i + 16] = velocity[comp, i] * (
                scale_zy * (mass_x[i % 8] * ends[i % 8])
            )

    row16 = lax.broadcasted_iota(jnp.int32, (16, 128), 0) % 8
    share_x = jnp.where(jnp.logical_or(row16 == 0, row16 == 7), 0.5, 1.0)
    half_y = jnp.broadcast_to(table[COUNT][:1], (8, 128))

    def fold(value):
        return value[:8] + value[8:]

    def apply(source, comp):
        return apply_all(source, (comp,))[0]

    def apply_all(source, comps):
        halves = [split(source[comp]) for comp in comps]
        highs = jnp.concatenate([high for high, _ in halves], axis=1)
        small = jnp.dot(flat[1], highs, preferred_element_type=jnp.float32)
        result = []
        for n, (high, low) in enumerate(halves):
            parts = jnp.concatenate([high, low], axis=1)
            along = jnp.dot(flat[0], parts, preferred_element_type=jnp.float32)
            along = along[:, :128] + along[:, 128:] + small[:, 128 * n : 128 * n + 128]
            across_y = jnp.dot(parts, normal[...], preferred_element_type=jnp.float32)
            result.append((along, across_y[:, :128] + across_y[:, 128:]))
        return result

    def send_face(turn, d, comp):
        push(
            face.at[turn, d, comp], face_in.at[turn, d, comp], send.at[2 + turn],
            recv.at[1 + turn], neighbours[d],
        )

    def operate(source, target, turn):
        for comp in range(3):
            along, across_y = apply(source, comp)
            for d in range(4):
                rows = slice(256 + 16 * d, 272 + 16 * d)
                face[turn, d, comp] = along[rows] * joined_y2
                if turn:
                    send_face(turn, d, comp)
            for i in range(16):
                rows = slice(16 * i, 16 * i + 16)
                target[comp, rows] = along[rows] * joined_y2 + across_y[rows] * both(
                    table[FLAT + i]
                )

    operate(res, one, 0)
    pl.semaphore_wait(barrier, len(near))

    for d in range(2):
        push(slab, slab_in.at[d], send.at[0], slab_recv.at[d], neighbours[d])
    for comp in range(3):
        for d in range(4):
            send_face(0, d, comp)
    tell(0)

    def regroup(blocks):
        upper = (lane // 8) % 2 == 1
        result = []
        for ex in range(2):
            low, high = blocks[ex], blocks[2 + ex]
            result.append(jnp.where(upper, pltpu.roll(high, 8, 1), low))
            result.append(jnp.where(upper, high, pltpu.roll(low, 120, 1)))
        return result

    def ungroup(values):
        upper = (lane // 8) % 2 == 1
        low, high = [], []
        for ex in range(2):
            a, b = values[2 * ex], values[2 * ex + 1]
            low.append(jnp.where(upper, pltpu.roll(b, 8, 1), a))
            high.append(jnp.where(upper, b, pltpu.roll(a, 120, 1)))
        return low + high

    wide = lambda row: jnp.broadcast_to(row, (8, 128))
    quarter = lambda ref, row, q: ref[row : row + 1, 128 * q : 128 * q + 128]
    distance = [(quarter(owner, 0, q) - wall + nw) % nw for q in range(4)]
    to_next = regroup([wide(jnp.where(d == 1, 1.0, 0.0)) for d in distance])
    to_prev = regroup([wide(jnp.where(d == nw - 1, 1.0, 0.0)) for d in distance])
    layer = regroup([wide((quarter(element, 0, q) % 2).astype(jnp.float32)) for q in range(4)])
    axes = [regroup([wide(quarter(coords, k, q)) for q in range(4)]) for k in range(3)]

    def lagrange(coord):
        value = table[LAG]
        for b in range(8):
            value = value * jnp.where(sub8 == b, 1.0, coord - GLL_NODES[b])
        return value

    basis = [[lagrange(axes[k][g]) for k in range(3)] for g in range(4)]
    second_wall = (lane // 8) % 2 == 1
    for g in range(4):
        ly = basis[g][2]
        blocks = []
        for side in range(2):
            for ey in range(2):
                chosen = jnp.logical_and(
                    wide(second_wall) == (side == 1), layer[g] == float(ey)
                )
                blocks.append(jnp.where(chosen, ly, 0.0))
        high, low = split(jnp.concatenate(blocks, axis=0))
        for kk in range(2):
            k = 2 * (g // 2) + kk
            column = slice(128 * kk, 128 * kk + 128)
            right[g, 32 * k : 32 * k + 32, column] = high
            right[g, 128 + 32 * k : 160 + 32 * k, column] = low

    masks = [[1.0 - to_next[g] - to_prev[g], to_prev[g], to_next[g]] for g in range(4)]

    def sample(source, g):
        ez = g % 2
        product = split_product(
            source[:, :, 8 * ez : 8 * ez + 8, :].reshape(64, 128), right[g]
        )
        total = [jnp.zeros((8, 128), jnp.float32) for _ in range(2)]
        for kk in range(2):
            values = product[:, 128 * kk : 128 * kk + 128].reshape(2, 4, 8, 128)
            for comp in range(2):
                for x in range(4):
                    a = 4 * kk + x
                    total[comp] = total[comp] + values[comp, x] * basis[g][0][a : a + 1]
        return total

    sums = []
    for g in range(4):
        own = sample(slab, g)
        sums.append([own[comp] * masks[g][0] for comp in range(2)])
    for d in range(2):
        wait_bytes(slab_in.at[d], slab_recv.at[d])
        for g in range(4):
            far = sample(slab_in.at[d], g)
            for comp in range(2):
                sums[g][comp] = sums[g][comp] + far[comp] * masks[g][1 + d]
    stream = ungroup(
        [wide(jnp.sum(sums[g][0] * basis[g][1], axis=0, keepdims=True)) for g in range(4)]
    )
    spanwise = ungroup(
        [wide(jnp.sum(sums[g][1] * basis[g][1], axis=0, keepdims=True)) for g in range(4)]
    )

    for q in range(4):
        u, v = stream[q], spanwise[q]
        speed = jnp.sqrt(u * u + v * v + speed_floor)
        ratio = karman / jnp.log(sample_height / wide(quarter(roughness, 0, q)))
        factor = -(ratio * ratio * speed / viscosity)
        for comp, value in enumerate((u, v)):
            slope = factor * value
            neumann[comp : comp + 1, 128 * q : 128 * q + 128] = slope[:1]
            plane[comp * 4 + q : comp * 4 + q + 1, :] = (viscosity * slope * table[PLANE])[:1]

    mine = plane[...]
    lines_x = jnp.zeros((8, 128), jnp.float32)
    for q in range(4):
        here = jnp.logical_and(sub8 == 2 * q + 1, lane8 // 16 == 3 - q)
        lines_x = jnp.where(here, pltpu.roll(mine, (16 * (3 - q) - 112) % 128, 1), lines_x)
        here = jnp.logical_and(sub8 == 2 * q, lane8 // 16 == 7 - q)
        lines_x = jnp.where(here, pltpu.roll(mine, (64 + 16 * (3 - q)) % 128, 1), lines_x)
    lines_z = jnp.zeros((8, 128), jnp.float32)
    for r in range(8):
        here = jnp.logical_and(sub8 == r, lane8 % 16 == 7 - r)
        lines_z = jnp.where(here, pltpu.roll(mine, (7 - r - 15) % 128, 1), lines_z)
        here = jnp.logical_and(sub8 == r, lane8 % 16 == 15 - r)
        lines_z = jnp.where(here, pltpu.roll(mine, (15 - r) % 128, 1), lines_z)
    verge[0] = jnp.sum(lines_x, axis=0, keepdims=True)
    verge[1] = jnp.sum(lines_z, axis=0, keepdims=True)
    hear(0)
    for d, (dw, ds) in enumerate(FAR_SHIFTS):
        push(
            verge.at[0 if abs(dw) == 2 else 1], verge_in.at[d], send.at[6], recv.at[5], distant[d]
        )
    for d in range(8):
        push(plane, plane_in.at[d], send.at[1], recv.at[0], neighbours[d])
    tell(1)

    node_z = lane8 % 16
    node_x = lane8 // 16
    half = sub8 % 2

    def join_span(mine, before, after):
        return (
            mine
            + jnp.where(node_z == 7, pltpu.roll(mine, 127, 1), 0.0)
            + jnp.where(node_z == 8, pltpu.roll(mine, 1, 1), 0.0)
            + jnp.where(node_z == 0, pltpu.roll(before, 113, 1), 0.0)
            + jnp.where(node_z == 15, pltpu.roll(after, 15, 1), 0.0)
        )

    def join_wall(mine, before, after):
        later = jnp.where(half == 0, pltpu.roll(mine, 7, 0), pltpu.roll(after, 1, 0))
        earlier = jnp.where(half == 0, pltpu.roll(before, 7, 0), pltpu.roll(mine, 1, 0))
        return (
            mine
            + jnp.where(node_x == 7, pltpu.roll(later, 112, 1), 0.0)
            + jnp.where(node_x == 0, pltpu.roll(earlier, 16, 1), 0.0)
        )

    def receive(target, turn):
        wait_bytes(face_in.at[turn], recv.at[1 + turn])
        into = (
            pl.ds(0, 16),
            pl.ds(240, 16),
            pl.ds(0, 16, stride=16),
            pl.ds(15, 16, stride=16),
        )
        for d in range(4):
            for comp in range(3):
                target[comp, into[d], :] = target[comp, into[d], :] + face_in[turn, d, comp]

    def note(k, value):
        mom[k : k + 1, :] = jnp.sum(value, axis=0, keepdims=True)

    def energy(source, index, comps):
        for comp, (along, across_y) in zip(comps, apply_all(source, comps)):
            inside = jnp.zeros((16, 128), jnp.float32)
            edges = jnp.zeros((16, 128), jnp.float32)
            for i in range(16):
                rows = slice(16 * i, 16 * i + 16)
                term = source[comp, rows] * (
                    along[rows] * joined_y2 + across_y[rows] * both(table[FLAT + i])
                )
                if i % 8 in (0, 7):
                    edges = edges + term
                else:
                    inside = inside + term
            for d, i in ((0, 15), (1, 0)):
                sent = along[256 + 16 * d : 272 + 16 * d] * joined_y2
                edges = edges + sent * source[comp, 16 * i : 16 * i + 16]
            total = fold((inside + 0.5 * edges) * count2)
            for d, first in ((2, 15), (3, 0)):
                sent = along[256 + 16 * d : 272 + 16 * d] * joined_y2
                term = sent * source[comp, pl.ds(first, 16, stride=16), :]
                total = total + fold(term * share_x) * half_y
            note(3 * index + comp, total)

    def weighted(pairs, comps):
        for comp in comps:
            totals = [jnp.zeros((16, 128), jnp.float32) for _ in pairs]
            edges = [jnp.zeros((16, 128), jnp.float32) for _ in pairs]
            for i in range(16):
                for n, (first, second, _) in enumerate(pairs):
                    term = (
                        first[comp, 16 * i : 16 * i + 16] * second[comp, 16 * i : 16 * i + 16]
                    )
                    if i % 8 in (0, 7):
                        edges[n] = edges[n] + term
                    else:
                        totals[n] = totals[n] + term
            for n, (_, _, index) in enumerate(pairs):
                note(3 * index + comp, fold((totals[n] + 0.5 * edges[n]) * count2))

    receive(one, 0)
    operate(one, two, 1)
    hear(1)
    tell(2)
    receive(two, 1)
    products = [(res, res, 0), (res, one, 1), (one, one, 2), (one, two, 3), (two, two, 4)]
    weighted(products, (1,))
    energy(two, 5, (1,))
    wait_bytes(plane_in, recv.at[0])
    wait_bytes(verge_in, recv.at[5])
    raw = {(-dw, -ds): plane_in[d] for d, (dw, ds) in enumerate(SHIFTS)}
    raw[0, 0] = plane[...]
    for d, (dw, ds) in enumerate(FAR_SHIFTS):
        row = wide(verge_in[d])
        if abs(dw) == 2:
            value = pltpu.roll(row, 56 if dw > 0 else 16, 1, stride=8, stride_axis=0)
        else:
            value = pltpu.roll(row, 8 if ds > 0 else 113, 1, stride=1, stride_axis=0)
        raw[-dw, -ds] = value
    none = jnp.zeros((8, 128), jnp.float32)
    square = [(dw, ds) for dw in (-1, 0, 1) for ds in (-1, 0, 1)]
    cross = [(0, 0), (-1, 0), (1, 0), (0, -1), (0, 1)]

    def spans(values, at):
        dw, ds = at
        return join_span(
            values[at], values.get((dw, ds - 1), none), values.get((dw, ds + 1), none)
        )

    def walls(values, at):
        dw, ds = at
        return join_wall(
            values[at], values.get((dw - 1, ds), none), values.get((dw + 1, ds), none)
        )

    def pulled(values):
        fill = [none] * (len(values) % 2)
        product = split_product(jnp.concatenate(list(values) + fill, axis=0), lines[...])
        return [
            (product[8 * n : 8 * n + 8, :128], product[8 * n : 8 * n + 8, 128:])
            for n in range(len(values))
        ]

    mass_flat = table[LANEX] * table[LANEZ]

    def plane_operator(in_x, in_z, value, at):
        return (
            table[LANEZ] * walls(in_x, at)
            + table[LANEX] * spans(in_z, at)
            + (SCALE * inverse_step) * mass_flat * value
        )

    line_of = {at: spans(raw, at) for at in square + [(-2, 0), (2, 0)]}
    stress = {at: walls(line_of, at) for at in square}
    pulls = pulled([stress[at] for at in square])
    in_x = {at: pulls[n][0] for n, at in enumerate(square)}
    in_z = {at: pulls[n][1] for n, at in enumerate(square)}
    first = {at: plane_operator(in_x, in_z, stress[at], at) for at in cross}
    mass_of = {at: mass_flat * stress[at] for at in cross}
    pulls = pulled([first[at] for at in cross] + [mass_of[at] for at in cross])
    seconds = []
    for offset, values in ((0, first), (5, mass_of)):
        in_x = {at: pulls[offset + n][0] for n, at in enumerate(cross)}
        in_z = {at: pulls[offset + n][1] for n, at in enumerate(cross)}
        seconds.append(plane_operator(in_x, in_z, values[0, 0], (0, 0)))

    def raised(doubles, triples, rights, rows):
        parts = []
        for value in doubles:
            parts += [coarse(value), value - coarse(value)]
        for value in triples:
            parts += [coarse(value), value - coarse(value), coarse(value)]
        parts += [none] * (rows // 8 - len(parts))
        return lax.dot_general(
            jnp.concatenate(parts, axis=0),
            rights[:rows],
            (((0,), (0,)), ((), ())),
            preferred_element_type=jnp.float32,
        )

    here, pull, mass_here = stress[0, 0], first[0, 0] * wall_mass, mass_of[0, 0]
    lifted = raised([here], [], lifting, 16)
    lifted_one = raised([pull], [mass_here], lifting, 48)
    lifted_two = raised(
        [seconds[0] * wall_mass * wall_mass],
        [seconds[1], mass_flat * pull, mass_flat * mass_here],
        lifting_two,
        96,
    )
    for comp in range(2):
        for ex in range(2):
            column = (comp * 2 + ex) * 128
            rows = slice(128 * ex, 128 * ex + 128)
            for target, value in ((res, lifted), (one, lifted_one), (two, lifted_two)):
                target[2 * comp, rows] = target[2 * comp, rows] + value[:, column : column + 128]

    weighted(products, (0, 2))
    energy(two, 5, (0, 2))

    mom[18:24, :] = jnp.zeros((6, 128), jnp.float32)
    total = jnp.sum(mom[...], axis=1, keepdims=True)
    row = jnp.zeros((8, 128), jnp.float32)
    for k in range(3):
        row = row + jnp.where(lane8 == 8 * k + sub8, total[8 * k : 8 * k + 8], 0.0)
    part[0] = jnp.sum(row, axis=0, keepdims=True)
    hear(2)
    line_slots, plane_slots = nc * ns, nx * ny
    for ds in sorted(deep_shifts, key=lambda k: -abs(k)):
        if ds:
            push(
                part.at[0], part_in.at[wc * ns + sp], send.at[4], recv.at[3], deep_peer(1, ds)
            )
    relays_sums = wc == 1

    @pl.when(jnp.logical_not(relays_sums))
    def _():
        push(part.at[0], part_in.at[wc * ns + sp], send.at[4], recv.at[3], deep_peer(1, 0))
        wait_bytes(part_in.at[pl.ds(line_slots, plane_slots)], recv.at[4])
        wait_bytes(part_in.at[pl.ds(0, ns)], send.at[4])

    @pl.when(relays_sums)
    def _():
        part_in[wc * ns + sp] = part[0]
        wait_bytes(part_in.at[pl.ds(0, line_slots - 1)], recv.at[3])
        row = part_in[0]
        for k in range(1, line_slots):
            row = row + part_in[k]
        part[1] = row
        slot = line_slots + wx * ny + wy
        for a, b in plain:
            for c in (0, 1):
                push(
                    part.at[1], part_in.at[slot], send.at[5 if c else 7], recv.at[4],
                    (place_x[a], place_y[b], c, sp),
                )
        push(part.at[1], part_in.at[slot], send.at[7], recv.at[4], (wx, wy, 0, sp))
        part_in[slot] = row
        wait_bytes(part_in.at[pl.ds(line_slots, plane_slots - 1)], recv.at[4])
        wait_bytes(part_in.at[pl.ds(0, ns - 1)], send.at[4])
        wait_bytes(part_in.at[pl.ds(line_slots, plane_slots - 1)], send.at[5])
        wait_bytes(part_in.at[pl.ds(line_slots, plane_slots)], send.at[7])

    row = part_in[line_slots]
    for k in range(1, plane_slots):
        row = row + part_in[line_slots + k]

    row = jnp.broadcast_to(row, (8, 128))
    moments = [row if j == 0 else pltpu.roll(row, 128 - 3 * j, 1) for j in range(6)]

    def inner(first, second, raise_by):
        total = None
        for i, a in enumerate(first):
            for j, b in enumerate(second):
                term = a * b * moments[i + j + raise_by]
                total = term if total is None else total + term
        return total

    unit = jnp.ones((8, 128), jnp.float32)
    direction, residual = [unit], [unit]
    answer = [jnp.zeros((8, 128), jnp.float32)] * 3
    norm = moments[0]
    for step in range(3):
        alpha = norm / inner(direction, direction, 1)
        for i, value in enumerate(direction):
            answer[i] = answer[i] + alpha * value
        if step == 2:
            break
        lowered = [-alpha * value for value in direction]
        residual = [residual[0]] + [
            lowered[i] + residual[i + 1] if i + 1 < len(residual) else lowered[i]
            for i in range(len(lowered))
        ]
        newer = inner(residual, residual, 0)
        growth = newer / norm
        direction = [
            value + growth * direction[i] if i < len(direction) else value
            for i, value in enumerate(residual)
        ]
        norm = newer
    for i, value in enumerate(answer):
        scalars[i : i + 1, :] = value[:1] * SCALE
    wait_bytes(slab_in, send.at[0])
    wait_bytes(plane_in, send.at[1])
    wait_bytes(verge_in, send.at[6])
    for turn in range(2):
        wait_bytes(face_in.at[turn], send.at[2 + turn])


def combine(res, one, two, scalars, slopes, out, neumann, sums, sent):
    copies = [pltpu.make_async_copy(slopes, neumann, sent.at[3])]
    copies[0].start()
    for comp in range(3):
        c0, c1, c2 = (
            jnp.broadcast_to(scalars[k : k + 1, comp : comp + 1], (16, 128)) for k in range(3)
        )
        for i in range(16):
            rows = pl.ds(16 * i, 16)
            sums[comp, i] = (
                c0 * res[comp, rows, :] + c1 * one[comp, rows, :] + c2 * two[comp, rows, :]
            )
        copy = pltpu.make_async_copy(sums.at[comp], out.at[comp], sent.at[comp])
        copy.start()
        copies.append(copy)
    for copy in copies:
        copy.wait()


def body(sizes, velocity_old, heights, owner_device, owner_element, ref_coords, roughness):
    nx, ny, nc, ns = sizes
    slots = nc * ns + nx * ny
    f32, i32 = jnp.float32, jnp.int32
    vmem = pl.BlockSpec(memory_space=pltpu.VMEM)
    anywhere = pl.BlockSpec(memory_space=pl.ANY)
    constants, flat, lines = (jnp.asarray(value) for value in tables())
    res, one, two, scalars, slopes = pl.pallas_call(
        functools.partial(kernel, sizes),
        out_shape=(
            pltpu.VMEM((3, 256, 128), f32),
            pltpu.VMEM((3, 256, 128), f32),
            pltpu.VMEM((3, 256, 128), f32),
            pltpu.VMEM((8, 128), f32),
            pltpu.VMEM((2, 512), f32),
        ),
        in_specs=[anywhere] * 9,
        out_specs=(vmem,) * 5,
        scratch_shapes=[
            pltpu.VMEM((3, 16, 16, 128), f32),
            pltpu.SMEM((16,), f32),
            pltpu.VMEM((1, 512), i32),
            pltpu.VMEM((1, 512), i32),
            pltpu.VMEM((3, 512), f32),
            pltpu.VMEM((1, 512), f32),
            pltpu.VMEM(constants.shape, f32),
            pltpu.VMEM(flat.shape, jnp.bfloat16),
            pltpu.VMEM(lines.shape, jnp.bfloat16),
            pltpu.VMEM((256, 256), jnp.bfloat16),
            pltpu.VMEM((48, 512), f32),
            pltpu.VMEM((96, 512), f32),
            pltpu.VMEM((4, 256, 256), jnp.bfloat16),
            pltpu.VMEM((2, 4, 16, 128), f32),
            pltpu.VMEM((2, 2, 4, 16, 128), f32),
            pltpu.VMEM((8, 128), f32),
            pltpu.VMEM((8, 8, 128), f32),
            pltpu.VMEM((2, 1, 128), f32),
            pltpu.VMEM((12, 1, 128), f32),
            pltpu.VMEM((2, 4, 3, 16, 128), f32),
            pltpu.VMEM((2, 4, 3, 16, 128), f32),
            pltpu.VMEM((24, 128), f32),
            pltpu.VMEM((2, 1, 128), f32),
            pltpu.VMEM((slots, 1, 128), f32),
            pltpu.SemaphoreType.DMA((9,)),
            pltpu.SemaphoreType.DMA((8,)),
            pltpu.SemaphoreType.DMA((2,)),
            pltpu.SemaphoreType.DMA((6,)),
            pltpu.SemaphoreType.REGULAR((3,)),
        ],
        compiler_params=pltpu.CompilerParams(collective_id=0, has_side_effects=True),
        name="channel_step",
    )(
        velocity_old,
        heights,
        owner_device.reshape(1, -1),
        owner_element.reshape(1, -1),
        ref_coords,
        roughness.reshape(1, -1),
        constants,
        flat,
        lines,
    )
    return pl.pallas_call(
        combine,
        out_shape=(
            jax.ShapeDtypeStruct((3, 16, 16, 128), f32),
            jax.ShapeDtypeStruct((2, 512), f32),
        ),
        in_specs=[vmem] * 5,
        out_specs=(anywhere, anywhere),
        scratch_shapes=[
            pltpu.VMEM((3, 16, 16, 128), f32),
            pltpu.SemaphoreType.DMA((4,)),
        ],
        name="combine",
    )(
        *(
            pltpu.with_memory_space_constraint(value, pltpu.VMEM)
            for value in (res, one, two, scalars, slopes)
        )
    )


def torus_program(torus):
    sizes = tuple(torus.shape[name] for name in AXES)
    return jax.shard_map(
        functools.partial(body, sizes),
        mesh=torus,
        in_specs=(
            P(None, WALL, "span", None),
            P(),
            P(WALL_SPAN, None),
            P(WALL_SPAN, None),
            P(None, WALL_SPAN),
            P(WALL_SPAN),
        ),
        out_specs=(P(None, WALL, "span", None), P(None, WALL_SPAN)),
        check_vma=False,
    )


def solution(mesh):
    return torus_program(Mesh(mesh.devices.reshape(4, 8, 2, mesh.shape["span"]), AXES))
```

```python
import functools

import jax
import jax.numpy as jnp
import numpy as np
from jax import lax
from jax.experimental import pallas as pl
from jax.experimental.pallas import tpu as pltpu
from jax.sharding import Mesh
from jax.sharding import PartitionSpec as P

AXES = ("wall_0", "wall_1", "wall_2", "span")
WALL_SPAN = AXES
WALL = ("wall_0", "wall_1", "wall_2")
MESH_ID = pl.DeviceIdType.MESH

GLL_NODES = (
    -1.0,
    -0.8717401485096066,
    -0.5917001814331423,
    -0.2092992179024789,
    0.2092992179024789,
    0.5917001814331423,
    0.8717401485096066,
    1.0,
)
GLL_WEIGHTS = (
    0.03571428571428571,
    0.2107042271435061,
    0.3411226924835044,
    0.4124587946587038,
    0.4124587946587038,
    0.3411226924835044,
    0.2107042271435061,
    0.03571428571428571,
)
viscosity = 0.02
inverse_step = 20.0
karman = 0.41
sample_height = 0.1
speed_floor = 0.01
element_dx = 0.05
element_dz = 0.13
precise = lax.Precision.HIGHEST

SCALE = 64.0

SHIFTS = ((1, 0), (-1, 0), (0, 1), (0, -1), (1, 1), (1, -1), (-1, 1), (-1, -1))

FAR_SHIFTS = (
    (2, 0), (2, 1), (2, -1), (-2, 0), (-2, 1), (-2, -1),
    (0, 2), (1, 2), (-1, 2), (0, -2), (1, -2), (-1, -2),
)

MZ, QMZ, COUNT, LAG, PLANE, HALFW, LAST, FIRST, LANEX, LANEZ = range(10)
BLOCK, LIFT, FLAT = 10, 26, 30


def stiffness_table():
    points = np.array(GLL_NODES)
    weights = np.array(GLL_WEIGHTS)
    previous = np.ones(8)
    current = points.copy()
    for degree in range(1, 7):
        previous, current = (
            current,
            ((2 * degree + 1) * points * current - degree * previous) / (degree + 1),
        )
    derivative = np.zeros((8, 8))
    for target in range(8):
        for source in range(8):
            if target != source:
                derivative[target, source] = (
                    current[target] / current[source] / (points[target] - points[source])
                )
    derivative[0, 0] = -14.0
    derivative[7, 7] = 14.0
    return derivative.T @ (weights[:, None] * derivative)


def tables():
    weights = np.array(GLL_WEIGHTS)
    points = np.array(GLL_NODES)
    stiffness = stiffness_table()
    ones = np.ones((8, 128))
    lane = np.arange(128)
    ends = np.array([2.0, 1, 1, 1, 1, 1, 1, 2.0])
    mass_x = 0.5 * element_dx * weights
    mass_z = 0.5 * element_dz * weights
    count_y = np.where((lane % 8 == 0) | (lane % 8 == 7), 0.5, 1.0)
    count_y[0] = count_y[127] = 1.0
    gaps = points[:, None] - points[None, :] + np.eye(8)
    rows = [
        mass_z[:, None] * ones,
        (mass_z * ends)[:, None] * ones,
        (1.0 / ends)[:, None] * count_y[None, :],
        (1.0 / np.prod(gaps, axis=1))[:, None] * ones,
        ones * (mass_x[lane // 16] * mass_z[lane % 8])[None, :],
        ones * (0.5 * weights[lane % 8])[None, :],
        ones * ((lane % 8 == 7) & (lane < 127))[None, :],
        ones * ((lane % 8 == 0) & (lane > 0))[None, :],
    ]
    block = np.kron(np.eye(16), SCALE * viscosity * 2.0 * stiffness)
    lift = np.zeros((8, 512))
    for comp in range(2):
        for half in range(2):
            column = (comp * 2 + half) * 128
            lift[comp * 4 + half, column] = 1.0
            lift[comp * 4 + 2 + half, column + 127] = 1.0
    joined_x = np.tile(mass_x * ends, 2)
    joined_z = np.tile(mass_z * ends, 2)

    def chain(length):
        scaled = SCALE * viscosity * (2.0 / length) * stiffness
        full = np.kron(np.eye(2), scaled)
        ends_only = full[[15, 0]]
        full[7] = full[8] = full[7] + full[8]
        return full, ends_only

    chain_x, ends_x = chain(element_dx)
    chain_z, ends_z = chain(element_dz)
    flat = np.kron(chain_x, np.diag(joined_z)) + np.kron(np.diag(joined_x), chain_z)
    flat += SCALE * inverse_step * np.diag(np.kron(joined_x, joined_z))
    faces = [np.kron(ends_x[d : d + 1], np.diag(joined_z)) for d in range(2)]
    faces += [np.kron(np.diag(joined_x), ends_z[d : d + 1]) for d in range(2)]
    flat = np.concatenate([flat] + faces).astype(np.float32)
    flat_high = flat.astype(jnp.bfloat16)
    flat_low = (flat - flat_high.astype(np.float32)).astype(jnp.bfloat16)
    line_x = SCALE * viscosity * (2.0 / element_dx) * stiffness
    line_z = SCALE * viscosity * (2.0 / element_dz) * stiffness
    line = np.concatenate([np.kron(line_x.T, np.eye(16)), np.kron(np.eye(16), line_z.T)], axis=1)
    line_high = line.astype(np.float32).astype(jnp.bfloat16)
    line_low = (line.astype(np.float32) - line_high.astype(np.float32)).astype(jnp.bfloat16)
    lines = np.concatenate([line_high, line_low])
    rows += [
        ones * (mass_x * ends)[lane // 16][None, :],
        ones * (mass_z * ends)[lane % 8][None, :],
    ]
    pieces = [np.stack(rows), block.reshape(16, 8, 128), lift.reshape(8, 4, 128).transpose(1, 0, 2)]
    pieces += [joined_x[:, None, None] * (mass_z * ends)[None, :, None] * np.ones((16, 8, 128))]
    return np.concatenate(pieces).astype(np.float32), np.stack([flat_high, flat_low]), lines


def kernel(sizes, *refs):
    operands, refs = refs[:9], refs[9:]
    (res, one, two, scalars, neumann), refs = refs[:5], refs[5:]
    local, refs = refs[:9], refs[9:]
    velocity, heights, owner, element, coords, roughness, table, flat, lines = local
    (normal, lifting, lifting_two, right, slab, slab_in, plane, plane_in,
     verge, verge_in, face, face_in, mom, part, part_in,
     load, send, slab_recv, recv, ready) = refs
    nx, ny, nc, ns = sizes
    nw = nx * ny * nc
    loads = [
        pltpu.make_async_copy(source, target, load.at[n])
        for n, (source, target) in enumerate(zip(operands, local))
    ]
    for copy in loads:
        copy.start()
    wx, wy, wc, sp = (lax.axis_index(name) for name in AXES)
    wall = (wx * ny + wy) * nc + wc
    weights = np.array(GLL_WEIGHTS)
    stiffness = stiffness_table()
    mass_x = [float(v) for v in 0.5 * element_dx * weights]
    ends = [2.0, 1.0, 1.0, 1.0, 1.0, 1.0, 1.0, 2.0]

    def ring(value, shift, count):
        if shift > 0:
            return jnp.where(value >= count - shift, value + shift - count, value + shift)
        return jnp.where(value < -shift, value + shift + count, value + shift)

    def beside(dw):
        if dw == 0:
            return wx, wy, wc
        sign = 1 if dw > 0 else -1
        if abs(dw) == 2:
            turn_y = wy == (ny - 1 if dw > 0 else 0)
            return jnp.where(turn_y, ring(wx, sign, nx), wx), ring(wy, sign, ny), wc
        turn = wc == (nc - 1 if dw > 0 else 0)
        turn_y = jnp.logical_and(turn, wy == (ny - 1 if dw > 0 else 0))
        return (
            jnp.where(turn_y, ring(wx, dw, nx), wx),
            jnp.where(turn, ring(wy, dw, ny), wy),
            ring(wc, dw, nc),
        )

    along = {dw: beside(dw) for dw in (-2, -1, 0, 1, 2)}
    across = {k: ring(sp, k, ns) if k else sp for k in (-2, -1, 0, 1, 2)}
    neighbours = [(*along[dw], across[ds]) for dw, ds in SHIFTS]
    distant = [(*along[dw], across[ds]) for dw, ds in FAR_SHIFTS]
    place_x = {0: wx, 1: ring(wx, 1, nx), -1: ring(wx, -1, nx), 2: ring(wx, 2, nx)}
    place_y = {k: ring(wy, k, ny) if k else wy for k in range(-(ny // 2) + 1, ny // 2 + 1)}
    place_y[-2] = ring(wy, -2, ny)
    place_z = {k: ring(sp, k, ns) if k else sp for k in range(-(ns // 2) + 1, ns // 2 + 1)}
    place_z[-2] = ring(sp, -2, ns)
    other = ring(wc, 1, nc)
    flat_peer = lambda dx, dy: (place_x[dx], place_y[dy], wc, sp)
    deep_peer = lambda c, ds: (wx, wy, c, place_z[ds])

    def far_first(keys):
        return sorted(keys, key=lambda key: -abs(key[0]) - abs(key[1]))

    deep_shifts = range(-(ns // 2) + 1, ns // 2 + 1)
    wide_x = [k for k in (-1, 0, 1, 2) if -(nx // 2) < k <= nx // 2]
    plain = far_first([(a, b) for a in wide_x for b in range(-(ny // 2) + 1, ny // 2 + 1)])
    plain = [key for key in plain if key != (0, 0)]

    barrier = pltpu.get_barrier_semaphore()
    near = neighbours[:4] + [deep_peer(other, 0)]
    near += [(*along[2], sp), (*along[-2], sp), (*along[0], across[2]), (*along[0], across[-2])]
    near += [flat_peer(1, 0), flat_peer(-1, 0), flat_peer(0, 1), flat_peer(0, -1)]
    for peer in near:
        pl.semaphore_signal(barrier, inc=1, device_id=peer, device_id_type=MESH_ID)
    relays = [
        near,
        [flat_peer(1, 0), flat_peer(-1, 0), flat_peer(0, 2), flat_peer(0, -2)]
        + [deep_peer(wc, 2), deep_peer(wc, -2)],
        [flat_peer(1, 0), flat_peer(-1, 0), flat_peer(0, 2), flat_peer(0, -2)]
        + [flat_peer(2, 2), flat_peer(2, -2), deep_peer(wc, 4), deep_peer(wc, -4)],
    ]

    def tell(n):
        for peer in relays[n]:
            pl.semaphore_signal(ready.at[n], inc=1, device_id=peer, device_id_type=MESH_ID)

    def hear(n):
        pl.semaphore_wait(ready.at[n], len(relays[n]))

    def push(source, target, send_sem, recv_sem, peer):
        pltpu.make_async_remote_copy(
            src_ref=source,
            dst_ref=target,
            send_sem=send_sem,
            recv_sem=recv_sem,
            device_id=peer,
            device_id_type=MESH_ID,
        ).start()

    def wait_bytes(like, sem):
        pltpu.make_async_copy(like, like, sem).wait()

    loads[0].wait()

    lane = lax.broadcasted_iota(jnp.int32, (1, 128), 1)
    sub8 = lax.broadcasted_iota(jnp.int32, (8, 128), 0)
    lane8 = lax.broadcasted_iota(jnp.int32, (8, 128), 1)

    for comp in range(2):
        quarters = []
        for k in range(4):
            quarters.append(velocity[2 * comp, 4 * k : 4 * k + 4].reshape(64, 128))
        packed = jnp.zeros((64, 128), jnp.float32)
        where_to = lax.broadcasted_iota(jnp.int32, (64, 128), 1)
        for k in range(4):
            low = pltpu.roll(quarters[k], 32 * k, 1) if k else quarters[k]
            shift = (32 * k + 32) % 128
            high = pltpu.roll(quarters[k], shift, 1) if shift else quarters[k]
            packed = jnp.where(where_to // 16 == 2 * k, low, packed)
            packed = jnp.where(where_to // 16 == 2 * k + 1, high, packed)
        slab[comp] = packed.reshape(4, 16, 128)

    for copy in loads[1:]:
        copy.wait()
    height = jnp.zeros((8, 128), jnp.float32)
    for layer in range(16):
        height = jnp.where(lane8 // 8 == layer, heights[layer], height)
    mass_y = height * table[HALFW]
    block = table[BLOCK : BLOCK + 16].reshape(128, 128) * (1.0 / height)[:1]
    block = (
        block
        + table[LAST][:1] * pltpu.roll(block, 127, 1)
        + table[FIRST][:1] * pltpu.roll(block, 1, 1)
    )

    def split(value):
        high = value.astype(jnp.bfloat16)
        return high, (value - high.astype(jnp.float32)).astype(jnp.bfloat16)

    def split_product(left, right):
        rows = left.shape[0]
        high, low = split(left)
        product = jnp.dot(
            jnp.concatenate(
                [
                    jnp.concatenate([high, high], axis=1),
                    jnp.concatenate([low, jnp.zeros_like(low)], axis=1),
                ],
                axis=0,
            ),
            right,
            preferred_element_type=jnp.float32,
        )
        return product[:rows] + product[rows:]

    block_high, block_low = split(block)
    normal[:128, :128] = block_high
    normal[128:, :128] = block_high
    normal[:128, 128:] = block_low
    normal[128:, 128:] = jnp.zeros((128, 128), jnp.bfloat16)
    right[...] = jnp.zeros(right.shape, jnp.bfloat16)
    side = sub8 // 2 % 2
    wall_row = jnp.where(side == 0, block[:1], block[127:])
    lift = jnp.concatenate([table[LIFT + k] for k in range(4)], axis=1)
    home = (sub8 // 4 * 2 + sub8 % 2)[:, :1]
    joined_y = (
        mass_y
        + table[LAST] * pltpu.roll(mass_y, 127, 1)
        + table[FIRST] * pltpu.roll(mass_y, 1, 1)
    )
    both = lambda value: jnp.concatenate([value, value], axis=0)
    joined_y2 = both(joined_y)
    count2 = both(table[COUNT])

    def at_home(value):
        return jnp.concatenate([jnp.where(home == k, value, 0.0) for k in range(4)], axis=1)

    def coarse(value):
        return value.astype(jnp.bfloat16).astype(jnp.float32)

    twice = jnp.dot(wall_row, block, precision=precise, preferred_element_type=jnp.float32)
    pieces, pieces_two = [lift, lift], [lift, lift]
    for n, value in enumerate((wall_row, joined_y * wall_row, wall_row, twice)):
        rises = at_home(value)
        high = coarse(rises)
        triple = [high, high, rises - high]
        if n == 0:
            pieces += triple
        else:
            pieces_two += triple
    for n, value in enumerate(pieces):
        lifting[8 * n : 8 * n + 8] = value
    lifting[40:] = jnp.zeros((8, 512), jnp.float32)
    for n, value in enumerate(pieces_two):
        lifting_two[8 * n : 8 * n + 8] = value
    lifting_two[88:] = jnp.zeros((8, 512), jnp.float32)
    wall_mass = jnp.where(side == 0, joined_y[:, :1], joined_y[:, 127:])
    scale_zy = both(table[QMZ] * joined_y) * inverse_step
    for comp in range(3):
        for i in range(16):
            res[comp, 16 * i : 16 * i + 16] = velocity[comp, i] * (
                scale_zy * (mass_x[i % 8] * ends[i % 8])
            )

    row16 = lax.broadcasted_iota(jnp.int32, (16, 128), 0) % 8
    share_x = jnp.where(jnp.logical_or(row16 == 0, row16 == 7), 0.5, 1.0)
    half_y = jnp.broadcast_to(table[COUNT][:1], (8, 128))

    def fold(value):
        return value[:8] + value[8:]

    def apply(source, comp):
        high, low = split(source[comp])
        parts = jnp.concatenate([high, low], axis=1)
        along = jnp.dot(flat[0], parts, preferred_element_type=jnp.float32)
        along = along[:, :128] + along[:, 128:]
        along = along + jnp.dot(flat[1], high, preferred_element_type=jnp.float32)
        across_y = jnp.dot(parts, normal[...], preferred_element_type=jnp.float32)
        return along, across_y[:, :128] + across_y[:, 128:]

    def send_face(turn, d, comp):
        push(
            face.at[turn, d, comp], face_in.at[turn, d, comp], send.at[2 + turn],
            recv.at[1 + turn], neighbours[d],
        )

    def operate(source, target, turn):
        for comp in range(3):
            along, across_y = apply(source, comp)
            for d in range(4):
                rows = slice(256 + 16 * d, 272 + 16 * d)
                face[turn, d, comp] = along[rows] * joined_y2
                if turn:
                    send_face(turn, d, comp)
            for i in range(16):
                rows = slice(16 * i, 16 * i + 16)
                target[comp, rows] = along[rows] * joined_y2 + across_y[rows] * both(
                    table[FLAT + i]
                )

    operate(res, one, 0)
    pl.semaphore_wait(barrier, len(near))

    for d in range(2):
        push(slab, slab_in.at[d], send.at[0], slab_recv.at[d], neighbours[d])
    tell(0)
    for comp in range(3):
        for d in range(4):
            send_face(0, d, comp)

    def regroup(blocks):
        upper = (lane // 8) % 2 == 1
        result = []
        for ex in range(2):
            low, high = blocks[ex], blocks[2 + ex]
            result.append(jnp.where(upper, pltpu.roll(high, 8, 1), low))
            result.append(jnp.where(upper, high, pltpu.roll(low, 120, 1)))
        return result

    def ungroup(values):
        upper = (lane // 8) % 2 == 1
        low, high = [], []
        for ex in range(2):
            a, b = values[2 * ex], values[2 * ex + 1]
            low.append(jnp.where(upper, pltpu.roll(b, 8, 1), a))
            high.append(jnp.where(upper, b, pltpu.roll(a, 120, 1)))
        return low + high

    wide = lambda row: jnp.broadcast_to(row, (8, 128))
    quarter = lambda ref, row, q: ref[row : row + 1, 128 * q : 128 * q + 128]
    distance = [(quarter(owner, 0, q) - wall + nw) % nw for q in range(4)]
    to_next = regroup([wide(jnp.where(d == 1, 1.0, 0.0)) for d in distance])
    to_prev = regroup([wide(jnp.where(d == nw - 1, 1.0, 0.0)) for d in distance])
    layer = regroup([wide((quarter(element, 0, q) % 2).astype(jnp.float32)) for q in range(4)])
    axes = [regroup([wide(quarter(coords, k, q)) for q in range(4)]) for k in range(3)]

    def lagrange(coord):
        value = table[LAG]
        for b in range(8):
            value = value * jnp.where(sub8 == b, 1.0, coord - GLL_NODES[b])
        return value

    basis = [[lagrange(axes[k][g]) for k in range(3)] for g in range(4)]
    second_wall = (lane // 8) % 2 == 1
    for g in range(4):
        ly = basis[g][2]
        blocks = []
        for side in range(2):
            for ey in range(2):
                chosen = jnp.logical_and(
                    wide(second_wall) == (side == 1), layer[g] == float(ey)
                )
                blocks.append(jnp.where(chosen, ly, 0.0))
        high, low = split(jnp.concatenate(blocks, axis=0))
        for kk in range(2):
            k = 2 * (g // 2) + kk
            column = slice(128 * kk, 128 * kk + 128)
            right[g, 32 * k : 32 * k + 32, column] = high
            right[g, 128 + 32 * k : 160 + 32 * k, column] = low

    masks = [[1.0 - to_next[g] - to_prev[g], to_prev[g], to_next[g]] for g in range(4)]

    def sample(source, g):
        ez = g % 2
        product = split_product(
            source[:, :, 8 * ez : 8 * ez + 8, :].reshape(64, 128), right[g]
        )
        total = [jnp.zeros((8, 128), jnp.float32) for _ in range(2)]
        for kk in range(2):
            values = product[:, 128 * kk : 128 * kk + 128].reshape(2, 4, 8, 128)
            for comp in range(2):
                for x in range(4):
                    a = 4 * kk + x
                    total[comp] = total[comp] + values[comp, x] * basis[g][0][a : a + 1]
        return total

    sums = []
    for g in range(4):
        own = sample(slab, g)
        sums.append([own[comp] * masks[g][0] for comp in range(2)])
    for d in range(2):
        wait_bytes(slab_in.at[d], slab_recv.at[d])
        for g in range(4):
            far = sample(slab_in.at[d], g)
            for comp in range(2):
                sums[g][comp] = sums[g][comp] + far[comp] * masks[g][1 + d]
    stream = ungroup(
        [wide(jnp.sum(sums[g][0] * basis[g][1], axis=0, keepdims=True)) for g in range(4)]
    )
    spanwise = ungroup(
        [wide(jnp.sum(sums[g][1] * basis[g][1], axis=0, keepdims=True)) for g in range(4)]
    )

    for q in range(4):
        u, v = stream[q], spanwise[q]
        speed = jnp.sqrt(u * u + v * v + speed_floor)
        ratio = karman / jnp.log(sample_height / wide(quarter(roughness, 0, q)))
        factor = -(ratio * ratio * speed / viscosity)
        for comp, value in enumerate((u, v)):
            slope = factor * value
            neumann[comp : comp + 1, 128 * q : 128 * q + 128] = slope[:1]
            plane[comp * 4 + q : comp * 4 + q + 1, :] = (viscosity * slope * table[PLANE])[:1]

    mine = plane[...]
    lines_x = jnp.zeros((8, 128), jnp.float32)
    for q in range(4):
        here = jnp.logical_and(sub8 == 2 * q + 1, lane8 // 16 == 3 - q)
        lines_x = jnp.where(here, pltpu.roll(mine, (16 * (3 - q) - 112) % 128, 1), lines_x)
        here = jnp.logical_and(sub8 == 2 * q, lane8 // 16 == 7 - q)
        lines_x = jnp.where(here, pltpu.roll(mine, (64 + 16 * (3 - q)) % 128, 1), lines_x)
    lines_z = jnp.zeros((8, 128), jnp.float32)
    for r in range(8):
        here = jnp.logical_and(sub8 == r, lane8 % 16 == 7 - r)
        lines_z = jnp.where(here, pltpu.roll(mine, (7 - r - 15) % 128, 1), lines_z)
        here = jnp.logical_and(sub8 == r, lane8 % 16 == 15 - r)
        lines_z = jnp.where(here, pltpu.roll(mine, (15 - r) % 128, 1), lines_z)
    verge[0] = jnp.sum(lines_x, axis=0, keepdims=True)
    verge[1] = jnp.sum(lines_z, axis=0, keepdims=True)
    hear(0)
    for d, (dw, ds) in enumerate(FAR_SHIFTS):
        push(
            verge.at[0 if abs(dw) == 2 else 1], verge_in.at[d], send.at[6], recv.at[5], distant[d]
        )
    for d in range(8):
        push(plane, plane_in.at[d], send.at[1], recv.at[0], neighbours[d])
    tell(1)

    node_z = lane8 % 16
    node_x = lane8 // 16
    half = sub8 % 2

    def join_span(mine, before, after):
        return (
            mine
            + jnp.where(node_z == 7, pltpu.roll(mine, 127, 1), 0.0)
            + jnp.where(node_z == 8, pltpu.roll(mine, 1, 1), 0.0)
            + jnp.where(node_z == 0, pltpu.roll(before, 113, 1), 0.0)
            + jnp.where(node_z == 15, pltpu.roll(after, 15, 1), 0.0)
        )

    def join_wall(mine, before, after):
        later = jnp.where(half == 0, pltpu.roll(mine, 7, 0), pltpu.roll(after, 1, 0))
        earlier = jnp.where(half == 0, pltpu.roll(before, 7, 0), pltpu.roll(mine, 1, 0))
        return (
            mine
            + jnp.where(node_x == 7, pltpu.roll(later, 112, 1), 0.0)
            + jnp.where(node_x == 0, pltpu.roll(earlier, 16, 1), 0.0)
        )

    def receive(target, turn):
        wait_bytes(face_in.at[turn], recv.at[1 + turn])
        into = (
            pl.ds(0, 16),
            pl.ds(240, 16),
            pl.ds(0, 16, stride=16),
            pl.ds(15, 16, stride=16),
        )
        for d in range(4):
            for comp in range(3):
                target[comp, into[d], :] = target[comp, into[d], :] + face_in[turn, d, comp]

    def note(k, value):
        mom[k : k + 1, :] = jnp.sum(value, axis=0, keepdims=True)

    def energy(source, index, comps):
        for comp in comps:
            along, across_y = apply(source, comp)
            inside = jnp.zeros((16, 128), jnp.float32)
            edges = jnp.zeros((16, 128), jnp.float32)
            for i in range(16):
                rows = slice(16 * i, 16 * i + 16)
                term = source[comp, rows] * (
                    along[rows] * joined_y2 + across_y[rows] * both(table[FLAT + i])
                )
                if i % 8 in (0, 7):
                    edges = edges + term
                else:
                    inside = inside + term
            for d, i in ((0, 15), (1, 0)):
                sent = along[256 + 16 * d : 272 + 16 * d] * joined_y2
                edges = edges + sent * source[comp, 16 * i : 16 * i + 16]
            total = fold((inside + 0.5 * edges) * count2)
            for d, first in ((2, 15), (3, 0)):
                sent = along[256 + 16 * d : 272 + 16 * d] * joined_y2
                term = sent * source[comp, pl.ds(first, 16, stride=16), :]
                total = total + fold(term * share_x) * half_y
            note(3 * index + comp, total)

    def weighted(pairs, comps):
        for comp in comps:
            totals = [jnp.zeros((16, 128), jnp.float32) for _ in pairs]
            edges = [jnp.zeros((16, 128), jnp.float32) for _ in pairs]
            for i in range(16):
                for n, (first, second, _) in enumerate(pairs):
                    term = (
                        first[comp, 16 * i : 16 * i + 16] * second[comp, 16 * i : 16 * i + 16]
                    )
                    if i % 8 in (0, 7):
                        edges[n] = edges[n] + term
                    else:
                        totals[n] = totals[n] + term
            for n, (_, _, index) in enumerate(pairs):
                note(3 * index + comp, fold((totals[n] + 0.5 * edges[n]) * count2))

    receive(one, 0)
    operate(one, two, 1)
    hear(1)
    tell(2)
    receive(two, 1)
    products = [(res, res, 0), (res, one, 1), (one, one, 2), (one, two, 3), (two, two, 4)]
    weighted(products, (1,))
    energy(two, 5, (1,))
    wait_bytes(plane_in, recv.at[0])
    wait_bytes(verge_in, recv.at[5])
    raw = {(-dw, -ds): plane_in[d] for d, (dw, ds) in enumerate(SHIFTS)}
    raw[0, 0] = plane[...]
    for d, (dw, ds) in enumerate(FAR_SHIFTS):
        row = wide(verge_in[d])
        if abs(dw) == 2:
            value = pltpu.roll(row, 56 if dw > 0 else 16, 1, stride=8, stride_axis=0)
        else:
            value = pltpu.roll(row, 8 if ds > 0 else 113, 1, stride=1, stride_axis=0)
        raw[-dw, -ds] = value
    none = jnp.zeros((8, 128), jnp.float32)
    square = [(dw, ds) for dw in (-1, 0, 1) for ds in (-1, 0, 1)]
    cross = [(0, 0), (-1, 0), (1, 0), (0, -1), (0, 1)]

    def spans(values, at):
        dw, ds = at
        return join_span(
            values[at], values.get((dw, ds - 1), none), values.get((dw, ds + 1), none)
        )

    def walls(values, at):
        dw, ds = at
        return join_wall(
            values[at], values.get((dw - 1, ds), none), values.get((dw + 1, ds), none)
        )

    def pulled(values):
        fill = [none] * (len(values) % 2)
        product = split_product(jnp.concatenate(list(values) + fill, axis=0), lines[...])
        return [
            (product[8 * n : 8 * n + 8, :128], product[8 * n : 8 * n + 8, 128:])
            for n in range(len(values))
        ]

    mass_flat = table[LANEX] * table[LANEZ]

    def plane_operator(in_x, in_z, value, at):
        return (
            table[LANEZ] * walls(in_x, at)
            + table[LANEX] * spans(in_z, at)
            + (SCALE * inverse_step) * mass_flat * value
        )

    line_of = {at: spans(raw, at) for at in square + [(-2, 0), (2, 0)]}
    stress = {at: walls(line_of, at) for at in square}
    pulls = pulled([stress[at] for at in square])
    in_x = {at: pulls[n][0] for n, at in enumerate(square)}
    in_z = {at: pulls[n][1] for n, at in enumerate(square)}
    first = {at: plane_operator(in_x, in_z, stress[at], at) for at in cross}
    mass_of = {at: mass_flat * stress[at] for at in cross}
    pulls = pulled([first[at] for at in cross] + [mass_of[at] for at in cross])
    seconds = []
    for offset, values in ((0, first), (5, mass_of)):
        in_x = {at: pulls[offset + n][0] for n, at in enumerate(cross)}
        in_z = {at: pulls[offset + n][1] for n, at in enumerate(cross)}
        seconds.append(plane_operator(in_x, in_z, values[0, 0], (0, 0)))

    def raised(doubles, triples, rights, rows):
        parts = []
        for value in doubles:
            parts += [coarse(value), value - coarse(value)]
        for value in triples:
            parts += [coarse(value), value - coarse(value), coarse(value)]
        parts += [none] * (rows // 8 - len(parts))
        return lax.dot_general(
            jnp.concatenate(parts, axis=0),
            rights[:rows],
            (((0,), (0,)), ((), ())),
            preferred_element_type=jnp.float32,
        )

    here, pull, mass_here = stress[0, 0], first[0, 0] * wall_mass, mass_of[0, 0]
    lifted = raised([here], [], lifting, 16)
    lifted_one = raised([pull], [mass_here], lifting, 48)
    lifted_two = raised(
        [seconds[0] * wall_mass * wall_mass],
        [seconds[1], mass_flat * pull, mass_flat * mass_here],
        lifting_two,
        96,
    )
    for comp in range(2):
        for ex in range(2):
            column = (comp * 2 + ex) * 128
            rows = slice(128 * ex, 128 * ex + 128)
            for target, value in ((res, lifted), (one, lifted_one), (two, lifted_two)):
                target[2 * comp, rows] = target[2 * comp, rows] + value[:, column : column + 128]

    weighted(products, (0, 2))
    energy(two, 5, (0, 2))

    mom[18:24, :] = jnp.zeros((6, 128), jnp.float32)
    total = jnp.sum(mom[...], axis=1, keepdims=True)
    row = jnp.zeros((8, 128), jnp.float32)
    for k in range(3):
        row = row + jnp.where(lane8 == 8 * k + sub8, total[8 * k : 8 * k + 8], 0.0)
    part[0] = jnp.sum(row, axis=0, keepdims=True)
    hear(2)
    line_slots, plane_slots = nc * ns, nx * ny
    for ds in sorted(deep_shifts, key=lambda k: -abs(k)):
        if ds:
            push(
                part.at[0], part_in.at[wc * ns + sp], send.at[4], recv.at[3], deep_peer(1, ds)
            )
    relays_sums = wc == 1

    @pl.when(jnp.logical_not(relays_sums))
    def _():
        push(part.at[0], part_in.at[wc * ns + sp], send.at[4], recv.at[3], deep_peer(1, 0))
        wait_bytes(part_in.at[pl.ds(line_slots, plane_slots)], recv.at[4])
        wait_bytes(part_in.at[pl.ds(0, ns)], send.at[4])

    @pl.when(relays_sums)
    def _():
        part_in[wc * ns + sp] = part[0]
        wait_bytes(part_in.at[pl.ds(0, line_slots - 1)], recv.at[3])
        row = part_in[0]
        for k in range(1, line_slots):
            row = row + part_in[k]
        part[1] = row
        slot = line_slots + wx * ny + wy
        for a, b in plain:
            for c in (0, 1):
                push(
                    part.at[1], part_in.at[slot], send.at[5 if c else 7], recv.at[4],
                    (place_x[a], place_y[b], c, sp),
                )
        push(part.at[1], part_in.at[slot], send.at[7], recv.at[4], (wx, wy, 0, sp))
        part_in[slot] = row
        wait_bytes(part_in.at[pl.ds(line_slots, plane_slots - 1)], recv.at[4])
        wait_bytes(part_in.at[pl.ds(0, ns - 1)], send.at[4])
        wait_bytes(part_in.at[pl.ds(line_slots, plane_slots - 1)], send.at[5])
        wait_bytes(part_in.at[pl.ds(line_slots, plane_slots)], send.at[7])

    row = part_in[line_slots]
    for k in range(1, plane_slots):
        row = row + part_in[line_slots + k]

    row = jnp.broadcast_to(row, (8, 128))
    moments = [row if j == 0 else pltpu.roll(row, 128 - 3 * j, 1) for j in range(6)]

    def inner(first, second, raise_by):
        total = None
        for i, a in enumerate(first):
            for j, b in enumerate(second):
                term = a * b * moments[i + j + raise_by]
                total = term if total is None else total + term
        return total

    unit = jnp.ones((8, 128), jnp.float32)
    direction, residual = [unit], [unit]
    answer = [jnp.zeros((8, 128), jnp.float32)] * 3
    norm = moments[0]
    for step in range(3):
        alpha = norm / inner(direction, direction, 1)
        for i, value in enumerate(direction):
            answer[i] = answer[i] + alpha * value
        if step == 2:
            break
        lowered = [-alpha * value for value in direction]
        residual = [residual[0]] + [
            lowered[i] + residual[i + 1] if i + 1 < len(residual) else lowered[i]
            for i in range(len(lowered))
        ]
        newer = inner(residual, residual, 0)
        growth = newer / norm
        direction = [
            value + growth * direction[i] if i < len(direction) else value
            for i, value in enumerate(residual)
        ]
        norm = newer
    for i, value in enumerate(answer):
        scalars[i : i + 1, :] = value[:1] * SCALE
    wait_bytes(slab_in, send.at[0])
    wait_bytes(plane_in, send.at[1])
    wait_bytes(verge_in, send.at[6])
    for turn in range(2):
        wait_bytes(face_in.at[turn], send.at[2 + turn])


def combine(res, one, two, scalars, slopes, out, neumann, sums, sent):
    copies = [pltpu.make_async_copy(slopes, neumann, sent.at[3])]
    copies[0].start()
    for comp in range(3):
        c0, c1, c2 = (
            jnp.broadcast_to(scalars[k : k + 1, comp : comp + 1], (16, 128)) for k in range(3)
        )
        for i in range(16):
            rows = pl.ds(16 * i, 16)
            sums[comp, i] = (
                c0 * res[comp, rows, :] + c1 * one[comp, rows, :] + c2 * two[comp, rows, :]
            )
        copy = pltpu.make_async_copy(sums.at[comp], out.at[comp], sent.at[comp])
        copy.start()
        copies.append(copy)
    for copy in copies:
        copy.wait()


def body(sizes, velocity_old, heights, owner_device, owner_element, ref_coords, roughness):
    nx, ny, nc, ns = sizes
    slots = nc * ns + nx * ny
    f32, i32 = jnp.float32, jnp.int32
    vmem = pl.BlockSpec(memory_space=pltpu.VMEM)
    anywhere = pl.BlockSpec(memory_space=pl.ANY)
    constants, flat, lines = (jnp.asarray(value) for value in tables())
    res, one, two, scalars, slopes = pl.pallas_call(
        functools.partial(kernel, sizes),
        out_shape=(
            pltpu.VMEM((3, 256, 128), f32),
            pltpu.VMEM((3, 256, 128), f32),
            pltpu.VMEM((3, 256, 128), f32),
            pltpu.VMEM((8, 128), f32),
            pltpu.VMEM((2, 512), f32),
        ),
        in_specs=[anywhere] * 9,
        out_specs=(vmem,) * 5,
        scratch_shapes=[
            pltpu.VMEM((3, 16, 16, 128), f32),
            pltpu.SMEM((16,), f32),
            pltpu.VMEM((1, 512), i32),
            pltpu.VMEM((1, 512), i32),
            pltpu.VMEM((3, 512), f32),
            pltpu.VMEM((1, 512), f32),
            pltpu.VMEM(constants.shape, f32),
            pltpu.VMEM(flat.shape, jnp.bfloat16),
            pltpu.VMEM(lines.shape, jnp.bfloat16),
            pltpu.VMEM((256, 256), jnp.bfloat16),
            pltpu.VMEM((48, 512), f32),
            pltpu.VMEM((96, 512), f32),
            pltpu.VMEM((4, 256, 256), jnp.bfloat16),
            pltpu.VMEM((2, 4, 16, 128), f32),
            pltpu.VMEM((2, 2, 4, 16, 128), f32),
            pltpu.VMEM((8, 128), f32),
            pltpu.VMEM((8, 8, 128), f32),
            pltpu.VMEM((2, 1, 128), f32),
            pltpu.VMEM((12, 1, 128), f32),
            pltpu.VMEM((2, 4, 3, 16, 128), f32),
            pltpu.VMEM((2, 4, 3, 16, 128), f32),
            pltpu.VMEM((24, 128), f32),
            pltpu.VMEM((2, 1, 128), f32),
            pltpu.VMEM((slots, 1, 128), f32),
            pltpu.SemaphoreType.DMA((9,)),
            pltpu.SemaphoreType.DMA((8,)),
            pltpu.SemaphoreType.DMA((2,)),
            pltpu.SemaphoreType.DMA((6,)),
            pltpu.SemaphoreType.REGULAR((3,)),
        ],
        compiler_params=pltpu.CompilerParams(collective_id=0, has_side_effects=True),
        name="channel_step",
    )(
        velocity_old,
        heights,
        owner_device.reshape(1, -1),
        owner_element.reshape(1, -1),
        ref_coords,
        roughness.reshape(1, -1),
        constants,
        flat,
        lines,
    )
    return pl.pallas_call(
        combine,
        out_shape=(
            jax.ShapeDtypeStruct((3, 16, 16, 128), f32),
            jax.ShapeDtypeStruct((2, 512), f32),
        ),
        in_specs=[vmem] * 5,
        out_specs=(anywhere, anywhere),
        scratch_shapes=[
            pltpu.VMEM((3, 16, 16, 128), f32),
            pltpu.SemaphoreType.DMA((4,)),
        ],
        name="combine",
    )(
        *(
            pltpu.with_memory_space_constraint(value, pltpu.VMEM)
            for value in (res, one, two, scalars, slopes)
        )
    )


def torus_program(torus):
    sizes = tuple(torus.shape[name] for name in AXES)
    return jax.shard_map(
        functools.partial(body, sizes),
        mesh=torus,
        in_specs=(
            P(None, WALL, "span", None),
            P(),
            P(WALL_SPAN, None),
            P(WALL_SPAN, None),
            P(None, WALL_SPAN),
            P(WALL_SPAN),
        ),
        out_specs=(P(None, WALL, "span", None), P(None, WALL_SPAN)),
        check_vma=False,
    )


def solution(mesh):
    return torus_program(Mesh(mesh.devices.reshape(4, 8, 2, mesh.shape["span"]), AXES))
```
